32 devices in a mesh: group: 4 (over y, x), fsdp: 2 (over core), tensor: 4 (over z).
Axes of the slice: x: 2, y: 2, z: 4, core: 2. Of those that a mesh axis runs over, the one named last changes fastest.
Arguments:
- patches: bfloat16 [4, 2, 8, 577, 1024], P('group', None, ('fsdp', 'tensor')), may hold values from -6 to 6
- output_grad: bfloat16 [4, 2, 8, 577, 1024], P('group', None, ('fsdp', 'tensor')), may hold values from -6 to 6
- live_counts: int32 [4, 2, 2], P('group'), may hold values from 1 to 4, as said below
- attn_master: float32 [4, 1024, 1024], P(None, 'fsdp', 'tensor')
- mlp_master: float32 [2, 1024, 4096], P(None, 'fsdp', 'tensor')
- vector_master: float32 [12, 1024], replicated
- attn_moments: float32 [4, 2, 4, 1024, 1024], P('group', None, None, 'fsdp', 'tensor'), as said below
- mlp_moments: float32 [4, 2, 2, 1024, 4096], P('group', None, None, 'fsdp', 'tensor'), as said below
- vector_moments: float32 [4, 2, 12, 1024], P('group'), as said below
- attn_outer: float32 [4, 1024, 1024], P(None, 'fsdp', 'tensor'), may hold values from -0.125 to 0.125
- mlp_outer: float32 [2, 1024, 4096], P(None, 'fsdp', 'tensor'), may hold values from -0.125 to 0.125
- vector_outer: float32 [12, 1024], replicated, may hold values from -0.625 to 0.625
Outputs:
- block_output: bfloat16 [4, 2, 8, 577, 1024], P('group', None, ('fsdp', 'tensor'))
- patches_grad: float32 [4, 2, 8, 577, 1024], P('group', None, ('fsdp', 'tensor'))
- attn_inner: float32 [4, 2, 4, 1024, 1024], P('group', None, None, 'fsdp', 'tensor')
- attn_state: float32 [3, 4, 1024, 1024], P(None, None, 'fsdp', 'tensor')
- attn_copy: bfloat16 [4, 1024, 1024], P(None, 'fsdp', 'tensor')
- mlp_inner: float32 [4, 2, 2, 1024, 4096], P('group', None, None, 'fsdp', 'tensor')
- mlp_state: float32 [3, 2, 1024, 4096], P(None, None, 'fsdp', 'tensor')
- mlp_copy: bfloat16 [2, 1024, 4096], P(None, 'fsdp', 'tensor')
- vector_inner: float32 [4, 2, 12, 1024], P('group')
- vector_state: float32 [3, 12, 1024], replicated
- vector_copy: bfloat16 [12, 1024], replicated
The draws below stay inside these ranges and needn't reach their ends.
Inputs may be any that keep to these rules, and one draw needn't show every extreme that they name: live_counts[g, m, f] images are live, and they stand first, among the f-th block of 4 image slots of micro-batch m in group g; some entry equals 4. `attn_moments`: second moments are positive. `mlp_moments`: second moments are positive. `vector_moments`: second moments are positive.
All inputs are finite; a program needn't handle non-finite values.
Results may differ from the reference program's by a relative error of at most 0.012.
The reference program's roundings to bfloat16 on the way count: a program that leaves them out, or rounds other values in their place, can miss the bound.
Values may be sent and summed in bfloat16 or wider, within the bound.
A program may use at most 320 MiB of HBM per device.

```python
import math
import jax
import jax.numpy as jnp
from jax import lax

D = 1024
HD = 64
FF = 4096
SEQ = 577
MICRO = 2
STEP = 8
IMG_DEV = 4
IMAGES = 8
GROUPS = 4
NV = 12


def draw_live_counts(key, part):
    owners = IMAGES // IMG_DEV
    drawn = jax.random.randint(key, (GROUPS, MICRO, owners), 1, IMG_DEV + 1)
    picked = jax.random.randint(jax.random.fold_in(key, 11), (3,), 0, 1 << 20)
    return drawn.at[picked[0] % GROUPS, picked[1] % MICRO, picked[2] % owners].set(IMG_DEV).astype(jnp.int32)


def draw_attn_master(key, part):
    factor = jnp.array([1.3, 1.3, 1.0, 8.0], jnp.float32) * D ** (-0.5)
    noise = jax.random.truncated_normal(key, -4.0, 4.0, (4, D, D), jnp.float32)
    return noise * factor[:, None, None]


def draw_mlp_master(key, part):
    factor = jnp.array([D ** (-0.5), FF ** (-0.5)], jnp.float32)
    noise = jax.random.truncated_normal(key, -4.0, 4.0, (2, D, FF), jnp.float32)
    return noise * factor[:, None, None]


def draw_vector_master(key, part):
    gain_rows = jax.random.uniform(key, (NV, D), jnp.float32, 0.5, 1.5)
    shifts = jax.random.truncated_normal(jax.random.fold_in(key, 1), -4.0, 4.0, (NV, D), jnp.float32)
    row_index = jnp.arange(NV)[:, None]
    spread = jnp.where(row_index == 5, 0.1, 0.3)
    is_gain = (row_index == 0) | (row_index == 2)
    return jnp.where(is_gain, gain_rows, shifts * spread)


def moments_from(key, factor, shape):
    magnitude = factor * math.sqrt(MICRO * IMAGES * SEQ * 0.6)
    first_moment = jax.random.normal(jax.random.fold_in(key, 1), shape, jnp.float32) * magnitude * (0.1 / 0.9)
    spread = jnp.exp(jax.random.uniform(jax.random.fold_in(key, 2), shape, jnp.float32, 0.0, math.log(4.0)))
    second_moment = magnitude * magnitude * (0.05 / 0.95) * spread
    return jnp.stack([first_moment, second_moment], axis=1)


def draw_attn_moments(key, part):
    factor = jnp.array([1.2, 1.2, 0.8, 0.2], jnp.float32)[None, :, None, None]
    return moments_from(key, factor, (GROUPS, 4, D, D))


def draw_mlp_moments(key, part):
    factor = jnp.array([0.35, 0.6], jnp.float32)[None, :, None, None]
    return moments_from(key, factor, (GROUPS, 2, D, FF))


def draw_vector_moments(key, part):
    leading = jnp.array([2.3, 2.3, 0.7, 0.7, 1.2, 0.8, 1.5, 1.0], jnp.float32)
    factor = jnp.concatenate([leading, jnp.full((NV - 8,), 0.35, jnp.float32)])[None, :, None]
    return moments_from(key, factor, (GROUPS, NV, D))


def level_of(own_key, dims, split, low, largest):
    gain, own = 1.0, jax.random.fold_in(own_key, 6)
    for axis_at, shards_of in split:
        heights = jnp.exp(jax.random.uniform(jax.random.fold_in(own, axis_at), (shards_of,), jnp.float32, low / len(split), largest / len(split)))
        gain = gain * jnp.repeat(heights, dims[axis_at] // shards_of).reshape([-1 if axis == axis_at else 1 for axis in range(len(dims))])
    return gain


def gaussian(own_key, extent, scale, bound, cuts=(), dtype=jnp.bfloat16):
    values = scale * jax.random.normal(own_key, extent, jnp.float32)
    if cuts:
        values = values * level_of(own_key, extent, cuts, -0.22, 0.18)
    return jnp.clip(values, -bound, bound).astype(dtype)


def setup_inputs(seed: int = 0) -> dict:
    streams_of = jax.random.split(jax.random.key(seed), 13)
    return {
        "patches": gaussian(streams_of[0], (GROUPS, MICRO, IMAGES, SEQ, D), 1.0, 6.0, ((0, 4), (2, 8))),
        "output_grad": gaussian(streams_of[1], (GROUPS, MICRO, IMAGES, SEQ, D), 1.0, 6.0, ((0, 4), (2, 8))),
        "live_counts": draw_live_counts(jax.random.fold_in(streams_of[12], 71), 0),
        "attn_master": draw_attn_master(jax.random.fold_in(streams_of[12], 71), 0),
        "mlp_master": draw_mlp_master(jax.random.fold_in(streams_of[12], 71), 0),
        "vector_master": draw_vector_master(jax.random.fold_in(streams_of[12], 71), 0),
        "attn_moments": draw_attn_moments(jax.random.fold_in(streams_of[12], 71), 0),
        "mlp_moments": draw_mlp_moments(jax.random.fold_in(streams_of[12], 71), 0),
        "vector_moments": draw_vector_moments(jax.random.fold_in(streams_of[12], 71), 0),
        "attn_outer": gaussian(streams_of[9], (4, D, D), 0.02, 0.125, ((1, 2), (2, 4)), jnp.float32),
        "mlp_outer": gaussian(streams_of[10], (2, D, FF), 0.02, 0.125, ((1, 2), (2, 4)), jnp.float32),
        "vector_outer": gaussian(streams_of[11], (NV, D), 0.1, 0.625, (), jnp.float32),
    }


EPSILON = 1e-06
PRECISE = lax.Precision.HIGHEST
INNER_RATE = 0.02
VECTOR_RATE = 0.2
WEIGHT_DECAY = 0.1
OUTER_RATE = 0.7
OUTER_MOMENTUM = 0.9

@jax.custom_vjp
def low(v):
    return lax.optimization_barrier(v.astype(jnp.bfloat16)).astype(jnp.float32)

@jax.custom_vjp
def low_back(v):
    return v

def low_keep(v):
    return (low(v), None)

def low_pass(kept, grad):
    return (grad,)

def back_keep(v):
    return (v, None)

def back_low(kept, grad):
    return (low(grad),)
low.defvjp(low_keep, low_pass)
low_back.defvjp(back_keep, back_low)

def normalize(source, gain_row, shift_row):
    centre = source - lax.optimization_barrier(jnp.mean(source, axis=-1, keepdims=True))
    spread = lax.optimization_barrier(jnp.mean(centre * centre, axis=-1, keepdims=True))
    return centre * lax.rsqrt(spread + EPSILON) * gain_row + shift_row

def inner_adamw(master, gradient, moments, step_rate, decay_rate):
    first_moment = 0.9 * moments[0] + 0.1 * gradient
    second_moment = 0.95 * moments[1] + 0.05 * gradient * gradient
    step_ratio = first_moment / (1.0 - 0.9 ** STEP) / (jnp.sqrt(second_moment / (1.0 - 0.95 ** STEP)) + 1e-08)
    return (master - step_rate * (step_ratio + decay_rate * master), second_moment)

def outer_nesterov(master, outer_old, difference):
    momentum = OUTER_MOMENTUM * outer_old + difference
    updated = master - OUTER_RATE * (difference + OUTER_MOMENTUM * momentum)
    return (jnp.stack([difference, momentum, updated]), updated.astype(jnp.bfloat16))

def block_forward(attn, mlp_weights, vector, row_block):
    image_count, seq_len, width = row_block.shape
    head_count = width // HD
    score_scale = HD ** (-0.5)
    normed_one = low(normalize(row_block, vector[0], vector[1]))
    queries = low(low_back(jnp.einsum('isd,de->ise', normed_one, attn[0], precision=PRECISE) + vector[4]))
    keys_low = low(low_back(jnp.einsum('isd,de->ise', normed_one, attn[1], precision=PRECISE)))
    values_low = low(low_back(jnp.einsum('isd,de->ise', normed_one, attn[2], precision=PRECISE) + vector[5]))
    shape_heads = (image_count, seq_len, head_count, HD)
    scores = low_back(jnp.einsum('iqhe,ikhe->ihqk', queries.reshape(shape_heads), keys_low.reshape(shape_heads), precision=PRECISE) * score_scale)
    probs_full = jax.nn.softmax(scores, axis=-1)
    attended = jnp.einsum('ihqk,ikhe->iqhe', low(probs_full), values_low.reshape(shape_heads), precision=PRECISE)
    attended = low(low_back(attended.reshape(image_count, seq_len, width)))
    branch_one = low_back(jnp.einsum('ise,de->isd', attended, attn[3], precision=PRECISE))
    resid_one = row_block + branch_one + vector[6]
    normed_two = low(normalize(resid_one, vector[2], vector[3]))
    pre_act = low_back(jnp.einsum('isd,df->isf', normed_two, mlp_weights[0], precision=PRECISE) + vector[8:].reshape(-1))
    hidden = low(jax.nn.gelu(pre_act, approximate=False))
    branch_two = low_back(jnp.einsum('isf,df->isd', hidden, mlp_weights[1], precision=PRECISE))
    return resid_one + branch_two + vector[7]

def reference(patches, output_grad, live_counts, attn_master, mlp_master, vector_master, attn_moments, mlp_moments, vector_moments, attn_outer, mlp_outer, vector_outer):
    attn_low = low(attn_master)
    mlp_low = low(mlp_master)
    slot_index = jnp.arange(IMAGES)
    block_size = math.gcd(MICRO * IMAGES, 4)
    mixed_groups = []
    input_groups = []
    attn_inner = []
    mlp_inner = []
    vector_inner = []
    attn_diff = jnp.zeros_like(attn_master)
    mlp_diff = jnp.zeros_like(mlp_master)
    vector_diff = jnp.zeros_like(vector_master)
    for group_index in range(GROUPS):
        alive = (slot_index[None, :] % IMG_DEV < live_counts[group_index][:, slot_index // IMG_DEV]).astype(jnp.float32)
        row_blocks = patches[group_index].astype(jnp.float32).reshape(-1, block_size, SEQ, D)
        cotangents = output_grad[group_index].astype(jnp.float32).reshape(-1, block_size, SEQ, D)
        alive_blocks = alive.reshape(-1, block_size)

        def scan_step(totals_now, block_item):
            rows_now, back_now, alive_block = block_item

            def forward(attn, mlp_weights, vector, inputs):
                return block_forward(attn, mlp_weights, vector, inputs) * alive_block[:, None, None]
            result, pullback = jax.vjp(forward, attn_low, mlp_low, vector_master, rows_now)
            gradients = pullback(back_now)
            totals_next = (totals_now[0] + gradients[0], totals_now[1] + gradients[1], totals_now[2] + gradients[2])
            return (totals_next, (result.astype(jnp.bfloat16), gradients[3]))
        zero_sums = (jnp.zeros_like(attn_master), jnp.zeros_like(mlp_master), jnp.zeros_like(vector_master))
        grad_sums, block_outputs = lax.scan(scan_step, zero_sums, (row_blocks, cotangents, alive_blocks))
        mixed_groups.append(block_outputs[0].reshape(MICRO, IMAGES, SEQ, D))
        input_groups.append(block_outputs[1].reshape(MICRO, IMAGES, SEQ, D))
        new_attn, second_attn = inner_adamw(attn_master, grad_sums[0], attn_moments[group_index], INNER_RATE, WEIGHT_DECAY)
        new_mlp, second_mlp = inner_adamw(mlp_master, grad_sums[1], mlp_moments[group_index], INNER_RATE, WEIGHT_DECAY)
        new_vector, second_vector = inner_adamw(vector_master, grad_sums[2], vector_moments[group_index], VECTOR_RATE, 0.0)
        attn_inner.append(jnp.stack([grad_sums[0], second_attn]))
        mlp_inner.append(jnp.stack([grad_sums[1], second_mlp]))
        vector_inner.append(jnp.stack([grad_sums[2], second_vector]))
        attn_diff = attn_diff + (attn_master - new_attn)
        mlp_diff = mlp_diff + (mlp_master - new_mlp)
        vector_diff = vector_diff + (vector_master - new_vector)
    attn_state, attn_copy = outer_nesterov(attn_master, attn_outer, attn_diff / GROUPS)
    mlp_state, mlp_copy = outer_nesterov(mlp_master, mlp_outer, mlp_diff / GROUPS)
    vector_state, vector_copy = outer_nesterov(vector_master, vector_outer, vector_diff / GROUPS)
    return (jnp.stack(mixed_groups), jnp.stack(input_groups), jnp.stack(attn_inner), attn_state, attn_copy, jnp.stack(mlp_inner), mlp_state, mlp_copy, jnp.stack(vector_inner), vector_state, vector_copy)
```

```python
import jax
import jax.numpy as jnp
from jax import lax
from jax.sharding import PartitionSpec as P

HD = 64
STEP = 8
IMG_DEV = 4


EPSILON = 1e-06
INNER_RATE = 0.02
VECTOR_RATE = 0.2
WEIGHT_DECAY = 0.1
OUTER_RATE = 0.7
OUTER_MOMENTUM = 0.9


def normalize(source, gain_row, shift_row):
    centre = source - jnp.mean(source, axis=-1, keepdims=True)
    spread = jnp.mean(centre * centre, axis=-1, keepdims=True)
    return centre * lax.rsqrt(spread + EPSILON) * gain_row + shift_row


def gelu_exact(source):
    return jax.nn.gelu(source, approximate=False)


def gelu_slope(source):
    return (
        0.5 * (1.0 + lax.erf(source * 0.7071067811865476))
        + source * jnp.exp(-0.5 * source * source) * 0.3989422804014327
    )


def inner_adamw(master, gradient, moments, step_rate, decay_rate):
    first_moment = 0.9 * moments[0] + 0.1 * gradient
    second_moment = 0.95 * moments[1] + 0.05 * gradient * gradient
    step_ratio = (
        first_moment / (1.0 - 0.9**STEP) / (jnp.sqrt(second_moment / (1.0 - 0.95**STEP)) + 1e-08)
    )
    return (master - step_rate * (step_ratio + decay_rate * master), second_moment)


def outer_nesterov(master, outer_old, difference):
    momentum = OUTER_MOMENTUM * outer_old + difference
    updated = master - OUTER_RATE * (difference + OUTER_MOMENTUM * momentum)
    return (jnp.stack([difference, momentum, updated]), updated.astype(jnp.bfloat16))


def attend(queries, keys, values, score_scale):
    scores = jnp.einsum("iqhe,ikhe->ihqk", queries, keys, preferred_element_type=jnp.float32) * score_scale
    highest = jnp.max(scores, axis=-1, keepdims=True)
    exponent = jnp.exp(scores - highest)
    totals = jnp.sum(exponent, axis=-1, keepdims=True)
    return exponent / totals


def gather_weight(low):
    whole = lax.all_gather(low, "tensor", axis=2, tiled=True)
    return lax.all_gather(whole, "fsdp", axis=1, tiled=True)


def scatter_gradient(gradient):
    low = gradient.astype(jnp.bfloat16)
    half = lax.psum_scatter(low, "fsdp", scatter_dimension=1, tiled=True)
    return lax.psum_scatter(half, "tensor", scatter_dimension=2, tiled=True).astype(jnp.float32)


def local(
    patches,
    output_grad,
    live_counts,
    attn_master,
    mlp_master,
    vector_master,
    attn_moments,
    mlp_moments,
    vector_moments,
    attn_outer,
    mlp_outer,
    vector_outer,
):
    narrow = jnp.bfloat16
    single = jnp.float32
    tensor_index = lax.axis_index("tensor")
    fsdp_index = lax.axis_index("fsdp")
    micro_count, local_images, seq_len, width = patches.shape[1:]
    score_scale = HD ** (-0.5)
    attn_low = attn_master.astype(narrow)
    mlp_low = mlp_master.astype(narrow)
    tensor_size = lax.axis_size("tensor")
    image_slot = (fsdp_index * tensor_size + tensor_index) * local_images + jnp.arange(local_images)
    block = IMG_DEV
    counts = jnp.take(live_counts[0], image_slot // block, axis=1)
    alive = ((image_slot % block)[None, :] < counts).astype(single).reshape(-1, 1, 1)
    inputs = patches[0].astype(single).reshape(-1, seq_len, width)
    cotangent = output_grad[0].astype(single).reshape(-1, seq_len, width)
    image_count = inputs.shape[0]
    w_qkv = gather_weight(attn_low[:3])
    w_out = gather_weight(attn_low[3:])[0]
    w_in = gather_weight(mlp_low[:1])[0]
    w_down = gather_weight(mlp_low[1:])[0]
    vec = vector_master
    bias_hidden = vec[8:].reshape(-1)
    normed_one = normalize(inputs, vec[0], vec[1]).astype(narrow)
    projected = jnp.einsum("isd,jde->jise", normed_one, w_qkv, preferred_element_type=single)
    heads = width // HD
    shape_heads = (image_count, seq_len, heads, HD)
    queries = (projected[0] + vec[4]).astype(narrow).reshape(shape_heads)
    keys = projected[1].astype(narrow).reshape(shape_heads)
    values = (projected[2] + vec[5]).astype(narrow).reshape(shape_heads)
    probs = attend(queries, keys, values, score_scale)
    probs_low = probs.astype(narrow)
    attended = jnp.einsum("ihqk,ikhe->iqhe", probs_low, values, preferred_element_type=single)
    attended = attended.astype(narrow).reshape(image_count, seq_len, width)
    branch_one = jnp.einsum("ise,de->isd", attended, w_out, preferred_element_type=single)
    resid_one = inputs + branch_one + vec[6]
    normed_two = normalize(resid_one, vec[2], vec[3]).astype(narrow)
    pre_act = jnp.einsum("isd,df->isf", normed_two, w_in, preferred_element_type=single) + bias_hidden
    hidden = gelu_exact(pre_act).astype(narrow)
    grad_out = alive * cotangent
    grad_two = grad_out.astype(narrow)
    grad_down = jnp.einsum("isd,isf->df", grad_two, hidden, preferred_element_type=single)
    g_down = scatter_gradient(grad_down[None])
    branch_two = jnp.einsum("isf,df->isd", hidden, w_down, preferred_element_type=single)
    block_output = (alive * (resid_one + branch_two + vec[7])).astype(narrow)
    grad_hidden = jnp.einsum("isd,df->isf", grad_two, w_down, preferred_element_type=single)
    grad_pre = (grad_hidden * gelu_slope(pre_act)).astype(narrow)
    grad_in = jnp.einsum("isd,isf->df", normed_two, grad_pre, preferred_element_type=single)
    g_in = scatter_gradient(grad_in[None])
    grad_normed_two = jnp.einsum("isf,df->isd", grad_pre, w_in, preferred_element_type=single)
    unused_two, pull_two = jax.vjp(normalize, resid_one, vec[2], vec[3])
    back_resid, gain_two, shift_two = pull_two(grad_normed_two)
    grad_resid = grad_out + back_resid
    grad_one = grad_resid.astype(narrow)
    grad_wo = jnp.einsum("isd,ise->de", grad_one, attended, preferred_element_type=single)
    g_out = scatter_gradient(grad_wo[None])
    grad_attended = jnp.einsum("isd,de->ise", grad_one, w_out, preferred_element_type=single)
    grad_attended = grad_attended.astype(narrow).reshape(shape_heads)
    grad_probs = jnp.einsum("iqhe,ikhe->ihqk", grad_attended, values, preferred_element_type=single)
    grad_values = jnp.einsum("ihqk,iqhe->ikhe", probs_low, grad_attended, preferred_element_type=single)
    weighted = jnp.sum(probs * grad_probs, axis=-1, keepdims=True)
    grad_scores = (probs * (grad_probs - weighted)).astype(narrow)
    grad_queries = jnp.einsum("ihqk,ikhe->iqhe", grad_scores, keys, preferred_element_type=single) * score_scale
    grad_keys = jnp.einsum("ihqk,iqhe->ikhe", grad_scores, queries, preferred_element_type=single) * score_scale
    stack = jnp.stack([grad_queries.astype(narrow), grad_keys.astype(narrow), grad_values.astype(narrow)])
    stack = stack.reshape(3, image_count, seq_len, width)
    grad_qkv = jnp.einsum("isd,jise->jde", normed_one, stack, preferred_element_type=single)
    g_qkv = scatter_gradient(grad_qkv)
    grad_normed_one = jnp.einsum("jise,jde->isd", stack, w_qkv, preferred_element_type=single)
    unused_one, pull_one = jax.vjp(normalize, inputs, vec[0], vec[1])
    back_inputs, gain_one, shift_one = pull_one(grad_normed_one)
    patches_grad = grad_resid + back_inputs
    vector_part = jnp.concatenate(
        [
            jnp.stack(
                [
                    gain_one,
                    shift_one,
                    gain_two,
                    shift_two,
                    jnp.sum(stack[0].astype(single), axis=(0, 1)),
                    jnp.sum(stack[2].astype(single), axis=(0, 1)),
                    jnp.sum(grad_resid, axis=(0, 1)),
                    jnp.sum(grad_out, axis=(0, 1)),
                ]
            ),
            jnp.sum(grad_pre.astype(single), axis=(0, 1)).reshape(-1, width),
        ]
    )
    vector_grad = lax.psum(vector_part, ("fsdp", "tensor"))
    attn_grad = jnp.concatenate([g_qkv, g_out])
    mlp_grad = jnp.concatenate([g_in, g_down])
    new_attn, second_attn = inner_adamw(attn_master, attn_grad, attn_moments[0], INNER_RATE, WEIGHT_DECAY)
    new_mlp, second_mlp = inner_adamw(mlp_master, mlp_grad, mlp_moments[0], INNER_RATE, WEIGHT_DECAY)
    new_vector, second_vector = inner_adamw(vec, vector_grad, vector_moments[0], VECTOR_RATE, 0.0)
    diff_attn, diff_mlp = lax.psum(
        ((attn_master - new_attn).astype(narrow), (mlp_master - new_mlp).astype(narrow)), "group"
    )
    diff_vector = lax.psum(vec - new_vector, "group")
    groups = lax.axis_size("group")
    attn_state, attn_copy = outer_nesterov(attn_master, attn_outer, diff_attn.astype(single) / groups)
    mlp_state, mlp_copy = outer_nesterov(mlp_master, mlp_outer, diff_mlp.astype(single) / groups)
    vector_state, vector_copy = outer_nesterov(vec, vector_outer, diff_vector / groups)
    shape_out = patches.shape
    return (
        block_output.reshape(shape_out),
        patches_grad.reshape(shape_out),
        jnp.stack([attn_grad, second_attn])[None],
        attn_state,
        attn_copy,
        jnp.stack([mlp_grad, second_mlp])[None],
        mlp_state,
        mlp_copy,
        jnp.stack([vector_grad, second_vector])[None],
        vector_state,
        vector_copy,
    )


def solution(mesh):
    placed = (
        P("group", None, ("fsdp", "tensor"), None, None),
        P("group", None, ("fsdp", "tensor"), None, None),
        P("group", None, None),
        P(None, "fsdp", "tensor"),
        P(None, "fsdp", "tensor"),
        P(),
        P("group", None, None, "fsdp", "tensor"),
        P("group", None, None, "fsdp", "tensor"),
        P("group", None, None, None),
        P(None, "fsdp", "tensor"),
        P(None, "fsdp", "tensor"),
        P(),
    )
    return jax.shard_map(
        local,
        mesh=mesh,
        in_specs=placed,
        out_specs=(
            P("group", None, ("fsdp", "tensor"), None, None),
            P("group", None, ("fsdp", "tensor"), None, None),
            P("group", None, None, "fsdp", "tensor"),
            P(None, None, "fsdp", "tensor"),
            P(None, "fsdp", "tensor"),
            P("group", None, None, "fsdp", "tensor"),
            P(None, None, "fsdp", "tensor"),
            P(None, "fsdp", "tensor"),
            P("group", None, None, None),
            P(),
            P(),
        ),
        check_vma=False,
    )
```

```python
import functools

import jax
import jax.numpy as jnp
from jax import lax
from jax.experimental import pallas as pl
from jax.experimental.pallas import tpu as pltpu
from jax.sharding import PartitionSpec as P

HD = 64
STEP = 8
IMG_DEV = 4
EPSILON = 1e-06
INNER_RATE = 0.02
VECTOR_RATE = 0.2
WEIGHT_DECAY = 0.1
OUTER_RATE = 0.7
OUTER_MOMENTUM = 0.9
QUARTERS = 4
LOW = jnp.bfloat16
F32 = jnp.float32
NN = (((1,), (0,)), ((), ()))
NT = (((1,), (1,)), ((), ()))
TN = (((0,), (0,)), ((), ()))


def dot(a, b, dims=NN):
    return lax.dot_general(a, b, dims, preferred_element_type=F32)


MESH = pl.DeviceIdType.MESH


def params(identity=None):
    if identity is None:
        return pltpu.CompilerParams(vmem_limit_bytes=60 * 2**20)
    return pltpu.CompilerParams(vmem_limit_bytes=60 * 2**20, collective_id=identity, has_side_effects=True)


def partner():
    return (lax.axis_index("group"), 1 - lax.axis_index("fsdp"), lax.axis_index("tensor"))


def greet_partner():
    barrier = pltpu.get_barrier_semaphore()
    pl.semaphore_signal(barrier, inc=1, device_id=partner(), device_id_type=MESH)
    pl.semaphore_wait(barrier, 1)


def to_partner(sent, received, sends, receives, n):
    return pltpu.make_async_remote_copy(
        src_ref=sent.at[n],
        dst_ref=received.at[n],
        send_sem=sends.at[n],
        recv_sem=receives.at[n],
        device_id=partner(),
        device_id_type=MESH,
    )


def bands(depth):
    f = lax.axis_index("fsdp")
    return pl.ds(pl.multiple_of(f * depth, depth), depth), pl.ds(pl.multiple_of((1 - f) * depth, depth), depth)


def exchange_scratch(steps, shape):
    dma = pltpu.SemaphoreType.DMA
    return [
        pltpu.VMEM((steps, *shape), F32),
        pltpu.VMEM((steps, *shape), LOW),
        pltpu.VMEM((steps, *shape), LOW),
        dma((steps,)),
        dma((steps,)),
    ]


def cost(flops, moved, special=0):
    return pl.CostEstimate(flops=int(flops), bytes_accessed=int(moved), transcendentals=int(special))


def padded(rows):
    return -(-rows // 16) * 16


def centred(source):
    centre = source - jnp.mean(source, axis=-1, keepdims=True)
    spread = jnp.mean(centre * centre, axis=-1, keepdims=True)
    inverse = lax.rsqrt(spread + EPSILON)
    return centre * inverse, inverse


def norm_back(upstream, normal, inverse, gain):
    pulled = upstream * gain
    mean_one = jnp.mean(pulled, axis=-1, keepdims=True)
    mean_two = jnp.mean(pulled * normal, axis=-1, keepdims=True)
    return inverse * (pulled - mean_one - normal * mean_two)


def project_kernel(images, seq, x_ref, w_ref, vec_ref, n_ref, out_ref, n_scr):
    j, t = pl.program_id(0), pl.program_id(1)
    span = n_scr.shape[0] // images

    @pl.when((j == 0) & (t == 0))
    def _():
        n_scr[...] = jnp.zeros_like(n_scr)
        for i in range(images):
            normal, _ = centred(x_ref[i].astype(F32))
            n_scr[pl.ds(i * span, seq), :] = (normal * vec_ref[0:1] + vec_ref[1:2]).astype(LOW)
        n_ref[...] = n_scr[...]

    cols = out_ref.shape[-1]
    out = dot(n_scr[...], w_ref[0, 0])
    at = pl.ds(pl.multiple_of(t * cols, cols), cols)
    bias = jnp.where(j == 0, vec_ref[4:5, at], jnp.where(j == 2, vec_ref[5:6, at], 0.0))
    out_ref[0] = (out + bias).astype(LOW)


def project(patches, w_attn, vec):
    images, seq, width = patches.shape
    shards, _, _, cols = w_attn.shape
    rows = images * padded(seq)
    return pl.pallas_call(
        functools.partial(project_kernel, images, seq),
        grid=(3, shards),
        in_specs=[
            pl.BlockSpec((images, seq, width), lambda j, t: (0, 0, 0)),
            pl.BlockSpec((1, 1, width, cols), lambda j, t: (t, j, 0, 0)),
            pl.BlockSpec(vec.shape, lambda j, t: (0, 0)),
        ],
        out_specs=[
            pl.BlockSpec((rows, width), lambda j, t: (0, 0)),
            pl.BlockSpec((1, rows, cols), lambda j, t: (j, 0, t)),
        ],
        out_shape=[
            jax.ShapeDtypeStruct((rows, width), LOW),
            jax.ShapeDtypeStruct((3, rows, width), LOW),
        ],
        scratch_shapes=[pltpu.VMEM((rows, width), LOW)],
        compiler_params=params(),
        cost_estimate=cost(6 * rows * width * width, 16 * rows * width),
        name="project",
    )(patches, w_attn, vec)


def half_lanes(value, which):
    lane = lax.broadcasted_iota(jnp.int32, value.shape, 1)
    return jnp.where((lane >= HD) == bool(which), value, jnp.zeros_like(value))


def attend_kernel(seq, q_ref, k_ref, v_ref, out_ref):
    span = q_ref.shape[1]
    scale = HD**-0.5
    q, k, v = q_ref[0], k_ref[0], v_ref[0]
    parts = []
    for h in range(2):
        scores = dot(q, half_lanes(k, h), NT)
        lane = lax.broadcasted_iota(jnp.int32, scores.shape, 1)
        scores = jnp.where(lane < seq, scores, -1e30)
        top = jnp.max(scores, axis=1, keepdims=True)
        raised = jnp.exp((scores - top) * scale)
        total = jnp.sum(raised, axis=1, keepdims=True)
        probs = (raised * (1.0 / total)).astype(LOW)
        parts.append(dot(probs, v))
    lane = lax.broadcasted_iota(jnp.int32, (span, 2 * HD), 1)
    out_ref[...] = jnp.where(lane < HD, parts[0], parts[1]).astype(LOW)


def attend(qkv, images, seq):
    _, rows, width = qkv.shape
    span = rows // images
    pair = 2 * HD

    def take(j):
        return pl.BlockSpec((1, span, pair), lambda i, h: (j, i, h))

    return pl.pallas_call(
        functools.partial(attend_kernel, seq),
        grid=(images, width // pair),
        in_specs=[take(0), take(1), take(2)],
        out_specs=pl.BlockSpec((span, pair), lambda i, h: (i, h)),
        out_shape=jax.ShapeDtypeStruct((rows, width), LOW),
        compiler_params=params(),
        cost_estimate=cost(16 * rows * span * width, 8 * rows * width, rows * span * (width // HD)),
        name="attend",
    )(qkv, qkv, qkv)


def mix_kernel(seq, alive_ref, att_ref, x_ref, g_ref, w_ref, vec_ref, resid_ref, n_ref, g2_ref, x_scr):
    i = pl.program_id(0)
    shards, _, _, cols = w_ref.shape
    x_scr[...] = jnp.zeros_like(x_scr)
    x_scr[0:seq, :] = x_ref[0].astype(F32)
    total = x_scr[...] + vec_ref[6:7]
    for t in range(shards):
        total = total + dot(att_ref[:, t * cols : (t + 1) * cols], w_ref[t, 0], NT)
    resid_ref[...] = total
    normal, _ = centred(total)
    n_ref[...] = (normal * vec_ref[2:3] + vec_ref[3:4]).astype(LOW)
    x_scr[0:seq, :] = g_ref[0].astype(F32) * alive_ref[i]
    g2_ref[...] = x_scr[...].astype(LOW)


def mix(alive, attended, patches, cotangent, w_attn, vec):
    images, seq, width = patches.shape
    rows = attended.shape[0]
    span = rows // images
    shards, _, _, cols = w_attn.shape
    block = pl.BlockSpec((span, width), lambda i: (i, 0))
    whole = jax.ShapeDtypeStruct((rows, width), LOW)
    return pl.pallas_call(
        functools.partial(mix_kernel, seq),
        grid=(images,),
        in_specs=[
            pl.BlockSpec(memory_space=pltpu.SMEM),
            block,
            pl.BlockSpec((1, seq, width), lambda i: (i, 0, 0)),
            pl.BlockSpec((1, seq, width), lambda i: (i, 0, 0)),
            pl.BlockSpec((shards, 1, width, cols), lambda i: (0, 3, 0, 0)),
            pl.BlockSpec(vec.shape, lambda i: (0, 0)),
        ],
        out_specs=[block, block, block],
        out_shape=[jax.ShapeDtypeStruct((rows, width), F32), whole, whole],
        scratch_shapes=[pltpu.VMEM((span, width), F32)],
        compiler_params=params(),
        cost_estimate=cost(2 * rows * width * width, 16 * rows * width),
        name="mix",
    )(alive, attended, patches, cotangent, w_attn, vec)


def mlp_kernel(first, pairwise, chunk, n_ref, g_ref, w1_ref, w2_ref, bias_ref, *refs):
    if not first:
        yi_ref, gi_ref, *refs = refs
    y_ref, gn_ref, dw_ref, db_ref, h_scr, p_scr, nt_scr, gt_scr, *exchange = refs
    step = pl.program_id(0)
    rows = n_ref.shape[0]
    each, _, width, cols = w1_ref.shape

    @pl.when(step == 0)
    def _():
        if pairwise:
            greet_partner()
        nt_scr[...] = n_ref[...].T
        gt_scr[...] = g_ref[...].T
        if first:
            y_ref[...] = jnp.zeros_like(y_ref)
            gn_ref[...] = jnp.zeros_like(gn_ref)
        else:
            y_ref[...] = yi_ref[...]
            gn_ref[...] = gi_ref[...]

    w1 = jnp.concatenate([w1_ref[t, 0] for t in range(each)], axis=1)
    w2 = jnp.concatenate([w2_ref[t, 0] for t in range(each)], axis=1)
    bias = jnp.concatenate([bias_ref[t] for t in range(each)], axis=1)

    def body(c, sums):
        at = pl.ds(pl.multiple_of(c * chunk, chunk), chunk)
        pre = dot(n_ref[at, :], w1) + bias
        cdf = 0.5 * (1.0 + lax.erf(pre * 0.7071067811865476))
        hidden = (pre * cdf).astype(LOW)
        slope = cdf + pre * jnp.exp(-0.5 * pre * pre) * 0.3989422804014327
        gp = dot(g_ref[at, :], w2) * slope
        gl = gp.astype(LOW)
        h_scr[at, :] = hidden
        p_scr[at, :] = gl
        y_ref[at, :] += dot(hidden, w2, NT)
        gn_ref[at, :] += dot(gl, w1, NT)
        return sums + jnp.sum(gl.astype(F32), axis=0, keepdims=True)

    sums = lax.fori_loop(0, rows // chunk, body, jnp.zeros((1, each * cols), F32))
    for t in range(each):
        db_ref[t] = sums[:, t * cols : (t + 1) * cols]
    if pairwise:
        own, sent, received, sends, receives = exchange
        ours, theirs = bands(width // 2)
        sent[step, 0] = dot(nt_scr[theirs, :], p_scr[...]).astype(LOW)
        sent[step, 1] = dot(gt_scr[theirs, :], h_scr[...]).astype(LOW)
        to_partner(sent, received, sends, receives, step).start()
        own[step, 0] = dot(nt_scr[ours, :], p_scr[...])
        own[step, 1] = dot(gt_scr[ours, :], h_scr[...])

        @pl.when(step == pl.num_programs(0) - 1)
        def _():
            for n in range(own.shape[0]):
                to_partner(sent, received, sends, receives, n).wait()
                for which in range(2):
                    total = (own[n, which] + received[n, which].astype(F32)).astype(LOW)
                    for t in range(each):
                        dw_ref[n * each + t, which] = total[:, t * cols : (t + 1) * cols]

        return
    shards, depth = dw_ref.shape[0], dw_ref.shape[3]
    d1 = dot(nt_scr[...], p_scr[...]).astype(LOW)
    d2 = dot(gt_scr[...], h_scr[...]).astype(LOW)
    for f in range(shards):
        for t in range(each):
            dw_ref[f, t, 0] = d1[f * depth : (f + 1) * depth, t * cols : (t + 1) * cols]
            dw_ref[f, t, 1] = d2[f * depth : (f + 1) * depth, t * cols : (t + 1) * cols]


def mlp(quarter, quarters, normed, grad_two, w_mlp, bias, carried, fsdp):
    rows, width = normed.shape
    shards, _, _, hidden = w_mlp.shape
    cols = hidden // quarters
    each = 2
    first, pairwise = carried is None, fsdp == 2
    single = pl.Buffered(1)
    full = pl.BlockSpec((rows, width), lambda s: (0, 0), pipeline_mode=single)
    depth = width // fsdp
    steps = shards // each
    acc_shape = jax.ShapeDtypeStruct((rows, width), F32)
    if pairwise:
        out_w = pl.BlockSpec((shards, 2, depth, cols), lambda s: (0, 0, 0, 0), pipeline_mode=single)
        w_shape = jax.ShapeDtypeStruct((shards, 2, depth, cols), LOW)
        extra = exchange_scratch(steps, (2, depth, each * cols))
    else:
        out_w = pl.BlockSpec((fsdp, each, 2, depth, cols), lambda s: (0, s, 0, 0, 0))
        w_shape = jax.ShapeDtypeStruct((fsdp, shards, 2, depth, cols), LOW)
        extra = []
    return pl.pallas_call(
        functools.partial(mlp_kernel, first, pairwise, rows // 4),
        grid=(steps,),
        in_specs=[
            full,
            full,
            pl.BlockSpec((each, 1, width, cols), lambda s: (s, 0, 0, quarter)),
            pl.BlockSpec((each, 1, width, cols), lambda s: (s, 1, 0, quarter)),
            pl.BlockSpec((each, 1, cols), lambda s: (s, 0, quarter)),
        ]
        + ([] if first else [full, full]),
        out_specs=[full, full, out_w, pl.BlockSpec((each, 1, cols), lambda s: (s, 0, 0))],
        out_shape=[acc_shape, acc_shape, w_shape, jax.ShapeDtypeStruct((shards, 1, cols), F32)],
        scratch_shapes=[
            pltpu.VMEM((rows, each * cols), LOW),
            pltpu.VMEM((rows, each * cols), LOW),
            pltpu.VMEM((width, rows), LOW),
            pltpu.VMEM((width, rows), LOW),
            *extra,
        ],
        compiler_params=params(2 + quarter if pairwise else None),
        cost_estimate=cost(12 * rows * width * cols * shards, 24 * rows * width),
        name=f"mlp_{quarter}",
    )(normed, grad_two, w_mlp, w_mlp, bias, *([] if first else carried))


def turn_kernel(seq, pairwise, alive_ref, resid_ref, y_ref, gn_ref, g2_ref, att_ref, w_ref, vec_ref,
                out_ref, gr_ref, ga_ref, dw_ref, sums_ref, dw_scr, *exchange):
    i = pl.program_id(0)
    if pairwise:
        pl.when(i == 0)(greet_partner)
    shards, _, _, cols = w_ref.shape
    resid = resid_ref[...]
    out_ref[0] = ((resid + y_ref[...] + vec_ref[7:8]) * alive_ref[i]).astype(LOW)[0:seq]
    normal, inverse = centred(resid)
    upstream = gn_ref[...]
    grad_out = g2_ref[...].astype(F32)
    grad_resid = grad_out + norm_back(upstream, normal, inverse, vec_ref[2:3])
    gr_ref[...] = grad_resid
    low = grad_resid.astype(LOW)
    rows = [
        jnp.sum(upstream * normal, axis=0, keepdims=True),
        jnp.sum(upstream, axis=0, keepdims=True),
        jnp.sum(grad_resid, axis=0, keepdims=True),
        jnp.sum(grad_out, axis=0, keepdims=True),
    ]
    rows = jnp.concatenate(rows, axis=0)

    @pl.when(i == 0)
    def _():
        sums_ref[...] = rows

    @pl.when(i != 0)
    def _():
        sums_ref[...] += rows

    for t in range(shards):
        ga_ref[:, t * cols : (t + 1) * cols] = dot(low, w_ref[t, 0]).astype(LOW)
    part = dot(low.T, att_ref[...])

    @pl.when(i == 0)
    def _():
        dw_scr[...] = part

    @pl.when(i != 0)
    def _():
        dw_scr[...] += part

    @pl.when(i == pl.num_programs(0) - 1)
    def _():
        if pairwise:
            sent, received, sends, receives = exchange
            ours, theirs = bands(dw_scr.shape[0] // 2)
            sent[0] = dw_scr[theirs, :].astype(LOW)
            copy = to_partner(sent, received, sends, receives, 0)
            copy.start()
            copy.wait()
            total = (dw_scr[ours, :] + received[0].astype(F32)).astype(LOW)
            for t in range(shards):
                dw_ref[t, 0] = total[:, t * cols : (t + 1) * cols]
            return
        depth = dw_ref.shape[3]
        for f in range(dw_ref.shape[0]):
            for t in range(shards):
                dw_ref[f, t, 0] = dw_scr[f * depth : (f + 1) * depth, t * cols : (t + 1) * cols].astype(LOW)


def turn(alive, resid, branch, grad_normed, grad_two, attended, w_attn, vec, images, seq, fsdp):
    rows, width = resid.shape
    span = rows // images
    shards, _, _, cols = w_attn.shape
    depth = width // fsdp
    pairwise = fsdp == 2
    lead = () if pairwise else (fsdp,)
    block = pl.BlockSpec((span, width), lambda i: (i, 0))
    return pl.pallas_call(
        functools.partial(turn_kernel, seq, pairwise),
        grid=(images,),
        in_specs=[
            pl.BlockSpec(memory_space=pltpu.SMEM),
            block, block, block, block, block,
            pl.BlockSpec((shards, 1, width, cols), lambda i: (0, 3, 0, 0)),
            pl.BlockSpec(vec.shape, lambda i: (0, 0)),
        ],
        out_specs=[
            pl.BlockSpec((1, seq, width), lambda i: (i, 0, 0)),
            block, block,
            pl.BlockSpec((*lead, shards, 1, depth, cols), lambda i: (0,) * (4 + len(lead))),
            pl.BlockSpec((4, width), lambda i: (0, 0)),
        ],
        out_shape=[
            jax.ShapeDtypeStruct((images, seq, width), LOW),
            jax.ShapeDtypeStruct((rows, width), F32),
            jax.ShapeDtypeStruct((rows, width), LOW),
            jax.ShapeDtypeStruct((*lead, shards, 1, depth, cols), LOW),
            jax.ShapeDtypeStruct((4, width), F32),
        ],
        scratch_shapes=[pltpu.VMEM((width, width), F32)] + (exchange_scratch(1, (depth, width))[1:] if pairwise else []),
        compiler_params=params(6 if pairwise else None),
        cost_estimate=cost(4 * rows * width * width, 24 * rows * width),
        name="turn",
    )(alive, resid, branch, grad_normed, grad_two, attended, w_attn, vec)


def unattend_kernel(seq, q_ref, k_ref, v_ref, g_ref, dq_ref, dk_ref, dv_ref):
    span = q_ref.shape[1]
    scale = HD**-0.5
    q, k, v, g = q_ref[0], k_ref[0], v_ref[0], g_ref[...]
    parts = []
    for h in range(2):
        scores = dot(half_lanes(k, h), q, NT)
        row = lax.broadcasted_iota(jnp.int32, scores.shape, 0)
        scores = jnp.where(row < seq, scores, -1e30)
        top = jnp.max(scores, axis=0, keepdims=True)
        raised = jnp.exp((scores - top) * scale)
        total = jnp.sum(raised, axis=0, keepdims=True)
        probs = raised * (1.0 / total)
        gp = dot(half_lanes(v, h), g, NT)
        delta = jnp.sum(probs * gp, axis=0, keepdims=True)
        gs = (probs * (gp - delta)).astype(LOW)
        dv = dot(probs.astype(LOW), g)
        dk = dot(gs, q)
        dq = dot(gs, k, TN)
        parts.append((dq, dk, dv))
    lane = lax.broadcasted_iota(jnp.int32, (span, 2 * HD), 1) < HD
    dq_ref[0] = (jnp.where(lane, parts[0][0], parts[1][0]) * scale).astype(LOW)
    dk_ref[0] = (jnp.where(lane, parts[0][1], parts[1][1]) * scale).astype(LOW)
    dv_ref[0] = jnp.where(lane, parts[0][2], parts[1][2]).astype(LOW)


def unattend(qkv, grad_attended, images, seq):
    _, rows, width = qkv.shape
    span = rows // images
    pair = 2 * HD

    def take(j):
        return pl.BlockSpec((1, span, pair), lambda i, h: (j, i, h))

    out = pl.BlockSpec((1, span, pair), lambda i, h: (0, i, h))
    shape = jax.ShapeDtypeStruct((1, rows, width), LOW)
    return pl.pallas_call(
        functools.partial(unattend_kernel, seq),
        grid=(images, width // pair),
        in_specs=[take(0), take(1), take(2), pl.BlockSpec((span, pair), lambda i, h: (i, h))],
        out_specs=[out, out, out],
        out_shape=[shape, shape, shape],
        compiler_params=params(),
        cost_estimate=cost(40 * rows * span * width, 14 * rows * width, rows * span * (width // HD)),
        name="unattend",
    )(qkv, qkv, qkv, grad_attended)


def close_kernel(seq, images, pairwise, n_ref, dq_ref, dk_ref, dv_ref, w_ref, x_ref, gr_ref, vec_ref,
                 out_ref, dw_ref, sums_ref, acc_scr, nt_scr, *exchange):
    j = pl.program_id(0)
    if pairwise:
        own, sent, received, sends, receives = exchange
        pl.when(j == 0)(greet_partner)
    shards, _, _, cols = w_ref.shape
    span = n_ref.shape[0] // images

    @pl.when(j == 0)
    def _():
        nt_scr[...] = n_ref[...].T
        acc_scr[...] = jnp.zeros_like(acc_scr)
        sums_ref[2:3, :] = jnp.sum(dq_ref[0].astype(F32), axis=0, keepdims=True)
        sums_ref[3:4, :] = jnp.sum(dv_ref[0].astype(F32), axis=0, keepdims=True)

    def part(ref):
        if pairwise:
            ours, theirs = bands(nt_scr.shape[0] // 2)
            for t in range(shards):
                sent[j, t] = dot(nt_scr[theirs, :], ref[0, :, t * cols : (t + 1) * cols]).astype(LOW)
            to_partner(sent, received, sends, receives, j).start()
        for t in range(shards):
            block = ref[0, :, t * cols : (t + 1) * cols]
            acc_scr[...] += dot(block, w_ref[t, 0], NT)
            if pairwise:
                own[j, t] = dot(nt_scr[ours, :], block)
                continue
            depth = dw_ref.shape[3]
            dw = dot(nt_scr[...], block).astype(LOW)
            for f in range(dw_ref.shape[0]):
                dw_ref[f, t, 0] = dw[f * depth : (f + 1) * depth]

    @pl.when(j == 0)
    def _():
        part(dq_ref)

    @pl.when(j == 1)
    def _():
        part(dk_ref)

    @pl.when(j == 2)
    def _():
        part(dv_ref)
        gain = jnp.zeros((1, vec_ref.shape[1]), F32)
        shift = jnp.zeros((1, vec_ref.shape[1]), F32)
        for i in range(images):
            normal, inverse = centred(x_ref[i].astype(F32))
            upstream = acc_scr[i * span : i * span + seq, :]
            out_ref[i] = gr_ref[i * span : i * span + seq, :] + norm_back(upstream, normal, inverse, vec_ref[0:1])
            gain += jnp.sum(upstream * normal, axis=0, keepdims=True)
            shift += jnp.sum(upstream, axis=0, keepdims=True)
        sums_ref[0:1, :] = gain
        sums_ref[1:2, :] = shift
        if pairwise:
            for n in range(own.shape[0]):
                to_partner(sent, received, sends, receives, n).wait()
                for t in range(shards):
                    dw_ref[t, n] = (own[n, t] + received[n, t].astype(F32)).astype(LOW)


def close(normed, grads, w_attn, patches, grad_resid, vec, fsdp):
    images, seq, width = patches.shape
    rows = normed.shape[0]
    shards, _, _, cols = w_attn.shape
    depth = width // fsdp
    pairwise = fsdp == 2
    if pairwise:
        dw_spec = pl.BlockSpec((shards, 3, depth, cols), lambda j: (0, 0, 0, 0), pipeline_mode=pl.Buffered(1))
        dw_shape = jax.ShapeDtypeStruct((shards, 3, depth, cols), LOW)
        extra = exchange_scratch(3, (shards, depth, cols))
    else:
        dw_spec = pl.BlockSpec((fsdp, shards, 1, depth, cols), lambda j: (0, 0, j, 0, 0))
        dw_shape = jax.ShapeDtypeStruct((fsdp, shards, 3, depth, cols), LOW)
        extra = []
    single = pl.Buffered(1)
    stack = pl.BlockSpec((1, rows, width), lambda j: (0, 0, 0), pipeline_mode=single)
    full = pl.BlockSpec((rows, width), lambda j: (0, 0), pipeline_mode=single)
    return pl.pallas_call(
        functools.partial(close_kernel, seq, images, pairwise),
        grid=(3,),
        in_specs=[
            full, stack, stack, stack,
            pl.BlockSpec((shards, 1, width, cols), lambda j: (0, j, 0, 0)),
            pl.BlockSpec((images, seq, width), lambda j: (0, 0, 0), pipeline_mode=single),
            full,
            pl.BlockSpec(vec.shape, lambda j: (0, 0)),
        ],
        out_specs=[
            pl.BlockSpec((images, seq, width), lambda j: (0, 0, 0), pipeline_mode=single),
            dw_spec,
            pl.BlockSpec((4, width), lambda j: (0, 0)),
        ],
        out_shape=[
            jax.ShapeDtypeStruct((images, seq, width), F32),
            dw_shape,
            jax.ShapeDtypeStruct((4, width), F32),
        ],
        scratch_shapes=[pltpu.VMEM((rows, width), F32), pltpu.VMEM((width, rows), LOW), *extra],
        compiler_params=params(7 if pairwise else None),
        cost_estimate=cost(12 * rows * width * width, 30 * rows * width),
        name="close",
    )(normed, *grads, w_attn, patches, grad_resid, vec)


def gather_kernel(a_in, m_in, a_out, m_out, a_hold, m_hold, zs, zr, xs, xr, ys, yr, xfs, xfr, yfs, yfr, cs, cr, ls):
    g, f, z = lax.axis_index("group"), lax.axis_index("fsdp"), lax.axis_index("tensor")
    last = lax.axis_size("tensor") - 1
    x_at, y_at = g % 2, g // 2
    east, north = y_at * 2 + (1 - x_at), (1 - y_at) * 2 + x_at
    depth = a_in.shape[1]
    band = depth // 4
    shared = band * 3 // 8
    rest = band - 2 * shared

    def place(column):
        cx, cy = column % 2, column // 2
        return 2 * (cx + cy - 2 * cx * cy) + cy

    mine, of_east, of_north = place(g), place(east), place(north)
    z_row = mine * band - shared * (mine % 2)
    lead_east = of_east * band + shared * (of_east % 2)
    lead_north = of_north * band + shared * (of_north % 2)
    chunks = ((a_in, a_out, 0, a_in.shape[0]), (m_in, m_out, 0, 1), (m_in, m_out, 1, 1))

    def tile(n):
        return pl.multiple_of(n, 16)

    def held(n, t, row, rows):
        _, out, j, many = chunks[n]
        return out.at[t, pl.ds(j, many), pl.ds(tile(f * depth + row), rows), :]

    def owned(n, row, rows):
        source, _, j, many = chunks[n]
        return source.at[pl.ds(j, many), pl.ds(tile(row), rows), :]

    def send(src, dst, sems, semr, n, t, to):
        return pltpu.make_async_remote_copy(
            src_ref=src, dst_ref=dst, send_sem=sems.at[n, t], recv_sem=semr.at[n, t], device_id=to, device_id_type=MESH
        )

    def along(n, t, up, src):
        return pltpu.make_async_remote_copy(
            src_ref=src,
            dst_ref=held(n, t, z_row, band + shared),
            send_sem=zs.at[n, t, 0 if up else 1],
            recv_sem=zr.at[n, t],
            device_id=(g, f, z + 1 if up else z - 1),
            device_id_type=MESH,
        )

    def to_east(n, t):
        part = held(n, t, mine * band, band)
        return send(part, part, xs, xr, n, t, (east, f, z))

    def to_north(n, t):
        part = held(n, t, mine * band, band)
        return send(part, part, ys, yr, n, t, (north, f, z))

    def north_to_east(n, t):
        part = held(n, t, lead_north, shared)
        return send(part, part, xfs, xfr, n, t, (east, f, z))

    def east_to_north(n, t):
        part = held(n, t, lead_east + shared, rest)
        return send(part, part, yfs, yfr, n, t, (north, f, z))

    def across(n, t, src):
        return send(src, held(n, t, 0, depth), cs, cr, n, t, (g, 1 - f, z))

    barrier = pltpu.get_barrier_semaphore()

    def greet(to):
        pl.semaphore_signal(barrier, inc=1, device_id=to, device_id_type=MESH)

    for to in ((east, f, z), (north, f, z), (g, 1 - f, z)):
        greet(to)

    @pl.when(z > 0)
    def _():
        greet((g, f, z - 1))

    @pl.when(z < last)
    def _():
        greet((g, f, z + 1))

    pl.semaphore_wait(barrier, 3 + jnp.minimum(z, 1) + jnp.minimum(last - z, 1))

    load_a = pltpu.make_async_copy(a_in, a_hold, ls.at[0])
    load_m = pltpu.make_async_copy(m_in, m_hold, ls.at[1])
    load_a.start()
    load_m.start()

    items = [(n, k, up) for n in range(3) for k in range(1, last + 1) for up in (True, False)]

    def when_real(k, up, run):
        @pl.when(z - k >= 0 if up else z + k <= last)
        def _():
            run(z - k if up else z + k)

    def own(n):
        @pl.when(z < last)
        def _():
            along(n, z, True, owned(n, z_row, band + shared)).start()

        @pl.when(z > 0)
        def _():
            along(n, z, False, owned(n, z_row, band + shared)).start()

        across(n, z, owned(n, 0, depth)).start()

    def land(n, k, up):
        def run(t):
            along(n, t, up, held(n, t, z_row, band + shared)).wait_recv()

            @pl.when(z < last if up else z > 0)
            def _():
                along(n, t, up, held(n, t, z_row, band + shared)).start()

            to_east(n, t).start()
            to_north(n, t).start()

        when_real(k, up, run)

    def relay(n, k, up):
        def run(t):
            to_east(n, t).wait_recv()
            east_to_north(n, t).start()
            to_north(n, t).wait_recv()
            north_to_east(n, t).start()

        when_real(k, up, run)

    def finish(n, k, up):
        def run(t):
            east_to_north(n, t).wait_recv()
            north_to_east(n, t).wait_recv()
            across(n, t, held(n, t, 0, depth)).start()

        when_real(k, up, run)

    for at in range(len(items) + 4):
        if at % (2 * last) == 0 and at // (2 * last) < 3:
            own(at // (2 * last))
        if at < len(items):
            land(*items[at])
        if 0 <= at - 2 < len(items):
            relay(*items[at - 2])
        if 0 <= at - 4 < len(items):
            finish(*items[at - 4])

    load_a.wait()
    load_m.wait()
    rows = pl.ds(tile(f * depth), depth)
    keep_a = pltpu.make_async_copy(a_hold, a_out.at[z, :, rows, :], ls.at[2])
    keep_m = pltpu.make_async_copy(m_hold, m_out.at[z, :, rows, :], ls.at[3])
    keep_a.start()
    keep_m.start()
    keep_a.wait()
    keep_m.wait()

    for n in range(3):
        @pl.when(z < last)
        def _():
            along(n, z, True, owned(n, z_row, band + shared)).wait_send()

        @pl.when(z > 0)
        def _():
            along(n, z, False, owned(n, z_row, band + shared)).wait_send()

        across(n, z, owned(n, 0, depth)).wait()

    def settle(n, k, up):
        def run(t):
            @pl.when(z < last if up else z > 0)
            def _():
                along(n, t, up, held(n, t, z_row, band + shared)).wait_send()

            to_east(n, t).wait_send()
            to_north(n, t).wait_send()
            east_to_north(n, t).wait_send()
            north_to_east(n, t).wait_send()
            across(n, t, held(n, t, 0, depth)).wait()

        when_real(k, up, run)

    for item in items:
        settle(*item)


def gather(attn_low, mlp_low, shards):
    _, depth, a_cols = attn_low.shape
    _, _, m_cols = mlp_low.shape
    width = 2 * depth
    anywhere = pl.BlockSpec(memory_space=pl.ANY)
    dma = pltpu.SemaphoreType.DMA
    return pl.pallas_call(
        gather_kernel,
        in_specs=[anywhere, anywhere],
        out_specs=[anywhere, anywhere],
        out_shape=[
            jax.ShapeDtypeStruct((shards, 4, width, a_cols), LOW),
            jax.ShapeDtypeStruct((shards, 2, width, m_cols), LOW),
        ],
        scratch_shapes=[
            pltpu.VMEM(attn_low.shape, LOW),
            pltpu.VMEM(mlp_low.shape, LOW),
            dma((3, shards, 2)),
        ]
        + [dma((3, shards))] * 11
        + [dma((4,))],
        compiler_params=pltpu.CompilerParams(
            collective_id=1, has_side_effects=True, vmem_limit_bytes=60 * 2**20
        ),
        name="gather",
    )(attn_low, mlp_low)


def inner_adamw(master, gradient, first, second, step_rate, decay_rate):
    first_moment = 0.9 * first + 0.1 * gradient
    second_moment = 0.95 * second + 0.05 * gradient * gradient
    step_ratio = (
        first_moment / (1.0 - 0.9**STEP) / (jnp.sqrt(second_moment / (1.0 - 0.95**STEP)) + 1e-08)
    )
    return (master - step_rate * (step_ratio + decay_rate * master), second_moment)


def outer_nesterov(master, outer_old, difference):
    momentum = OUTER_MOMENTUM * outer_old + difference
    updated = master - OUTER_RATE * (difference + OUTER_MOMENTUM * momentum)
    return (jnp.stack([difference, momentum, updated]), updated.astype(LOW))


def gather_weights(shard):
    whole = lax.all_gather(shard, "tensor", axis=0)
    return lax.all_gather(whole, "fsdp", axis=2, tiled=True)


def scatter_gradient(gradient):
    half = gradient if gradient.ndim == 4 else lax.psum_scatter(gradient, "fsdp", scatter_dimension=0)
    return lax.psum_scatter(half, "tensor", scatter_dimension=0)


def local(
    patches,
    output_grad,
    live_counts,
    attn_master,
    mlp_master,
    vector_master,
    attn_moments,
    mlp_moments,
    vector_moments,
    attn_outer,
    mlp_outer,
    vector_outer,
):
    vec = vector_master
    tensor_size, fsdp = lax.axis_size("tensor"), lax.axis_size("fsdp")
    groups = lax.axis_size("group")
    local_images, seq, width = patches.shape[2:]
    slot = (lax.axis_index("fsdp") * tensor_size + lax.axis_index("tensor")) * local_images
    slot = slot + jnp.arange(local_images)
    counts = jnp.take(live_counts[0], slot // IMG_DEV, axis=1)
    alive = ((slot % IMG_DEV)[None, :] < counts).astype(F32).reshape(-1)
    x = patches.reshape(-1, seq, width)
    cotangent = output_grad.reshape(-1, seq, width)
    images = x.shape[0]

    if (groups, fsdp) == (4, 2):
        w_attn, w_mlp = gather(attn_master.astype(LOW), mlp_master.astype(LOW), tensor_size)
    else:
        w_attn = gather_weights(attn_master.astype(LOW))
        w_mlp = gather_weights(mlp_master.astype(LOW))

    normed_one, qkv = project(x, w_attn, vec)
    attended = attend(qkv, images, seq)
    resid, normed_two, grad_two = mix(alive, attended, x, cotangent, w_attn, vec)
    bias = vec[8:].reshape(tensor_size, 1, -1)
    carried = None
    mlp_grads, bias_parts = [], []
    for quarter in range(QUARTERS):
        *carried, dw, db = mlp(quarter, QUARTERS, normed_two, grad_two, w_mlp, bias, carried, fsdp)
        mlp_grads.append(scatter_gradient(dw))
        bias_parts.append(db)
    branch, grad_normed = carried
    block_output, grad_resid, grad_attended, dw_out, sums_two = turn(
        alive, resid, branch, grad_normed, grad_two, attended, w_attn, vec, images, seq, fsdp
    )
    out_grad = scatter_gradient(dw_out)
    grads = unattend(qkv, grad_attended, images, seq)
    patches_grad, dw_qkv, sums_one = close(normed_one, grads, w_attn, x, grad_resid, vec, fsdp)
    qkv_grad = scatter_gradient(dw_qkv)

    hidden_bias = jnp.concatenate(bias_parts, axis=-1).reshape(-1, width)
    vector_part = jnp.concatenate([sums_one[:2], sums_two[:2], sums_one[2:], sums_two[2:], hidden_bias])
    vector_grad = lax.psum(vector_part, ("fsdp", "tensor"))

    attn_grad = jnp.concatenate([qkv_grad, out_grad]).astype(F32)
    mlp_grad = jnp.concatenate(mlp_grads, axis=-1).astype(F32)
    attn_first, attn_second = attn_moments[0]
    mlp_first, mlp_second = mlp_moments[0]
    new_attn, second_attn = inner_adamw(
        attn_master, attn_grad, attn_first, attn_second, INNER_RATE, WEIGHT_DECAY
    )
    new_mlp, second_mlp = inner_adamw(mlp_master, mlp_grad, mlp_first, mlp_second, INNER_RATE, WEIGHT_DECAY)
    new_vector, second_vector = inner_adamw(
        vec, vector_grad, vector_moments[0, 0], vector_moments[0, 1], VECTOR_RATE, 0.0
    )
    diff_attn, diff_mlp = lax.psum(((attn_master - new_attn).astype(LOW), (mlp_master - new_mlp).astype(LOW)), "group")
    diff_vector = lax.psum(vec - new_vector, "group")
    attn_state, attn_copy = outer_nesterov(attn_master, attn_outer, diff_attn.astype(F32) / groups)
    mlp_state, mlp_copy = outer_nesterov(mlp_master, mlp_outer, diff_mlp.astype(F32) / groups)
    vector_state, vector_copy = outer_nesterov(vec, vector_outer, diff_vector / groups)
    return (
        block_output.reshape(patches.shape),
        patches_grad.reshape(patches.shape),
        jnp.stack([attn_grad, second_attn])[None],
        attn_state,
        attn_copy,
        jnp.stack([mlp_grad, second_mlp])[None],
        mlp_state,
        mlp_copy,
        jnp.stack([vector_grad, second_vector])[None],
        vector_state,
        vector_copy,
    )


def solution(mesh):
    placed = (
        P("group", None, ("fsdp", "tensor"), None, None),
        P("group", None, ("fsdp", "tensor"), None, None),
        P("group", None, None),
        P(None, "fsdp", "tensor"),
        P(None, "fsdp", "tensor"),
        P(),
        P("group", None, None, "fsdp", "tensor"),
        P("group", None, None, "fsdp", "tensor"),
        P("group", None, None, None),
        P(None, "fsdp", "tensor"),
        P(None, "fsdp", "tensor"),
        P(),
    )
    return jax.shard_map(
        local,
        mesh=mesh,
        in_specs=placed,
        out_specs=(
            P("group", None, ("fsdp", "tensor"), None, None),
            P("group", None, ("fsdp", "tensor"), None, None),
            P("group", None, None, "fsdp", "tensor"),
            P(None, None, "fsdp", "tensor"),
            P(None, "fsdp", "tensor"),
            P("group", None, None, "fsdp", "tensor"),
            P(None, None, "fsdp", "tensor"),
            P(None, "fsdp", "tensor"),
            P("group", None, None, None),
            P(),
            P(),
        ),
        check_vma=False,
    )
```

```python
import functools

import jax
import jax.numpy as jnp
from jax import lax
from jax.experimental import pallas as pl
from jax.experimental.pallas import tpu as pltpu
from jax.sharding import PartitionSpec as P

HD = 64
STEP = 8
IMG_DEV = 4
EPSILON = 1e-06
INNER_RATE = 0.02
VECTOR_RATE = 0.2
WEIGHT_DECAY = 0.1
OUTER_RATE = 0.7
OUTER_MOMENTUM = 0.9
QUARTERS = 4
PARTS = 2
LOW = jnp.bfloat16
F32 = jnp.float32
NN = (((1,), (0,)), ((), ()))
NT = (((1,), (1,)), ((), ()))
TN = (((0,), (0,)), ((), ()))


def dot(a, b, dims=NN):
    return lax.dot_general(a, b, dims, preferred_element_type=F32)


MESH = pl.DeviceIdType.MESH


def params(identity=None):
    if identity is None:
        return pltpu.CompilerParams(vmem_limit_bytes=60 * 2**20)
    return pltpu.CompilerParams(vmem_limit_bytes=60 * 2**20, collective_id=identity, has_side_effects=True)


def partner():
    return (lax.axis_index("group"), 1 - lax.axis_index("fsdp"), lax.axis_index("tensor"))


def greet_partner():
    barrier = pltpu.get_barrier_semaphore()
    pl.semaphore_signal(barrier, inc=1, device_id=partner(), device_id_type=MESH)
    pl.semaphore_wait(barrier, 1)


def to_partner(sent, received, sends, receives, n):
    return pltpu.make_async_remote_copy(
        src_ref=sent.at[n],
        dst_ref=received.at[n],
        send_sem=sends.at[n],
        recv_sem=receives.at[n],
        device_id=partner(),
        device_id_type=MESH,
    )


def bands(depth):
    f = lax.axis_index("fsdp")
    return pl.ds(pl.multiple_of(f * depth, depth), depth), pl.ds(pl.multiple_of((1 - f) * depth, depth), depth)


def exchange_scratch(steps, shape):
    dma = pltpu.SemaphoreType.DMA
    return [
        pltpu.VMEM((steps, *shape), F32),
        pltpu.VMEM((steps, *shape), LOW),
        pltpu.VMEM((steps, *shape), LOW),
        dma((steps,)),
        dma((steps,)),
    ]


def cost(flops, moved, special=0):
    return pl.CostEstimate(flops=int(flops), bytes_accessed=int(moved), transcendentals=int(special))


def padded(rows):
    return -(-rows // 16) * 16


def centred(source):
    centre = source - jnp.mean(source, axis=-1, keepdims=True)
    spread = jnp.mean(centre * centre, axis=-1, keepdims=True)
    inverse = lax.rsqrt(spread + EPSILON)
    return centre * inverse, inverse


def norm_back(upstream, normal, inverse, gain):
    pulled = upstream * gain
    mean_one = jnp.mean(pulled, axis=-1, keepdims=True)
    mean_two = jnp.mean(pulled * normal, axis=-1, keepdims=True)
    return inverse * (pulled - mean_one - normal * mean_two)


def project_kernel(images, seq, x_ref, w_ref, vec_ref, n_ref, out_ref, n_scr):
    j, t = pl.program_id(0), pl.program_id(1)
    span = n_scr.shape[0] // images

    @pl.when((j == 0) & (t == 0))
    def _():
        n_scr[...] = jnp.zeros_like(n_scr)
        for i in range(images):
            normal, _ = centred(x_ref[i].astype(F32))
            n_scr[pl.ds(i * span, seq), :] = (normal * vec_ref[0:1] + vec_ref[1:2]).astype(LOW)
        n_ref[...] = n_scr[...]

    cols = out_ref.shape[-1]
    out = dot(n_scr[...], w_ref[0, 0])
    at = pl.ds(pl.multiple_of(t * cols, cols), cols)
    bias = jnp.where(j == 0, vec_ref[4:5, at], jnp.where(j == 2, vec_ref[5:6, at], 0.0))
    out_ref[0] = (out + bias).astype(LOW)


def project(patches, w_attn, vec):
    images, seq, width = patches.shape
    shards, _, _, cols = w_attn.shape
    rows = images * padded(seq)
    return pl.pallas_call(
        functools.partial(project_kernel, images, seq),
        grid=(3, shards),
        in_specs=[
            pl.BlockSpec((images, seq, width), lambda j, t: (0, 0, 0)),
            pl.BlockSpec((1, 1, width, cols), lambda j, t: (t, j, 0, 0)),
            pl.BlockSpec(vec.shape, lambda j, t: (0, 0)),
        ],
        out_specs=[
            pl.BlockSpec((rows, width), lambda j, t: (0, 0)),
            pl.BlockSpec((1, rows, cols), lambda j, t: (j, 0, t)),
        ],
        out_shape=[
            jax.ShapeDtypeStruct((rows, width), LOW),
            jax.ShapeDtypeStruct((3, rows, width), LOW),
        ],
        scratch_shapes=[pltpu.VMEM((rows, width), LOW)],
        compiler_params=params(),
        cost_estimate=cost(6 * rows * width * width, 16 * rows * width),
        name="project",
    )(patches, w_attn, vec)


def half_lanes(value, which):
    lane = lax.broadcasted_iota(jnp.int32, value.shape, 1)
    return jnp.where((lane >= HD) == bool(which), value, jnp.zeros_like(value))


def attend_kernel(seq, q_ref, k_ref, v_ref, out_ref):
    span = q_ref.shape[1]
    scale = HD**-0.5
    q, k, v = q_ref[0], k_ref[0], v_ref[0]
    parts = []
    for h in range(2):
        scores = dot(q, half_lanes(k, h), NT)
        lane = lax.broadcasted_iota(jnp.int32, scores.shape, 1)
        scores = jnp.where(lane < seq, scores, -1e30)
        top = jnp.max(scores, axis=1, keepdims=True)
        raised = jnp.exp((scores - top) * scale)
        total = jnp.sum(raised, axis=1, keepdims=True)
        probs = (raised * (1.0 / total)).astype(LOW)
        parts.append(dot(probs, v))
    lane = lax.broadcasted_iota(jnp.int32, (span, 2 * HD), 1)
    out_ref[...] = jnp.where(lane < HD, parts[0], parts[1]).astype(LOW)


def attend(qkv, images, seq):
    _, rows, width = qkv.shape
    span = rows // images
    pair = 2 * HD

    def take(j):
        return pl.BlockSpec((1, span, pair), lambda i, h: (j, i, h))

    return pl.pallas_call(
        functools.partial(attend_kernel, seq),
        grid=(images, width // pair),
        in_specs=[take(0), take(1), take(2)],
        out_specs=pl.BlockSpec((span, pair), lambda i, h: (i, h)),
        out_shape=jax.ShapeDtypeStruct((rows, width), LOW),
        compiler_params=params(),
        cost_estimate=cost(16 * rows * span * width, 8 * rows * width, rows * span * (width // HD)),
        name="attend",
    )(qkv, qkv, qkv)


def mix_kernel(seq, alive_ref, att_ref, x_ref, g_ref, w_ref, vec_ref, resid_ref, n_ref, g2_ref, x_scr):
    i = pl.program_id(0)
    shards, _, _, cols = w_ref.shape
    x_scr[...] = jnp.zeros_like(x_scr)
    x_scr[0:seq, :] = x_ref[0].astype(F32)
    total = x_scr[...] + vec_ref[6:7]
    for t in range(shards):
        total = total + dot(att_ref[:, t * cols : (t + 1) * cols], w_ref[t, 0], NT)
    resid_ref[...] = total
    normal, _ = centred(total)
    n_ref[...] = (normal * vec_ref[2:3] + vec_ref[3:4]).astype(LOW)
    x_scr[0:seq, :] = g_ref[0].astype(F32) * alive_ref[i]
    g2_ref[...] = x_scr[...].astype(LOW)


def mix(alive, attended, patches, cotangent, w_attn, vec):
    images, seq, width = patches.shape
    rows = attended.shape[0]
    span = rows // images
    shards, _, _, cols = w_attn.shape
    block = pl.BlockSpec((span, width), lambda i: (i, 0))
    whole = jax.ShapeDtypeStruct((rows, width), LOW)
    return pl.pallas_call(
        functools.partial(mix_kernel, seq),
        grid=(images,),
        in_specs=[
            pl.BlockSpec(memory_space=pltpu.SMEM),
            block,
            pl.BlockSpec((1, seq, width), lambda i: (i, 0, 0)),
            pl.BlockSpec((1, seq, width), lambda i: (i, 0, 0)),
            pl.BlockSpec((shards, 1, width, cols), lambda i: (0, 3, 0, 0)),
            pl.BlockSpec(vec.shape, lambda i: (0, 0)),
        ],
        out_specs=[block, block, block],
        out_shape=[jax.ShapeDtypeStruct((rows, width), F32), whole, whole],
        scratch_shapes=[pltpu.VMEM((span, width), F32)],
        compiler_params=params(),
        cost_estimate=cost(2 * rows * width * width, 16 * rows * width),
        name="mix",
    )(alive, attended, patches, cotangent, w_attn, vec)


def mlp_kernel(first, pairwise, chunk, n_ref, g_ref, w1_ref, w2_ref, bias_ref, *refs):
    if not first:
        yi_ref, gi_ref, *refs = refs
    y_ref, gn_ref, dw_ref, db_ref, h_scr, p_scr, nt_scr, gt_scr, *exchange = refs
    step = pl.program_id(0)
    rows = n_ref.shape[0]
    each, _, width, cols = w1_ref.shape

    @pl.when(step == 0)
    def _():
        if pairwise:
            greet_partner()
        nt_scr[...] = n_ref[...].T
        gt_scr[...] = g_ref[...].T
        if first:
            y_ref[...] = jnp.zeros_like(y_ref)
            gn_ref[...] = jnp.zeros_like(gn_ref)
        else:
            y_ref[...] = yi_ref[...]
            gn_ref[...] = gi_ref[...]

    w1 = jnp.concatenate([w1_ref[t, 0] for t in range(each)], axis=1)
    w2 = jnp.concatenate([w2_ref[t, 0] for t in range(each)], axis=1)
    bias = jnp.concatenate([bias_ref[t] for t in range(each)], axis=1)

    def body(c, sums):
        at = pl.ds(pl.multiple_of(c * chunk, chunk), chunk)
        pre = dot(n_ref[at, :], w1) + bias
        cdf = 0.5 * (1.0 + lax.erf(pre * 0.7071067811865476))
        hidden = (pre * cdf).astype(LOW)
        slope = cdf + pre * jnp.exp(-0.5 * pre * pre) * 0.3989422804014327
        gp = dot(g_ref[at, :], w2) * slope
        gl = gp.astype(LOW)
        h_scr[at, :] = hidden
        p_scr[at, :] = gl
        y_ref[at, :] += dot(hidden, w2, NT)
        gn_ref[at, :] += dot(gl, w1, NT)
        return sums + jnp.sum(gl.astype(F32), axis=0, keepdims=True)

    sums = lax.fori_loop(0, rows // chunk, body, jnp.zeros((1, each * cols), F32))
    for t in range(each):
        db_ref[t] = sums[:, t * cols : (t + 1) * cols]
    if pairwise:
        own, sent, received, sends, receives = exchange
        ours, theirs = bands(width // 2)
        sent[step, 0] = dot(nt_scr[theirs, :], p_scr[...]).astype(LOW)
        sent[step, 1] = dot(gt_scr[theirs, :], h_scr[...]).astype(LOW)
        to_partner(sent, received, sends, receives, step).start()
        own[step, 0] = dot(nt_scr[ours, :], p_scr[...])
        own[step, 1] = dot(gt_scr[ours, :], h_scr[...])

        @pl.when(step == pl.num_programs(0) - 1)
        def _():
            for n in range(own.shape[0]):
                to_partner(sent, received, sends, receives, n).wait()
                for which in range(2):
                    total = (own[n, which] + received[n, which].astype(F32)).astype(LOW)
                    for t in range(each):
                        dw_ref[n * each + t, which] = total[:, t * cols : (t + 1) * cols]

        return
    shards, depth = dw_ref.shape[0], dw_ref.shape[3]
    d1 = dot(nt_scr[...], p_scr[...]).astype(LOW)
    d2 = dot(gt_scr[...], h_scr[...]).astype(LOW)
    for f in range(shards):
        for t in range(each):
            dw_ref[f, t, 0] = d1[f * depth : (f + 1) * depth, t * cols : (t + 1) * cols]
            dw_ref[f, t, 1] = d2[f * depth : (f + 1) * depth, t * cols : (t + 1) * cols]


def mlp(quarter, quarters, normed, grad_two, w_mlp, bias, carried, fsdp):
    rows, width = normed.shape
    shards, _, _, hidden = w_mlp.shape
    cols = hidden // quarters
    each = 2
    first, pairwise = carried is None, fsdp == 2
    single = pl.Buffered(1)
    full = pl.BlockSpec((rows, width), lambda s: (0, 0), pipeline_mode=single)
    depth = width // fsdp
    steps = shards // each
    acc_shape = jax.ShapeDtypeStruct((rows, width), F32)
    if pairwise:
        out_w = pl.BlockSpec((shards, 2, depth, cols), lambda s: (0, 0, 0, 0), pipeline_mode=single)
        w_shape = jax.ShapeDtypeStruct((shards, 2, depth, cols), LOW)
        extra = exchange_scratch(steps, (2, depth, each * cols))
    else:
        out_w = pl.BlockSpec((fsdp, each, 2, depth, cols), lambda s: (0, s, 0, 0, 0))
        w_shape = jax.ShapeDtypeStruct((fsdp, shards, 2, depth, cols), LOW)
        extra = []
    return pl.pallas_call(
        functools.partial(mlp_kernel, first, pairwise, rows // 4),
        grid=(steps,),
        in_specs=[
            full,
            full,
            pl.BlockSpec((each, 1, width, cols), lambda s: (s, 0, 0, quarter)),
            pl.BlockSpec((each, 1, width, cols), lambda s: (s, 1, 0, quarter)),
            pl.BlockSpec((each, 1, cols), lambda s: (s, 0, quarter)),
        ]
        + ([] if first else [full, full]),
        out_specs=[full, full, out_w, pl.BlockSpec((each, 1, cols), lambda s: (s, 0, 0))],
        out_shape=[acc_shape, acc_shape, w_shape, jax.ShapeDtypeStruct((shards, 1, cols), F32)],
        scratch_shapes=[
            pltpu.VMEM((rows, each * cols), LOW),
            pltpu.VMEM((rows, each * cols), LOW),
            pltpu.VMEM((width, rows), LOW),
            pltpu.VMEM((width, rows), LOW),
            *extra,
        ],
        compiler_params=params(2 + quarter if pairwise else None),
        cost_estimate=cost(12 * rows * width * cols * shards, 24 * rows * width),
        name=f"mlp_{quarter}",
    )(normed, grad_two, w_mlp, w_mlp, bias, *([] if first else carried))


def turn_kernel(seq, pairwise, alive_ref, resid_ref, y_ref, gn_ref, g2_ref, att_ref, w_ref, vec_ref,
                out_ref, gr_ref, ga_ref, dw_ref, sums_ref, dw_scr, *exchange):
    i = pl.program_id(0)
    if pairwise:
        pl.when(i == 0)(greet_partner)
    shards, _, _, cols = w_ref.shape
    resid = resid_ref[...]
    out_ref[0] = ((resid + y_ref[...] + vec_ref[7:8]) * alive_ref[i]).astype(LOW)[0:seq]
    normal, inverse = centred(resid)
    upstream = gn_ref[...]
    grad_out = g2_ref[...].astype(F32)
    grad_resid = grad_out + norm_back(upstream, normal, inverse, vec_ref[2:3])
    gr_ref[...] = grad_resid
    low = grad_resid.astype(LOW)
    rows = [
        jnp.sum(upstream * normal, axis=0, keepdims=True),
        jnp.sum(upstream, axis=0, keepdims=True),
        jnp.sum(grad_resid, axis=0, keepdims=True),
        jnp.sum(grad_out, axis=0, keepdims=True),
    ]
    rows = jnp.concatenate(rows, axis=0)

    @pl.when(i == 0)
    def _():
        sums_ref[...] = rows

    @pl.when(i != 0)
    def _():
        sums_ref[...] += rows

    for t in range(shards):
        ga_ref[:, t * cols : (t + 1) * cols] = dot(low, w_ref[t, 0]).astype(LOW)
    part = dot(low.T, att_ref[...])

    @pl.when(i == 0)
    def _():
        dw_scr[...] = part

    @pl.when(i != 0)
    def _():
        dw_scr[...] += part

    @pl.when(i == pl.num_programs(0) - 1)
    def _():
        if pairwise:
            sent, received, sends, receives = exchange
            ours, theirs = bands(dw_scr.shape[0] // 2)
            sent[0] = dw_scr[theirs, :].astype(LOW)
            copy = to_partner(sent, received, sends, receives, 0)
            copy.start()
            copy.wait()
            total = (dw_scr[ours, :] + received[0].astype(F32)).astype(LOW)
            for t in range(shards):
                dw_ref[t, 0] = total[:, t * cols : (t + 1) * cols]
            return
        depth = dw_ref.shape[3]
        for f in range(dw_ref.shape[0]):
            for t in range(shards):
                dw_ref[f, t, 0] = dw_scr[f * depth : (f + 1) * depth, t * cols : (t + 1) * cols].astype(LOW)


def turn(alive, resid, branch, grad_normed, grad_two, attended, w_attn, vec, images, seq, fsdp):
    rows, width = resid.shape
    span = rows // images
    shards, _, _, cols = w_attn.shape
    depth = width // fsdp
    pairwise = fsdp == 2
    lead = () if pairwise else (fsdp,)
    block = pl.BlockSpec((span, width), lambda i: (i, 0))
    return pl.pallas_call(
        functools.partial(turn_kernel, seq, pairwise),
        grid=(images,),
        in_specs=[
            pl.BlockSpec(memory_space=pltpu.SMEM),
            block, block, block, block, block,
            pl.BlockSpec((shards, 1, width, cols), lambda i: (0, 3, 0, 0)),
            pl.BlockSpec(vec.shape, lambda i: (0, 0)),
        ],
        out_specs=[
            pl.BlockSpec((1, seq, width), lambda i: (i, 0, 0)),
            block, block,
            pl.BlockSpec((*lead, shards, 1, depth, cols), lambda i: (0,) * (4 + len(lead))),
            pl.BlockSpec((4, width), lambda i: (0, 0)),
        ],
        out_shape=[
            jax.ShapeDtypeStruct((images, seq, width), LOW),
            jax.ShapeDtypeStruct((rows, width), F32),
            jax.ShapeDtypeStruct((rows, width), LOW),
            jax.ShapeDtypeStruct((*lead, shards, 1, depth, cols), LOW),
            jax.ShapeDtypeStruct((4, width), F32),
        ],
        scratch_shapes=[pltpu.VMEM((width, width), F32)] + (exchange_scratch(1, (depth, width))[1:] if pairwise else []),
        compiler_params=params(6 if pairwise else None),
        cost_estimate=cost(4 * rows * width * width, 24 * rows * width),
        name="turn",
    )(alive, resid, branch, grad_normed, grad_two, attended, w_attn, vec)


def unattend_kernel(seq, q_ref, k_ref, v_ref, g_ref, dq_ref, dk_ref, dv_ref):
    span = q_ref.shape[1]
    scale = HD**-0.5
    q, k, v, g = q_ref[0], k_ref[0], v_ref[0], g_ref[...]
    parts = []
    for h in range(2):
        scores = dot(half_lanes(k, h), q, NT)
        row = lax.broadcasted_iota(jnp.int32, scores.shape, 0)
        scores = jnp.where(row < seq, scores, -1e30)
        top = jnp.max(scores, axis=0, keepdims=True)
        raised = jnp.exp((scores - top) * scale)
        total = jnp.sum(raised, axis=0, keepdims=True)
        probs = raised * (1.0 / total)
        gp = dot(half_lanes(v, h), g, NT)
        delta = jnp.sum(probs * gp, axis=0, keepdims=True)
        gs = (probs * (gp - delta)).astype(LOW)
        dv = dot(probs.astype(LOW), g)
        dk = dot(gs, q)
        dq = dot(gs, k, TN)
        parts.append((dq, dk, dv))
    lane = lax.broadcasted_iota(jnp.int32, (span, 2 * HD), 1) < HD
    dq_ref[0] = (jnp.where(lane, parts[0][0], parts[1][0]) * scale).astype(LOW)
    dk_ref[0] = (jnp.where(lane, parts[0][1], parts[1][1]) * scale).astype(LOW)
    dv_ref[0] = jnp.where(lane, parts[0][2], parts[1][2]).astype(LOW)


def unattend(qkv, grad_attended, images, seq, part, parts, shards):
    _, rows, width = qkv.shape
    span = rows // images
    pair = 2 * HD
    each = width // shards // parts // pair

    def spot(h):
        return (h // each) * (each * parts) + part * each + h % each

    def take(j):
        return pl.BlockSpec((1, span, pair), lambda i, h: (j, i, spot(h)))

    out = pl.BlockSpec((1, span, pair), lambda i, h: (0, i, h))
    shape = jax.ShapeDtypeStruct((1, rows, width // parts), LOW)
    return pl.pallas_call(
        functools.partial(unattend_kernel, seq),
        grid=(images, width // pair // parts),
        in_specs=[take(0), take(1), take(2), pl.BlockSpec((span, pair), lambda i, h: (i, spot(h)))],
        out_specs=[out, out, out],
        out_shape=[shape, shape, shape],
        compiler_params=params(),
        cost_estimate=cost(
            40 * rows * span * width // parts, 14 * rows * width // parts, rows * span * (width // HD) // parts
        ),
        name=f"unattend_{part}",
    )(qkv, qkv, qkv, grad_attended)


def close_kernel(seq, images, pairwise, first, final, n_ref, dq_ref, dk_ref, dv_ref, w_ref, *refs):
    if not first:
        carry_ref, *refs = refs
    if final:
        x_ref, gr_ref, vec_ref, out_ref, norm_ref, *refs = refs
    else:
        acc_ref, *refs = refs
    dw_ref, sums_ref, acc_scr, nt_scr, *exchange = refs
    j = pl.program_id(0)
    shards, _, _, cols = w_ref.shape
    span = n_ref.shape[0] // images
    if pairwise:
        own, sent, received, sends, receives = exchange
        pl.when(j == 0)(greet_partner)

    @pl.when(j == 0)
    def _():
        nt_scr[...] = n_ref[...].T
        acc_scr[...] = jnp.zeros_like(acc_scr) if first else carry_ref[...]
        sums_ref[0:1, :] = jnp.sum(dq_ref[0].astype(F32), axis=0, keepdims=True)
        sums_ref[1:2, :] = jnp.sum(dv_ref[0].astype(F32), axis=0, keepdims=True)

    def spread(n, total, f=None):
        for t in range(shards):
            piece = total[:, t * cols : (t + 1) * cols]
            if f is None:
                dw_ref[t, n] = piece
            else:
                dw_ref[f, t, 0] = piece

    def step(ref):
        weight = jnp.concatenate([w_ref[t, 0] for t in range(shards)], axis=1)
        if pairwise:
            ours, theirs = bands(nt_scr.shape[0] // 2)
            sent[j] = dot(nt_scr[theirs, :], ref[0]).astype(LOW)
            to_partner(sent, received, sends, receives, j).start()
            own[j] = dot(nt_scr[ours, :], ref[0])
        else:
            depth = dw_ref.shape[3]
            dw = dot(nt_scr[...], ref[0]).astype(LOW)
            for f in range(dw_ref.shape[0]):
                spread(0, dw[f * depth : (f + 1) * depth], f)
        acc_scr[...] += dot(ref[0], weight, NT)

    @pl.when(j == 0)
    def _():
        step(dq_ref)

    @pl.when(j == 1)
    def _():
        step(dk_ref)

    @pl.when(j == 2)
    def _():
        step(dv_ref)
        if pairwise:
            for n in range(own.shape[0]):
                to_partner(sent, received, sends, receives, n).wait()
                spread(n, (own[n] + received[n].astype(F32)).astype(LOW))
        if not final:
            acc_ref[...] = acc_scr[...]
            return
        gain = jnp.zeros((1, vec_ref.shape[1]), F32)
        shift = jnp.zeros((1, vec_ref.shape[1]), F32)
        for i in range(images):
            normal, inverse = centred(x_ref[i].astype(F32))
            upstream = acc_scr[i * span : i * span + seq, :]
            out_ref[i] = gr_ref[i * span : i * span + seq, :] + norm_back(upstream, normal, inverse, vec_ref[0:1])
            gain += jnp.sum(upstream * normal, axis=0, keepdims=True)
            shift += jnp.sum(upstream, axis=0, keepdims=True)
        norm_ref[0:1, :] = gain
        norm_ref[1:2, :] = shift


def close(part, parts, normed, grads, w_attn, carry, ending, fsdp, images, seq):
    rows, width = normed.shape
    shards, _, _, cols = w_attn.shape
    cols = cols // parts
    lanes = shards * cols
    depth = width // fsdp
    pairwise, first, final = fsdp == 2, carry is None, ending is not None
    single = pl.Buffered(1)
    stack = pl.BlockSpec((1, rows, lanes), lambda j: (0, 0, 0), pipeline_mode=single)
    full = pl.BlockSpec((rows, width), lambda j: (0, 0), pipeline_mode=single)
    image = pl.BlockSpec((images, seq, width), lambda j: (0, 0, 0), pipeline_mode=single)
    if pairwise:
        dw_spec = pl.BlockSpec((shards, 3, depth, cols), lambda j: (0, 0, 0, 0), pipeline_mode=single)
        dw_shape = jax.ShapeDtypeStruct((shards, 3, depth, cols), LOW)
        extra = exchange_scratch(3, (depth, lanes))
    else:
        dw_spec = pl.BlockSpec((fsdp, shards, 1, depth, cols), lambda j: (0, 0, j, 0, 0))
        dw_shape = jax.ShapeDtypeStruct((fsdp, shards, 3, depth, cols), LOW)
        extra = []
    in_specs = [full, stack, stack, stack, pl.BlockSpec((shards, 1, width, cols), lambda j: (0, j, 0, part))]
    out_specs, out_shape = [], []
    if not first:
        in_specs.append(full)
    if final:
        in_specs += [image, full, pl.BlockSpec((12, width), lambda j: (0, 0))]
        out_specs += [image, pl.BlockSpec((2, width), lambda j: (0, 0))]
        out_shape += [jax.ShapeDtypeStruct((images, seq, width), F32), jax.ShapeDtypeStruct((2, width), F32)]
    else:
        out_specs.append(full)
        out_shape.append(jax.ShapeDtypeStruct((rows, width), F32))
    return pl.pallas_call(
        functools.partial(close_kernel, seq, images, pairwise, first, final),
        grid=(3,),
        in_specs=in_specs,
        out_specs=[*out_specs, dw_spec, pl.BlockSpec((2, lanes), lambda j: (0, 0))],
        out_shape=[*out_shape, dw_shape, jax.ShapeDtypeStruct((2, lanes), F32)],
        scratch_shapes=[pltpu.VMEM((rows, width), F32), pltpu.VMEM((width, rows), LOW), *extra],
        compiler_params=params(7 + part if pairwise else None),
        cost_estimate=cost(12 * rows * width * lanes, 20 * rows * width),
        name=f"close_{part}",
    )(normed, *grads, w_attn, *([] if first else [carry]), *(ending if final else []))


def gather_kernel(a_in, m_in, a_out, m_out, a_hold, m_hold, zs, zr, xs, xr, ys, yr, xfs, xfr, yfs, yfr, cs, cr, ls):
    g, f, z = lax.axis_index("group"), lax.axis_index("fsdp"), lax.axis_index("tensor")
    last = lax.axis_size("tensor") - 1
    x_at, y_at = g % 2, g // 2
    east, north = y_at * 2 + (1 - x_at), (1 - y_at) * 2 + x_at
    depth = a_in.shape[1]
    band = depth // 4
    shared = band * 3 // 8
    rest = band - 2 * shared

    def place(column):
        cx, cy = column % 2, column // 2
        return 2 * (cx + cy - 2 * cx * cy) + cy

    mine, of_east, of_north = place(g), place(east), place(north)
    z_row = mine * band - shared * (mine % 2)
    lead_east = of_east * band + shared * (of_east % 2)
    lead_north = of_north * band + shared * (of_north % 2)
    chunks = ((a_in, a_out, 0, a_in.shape[0]), (m_in, m_out, 0, 1), (m_in, m_out, 1, 1))

    def tile(n):
        return pl.multiple_of(n, 16)

    def held(n, t, row, rows):
        _, out, j, many = chunks[n]
        return out.at[t, pl.ds(j, many), pl.ds(tile(f * depth + row), rows), :]

    def owned(n, row, rows):
        source, _, j, many = chunks[n]
        return source.at[pl.ds(j, many), pl.ds(tile(row), rows), :]

    def send(src, dst, sems, semr, n, t, to):
        return pltpu.make_async_remote_copy(
            src_ref=src, dst_ref=dst, send_sem=sems.at[n, t], recv_sem=semr.at[n, t], device_id=to, device_id_type=MESH
        )

    def along(n, t, up, src):
        return pltpu.make_async_remote_copy(
            src_ref=src,
            dst_ref=held(n, t, z_row, band + shared),
            send_sem=zs.at[n, t, 0 if up else 1],
            recv_sem=zr.at[n, t],
            device_id=(g, f, z + 1 if up else z - 1),
            device_id_type=MESH,
        )

    def to_east(n, t):
        part = held(n, t, mine * band, band)
        return send(part, part, xs, xr, n, t, (east, f, z))

    def to_north(n, t):
        part = held(n, t, mine * band, band)
        return send(part, part, ys, yr, n, t, (north, f, z))

    def north_to_east(n, t):
        part = held(n, t, lead_north, shared)
        return send(part, part, xfs, xfr, n, t, (east, f, z))

    def east_to_north(n, t):
        part = held(n, t, lead_east + shared, rest)
        return send(part, part, yfs, yfr, n, t, (north, f, z))

    def across(n, t, src):
        return send(src, held(n, t, 0, depth), cs, cr, n, t, (g, 1 - f, z))

    barrier = pltpu.get_barrier_semaphore()

    def greet(to):
        pl.semaphore_signal(barrier, inc=1, device_id=to, device_id_type=MESH)

    for to in ((east, f, z), (north, f, z), (g, 1 - f, z)):
        greet(to)

    @pl.when(z > 0)
    def _():
        greet((g, f, z - 1))

    @pl.when(z < last)
    def _():
        greet((g, f, z + 1))

    pl.semaphore_wait(barrier, 3 + jnp.minimum(z, 1) + jnp.minimum(last - z, 1))

    load_a = pltpu.make_async_copy(a_in, a_hold, ls.at[0])
    load_m = pltpu.make_async_copy(m_in, m_hold, ls.at[1])
    load_a.start()
    load_m.start()

    items = [(n, k, up) for n in range(3) for k in range(1, last + 1) for up in (True, False)]

    def when_real(k, up, run):
        @pl.when(z - k >= 0 if up else z + k <= last)
        def _():
            run(z - k if up else z + k)

    def own(n):
        @pl.when(z < last)
        def _():
            along(n, z, True, owned(n, z_row, band + shared)).start()

        @pl.when(z > 0)
        def _():
            along(n, z, False, owned(n, z_row, band + shared)).start()

        across(n, z, owned(n, 0, depth)).start()

    def land(n, k, up):
        def run(t):
            along(n, t, up, held(n, t, z_row, band + shared)).wait_recv()

            @pl.when(z < last if up else z > 0)
            def _():
                along(n, t, up, held(n, t, z_row, band + shared)).start()

            to_east(n, t).start()
            to_north(n, t).start()

        when_real(k, up, run)

    def relay(n, k, up):
        def run(t):
            to_east(n, t).wait_recv()
            east_to_north(n, t).start()
            to_north(n, t).wait_recv()
            north_to_east(n, t).start()

        when_real(k, up, run)

    def finish(n, k, up):
        def run(t):
            east_to_north(n, t).wait_recv()
            north_to_east(n, t).wait_recv()
            across(n, t, held(n, t, 0, depth)).start()

        when_real(k, up, run)

    for at in range(len(items) + 4):
        if at % (2 * last) == 0 and at // (2 * last) < 3:
            own(at // (2 * last))
        if at < len(items):
            land(*items[at])
        if 0 <= at - 2 < len(items):
            relay(*items[at - 2])
        if 0 <= at - 4 < len(items):
            finish(*items[at - 4])

    load_a.wait()
    load_m.wait()
    rows = pl.ds(tile(f * depth), depth)
    keep_a = pltpu.make_async_copy(a_hold, a_out.at[z, :, rows, :], ls.at[2])
    keep_m = pltpu.make_async_copy(m_hold, m_out.at[z, :, rows, :], ls.at[3])
    keep_a.start()
    keep_m.start()
    keep_a.wait()
    keep_m.wait()

    for n in range(3):
        @pl.when(z < last)
        def _():
            along(n, z, True, owned(n, z_row, band + shared)).wait_send()

        @pl.when(z > 0)
        def _():
            along(n, z, False, owned(n, z_row, band + shared)).wait_send()

        across(n, z, owned(n, 0, depth)).wait()

    def settle(n, k, up):
        def run(t):
            @pl.when(z < last if up else z > 0)
            def _():
                along(n, t, up, held(n, t, z_row, band + shared)).wait_send()

            to_east(n, t).wait_send()
            to_north(n, t).wait_send()
            east_to_north(n, t).wait_send()
            north_to_east(n, t).wait_send()
            across(n, t, held(n, t, 0, depth)).wait()

        when_real(k, up, run)

    for item in items:
        settle(*item)


def gather(attn_low, mlp_low, shards):
    _, depth, a_cols = attn_low.shape
    _, _, m_cols = mlp_low.shape
    width = 2 * depth
    anywhere = pl.BlockSpec(memory_space=pl.ANY)
    dma = pltpu.SemaphoreType.DMA
    return pl.pallas_call(
        gather_kernel,
        in_specs=[anywhere, anywhere],
        out_specs=[anywhere, anywhere],
        out_shape=[
            jax.ShapeDtypeStruct((shards, 4, width, a_cols), LOW),
            jax.ShapeDtypeStruct((shards, 2, width, m_cols), LOW),
        ],
        scratch_shapes=[
            pltpu.VMEM(attn_low.shape, LOW),
            pltpu.VMEM(mlp_low.shape, LOW),
            dma((3, shards, 2)),
        ]
        + [dma((3, shards))] * 11
        + [dma((4,))],
        compiler_params=pltpu.CompilerParams(
            collective_id=1, has_side_effects=True, vmem_limit_bytes=60 * 2**20
        ),
        name="gather",
    )(attn_low, mlp_low)


def inner_adamw(master, gradient, first, second, step_rate, decay_rate):
    first_moment = 0.9 * first + 0.1 * gradient
    second_moment = 0.95 * second + 0.05 * gradient * gradient
    step_ratio = (
        first_moment / (1.0 - 0.9**STEP) / (jnp.sqrt(second_moment / (1.0 - 0.95**STEP)) + 1e-08)
    )
    return (master - step_rate * (step_ratio + decay_rate * master), second_moment)


def outer_nesterov(master, outer_old, difference):
    momentum = OUTER_MOMENTUM * outer_old + difference
    return momentum, master - OUTER_RATE * (difference + OUTER_MOMENTUM * momentum)


def inner_kernel(join, count, *refs):
    pieces, (master_ref, moment_ref, inner_ref, diff_ref) = refs[:count], refs[count:]
    gradient = join(*[piece[0] for piece in pieces]).astype(F32)
    master = master_ref[0]
    new, second = inner_adamw(master, gradient, moment_ref[0, 0, 0], moment_ref[0, 1, 0], INNER_RATE, WEIGHT_DECAY)
    inner_ref[0, 0, 0] = gradient
    inner_ref[0, 1, 0] = second
    diff_ref[0] = (master - new).astype(LOW)


def inner_step(join, places, pieces, master, moments, name):
    many, depth, cols = master.shape
    rows = min(depth, 131072 // cols)
    block = pl.BlockSpec((1, rows, cols), lambda j, r: (j, r, 0))
    both = pl.BlockSpec((1, 2, 1, rows, cols), lambda j, r: (0, 0, j, r, 0))

    def piece_spec(piece, place):
        return pl.BlockSpec((1, rows, piece.shape[2]), lambda j, r: (place(j), r, 0))

    return pl.pallas_call(
        functools.partial(inner_kernel, join, len(pieces)),
        grid=(many, depth // rows),
        in_specs=[piece_spec(piece, place) for piece, place in zip(pieces, places)] + [block, both],
        out_specs=[both, block],
        out_shape=[jax.ShapeDtypeStruct(moments.shape, F32), jax.ShapeDtypeStruct(master.shape, LOW)],
        compiler_params=params(),
        cost_estimate=cost(30 * master.size, 24 * master.size),
        name=name,
    )(*pieces, master, moments)


def outer_kernel(groups, total_ref, master_ref, outer_ref, state_ref, copy_ref):
    difference = total_ref[0].astype(F32) / groups
    momentum, fresh = outer_nesterov(master_ref[0], outer_ref[0], difference)
    state_ref[0, 0] = difference
    state_ref[1, 0] = momentum
    state_ref[2, 0] = fresh
    copy_ref[0] = fresh.astype(LOW)


def outer_step(groups, total, master, outer_old, name):
    many, depth, cols = master.shape
    rows = min(depth, 131072 // cols)
    block = pl.BlockSpec((1, rows, cols), lambda j, r: (j, r, 0))
    return pl.pallas_call(
        functools.partial(outer_kernel, groups),
        grid=(many, depth // rows),
        in_specs=[block, block, block],
        out_specs=[pl.BlockSpec((3, 1, rows, cols), lambda j, r: (0, j, r, 0)), block],
        out_shape=[jax.ShapeDtypeStruct((3, *master.shape), F32), jax.ShapeDtypeStruct(master.shape, LOW)],
        compiler_params=params(),
        cost_estimate=cost(10 * master.size, 24 * master.size),
        name=name,
    )(total, master, outer_old)


def group_kernel(groups, diff_ref, total_ref, landed, summed, sends, receives, sends_two, receives_two):
    g, f, t = lax.axis_index("group"), lax.axis_index("fsdp"), lax.axis_index("tensor")
    span = landed.shape[1]

    def rows(n):
        return pl.ds(pl.multiple_of(n * span, span), span)

    def other(k):
        return lax.rem(g + k, groups)

    barrier = pltpu.get_barrier_semaphore()
    for k in range(1, groups):
        pl.semaphore_signal(barrier, inc=1, device_id=(other(k), f, t), device_id_type=MESH)
    pl.semaphore_wait(barrier, groups - 1)

    def part(k):
        return pltpu.make_async_remote_copy(
            src_ref=diff_ref.at[rows(other(k)), :],
            dst_ref=landed.at[k],
            send_sem=sends.at[k],
            recv_sem=receives.at[k],
            device_id=(other(k), f, t),
            device_id_type=MESH,
        )

    def result(k):
        return pltpu.make_async_remote_copy(
            src_ref=summed,
            dst_ref=landed.at[groups + k],
            send_sem=sends_two.at[k],
            recv_sem=receives_two.at[k],
            device_id=(other(k), f, t),
            device_id_type=MESH,
        )

    for k in range(1, groups):
        part(k).start()
    total = diff_ref[rows(g), :].astype(F32)
    for k in range(1, groups):
        part(k).wait_recv()
        total = total + landed[k].astype(F32)
    summed[...] = total.astype(LOW)
    for k in range(1, groups):
        result(k).start()
    total_ref[rows(g), :] = summed[...]
    for k in range(1, groups):
        result(k).wait_recv()
        total_ref[rows(lax.rem(g + groups - k, groups)), :] = landed[groups + k]
    for k in range(1, groups):
        part(k).wait_send()
        result(k).wait_send()


def group_sum(diff, groups, identity, name):
    flat = diff.reshape(-1, diff.shape[-1])
    span, cols = flat.shape[0] // groups, flat.shape[1]
    dma = pltpu.SemaphoreType.DMA
    whole = pl.BlockSpec(memory_space=pltpu.VMEM)
    total = pl.pallas_call(
        functools.partial(group_kernel, groups),
        in_specs=[whole],
        out_specs=whole,
        out_shape=jax.ShapeDtypeStruct(flat.shape, LOW),
        scratch_shapes=[
            pltpu.VMEM((2 * groups, span, cols), LOW),
            pltpu.VMEM((span, cols), LOW),
            *[dma((groups,))] * 4,
        ],
        compiler_params=params(identity),
        cost_estimate=cost(4 * flat.size, 8 * flat.size),
        name=name,
    )(flat)
    return total.reshape(diff.shape)


def vector_kernel(groups, shards, fsdp, part_ref, master_ref, moment_ref, outer_ref, inner_ref, state_ref, copy_ref,
                  landed, mine, sends, receives, sends_two, receives_two):
    g, f, t = lax.axis_index("group"), lax.axis_index("fsdp"), lax.axis_index("tensor")
    me = f * shards + t
    members = fsdp * shards

    def place(k):
        at = lax.rem(me + k, members)
        return (g, at // shards, at % shards)

    def column(k):
        return (lax.rem(g + k, groups), f, t)

    barrier = pltpu.get_barrier_semaphore()
    for k in range(1, members):
        pl.semaphore_signal(barrier, inc=1, device_id=place(k), device_id_type=MESH)
    for k in range(1, groups):
        pl.semaphore_signal(barrier, inc=1, device_id=column(k), device_id_type=MESH)
    pl.semaphore_wait(barrier, members + groups - 2)

    def part(k):
        return pltpu.make_async_remote_copy(
            src_ref=part_ref, dst_ref=landed.at[k], send_sem=sends.at[k], recv_sem=receives.at[k],
            device_id=place(k), device_id_type=MESH,
        )

    def share(k):
        return pltpu.make_async_remote_copy(
            src_ref=mine, dst_ref=landed.at[members + k], send_sem=sends_two.at[k], recv_sem=receives_two.at[k],
            device_id=column(k), device_id_type=MESH,
        )

    for k in range(1, members):
        part(k).start()
    landed[0] = part_ref[...]
    for k in range(1, members):
        part(k).wait_recv()
    gradient = jnp.zeros(part_ref.shape, F32)
    for n in range(members):
        gradient = gradient + landed[lax.rem(me + members - n, members)]
    master = master_ref[...]
    new, second = inner_adamw(master, gradient, moment_ref[0], moment_ref[1], VECTOR_RATE, 0.0)
    inner_ref[0] = gradient
    inner_ref[1] = second
    mine[...] = master - new
    for k in range(1, groups):
        share(k).start()
    landed[members] = mine[...]
    for k in range(1, groups):
        share(k).wait_recv()
    difference = jnp.zeros(part_ref.shape, F32)
    for n in range(groups):
        difference = difference + landed[members + lax.rem(g + groups - n, groups)]
    difference = difference / groups
    momentum, fresh = outer_nesterov(master, outer_ref[...], difference)
    state_ref[0] = difference
    state_ref[1] = momentum
    state_ref[2] = fresh
    copy_ref[...] = fresh.astype(LOW)
    for k in range(1, members):
        part(k).wait_send()
    for k in range(1, groups):
        share(k).wait_send()


def vector_step(part, master, moments, outer_old, groups, shards, fsdp, identity):
    dma = pltpu.SemaphoreType.DMA
    whole = pl.BlockSpec(memory_space=pltpu.VMEM)
    return pl.pallas_call(
        functools.partial(vector_kernel, groups, shards, fsdp),
        in_specs=[whole] * 4,
        out_specs=[whole] * 3,
        out_shape=[
            jax.ShapeDtypeStruct((2, *part.shape), F32),
            jax.ShapeDtypeStruct((3, *part.shape), F32),
            jax.ShapeDtypeStruct(part.shape, LOW),
        ],
        scratch_shapes=[
            pltpu.VMEM((fsdp * shards + groups, *part.shape), F32),
            pltpu.VMEM(part.shape, F32),
            dma((fsdp * shards,)),
            dma((fsdp * shards,)),
            dma((groups,)),
            dma((groups,)),
        ],
        compiler_params=params(identity),
        name="vector_step",
    )(part, master, moments, outer_old)


def gather_weights(shard):
    whole = lax.all_gather(shard, "tensor", axis=0)
    return lax.all_gather(whole, "fsdp", axis=2, tiled=True)


def scatter_gradient(gradient):
    half = gradient if gradient.ndim == 4 else lax.psum_scatter(gradient, "fsdp", scatter_dimension=0)
    return lax.psum_scatter(half, "tensor", scatter_dimension=0)


def local(
    patches,
    output_grad,
    live_counts,
    attn_master,
    mlp_master,
    vector_master,
    attn_moments,
    mlp_moments,
    vector_moments,
    attn_outer,
    mlp_outer,
    vector_outer,
):
    vec = vector_master
    tensor_size, fsdp = lax.axis_size("tensor"), lax.axis_size("fsdp")
    groups = lax.axis_size("group")
    local_images, seq, width = patches.shape[2:]
    slot = (lax.axis_index("fsdp") * tensor_size + lax.axis_index("tensor")) * local_images
    slot = slot + jnp.arange(local_images)
    counts = jnp.take(live_counts[0], slot // IMG_DEV, axis=1)
    alive = ((slot % IMG_DEV)[None, :] < counts).astype(F32).reshape(-1)
    x = patches.reshape(-1, seq, width)
    cotangent = output_grad.reshape(-1, seq, width)
    images = x.shape[0]

    if (groups, fsdp) == (4, 2):
        w_attn, w_mlp = gather(attn_master.astype(LOW), mlp_master.astype(LOW), tensor_size)
    else:
        w_attn = gather_weights(attn_master.astype(LOW))
        w_mlp = gather_weights(mlp_master.astype(LOW))

    normed_one, qkv = project(x, w_attn, vec)
    attended = attend(qkv, images, seq)
    resid, normed_two, grad_two = mix(alive, attended, x, cotangent, w_attn, vec)
    bias = vec[8:].reshape(tensor_size, 1, -1)
    carried = None
    mlp_grads, bias_parts = [], []
    for quarter in range(QUARTERS):
        if quarter == 3:
            carried[0], mlp_grads[0] = lax.optimization_barrier((carried[0], mlp_grads[0]))
        *carried, dw, db = mlp(quarter, QUARTERS, normed_two, grad_two, w_mlp, bias, carried, fsdp)
        mlp_grads.append(scatter_gradient(dw))
        bias_parts.append(db)
    branch, grad_normed = carried
    branch, mlp_grads[1] = lax.optimization_barrier((branch, mlp_grads[1]))
    block_output, grad_resid, grad_attended, dw_out, sums_two = turn(
        alive, resid, branch, grad_normed, grad_two, attended, w_attn, vec, images, seq, fsdp
    )
    out_grad = scatter_gradient(dw_out)
    qkv_grads, head_sums, carry = [], [], None
    for part in range(PARTS):
        grads = unattend(qkv, grad_attended, images, seq, part, PARTS, tensor_size)
        final = part == PARTS - 1
        head_grad, mlp_grads[2 + part] = lax.optimization_barrier((grads[0], mlp_grads[2 + part]))
        grads = (head_grad, *grads[1:])
        ending = [x, grad_resid, vec] if final else None
        *carry, dw_qkv, sums = close(part, PARTS, normed_one, grads, w_attn, carry, ending, fsdp, images, seq)
        if not final:
            (carry,) = carry
        qkv_grads.append(scatter_gradient(dw_qkv))
        head_sums.append(sums.reshape(2, tensor_size, -1))
    patches_grad, sums_one = carry

    head_rows = jnp.concatenate(head_sums, axis=-1).reshape(2, width)
    hidden_bias = jnp.concatenate(bias_parts, axis=-1).reshape(-1, width)
    vector_part = jnp.concatenate([sums_one, sums_two[:2], head_rows, sums_two[2:], hidden_bias])
    if fsdp == 2:
        vector_inner, vector_state, vector_copy = vector_step(
            vector_part, vec, vector_moments[0], vector_outer, groups, tensor_size, fsdp, 12
        )
    else:
        vector_grad = lax.psum(vector_part, ("fsdp", "tensor"))
        new_vector, second_vector = inner_adamw(
            vec, vector_grad, vector_moments[0, 0], vector_moments[0, 1], VECTOR_RATE, 0.0
        )
        diff_vector = lax.psum(vec - new_vector, "group") / groups
        momentum, fresh = outer_nesterov(vec, vector_outer, diff_vector)
        vector_inner = jnp.stack([vector_grad, second_vector])
        vector_state, vector_copy = jnp.stack([diff_vector, momentum, fresh]), fresh.astype(LOW)

    def beside(*parts):
        return jnp.concatenate(parts, axis=-1)

    def beside_or_last(*parts):
        return jnp.where(pl.program_id(0) == 3, parts[-1], beside(*parts[:-1]))

    mlp_inner, mlp_diff = inner_step(beside, [lambda j: j] * QUARTERS, mlp_grads, mlp_master, mlp_moments, "inner_mlp")
    mlp_total = group_sum(mlp_diff, groups, 10, "group_mlp")
    mlp_state, mlp_copy = outer_step(groups, mlp_total, mlp_master, mlp_outer, "outer_mlp")
    out_grad, mlp_state = lax.optimization_barrier((out_grad, mlp_state))
    attn_inner, attn_diff = inner_step(
        beside_or_last,
        [lambda j: jnp.minimum(j, 2)] * PARTS + [lambda j: 0],
        [*qkv_grads, out_grad],
        attn_master,
        attn_moments,
        "inner_attn",
    )
    attn_total = group_sum(attn_diff, groups, 11, "group_attn")
    attn_state, attn_copy = outer_step(groups, attn_total, attn_master, attn_outer, "outer_attn")
    return (
        block_output.reshape(patches.shape),
        patches_grad.reshape(patches.shape),
        attn_inner,
        attn_state,
        attn_copy,
        mlp_inner,
        mlp_state,
        mlp_copy,
        vector_inner[None],
        vector_state,
        vector_copy,
    )


def solution(mesh):
    placed = (
        P("group", None, ("fsdp", "tensor"), None, None),
        P("group", None, ("fsdp", "tensor"), None, None),
        P("group", None, None),
        P(None, "fsdp", "tensor"),
        P(None, "fsdp", "tensor"),
        P(),
        P("group", None, None, "fsdp", "tensor"),
        P("group", None, None, "fsdp", "tensor"),
        P("group", None, None, None),
        P(None, "fsdp", "tensor"),
        P(None, "fsdp", "tensor"),
        P(),
    )
    return jax.shard_map(
        local,
        mesh=mesh,
        in_specs=placed,
        out_specs=(
            P("group", None, ("fsdp", "tensor"), None, None),
            P("group", None, ("fsdp", "tensor"), None, None),
            P("group", None, None, "fsdp", "tensor"),
            P(None, None, "fsdp", "tensor"),
            P(None, "fsdp", "tensor"),
            P("group", None, None, "fsdp", "tensor"),
            P(None, None, "fsdp", "tensor"),
            P(None, "fsdp", "tensor"),
            P("group", None, None, None),
            P(),
            P(),
        ),
        check_vma=False,
    )
```

```python
import functools

import jax
import jax.numpy as jnp
from jax import lax
from jax.experimental import pallas as pl
from jax.experimental.pallas import tpu as pltpu
from jax.sharding import PartitionSpec as P

HD = 64
STEP = 8
IMG_DEV = 4
EPSILON = 1e-06
INNER_RATE = 0.02
VECTOR_RATE = 0.2
WEIGHT_DECAY = 0.1
OUTER_RATE = 0.7
OUTER_MOMENTUM = 0.9
PIECES = ((0, 256), (256, 256), (512, 512))
PARTS = 2
LOW = jnp.bfloat16
F32 = jnp.float32
NN = (((1,), (0,)), ((), ()))
NT = (((1,), (1,)), ((), ()))
TN = (((0,), (0,)), ((), ()))


def dot(a, b, dims=NN):
    return lax.dot_general(a, b, dims, preferred_element_type=F32)


MESH = pl.DeviceIdType.MESH


def params(identity=None):
    if identity is None:
        return pltpu.CompilerParams(vmem_limit_bytes=60 * 2**20)
    return pltpu.CompilerParams(vmem_limit_bytes=60 * 2**20, collective_id=identity, has_side_effects=True)


def partner():
    return (lax.axis_index("group"), 1 - lax.axis_index("fsdp"), lax.axis_index("tensor"))


def greet_partner():
    barrier = pltpu.get_barrier_semaphore()
    pl.semaphore_signal(barrier, inc=1, device_id=partner(), device_id_type=MESH)
    pl.semaphore_wait(barrier, 1)


def to_partner(sent, received, sends, receives, n):
    return pltpu.make_async_remote_copy(
        src_ref=sent.at[n],
        dst_ref=received.at[n],
        send_sem=sends.at[n],
        recv_sem=receives.at[n],
        device_id=partner(),
        device_id_type=MESH,
    )


def bands(depth):
    f = lax.axis_index("fsdp")
    return pl.ds(pl.multiple_of(f * depth, depth), depth), pl.ds(pl.multiple_of((1 - f) * depth, depth), depth)


def exchange_scratch(steps, shape):
    dma = pltpu.SemaphoreType.DMA
    return [
        pltpu.VMEM((steps, *shape), F32),
        pltpu.VMEM((steps, *shape), LOW),
        pltpu.VMEM((steps, *shape), LOW),
        dma((steps,)),
        dma((steps,)),
    ]


def cost(flops, moved, special=0):
    return pl.CostEstimate(flops=int(flops), bytes_accessed=int(moved), transcendentals=int(special))


def padded(rows):
    return -(-rows // 16) * 16


def centred(source):
    centre = source - jnp.mean(source, axis=-1, keepdims=True)
    spread = jnp.mean(centre * centre, axis=-1, keepdims=True)
    inverse = lax.rsqrt(spread + EPSILON)
    return centre * inverse, inverse


def norm_back(upstream, normal, inverse, gain):
    pulled = upstream * gain
    mean_one = jnp.mean(pulled, axis=-1, keepdims=True)
    mean_two = jnp.mean(pulled * normal, axis=-1, keepdims=True)
    return inverse * (pulled - mean_one - normal * mean_two)


def project_kernel(images, seq, x_ref, w_ref, vec_ref, n_ref, out_ref, n_scr):
    j, t = pl.program_id(0), pl.program_id(1)
    span = n_scr.shape[0] // images

    @pl.when((j == 0) & (t == 0))
    def _():
        n_scr[...] = jnp.zeros_like(n_scr)
        for i in range(images):
            normal, _ = centred(x_ref[i].astype(F32))
            n_scr[pl.ds(i * span, seq), :] = (normal * vec_ref[0:1] + vec_ref[1:2]).astype(LOW)
        n_ref[...] = n_scr[...]

    cols = out_ref.shape[-1]
    out = dot(n_scr[...], w_ref[0, 0])
    at = pl.ds(pl.multiple_of(t * cols, cols), cols)
    bias = jnp.where(j == 0, vec_ref[4:5, at], jnp.where(j == 2, vec_ref[5:6, at], 0.0))
    out_ref[0] = (out + bias).astype(LOW)


def project(patches, w_attn, vec):
    images, seq, width = patches.shape
    shards, _, _, cols = w_attn.shape
    rows = images * padded(seq)
    return pl.pallas_call(
        functools.partial(project_kernel, images, seq),
        grid=(3, shards),
        in_specs=[
            pl.BlockSpec((images, seq, width), lambda j, t: (0, 0, 0)),
            pl.BlockSpec((1, 1, width, cols), lambda j, t: (t, j, 0, 0)),
            pl.BlockSpec(vec.shape, lambda j, t: (0, 0)),
        ],
        out_specs=[
            pl.BlockSpec((rows, width), lambda j, t: (0, 0)),
            pl.BlockSpec((1, rows, cols), lambda j, t: (j, 0, t)),
        ],
        out_shape=[
            jax.ShapeDtypeStruct((rows, width), LOW),
            jax.ShapeDtypeStruct((3, rows, width), LOW),
        ],
        scratch_shapes=[pltpu.VMEM((rows, width), LOW)],
        compiler_params=params(),
        cost_estimate=cost(6 * rows * width * width, 16 * rows * width),
        name="project",
    )(patches, w_attn, vec)


def half_lanes(value, which):
    lane = lax.broadcasted_iota(jnp.int32, value.shape, 1)
    return jnp.where((lane >= HD) == bool(which), value, jnp.zeros_like(value))


def attend_kernel(seq, q_ref, k_ref, v_ref, out_ref):
    span = q_ref.shape[1]
    scale = HD**-0.5
    q, k, v = q_ref[0], k_ref[0], v_ref[0]
    parts = []
    for h in range(2):
        scores = dot(q, half_lanes(k, h), NT)
        lane = lax.broadcasted_iota(jnp.int32, scores.shape, 1)
        scores = jnp.where(lane < seq, scores, -1e30)
        top = jnp.max(scores, axis=1, keepdims=True)
        raised = jnp.exp((scores - top) * scale)
        total = jnp.sum(raised, axis=1, keepdims=True)
        probs = (raised * (1.0 / total)).astype(LOW)
        parts.append(dot(probs, v))
    lane = lax.broadcasted_iota(jnp.int32, (span, 2 * HD), 1)
    out_ref[...] = jnp.where(lane < HD, parts[0], parts[1]).astype(LOW)


def attend(qkv, images, seq):
    _, rows, width = qkv.shape
    span = rows // images
    pair = 2 * HD

    def take(j):
        return pl.BlockSpec((1, span, pair), lambda i, h: (j, i, h))

    return pl.pallas_call(
        functools.partial(attend_kernel, seq),
        grid=(images, width // pair),
        in_specs=[take(0), take(1), take(2)],
        out_specs=pl.BlockSpec((span, pair), lambda i, h: (i, h)),
        out_shape=jax.ShapeDtypeStruct((rows, width), LOW),
        compiler_params=params(),
        cost_estimate=cost(16 * rows * span * width, 8 * rows * width, rows * span * (width // HD)),
        name="attend",
    )(qkv, qkv, qkv)


def mix_kernel(seq, alive_ref, att_ref, x_ref, g_ref, w_ref, vec_ref, resid_ref, n_ref, g2_ref, x_scr):
    i = pl.program_id(0)
    shards, _, _, cols = w_ref.shape
    x_scr[...] = jnp.zeros_like(x_scr)
    x_scr[0:seq, :] = x_ref[0].astype(F32)
    total = x_scr[...] + vec_ref[6:7]
    for t in range(shards):
        total = total + dot(att_ref[:, t * cols : (t + 1) * cols], w_ref[t, 0], NT)
    resid_ref[...] = total
    normal, _ = centred(total)
    n_ref[...] = (normal * vec_ref[2:3] + vec_ref[3:4]).astype(LOW)
    x_scr[0:seq, :] = g_ref[0].astype(F32) * alive_ref[i]
    g2_ref[...] = x_scr[...].astype(LOW)


def mix(alive, attended, patches, cotangent, w_attn, vec):
    images, seq, width = patches.shape
    rows = attended.shape[0]
    span = rows // images
    shards, _, _, cols = w_attn.shape
    block = pl.BlockSpec((span, width), lambda i: (i, 0))
    whole = jax.ShapeDtypeStruct((rows, width), LOW)
    return pl.pallas_call(
        functools.partial(mix_kernel, seq),
        grid=(images,),
        in_specs=[
            pl.BlockSpec(memory_space=pltpu.SMEM),
            block,
            pl.BlockSpec((1, seq, width), lambda i: (i, 0, 0)),
            pl.BlockSpec((1, seq, width), lambda i: (i, 0, 0)),
            pl.BlockSpec((shards, 1, width, cols), lambda i: (0, 3, 0, 0)),
            pl.BlockSpec(vec.shape, lambda i: (0, 0)),
        ],
        out_specs=[block, block, block],
        out_shape=[jax.ShapeDtypeStruct((rows, width), F32), whole, whole],
        scratch_shapes=[pltpu.VMEM((span, width), F32)],
        compiler_params=params(),
        cost_estimate=cost(2 * rows * width * width, 16 * rows * width),
        name="mix",
    )(alive, attended, patches, cotangent, w_attn, vec)


def mlp_kernel(first, pairwise, n_ref, g_ref, w1_ref, w2_ref, bias_ref, *refs):
    if not first:
        yi_ref, gi_ref, *refs = refs
    y_ref, gn_ref, dw_ref, db_ref, h_scr, p_scr, loaded, *exchange = refs
    step = pl.program_id(0)
    each, _, width, cols = w1_ref.shape
    if not first:
        loads = (
            pltpu.make_async_copy(yi_ref, y_ref, loaded.at[0]),
            pltpu.make_async_copy(gi_ref, gn_ref, loaded.at[1]),
        )

    @pl.when(step == 0)
    def _():
        if not first:
            for load in loads:
                load.start()
        else:
            y_ref[...] = jnp.zeros_like(y_ref)
            gn_ref[...] = jnp.zeros_like(gn_ref)
        if pairwise:
            greet_partner()

    w1 = jnp.concatenate([w1_ref[t, 0] for t in range(each)], axis=1)
    w2 = jnp.concatenate([w2_ref[t, 0] for t in range(each)], axis=1)
    bias = jnp.concatenate([bias_ref[t] for t in range(each)], axis=1)
    pre = dot(n_ref[...], w1) + bias
    cdf = 0.5 * (1.0 + lax.erf(pre * 0.7071067811865476))
    h_scr[...] = (pre * cdf).astype(LOW)
    slope = cdf + pre * jnp.exp(-0.5 * pre * pre) * 0.3989422804014327
    p_scr[...] = (dot(g_ref[...], w2) * slope).astype(LOW)
    sums = jnp.sum(p_scr[...].astype(F32), axis=0, keepdims=True)
    for t in range(each):
        db_ref[t] = sums[:, t * cols : (t + 1) * cols]

    if pairwise:
        own, sent, received, sends, receives = exchange
        ours, theirs = bands(width // 2)

        def collect(n):
            to_partner(sent, received, sends, receives, n % 2).wait()
            for which in range(2):
                total = (own[n % 2, which] + received[n % 2, which].astype(F32)).astype(LOW)
                for t in range(each):
                    dw_ref[n * each + t, which] = total[:, t * cols : (t + 1) * cols]

        for n in range(dw_ref.shape[0] // each):

            @pl.when(step == n)
            def _():
                if n:
                    collect(n - 1)
                sent[n % 2, 0] = dot(n_ref[:, theirs], p_scr[...], TN).astype(LOW)
                sent[n % 2, 1] = dot(g_ref[:, theirs], h_scr[...], TN).astype(LOW)
                to_partner(sent, received, sends, receives, n % 2).start()
                own[n % 2, 0] = dot(n_ref[:, ours], p_scr[...], TN)
                own[n % 2, 1] = dot(g_ref[:, ours], h_scr[...], TN)

    else:
        shards, depth = dw_ref.shape[0], dw_ref.shape[3]
        d1 = dot(n_ref[...], p_scr[...], TN).astype(LOW)
        d2 = dot(g_ref[...], h_scr[...], TN).astype(LOW)
        for f in range(shards):
            for t in range(each):
                dw_ref[f, t, 0] = d1[f * depth : (f + 1) * depth, t * cols : (t + 1) * cols]
                dw_ref[f, t, 1] = d2[f * depth : (f + 1) * depth, t * cols : (t + 1) * cols]

    if not first:

        @pl.when(step == 0)
        def _():
            for load in loads:
                load.wait()

    y_ref[...] += dot(h_scr[...], w2, NT)
    gn_ref[...] += dot(p_scr[...], w1, NT)
    if pairwise:

        @pl.when(step == pl.num_programs(0) - 1)
        def _():
            collect(dw_ref.shape[0] // each - 1)


def mlp(part, start, cols, normed, grad_two, w_mlp, bias, carried, fsdp):
    rows, width = normed.shape
    shards = w_mlp.shape[0]
    each = max(512 // cols, 1)
    at = start // cols
    first, pairwise = carried is None, fsdp == 2
    single = pl.Buffered(1)
    full = pl.BlockSpec((rows, width), lambda s: (0, 0), pipeline_mode=single)
    depth = width // fsdp
    steps = shards // each
    acc_shape = jax.ShapeDtypeStruct((rows, width), F32)
    if pairwise:
        out_w = pl.BlockSpec((shards, 2, depth, cols), lambda s: (0, 0, 0, 0), pipeline_mode=single)
        w_shape = jax.ShapeDtypeStruct((shards, 2, depth, cols), LOW)
        extra = exchange_scratch(2, (2, depth, each * cols))
    else:
        out_w = pl.BlockSpec((fsdp, each, 2, depth, cols), lambda s: (0, s, 0, 0, 0))
        w_shape = jax.ShapeDtypeStruct((fsdp, shards, 2, depth, cols), LOW)
        extra = []
    return pl.pallas_call(
        functools.partial(mlp_kernel, first, pairwise),
        grid=(steps,),
        in_specs=[
            full,
            full,
            pl.BlockSpec((each, 1, width, cols), lambda s: (s, 0, 0, at)),
            pl.BlockSpec((each, 1, width, cols), lambda s: (s, 1, 0, at)),
            pl.BlockSpec((each, 1, cols), lambda s: (s, 0, at)),
        ]
        + ([] if first else [pl.BlockSpec(memory_space=pl.ANY)] * 2),
        out_specs=[full, full, out_w, pl.BlockSpec((each, 1, cols), lambda s: (s, 0, 0))],
        out_shape=[acc_shape, acc_shape, w_shape, jax.ShapeDtypeStruct((shards, 1, cols), F32)],
        scratch_shapes=[
            pltpu.VMEM((rows, each * cols), LOW),
            pltpu.VMEM((rows, each * cols), LOW),
            pltpu.SemaphoreType.DMA((2,)),
            *extra,
        ],
        compiler_params=params(2 + part if pairwise else None),
        cost_estimate=cost(12 * rows * width * cols * shards, 24 * rows * width),
        name=f"mlp_{part}",
    )(normed, grad_two, w_mlp, w_mlp, bias, *([] if first else carried))


def turn_kernel(seq, pairwise, alive_ref, resid_ref, y_ref, gn_ref, g2_ref, att_ref, w_ref, vec_ref,
                out_ref, gr_ref, ga_ref, dw_ref, sums_ref, dw_scr, *exchange):
    i = pl.program_id(0)
    if pairwise:
        pl.when(i == 0)(greet_partner)
    shards, _, _, cols = w_ref.shape
    resid = resid_ref[...]
    out_ref[0] = ((resid + y_ref[...] + vec_ref[7:8]) * alive_ref[i]).astype(LOW)[0:seq]
    normal, inverse = centred(resid)
    upstream = gn_ref[...]
    grad_out = g2_ref[...].astype(F32)
    grad_resid = grad_out + norm_back(upstream, normal, inverse, vec_ref[2:3])
    gr_ref[...] = grad_resid
    low = grad_resid.astype(LOW)
    rows = [
        jnp.sum(upstream * normal, axis=0, keepdims=True),
        jnp.sum(upstream, axis=0, keepdims=True),
        jnp.sum(grad_resid, axis=0, keepdims=True),
        jnp.sum(grad_out, axis=0, keepdims=True),
    ]
    rows = jnp.concatenate(rows, axis=0)

    @pl.when(i == 0)
    def _():
        sums_ref[...] = rows

    @pl.when(i != 0)
    def _():
        sums_ref[...] += rows

    for t in range(shards):
        ga_ref[:, t * cols : (t + 1) * cols] = dot(low, w_ref[t, 0]).astype(LOW)
    part = dot(low, att_ref[...], TN)

    @pl.when(i == 0)
    def _():
        dw_scr[...] = part

    @pl.when(i != 0)
    def _():
        dw_scr[...] += part

    @pl.when(i == pl.num_programs(0) - 1)
    def _():
        if pairwise:
            sent, received, sends, receives = exchange
            ours, theirs = bands(dw_scr.shape[0] // 2)
            sent[0] = dw_scr[theirs, :].astype(LOW)
            copy = to_partner(sent, received, sends, receives, 0)
            copy.start()
            copy.wait()
            total = (dw_scr[ours, :] + received[0].astype(F32)).astype(LOW)
            for t in range(shards):
                dw_ref[t, 0] = total[:, t * cols : (t + 1) * cols]
            return
        depth = dw_ref.shape[3]
        for f in range(dw_ref.shape[0]):
            for t in range(shards):
                dw_ref[f, t, 0] = dw_scr[f * depth : (f + 1) * depth, t * cols : (t + 1) * cols].astype(LOW)


def turn(alive, resid, branch, grad_normed, grad_two, attended, w_attn, vec, images, seq, fsdp):
    rows, width = resid.shape
    span = rows // images
    shards, _, _, cols = w_attn.shape
    depth = width // fsdp
    pairwise = fsdp == 2
    lead = () if pairwise else (fsdp,)
    block = pl.BlockSpec((span, width), lambda i: (i, 0))
    return pl.pallas_call(
        functools.partial(turn_kernel, seq, pairwise),
        grid=(images,),
        in_specs=[
            pl.BlockSpec(memory_space=pltpu.SMEM),
            block, block, block, block, block,
            pl.BlockSpec((shards, 1, width, cols), lambda i: (0, 3, 0, 0)),
            pl.BlockSpec(vec.shape, lambda i: (0, 0)),
        ],
        out_specs=[
            pl.BlockSpec((1, seq, width), lambda i: (i, 0, 0)),
            block, block,
            pl.BlockSpec((*lead, shards, 1, depth, cols), lambda i: (0,) * (4 + len(lead))),
            pl.BlockSpec((4, width), lambda i: (0, 0)),
        ],
        out_shape=[
            jax.ShapeDtypeStruct((images, seq, width), LOW),
            jax.ShapeDtypeStruct((rows, width), F32),
            jax.ShapeDtypeStruct((rows, width), LOW),
            jax.ShapeDtypeStruct((*lead, shards, 1, depth, cols), LOW),
            jax.ShapeDtypeStruct((4, width), F32),
        ],
        scratch_shapes=[pltpu.VMEM((width, width), F32)] + (exchange_scratch(1, (depth, width))[1:] if pairwise else []),
        compiler_params=params(6 if pairwise else None),
        cost_estimate=cost(4 * rows * width * width, 24 * rows * width),
        name="turn",
    )(alive, resid, branch, grad_normed, grad_two, attended, w_attn, vec)


def unattend_kernel(seq, q_ref, k_ref, v_ref, g_ref, dq_ref, dk_ref, dv_ref):
    span = q_ref.shape[1]
    scale = HD**-0.5
    q, k, v, g = q_ref[0], k_ref[0], v_ref[0], g_ref[...]
    parts = []
    for h in range(2):
        scores = dot(half_lanes(k, h), q, NT)
        row = lax.broadcasted_iota(jnp.int32, scores.shape, 0)
        scores = jnp.where(row < seq, scores, -1e30)
        top = jnp.max(scores, axis=0, keepdims=True)
        raised = jnp.exp((scores - top) * scale)
        total = jnp.sum(raised, axis=0, keepdims=True)
        probs = raised * (1.0 / total)
        gp = dot(half_lanes(v, h), g, NT)
        delta = jnp.sum(probs * gp, axis=0, keepdims=True)
        gs = (probs * (gp - delta)).astype(LOW)
        dv = dot(probs.astype(LOW), g)
        dk = dot(gs, q)
        dq = dot(gs, k, TN)
        parts.append((dq, dk, dv))
    lane = lax.broadcasted_iota(jnp.int32, (span, 2 * HD), 1) < HD
    dq_ref[0] = (jnp.where(lane, parts[0][0], parts[1][0]) * scale).astype(LOW)
    dk_ref[0] = (jnp.where(lane, parts[0][1], parts[1][1]) * scale).astype(LOW)
    dv_ref[0] = jnp.where(lane, parts[0][2], parts[1][2]).astype(LOW)


def unattend(qkv, grad_attended, images, seq, part, parts, shards):
    _, rows, width = qkv.shape
    span = rows // images
    pair = 2 * HD
    each = width // shards // parts // pair

    def spot(h):
        return (h // each) * (each * parts) + part * each + h % each

    def take(j):
        return pl.BlockSpec((1, span, pair), lambda i, h: (j, i, spot(h)))

    out = pl.BlockSpec((1, span, pair), lambda i, h: (0, i, h))
    shape = jax.ShapeDtypeStruct((1, rows, width // parts), LOW)
    return pl.pallas_call(
        functools.partial(unattend_kernel, seq),
        grid=(images, width // pair // parts),
        in_specs=[take(0), take(1), take(2), pl.BlockSpec((span, pair), lambda i, h: (i, spot(h)))],
        out_specs=[out, out, out],
        out_shape=[shape, shape, shape],
        compiler_params=params(),
        cost_estimate=cost(
            40 * rows * span * width // parts, 14 * rows * width // parts, rows * span * (width // HD) // parts
        ),
        name=f"unattend_{part}",
    )(qkv, qkv, qkv, grad_attended)


def close_kernel(seq, images, pairwise, first, final, n_ref, dq_ref, dk_ref, dv_ref, w_ref, *refs):
    if not first:
        carry_ref, *refs = refs
    if final:
        x_ref, gr_ref, vec_ref, out_ref, norm_ref, *refs = refs
    else:
        acc_ref, *refs = refs
    dw_ref, sums_ref, acc_scr, *exchange = refs
    j = pl.program_id(0)
    shards, _, _, cols = w_ref.shape
    span = n_ref.shape[0] // images
    if pairwise:
        own, sent, received, sends, receives = exchange
        pl.when(j == 0)(greet_partner)

    @pl.when(j == 0)
    def _():
        acc_scr[...] = jnp.zeros_like(acc_scr) if first else carry_ref[...]
        sums_ref[0:1, :] = jnp.sum(dq_ref[0].astype(F32), axis=0, keepdims=True)
        sums_ref[1:2, :] = jnp.sum(dv_ref[0].astype(F32), axis=0, keepdims=True)

    def spread(n, total, f=None):
        for t in range(shards):
            piece = total[:, t * cols : (t + 1) * cols]
            if f is None:
                dw_ref[t, n] = piece
            else:
                dw_ref[f, t, 0] = piece

    def step(ref):
        weight = jnp.concatenate([w_ref[t, 0] for t in range(shards)], axis=1)
        if pairwise:
            ours, theirs = bands(n_ref.shape[1] // 2)
            sent[j] = dot(n_ref[:, theirs], ref[0], TN).astype(LOW)
            to_partner(sent, received, sends, receives, j).start()
            own[j] = dot(n_ref[:, ours], ref[0], TN)
        else:
            depth = dw_ref.shape[3]
            dw = dot(n_ref[...], ref[0], TN).astype(LOW)
            for f in range(dw_ref.shape[0]):
                spread(0, dw[f * depth : (f + 1) * depth], f)
        acc_scr[...] += dot(ref[0], weight, NT)

    @pl.when(j == 0)
    def _():
        step(dq_ref)

    @pl.when(j == 1)
    def _():
        step(dk_ref)

    @pl.when(j == 2)
    def _():
        step(dv_ref)
        if pairwise:
            for n in range(own.shape[0]):
                to_partner(sent, received, sends, receives, n).wait()
                spread(n, (own[n] + received[n].astype(F32)).astype(LOW))
        if not final:
            acc_ref[...] = acc_scr[...]
            return
        gain = jnp.zeros((1, vec_ref.shape[1]), F32)
        shift = jnp.zeros((1, vec_ref.shape[1]), F32)
        for i in range(images):
            normal, inverse = centred(x_ref[i].astype(F32))
            upstream = acc_scr[i * span : i * span + seq, :]
            out_ref[i] = gr_ref[i * span : i * span + seq, :] + norm_back(upstream, normal, inverse, vec_ref[0:1])
            gain += jnp.sum(upstream * normal, axis=0, keepdims=True)
            shift += jnp.sum(upstream, axis=0, keepdims=True)
        norm_ref[0:1, :] = gain
        norm_ref[1:2, :] = shift


def close(part, parts, normed, grads, w_attn, carry, ending, fsdp, images, seq):
    rows, width = normed.shape
    shards, _, _, cols = w_attn.shape
    cols = cols // parts
    lanes = shards * cols
    depth = width // fsdp
    pairwise, first, final = fsdp == 2, carry is None, ending is not None
    single = pl.Buffered(1)
    stack = pl.BlockSpec((1, rows, lanes), lambda j: (0, 0, 0), pipeline_mode=single)
    full = pl.BlockSpec((rows, width), lambda j: (0, 0), pipeline_mode=single)
    image = pl.BlockSpec((images, seq, width), lambda j: (0, 0, 0), pipeline_mode=single)
    if pairwise:
        dw_spec = pl.BlockSpec((shards, 3, depth, cols), lambda j: (0, 0, 0, 0), pipeline_mode=single)
        dw_shape = jax.ShapeDtypeStruct((shards, 3, depth, cols), LOW)
        extra = exchange_scratch(3, (depth, lanes))
    else:
        dw_spec = pl.BlockSpec((fsdp, shards, 1, depth, cols), lambda j: (0, 0, j, 0, 0))
        dw_shape = jax.ShapeDtypeStruct((fsdp, shards, 3, depth, cols), LOW)
        extra = []
    in_specs = [full, stack, stack, stack, pl.BlockSpec((shards, 1, width, cols), lambda j: (0, j, 0, part))]
    out_specs, out_shape = [], []
    if not first:
        in_specs.append(full)
    if final:
        in_specs += [image, full, pl.BlockSpec((12, width), lambda j: (0, 0))]
        out_specs += [image, pl.BlockSpec((2, width), lambda j: (0, 0))]
        out_shape += [jax.ShapeDtypeStruct((images, seq, width), F32), jax.ShapeDtypeStruct((2, width), F32)]
    else:
        out_specs.append(full)
        out_shape.append(jax.ShapeDtypeStruct((rows, width), F32))
    return pl.pallas_call(
        functools.partial(close_kernel, seq, images, pairwise, first, final),
        grid=(3,),
        in_specs=in_specs,
        out_specs=[*out_specs, dw_spec, pl.BlockSpec((2, lanes), lambda j: (0, 0))],
        out_shape=[*out_shape, dw_shape, jax.ShapeDtypeStruct((2, lanes), F32)],
        scratch_shapes=[pltpu.VMEM((rows, width), F32), *extra],
        compiler_params=params(7 + part if pairwise else None),
        cost_estimate=cost(12 * rows * width * lanes, 20 * rows * width),
        name=f"close_{part}",
    )(normed, *grads, w_attn, *([] if first else [carry]), *(ending if final else []))


def attend_pair(seq, q, k, v):
    scale = HD**-0.5
    parts = []
    for h in range(2):
        scores = dot(q, half_lanes(k, h), NT)
        lane = lax.broadcasted_iota(jnp.int32, scores.shape, 1)
        scores = jnp.where(lane < seq, scores, -1e30)
        top = jnp.max(scores, axis=1, keepdims=True)
        raised = jnp.exp((scores - top) * scale)
        total = jnp.sum(raised, axis=1, keepdims=True)
        probs = (raised * (1.0 / total)).astype(LOW)
        parts.append(dot(probs, v))
    lane = lax.broadcasted_iota(jnp.int32, parts[0].shape, 1)
    return jnp.where(lane < HD, parts[0], parts[1]).astype(LOW)


def front_kernel(
    images, seq, alive_ref, a_in, m_in, x_ref, g_ref, vec_ref,
    a_out, m_out, n_out, qkv_out, att_out, resid_out, n2_out, g2_out,
    a_wide, m_wide, a_hold, m_hold, n_scr, qkv_scr, att_scr, w_scr, o_scr, x_scr, resid_scr, n2_scr, g2_scr,
    zs, zr, xs, xr, ys, yr, xfs, xfr, yfs, yfr, cs, cr, ls, ws,
):
    g, f, z = lax.axis_index("group"), lax.axis_index("fsdp"), lax.axis_index("tensor")
    shards = lax.axis_size("tensor")
    last = shards - 1
    x_at, y_at = g % 2, g // 2
    east, north = y_at * 2 + (1 - x_at), (1 - y_at) * 2 + x_at
    depth, cols = a_in.shape[1:]
    band = depth // 4
    shared = band * 3 // 8
    rest = band - 2 * shared
    span = n_scr.shape[0] // images

    def place(column):
        cx, cy = column % 2, column // 2
        return 2 * (cx + cy - 2 * cx * cy) + cy

    mine, of_east, of_north = place(g), place(east), place(north)
    z_row = mine * band - shared * (mine % 2)
    lead_east = of_east * band + shared * (of_east % 2)
    lead_north = of_north * band + shared * (of_north % 2)
    chunks = ((a_out, 0, 3), (a_out, 3, 1), (m_out, 0, 1), (m_out, 1, 1))

    def tile(n):
        return pl.multiple_of(n, 16)

    def held(n, t, row, rows):
        out, j, many = chunks[n]
        return out.at[t, pl.ds(j, many), pl.ds(tile(f * depth + row), rows), :]

    def send(part, sems, semr, n, t, to):
        return pltpu.make_async_remote_copy(
            src_ref=part, dst_ref=part, send_sem=sems.at[n, t], recv_sem=semr.at[n, t], device_id=to, device_id_type=MESH
        )

    def along(n, t, up):
        part = held(n, t, z_row, band + shared)
        return pltpu.make_async_remote_copy(
            src_ref=part,
            dst_ref=part,
            send_sem=zs.at[n, t, 0 if up else 1],
            recv_sem=zr.at[n, t],
            device_id=(g, f, z + 1 if up else z - 1),
            device_id_type=MESH,
        )

    def to_east(n, t):
        return send(held(n, t, mine * band, band), xs, xr, n, t, (east, f, z))

    def to_north(n, t):
        return send(held(n, t, mine * band, band), ys, yr, n, t, (north, f, z))

    def north_to_east(n, t):
        return send(held(n, t, lead_north, shared), xfs, xfr, n, t, (east, f, z))

    def east_to_north(n, t):
        return send(held(n, t, lead_east + shared, rest), yfs, yfr, n, t, (north, f, z))

    def across(n, t):
        return send(held(n, t, 0, depth), cs, cr, n, t, (g, 1 - f, z))

    rows = pl.ds(tile(f * depth), depth)
    loads = (
        pltpu.make_async_copy(a_in, a_wide, ls.at[0]),
        pltpu.make_async_copy(m_in, m_wide, ls.at[1]),
    )
    keeps = (
        pltpu.make_async_copy(a_hold, a_out.at[z, :, rows, :], ls.at[2]),
        pltpu.make_async_copy(m_hold, m_out.at[z, :, rows, :], ls.at[3]),
    )
    loads[0].start()

    barrier = pltpu.get_barrier_semaphore()

    def greet(to):
        pl.semaphore_signal(barrier, inc=1, device_id=to, device_id_type=MESH)

    for to in ((east, f, z), (north, f, z), (g, 1 - f, z)):
        greet(to)

    @pl.when(z > 0)
    def _():
        greet((g, f, z - 1))

    @pl.when(z < last)
    def _():
        greet((g, f, z + 1))

    loads[0].wait()
    a_hold[...] = a_wide[...].astype(LOW)
    keeps[0].start()
    pl.semaphore_wait(barrier, 3 + jnp.minimum(z, 1) + jnp.minimum(last - z, 1))
    keeps[0].wait()

    count = len(chunks)

    def when_real(k, up, run):
        @pl.when(z - k >= 0 if up else z + k <= last)
        def _():
            run(z - k if up else z + k)

    def own(n):
        @pl.when(z < last)
        def _():
            along(n, z, True).start()

        @pl.when(z > 0)
        def _():
            along(n, z, False).start()

        across(n, z).start()

    def land(n, k, up):
        def run(t):
            along(n, t, up).wait_recv()

            @pl.when(z < last if up else z > 0)
            def _():
                along(n, t, up).start()

            to_east(n, t).start()
            to_north(n, t).start()

        when_real(k, up, run)

    def relay(n, k, up):
        def run(t):
            to_east(n, t).wait_recv()
            east_to_north(n, t).start()
            to_north(n, t).wait_recv()
            north_to_east(n, t).start()

        when_real(k, up, run)

    def finish(n, k, up):
        def run(t):
            east_to_north(n, t).wait_recv()
            north_to_east(n, t).wait_recv()
            across(n, t).start()

        when_real(k, up, run)

    def both(run, n, k):
        for up in (True, False):
            run(n, k, up)

    def fetch(t):
        return pltpu.make_async_copy(a_out.at[t, pl.ds(0, 3)], w_scr, ws.at[0])

    def maps(t):
        across(0, t).wait_recv()
        fetch(t).start()
        fetch(t).wait()
        here = pl.ds(pl.multiple_of(t * cols, cols), cols)
        for j in range(3):
            out = dot(n_scr[...], w_scr[j])
            if j != 1:
                out = out + vec_ref[4 + j // 2 : 5 + j // 2, here]
            qkv_scr[j, :, here] = out.astype(LOW)

    def project(n, k, up):
        when_real(k, up, maps)

    own(0)
    loads[1].start()
    n_scr[...] = jnp.zeros_like(n_scr)
    for i in range(images):
        normal, _ = centred(x_ref[i].astype(F32))
        n_scr[pl.ds(i * span, seq), :] = (normal * vec_ref[0:1] + vec_ref[1:2]).astype(LOW)
    puts = [pltpu.make_async_copy(n_scr, n_out, ws.at[1])]
    puts[0].start()
    both(land, 0, 1)
    loads[1].wait()
    m_hold[...] = m_wide[...].astype(LOW)
    keeps[1].start()
    maps(z)
    both(land, 0, 2)
    both(relay, 0, 1)
    keeps[1].wait()
    both(land, 0, 3)
    for n in range(1, count):
        own(n)
    both(relay, 0, 2)
    both(finish, 0, 1)
    both(relay, 0, 3)
    both(finish, 0, 2)
    both(project, 0, 1)
    both(finish, 0, 3)
    both(project, 0, 2)

    rest_items = [(n, k) for k in range(1, last + 1) for n in range(1, count)]
    total = len(rest_items) + 2

    def advance(at):
        if at < len(rest_items):
            both(land, *rest_items[at])
        if 0 <= at - 1 < len(rest_items):
            both(relay, *rest_items[at - 1])
        if 0 <= at - 2 < len(rest_items):
            both(finish, *rest_items[at - 2])

    advance(0)
    both(project, 0, 3)
    puts.append(pltpu.make_async_copy(qkv_scr, qkv_out, ws.at[2]))
    puts[-1].start()

    pair = 2 * HD
    pairs = qkv_scr.shape[2] // pair
    stretch = max(pairs // 4, 1)
    at = 1
    for i in range(images):
        for start in range(0, pairs, stretch):

            def body(h, carry):
                lanes = pl.ds(pl.multiple_of(h * pair, pair), pair)
                here = pl.ds(i * span, span)
                att_scr[here, lanes] = attend_pair(
                    seq, qkv_scr[0, here, lanes], qkv_scr[1, here, lanes], qkv_scr[2, here, lanes]
                )
                return carry

            lax.fori_loop(start, start + stretch, body, 0)
            if at < total:
                advance(at)
                at += 1
    puts.append(pltpu.make_async_copy(att_scr, att_out, ws.at[3]))
    puts[-1].start()
    while at < total - 2:
        advance(at)
        at += 1

    for t in range(shards):
        across(1, t).wait_recv()
    take = pltpu.make_async_copy(a_out.at[:, 3], o_scr, ws.at[0])
    take.start()
    take.wait()
    x_scr[...] = jnp.zeros_like(x_scr)
    for i in range(images):
        here = pl.ds(i * span, span)
        x_scr[0:seq, :] = x_ref[i].astype(F32)
        out = x_scr[...] + vec_ref[6:7]
        for t in range(shards):
            out = out + dot(att_scr[here, t * cols : (t + 1) * cols], o_scr[t], NT)
        resid_scr[here, :] = out
        normal, _ = centred(out)
        n2_scr[here, :] = (normal * vec_ref[2:3] + vec_ref[3:4]).astype(LOW)
        x_scr[0:seq, :] = g_ref[i].astype(F32) * alive_ref[i]
        g2_scr[here, :] = x_scr[...].astype(LOW)
        if at < total:
            advance(at)
            at += 1
    for n, (src, dst) in enumerate(((resid_scr, resid_out), (n2_scr, n2_out), (g2_scr, g2_out))):
        puts.append(pltpu.make_async_copy(src, dst, ws.at[4 + n]))
        puts[-1].start()
    while at < total:
        advance(at)
        at += 1
    for put in puts:
        put.wait()

    for n in range(count):
        @pl.when(z < last)
        def _():
            along(n, z, True).wait_send()

        @pl.when(z > 0)
        def _():
            along(n, z, False).wait_send()

        for t in range(shards):
            across(n, t).wait_send()
            if n > 1:
                across(n, t).wait_recv()

    def settle(n, k, up):
        def run(t):
            @pl.when(z < last if up else z > 0)
            def _():
                along(n, t, up).wait_send()

            to_east(n, t).wait_send()
            to_north(n, t).wait_send()
            east_to_north(n, t).wait_send()
            north_to_east(n, t).wait_send()

        when_real(k, up, run)

    for n in range(count):
        for k in range(1, last + 1):
            both(settle, n, k)


def front(alive, attn_master, mlp_master, patches, cotangent, vec, shards):
    _, depth, a_cols = attn_master.shape
    _, _, m_cols = mlp_master.shape
    images, seq, width = patches.shape
    rows = images * padded(seq)
    anywhere = pl.BlockSpec(memory_space=pl.ANY)
    inside = pl.BlockSpec(memory_space=pltpu.VMEM)
    dma = pltpu.SemaphoreType.DMA
    low = jax.ShapeDtypeStruct((rows, width), LOW)
    return pl.pallas_call(
        functools.partial(front_kernel, images, seq),
        in_specs=[pl.BlockSpec(memory_space=pltpu.SMEM), anywhere, anywhere, inside, inside, inside],
        out_specs=[anywhere] * 8,
        out_shape=[
            jax.ShapeDtypeStruct((shards, 4, width, a_cols), LOW),
            jax.ShapeDtypeStruct((shards, 2, width, m_cols), LOW),
            low,
            jax.ShapeDtypeStruct((3, rows, width), LOW),
            low,
            jax.ShapeDtypeStruct((rows, width), F32),
            low,
            low,
        ],
        scratch_shapes=[
            pltpu.VMEM(attn_master.shape, F32),
            pltpu.VMEM(mlp_master.shape, F32),
            pltpu.VMEM(attn_master.shape, LOW),
            pltpu.VMEM(mlp_master.shape, LOW),
            pltpu.VMEM((rows, width), LOW),
            pltpu.VMEM((3, rows, width), LOW),
            pltpu.VMEM((rows, width), LOW),
            pltpu.VMEM((3, width, a_cols), LOW),
            pltpu.VMEM((shards, width, a_cols), LOW),
            pltpu.VMEM((rows // images, width), F32),
            pltpu.VMEM((rows, width), F32),
            pltpu.VMEM((rows, width), LOW),
            pltpu.VMEM((rows, width), LOW),
            dma((4, shards, 2)),
        ]
        + [dma((4, shards))] * 11
        + [dma((4,)), dma((7,))],
        compiler_params=params(1),
        cost_estimate=cost(8 * rows * width * width, 30 * rows * width),
        name="front",
    )(alive, attn_master, mlp_master, patches, cotangent, vec)


def inner_adamw(master, gradient, first, second, step_rate, decay_rate):
    first_moment = 0.9 * first + 0.1 * gradient
    second_moment = 0.95 * second + 0.05 * gradient * gradient
    step_ratio = (
        first_moment / (1.0 - 0.9**STEP) / (jnp.sqrt(second_moment / (1.0 - 0.95**STEP)) + 1e-08)
    )
    return (master - step_rate * (step_ratio + decay_rate * master), second_moment)


def outer_nesterov(master, outer_old, difference):
    momentum = OUTER_MOMENTUM * outer_old + difference
    return momentum, master - OUTER_RATE * (difference + OUTER_MOMENTUM * momentum)


def inner_kernel(join, count, *refs):
    pieces, (master_ref, moment_ref, inner_ref, diff_ref) = refs[:count], refs[count:]
    gradient = join(*[piece[0] for piece in pieces]).astype(F32)
    master = master_ref[0]
    new, second = inner_adamw(master, gradient, moment_ref[0, 0, 0], moment_ref[0, 1, 0], INNER_RATE, WEIGHT_DECAY)
    inner_ref[0, 0, 0] = gradient
    inner_ref[0, 1, 0] = second
    diff_ref[0] = (master - new).astype(LOW)


def inner_step(join, places, pieces, master, moments, name):
    many, depth, cols = master.shape
    rows = min(depth, 131072 // cols)
    block = pl.BlockSpec((1, rows, cols), lambda j, r: (j, r, 0))
    both = pl.BlockSpec((1, 2, 1, rows, cols), lambda j, r: (0, 0, j, r, 0))

    def piece_spec(piece, place):
        return pl.BlockSpec((1, rows, piece.shape[2]), lambda j, r: (place(j), r, 0))

    return pl.pallas_call(
        functools.partial(inner_kernel, join, len(pieces)),
        grid=(many, depth // rows),
        in_specs=[piece_spec(piece, place) for piece, place in zip(pieces, places)] + [block, both],
        out_specs=[both, block],
        out_shape=[jax.ShapeDtypeStruct(moments.shape, F32), jax.ShapeDtypeStruct(master.shape, LOW)],
        compiler_params=params(),
        cost_estimate=cost(30 * master.size, 24 * master.size),
        name=name,
    )(*pieces, master, moments)


def outer_kernel(groups, total_ref, master_ref, outer_ref, state_ref, copy_ref):
    difference = total_ref[0].astype(F32) / groups
    momentum, fresh = outer_nesterov(master_ref[0], outer_ref[0], difference)
    state_ref[0, 0] = difference
    state_ref[1, 0] = momentum
    state_ref[2, 0] = fresh
    copy_ref[0] = fresh.astype(LOW)


def outer_step(groups, total, master, outer_old, name):
    many, depth, cols = master.shape
    rows = min(depth, 131072 // cols)
    block = pl.BlockSpec((1, rows, cols), lambda j, r: (j, r, 0))
    return pl.pallas_call(
        functools.partial(outer_kernel, groups),
        grid=(many, depth // rows),
        in_specs=[block, block, block],
        out_specs=[pl.BlockSpec((3, 1, rows, cols), lambda j, r: (0, j, r, 0)), block],
        out_shape=[jax.ShapeDtypeStruct((3, *master.shape), F32), jax.ShapeDtypeStruct(master.shape, LOW)],
        compiler_params=params(),
        cost_estimate=cost(10 * master.size, 24 * master.size),
        name=name,
    )(total, master, outer_old)


def group_kernel(groups, shards, fsdp, diff_ref, *refs):
    if fsdp:
        part_ref, master_ref, moment_ref, outer_ref, total_ref, inner_ref, state_ref, copy_ref, *refs = refs
    else:
        total_ref, *refs = refs
    landed, summed, sends, receives, sends_two, receives_two, *small = refs
    g, f, t = lax.axis_index("group"), lax.axis_index("fsdp"), lax.axis_index("tensor")
    span = landed.shape[1]

    def rows(n):
        return pl.ds(pl.multiple_of(n * span, span), span)

    def other(k):
        return lax.rem(g + k, groups)

    def back(k):
        return lax.rem(g + groups - k, groups)

    def copy(src, dst, sems, semr, k, to):
        return pltpu.make_async_remote_copy(
            src_ref=src, dst_ref=dst, send_sem=sems.at[k], recv_sem=semr.at[k], device_id=to, device_id_type=MESH
        )

    def part(k):
        return copy(diff_ref.at[rows(other(k)), :], landed.at[k], sends, receives, k, (other(k), f, t))

    def result(k):
        return copy(summed, landed.at[groups + k], sends_two, receives_two, k, (other(k), f, t))

    barrier = pltpu.get_barrier_semaphore()
    for k in range(1, groups):
        pl.semaphore_signal(barrier, inc=1, device_id=(other(k), f, t), device_id_type=MESH)
    members = shards * fsdp
    if fsdp:
        few, mine, one, two, three, four = small
        me = f * shards + t

        def place(k):
            at = lax.rem(me + k, members)
            return (g, at // shards, lax.rem(at, shards))

        def piece(k):
            return copy(part_ref, few.at[k], one, two, k, place(k))

        def share(k):
            return copy(mine, few.at[members + k], three, four, k, (other(k), f, t))

        for k in range(1, members):
            pl.semaphore_signal(barrier, inc=1, device_id=place(k), device_id_type=MESH)
    pl.semaphore_wait(barrier, groups - 1 + max(members - 1, 0))

    for k in range(1, groups):
        part(k).start()
    if fsdp:
        for k in range(1, members):
            piece(k).start()
        few[0] = part_ref[...]
        for k in range(1, members):
            piece(k).wait_recv()
        gradient = jnp.zeros(part_ref.shape, F32)
        for n in range(members):
            gradient = gradient + few[lax.rem(me + members - n, members)]
        master = master_ref[...]
        new, second = inner_adamw(master, gradient, moment_ref[0], moment_ref[1], VECTOR_RATE, 0.0)
        inner_ref[0] = gradient
        inner_ref[1] = second
        mine[...] = master - new
        for k in range(1, groups):
            share(k).start()
        few[members] = mine[...]
    total = diff_ref[rows(g), :].astype(F32)
    for k in range(1, groups):
        part(k).wait_recv()
        total = total + landed[k].astype(F32)
    summed[...] = total.astype(LOW)
    for k in range(1, groups):
        result(k).start()
    total_ref[rows(g), :] = summed[...]
    if fsdp:
        for k in range(1, groups):
            share(k).wait_recv()
        difference = jnp.zeros(part_ref.shape, F32)
        for n in range(groups):
            difference = difference + few[members + lax.rem(g + groups - n, groups)]
        difference = difference / groups
        momentum, fresh = outer_nesterov(master, outer_ref[...], difference)
        state_ref[0] = difference
        state_ref[1] = momentum
        state_ref[2] = fresh
        copy_ref[...] = fresh.astype(LOW)
    for k in range(1, groups):
        result(k).wait_recv()
        total_ref[rows(back(k)), :] = landed[groups + k]
    for k in range(1, groups):
        part(k).wait_send()
        result(k).wait_send()
    if fsdp:
        for k in range(1, members):
            piece(k).wait_send()
        for k in range(1, groups):
            share(k).wait_send()


def group_sum(diff, groups, identity, name, vectors=None, shards=0, fsdp=0):
    flat = diff.reshape(-1, diff.shape[-1])
    span, cols = flat.shape[0] // groups, flat.shape[1]
    dma = pltpu.SemaphoreType.DMA
    whole = pl.BlockSpec(memory_space=pltpu.VMEM)
    out_shape = [jax.ShapeDtypeStruct(flat.shape, LOW)]
    extra = []
    if fsdp:
        shape = vectors[0].shape
        out_shape += [
            jax.ShapeDtypeStruct((2, *shape), F32),
            jax.ShapeDtypeStruct((3, *shape), F32),
            jax.ShapeDtypeStruct(shape, LOW),
        ]
        extra = [
            pltpu.VMEM((fsdp * shards + groups, *shape), F32),
            pltpu.VMEM(shape, F32),
            dma((fsdp * shards,)),
            dma((fsdp * shards,)),
            dma((groups,)),
            dma((groups,)),
        ]
    total, *rest = pl.pallas_call(
        functools.partial(group_kernel, groups, shards, fsdp),
        in_specs=[whole] * (5 if fsdp else 1),
        out_specs=[whole] * len(out_shape),
        out_shape=out_shape,
        scratch_shapes=[
            pltpu.VMEM((2 * groups, span, cols), LOW),
            pltpu.VMEM((span, cols), LOW),
            *[dma((groups,))] * 4,
            *extra,
        ],
        compiler_params=params(identity),
        cost_estimate=cost(4 * flat.size, 8 * flat.size),
        name=name,
    )(flat, *(vectors or []))
    return total.reshape(diff.shape), *rest


def gather_weights(shard):
    whole = lax.all_gather(shard, "tensor", axis=0)
    return lax.all_gather(whole, "fsdp", axis=2, tiled=True)


def scatter_gradient(gradient):
    half = gradient if gradient.ndim == 4 else lax.psum_scatter(gradient, "fsdp", scatter_dimension=0)
    return lax.psum_scatter(half, "tensor", scatter_dimension=0)


def local(
    patches,
    output_grad,
    live_counts,
    attn_master,
    mlp_master,
    vector_master,
    attn_moments,
    mlp_moments,
    vector_moments,
    attn_outer,
    mlp_outer,
    vector_outer,
):
    vec = vector_master
    tensor_size, fsdp = lax.axis_size("tensor"), lax.axis_size("fsdp")
    groups = lax.axis_size("group")
    local_images, seq, width = patches.shape[2:]
    slot = (lax.axis_index("fsdp") * tensor_size + lax.axis_index("tensor")) * local_images
    slot = slot + jnp.arange(local_images)
    counts = jnp.take(live_counts[0], slot // IMG_DEV, axis=1)
    alive = ((slot % IMG_DEV)[None, :] < counts).astype(F32).reshape(-1)
    x = patches.reshape(-1, seq, width)
    cotangent = output_grad.reshape(-1, seq, width)
    images = x.shape[0]

    if (groups, fsdp) == (4, 2):
        w_attn, w_mlp, normed_one, qkv, attended, resid, normed_two, grad_two = front(
            alive, attn_master, mlp_master, x, cotangent, vec, tensor_size
        )
    else:
        w_attn = gather_weights(attn_master.astype(LOW))
        w_mlp = gather_weights(mlp_master.astype(LOW))
        normed_one, qkv = project(x, w_attn, vec)
        attended = attend(qkv, images, seq)
        resid, normed_two, grad_two = mix(alive, attended, x, cotangent, w_attn, vec)
    bias = vec[8:].reshape(tensor_size, 1, -1)
    carried = None
    mlp_grads, bias_parts = [], []
    for part, (start, cols) in enumerate(PIECES):
        *carried, dw, db = mlp(part, start, cols, normed_two, grad_two, w_mlp, bias, carried, fsdp)
        mlp_grads.append(scatter_gradient(dw))
        bias_parts.append(db)
    branch, grad_normed = carried
    block_output, grad_resid, grad_attended, dw_out, sums_two = turn(
        alive, resid, branch, grad_normed, grad_two, attended, w_attn, vec, images, seq, fsdp
    )
    out_grad = scatter_gradient(dw_out)

    def beside(*parts):
        return jnp.concatenate(parts, axis=-1)

    def beside_or_last(*parts):
        return jnp.where(pl.program_id(0) == 3, parts[-1], beside(*parts[:-1]))

    grads = unattend(qkv, grad_attended, images, seq, 0, PARTS, tensor_size)
    head_grad, mlp_grads[0] = lax.optimization_barrier((grads[0], mlp_grads[0]))
    carry, dw_qkv, head_sums = close(
        0, PARTS, normed_one, (head_grad, *grads[1:]), w_attn, None, None, fsdp, images, seq
    )
    qkv_grads, head_sums = [scatter_gradient(dw_qkv)], [head_sums]
    carry, mlp_grads[1] = lax.optimization_barrier((carry, mlp_grads[1]))
    grads = unattend(qkv, grad_attended, images, seq, 1, PARTS, tensor_size)
    mlp_grads[0], head_grad = lax.optimization_barrier((mlp_grads[0], grads[0]))
    mlp_inner, mlp_diff = inner_step(beside, [lambda j: j] * len(PIECES), mlp_grads, mlp_master, mlp_moments, "inner_mlp")
    carry, mlp_diff = lax.optimization_barrier((carry, mlp_diff))
    patches_grad, sums_one, dw_qkv, sums = close(
        1, PARTS, normed_one, (head_grad, *grads[1:]), w_attn, carry, [x, grad_resid, vec], fsdp, images, seq
    )
    qkv_grads.append(scatter_gradient(dw_qkv))
    head_sums.append(sums)
    mlp_diff, sums_one = lax.optimization_barrier((mlp_diff, sums_one))
    (mlp_total,) = group_sum(mlp_diff, groups, 10, "group_mlp")
    mlp_state, mlp_copy = outer_step(groups, mlp_total, mlp_master, mlp_outer, "outer_mlp")

    head_rows = jnp.concatenate([v.reshape(2, tensor_size, -1) for v in head_sums], axis=-1).reshape(2, width)
    hidden_bias = jnp.concatenate(bias_parts, axis=-1).reshape(-1, width)
    vector_part = jnp.concatenate([sums_one, sums_two[:2], head_rows, sums_two[2:], hidden_bias])

    out_grad, mlp_state = lax.optimization_barrier((out_grad, mlp_state))
    attn_inner, attn_diff = inner_step(
        beside_or_last,
        [lambda j: jnp.minimum(j, 2)] * PARTS + [lambda j: 0],
        [*qkv_grads, out_grad],
        attn_master,
        attn_moments,
        "inner_attn",
    )
    if fsdp == 2:
        attn_total, vector_inner, vector_state, vector_copy = group_sum(
            attn_diff,
            groups,
            11,
            "group_attn",
            [vector_part, vec, vector_moments[0], vector_outer],
            tensor_size,
            fsdp,
        )
    else:
        (attn_total,) = group_sum(attn_diff, groups, 11, "group_attn")
        vector_grad = lax.psum(vector_part, ("fsdp", "tensor"))
        new_vector, second_vector = inner_adamw(
            vec, vector_grad, vector_moments[0, 0], vector_moments[0, 1], VECTOR_RATE, 0.0
        )
        diff_vector = lax.psum(vec - new_vector, "group") / groups
        momentum, fresh = outer_nesterov(vec, vector_outer, diff_vector)
        vector_inner = jnp.stack([vector_grad, second_vector])
        vector_state, vector_copy = jnp.stack([diff_vector, momentum, fresh]), fresh.astype(LOW)
    attn_state, attn_copy = outer_step(groups, attn_total, attn_master, attn_outer, "outer_attn")
    return (
        block_output.reshape(patches.shape),
        patches_grad.reshape(patches.shape),
        attn_inner,
        attn_state,
        attn_copy,
        mlp_inner,
        mlp_state,
        mlp_copy,
        vector_inner[None],
        vector_state,
        vector_copy,
    )


def solution(mesh):
    placed = (
        P("group", None, ("fsdp", "tensor"), None, None),
        P("group", None, ("fsdp", "tensor"), None, None),
        P("group", None, None),
        P(None, "fsdp", "tensor"),
        P(None, "fsdp", "tensor"),
        P(),
        P("group", None, None, "fsdp", "tensor"),
        P("group", None, None, "fsdp", "tensor"),
        P("group", None, None, None),
        P(None, "fsdp", "tensor"),
        P(None, "fsdp", "tensor"),
        P(),
    )
    return jax.shard_map(
        local,
        mesh=mesh,
        in_specs=placed,
        out_specs=(
            P("group", None, ("fsdp", "tensor"), None, None),
            P("group", None, ("fsdp", "tensor"), None, None),
            P("group", None, None, "fsdp", "tensor"),
            P(None, None, "fsdp", "tensor"),
            P(None, "fsdp", "tensor"),
            P("group", None, None, "fsdp", "tensor"),
            P(None, None, "fsdp", "tensor"),
            P(None, "fsdp", "tensor"),
            P("group", None, None, None),
            P(),
            P(),
        ),
        check_vma=False,
    )
```

```python
import functools

import jax
import jax.numpy as jnp
from jax import lax
from jax.experimental import pallas as pl
from jax.experimental.pallas import tpu as pltpu
from jax.sharding import PartitionSpec as P

HD = 64
STEP = 8
IMG_DEV = 4
EPSILON = 1e-06
INNER_RATE = 0.02
VECTOR_RATE = 0.2
WEIGHT_DECAY = 0.1
OUTER_RATE = 0.7
OUTER_MOMENTUM = 0.9
PIECES = ((0, 256), (256, 256), (512, 512))
PARTS = 2
LOW = jnp.bfloat16
F32 = jnp.float32
NN = (((1,), (0,)), ((), ()))
NT = (((1,), (1,)), ((), ()))
TN = (((0,), (0,)), ((), ()))


def dot(a, b, dims=NN):
    return lax.dot_general(a, b, dims, preferred_element_type=F32)


MESH = pl.DeviceIdType.MESH


def params(identity=None):
    if identity is None:
        return pltpu.CompilerParams(vmem_limit_bytes=60 * 2**20)
    return pltpu.CompilerParams(vmem_limit_bytes=60 * 2**20, collective_id=identity, has_side_effects=True)


def partner():
    return (lax.axis_index("group"), 1 - lax.axis_index("fsdp"), lax.axis_index("tensor"))


def greet_partner():
    barrier = pltpu.get_barrier_semaphore()
    pl.semaphore_signal(barrier, inc=1, device_id=partner(), device_id_type=MESH)
    pl.semaphore_wait(barrier, 1)


def to_partner(sent, received, sends, receives, n):
    return pltpu.make_async_remote_copy(
        src_ref=sent.at[n],
        dst_ref=received.at[n],
        send_sem=sends.at[n],
        recv_sem=receives.at[n],
        device_id=partner(),
        device_id_type=MESH,
    )


def bands(depth):
    f = lax.axis_index("fsdp")
    return pl.ds(pl.multiple_of(f * depth, depth), depth), pl.ds(pl.multiple_of((1 - f) * depth, depth), depth)


def exchange_scratch(steps, shape):
    dma = pltpu.SemaphoreType.DMA
    return [
        pltpu.VMEM((steps, *shape), F32),
        pltpu.VMEM((steps, *shape), LOW),
        pltpu.VMEM((steps, *shape), LOW),
        dma((steps,)),
        dma((steps,)),
    ]


def cost(flops, moved, special=0):
    return pl.CostEstimate(flops=int(flops), bytes_accessed=int(moved), transcendentals=int(special))


def padded(rows):
    return -(-rows // 16) * 16


def centred(source):
    centre = source - jnp.mean(source, axis=-1, keepdims=True)
    spread = jnp.mean(centre * centre, axis=-1, keepdims=True)
    inverse = lax.rsqrt(spread + EPSILON)
    return centre * inverse, inverse


def norm_back(upstream, normal, inverse, gain):
    pulled = upstream * gain
    mean_one = jnp.mean(pulled, axis=-1, keepdims=True)
    mean_two = jnp.mean(pulled * normal, axis=-1, keepdims=True)
    return inverse * (pulled - mean_one - normal * mean_two)


def project_kernel(images, seq, x_ref, w_ref, vec_ref, n_ref, out_ref, n_scr):
    j, t = pl.program_id(0), pl.program_id(1)
    span = n_scr.shape[0] // images

    @pl.when((j == 0) & (t == 0))
    def _():
        n_scr[...] = jnp.zeros_like(n_scr)
        for i in range(images):
            normal, _ = centred(x_ref[i].astype(F32))
            n_scr[pl.ds(i * span, seq), :] = (normal * vec_ref[0:1] + vec_ref[1:2]).astype(LOW)
        n_ref[...] = n_scr[...]

    cols = out_ref.shape[-1]
    out = dot(n_scr[...], w_ref[0, 0])
    at = pl.ds(pl.multiple_of(t * cols, cols), cols)
    bias = jnp.where(j == 0, vec_ref[4:5, at], jnp.where(j == 2, vec_ref[5:6, at], 0.0))
    out_ref[0] = (out + bias).astype(LOW)


def project(patches, w_attn, vec):
    images, seq, width = patches.shape
    shards, _, _, cols = w_attn.shape
    rows = images * padded(seq)
    return pl.pallas_call(
        functools.partial(project_kernel, images, seq),
        grid=(3, shards),
        in_specs=[
            pl.BlockSpec((images, seq, width), lambda j, t: (0, 0, 0)),
            pl.BlockSpec((1, 1, width, cols), lambda j, t: (t, j, 0, 0)),
            pl.BlockSpec(vec.shape, lambda j, t: (0, 0)),
        ],
        out_specs=[
            pl.BlockSpec((rows, width), lambda j, t: (0, 0)),
            pl.BlockSpec((1, rows, cols), lambda j, t: (j, 0, t)),
        ],
        out_shape=[
            jax.ShapeDtypeStruct((rows, width), LOW),
            jax.ShapeDtypeStruct((3, rows, width), LOW),
        ],
        scratch_shapes=[pltpu.VMEM((rows, width), LOW)],
        compiler_params=params(),
        cost_estimate=cost(6 * rows * width * width, 16 * rows * width),
        name="project",
    )(patches, w_attn, vec)


def half_lanes(value, which):
    lane = lax.broadcasted_iota(jnp.int32, value.shape, 1)
    return jnp.where((lane >= HD) == bool(which), value, jnp.zeros_like(value))


def attend_kernel(seq, q_ref, k_ref, v_ref, out_ref):
    span = q_ref.shape[1]
    scale = HD**-0.5
    q, k, v = q_ref[0], k_ref[0], v_ref[0]
    parts = []
    for h in range(2):
        scores = dot(q, half_lanes(k, h), NT)
        lane = lax.broadcasted_iota(jnp.int32, scores.shape, 1)
        scores = jnp.where(lane < seq, scores, -1e30)
        top = jnp.max(scores, axis=1, keepdims=True)
        raised = jnp.exp((scores - top) * scale)
        total = jnp.sum(raised, axis=1, keepdims=True)
        probs = (raised * (1.0 / total)).astype(LOW)
        parts.append(dot(probs, v))
    lane = lax.broadcasted_iota(jnp.int32, (span, 2 * HD), 1)
    out_ref[...] = jnp.where(lane < HD, parts[0], parts[1]).astype(LOW)


def attend(qkv, images, seq):
    _, rows, width = qkv.shape
    span = rows // images
    pair = 2 * HD

    def take(j):
        return pl.BlockSpec((1, span, pair), lambda i, h: (j, i, h))

    return pl.pallas_call(
        functools.partial(attend_kernel, seq),
        grid=(images, width // pair),
        in_specs=[take(0), take(1), take(2)],
        out_specs=pl.BlockSpec((span, pair), lambda i, h: (i, h)),
        out_shape=jax.ShapeDtypeStruct((rows, width), LOW),
        compiler_params=params(),
        cost_estimate=cost(16 * rows * span * width, 8 * rows * width, rows * span * (width // HD)),
        name="attend",
    )(qkv, qkv, qkv)


def mix_kernel(seq, alive_ref, att_ref, x_ref, g_ref, w_ref, vec_ref, resid_ref, n_ref, g2_ref, x_scr):
    i = pl.program_id(0)
    shards, _, _, cols = w_ref.shape
    x_scr[...] = jnp.zeros_like(x_scr)
    x_scr[0:seq, :] = x_ref[0].astype(F32)
    total = x_scr[...] + vec_ref[6:7]
    for t in range(shards):
        total = total + dot(att_ref[:, t * cols : (t + 1) * cols], w_ref[t, 0], NT)
    resid_ref[...] = total
    normal, _ = centred(total)
    n_ref[...] = (normal * vec_ref[2:3] + vec_ref[3:4]).astype(LOW)
    x_scr[0:seq, :] = g_ref[0].astype(F32) * alive_ref[i]
    g2_ref[...] = x_scr[...].astype(LOW)


def mix(alive, attended, patches, cotangent, w_attn, vec):
    images, seq, width = patches.shape
    rows = attended.shape[0]
    span = rows // images
    shards, _, _, cols = w_attn.shape
    block = pl.BlockSpec((span, width), lambda i: (i, 0))
    whole = jax.ShapeDtypeStruct((rows, width), LOW)
    return pl.pallas_call(
        functools.partial(mix_kernel, seq),
        grid=(images,),
        in_specs=[
            pl.BlockSpec(memory_space=pltpu.SMEM),
            block,
            pl.BlockSpec((1, seq, width), lambda i: (i, 0, 0)),
            pl.BlockSpec((1, seq, width), lambda i: (i, 0, 0)),
            pl.BlockSpec((shards, 1, width, cols), lambda i: (0, 3, 0, 0)),
            pl.BlockSpec(vec.shape, lambda i: (0, 0)),
        ],
        out_specs=[block, block, block],
        out_shape=[jax.ShapeDtypeStruct((rows, width), F32), whole, whole],
        scratch_shapes=[pltpu.VMEM((span, width), F32)],
        compiler_params=params(),
        cost_estimate=cost(2 * rows * width * width, 16 * rows * width),
        name="mix",
    )(alive, attended, patches, cotangent, w_attn, vec)


def mlp_kernel(first, pairwise, n_ref, g_ref, w1_ref, w2_ref, bias_ref, *refs):
    if not first:
        yi_ref, gi_ref, *refs = refs
    y_ref, gn_ref, dw_ref, db_ref, h_scr, p_scr, loaded, *exchange = refs
    step = pl.program_id(0)
    each, _, width, cols = w1_ref.shape
    if not first:
        loads = (
            pltpu.make_async_copy(yi_ref, y_ref, loaded.at[0]),
            pltpu.make_async_copy(gi_ref, gn_ref, loaded.at[1]),
        )

    @pl.when(step == 0)
    def _():
        if not first:
            for load in loads:
                load.start()
        else:
            y_ref[...] = jnp.zeros_like(y_ref)
            gn_ref[...] = jnp.zeros_like(gn_ref)
        if pairwise:
            greet_partner()

    w1 = jnp.concatenate([w1_ref[t, 0] for t in range(each)], axis=1)
    w2 = jnp.concatenate([w2_ref[t, 0] for t in range(each)], axis=1)
    bias = jnp.concatenate([bias_ref[t] for t in range(each)], axis=1)
    pre = dot(n_ref[...], w1) + bias
    cdf = 0.5 * (1.0 + lax.erf(pre * 0.7071067811865476))
    h_scr[...] = (pre * cdf).astype(LOW)
    slope = cdf + pre * jnp.exp(-0.5 * pre * pre) * 0.3989422804014327
    p_scr[...] = (dot(g_ref[...], w2) * slope).astype(LOW)
    sums = jnp.sum(p_scr[...].astype(F32), axis=0, keepdims=True)
    for t in range(each):
        db_ref[t] = sums[:, t * cols : (t + 1) * cols]

    if pairwise:
        own, sent, received, sends, receives = exchange
        ours, theirs = bands(width // 2)

        def collect(n):
            to_partner(sent, received, sends, receives, n % 2).wait()
            for which in range(2):
                total = (own[n % 2, which] + received[n % 2, which].astype(F32)).astype(LOW)
                for t in range(each):
                    dw_ref[n * each + t, which] = total[:, t * cols : (t + 1) * cols]

        for n in range(dw_ref.shape[0] // each):

            @pl.when(step == n)
            def _():
                if n:
                    collect(n - 1)
                sent[n % 2, 0] = dot(n_ref[:, theirs], p_scr[...], TN).astype(LOW)
                sent[n % 2, 1] = dot(g_ref[:, theirs], h_scr[...], TN).astype(LOW)
                to_partner(sent, received, sends, receives, n % 2).start()
                own[n % 2, 0] = dot(n_ref[:, ours], p_scr[...], TN)
                own[n % 2, 1] = dot(g_ref[:, ours], h_scr[...], TN)

    else:
        shards, depth = dw_ref.shape[0], dw_ref.shape[3]
        d1 = dot(n_ref[...], p_scr[...], TN).astype(LOW)
        d2 = dot(g_ref[...], h_scr[...], TN).astype(LOW)
        for f in range(shards):
            for t in range(each):
                dw_ref[f, t, 0] = d1[f * depth : (f + 1) * depth, t * cols : (t + 1) * cols]
                dw_ref[f, t, 1] = d2[f * depth : (f + 1) * depth, t * cols : (t + 1) * cols]

    if not first:

        @pl.when(step == 0)
        def _():
            for load in loads:
                load.wait()

    y_ref[...] += dot(h_scr[...], w2, NT)
    gn_ref[...] += dot(p_scr[...], w1, NT)
    if pairwise:

        @pl.when(step == pl.num_programs(0) - 1)
        def _():
            collect(dw_ref.shape[0] // each - 1)


def mlp(part, start, cols, normed, grad_two, w_mlp, bias, carried, fsdp):
    rows, width = normed.shape
    shards = w_mlp.shape[0]
    each = max(512 // cols, 1)
    at = start // cols
    first, pairwise = carried is None, fsdp == 2
    single = pl.Buffered(1)
    full = pl.BlockSpec((rows, width), lambda s: (0, 0), pipeline_mode=single)
    depth = width // fsdp
    steps = shards // each
    acc_shape = jax.ShapeDtypeStruct((rows, width), F32)
    if pairwise:
        out_w = pl.BlockSpec((shards, 2, depth, cols), lambda s: (0, 0, 0, 0), pipeline_mode=single)
        w_shape = jax.ShapeDtypeStruct((shards, 2, depth, cols), LOW)
        extra = exchange_scratch(2, (2, depth, each * cols))
    else:
        out_w = pl.BlockSpec((fsdp, each, 2, depth, cols), lambda s: (0, s, 0, 0, 0))
        w_shape = jax.ShapeDtypeStruct((fsdp, shards, 2, depth, cols), LOW)
        extra = []
    return pl.pallas_call(
        functools.partial(mlp_kernel, first, pairwise),
        grid=(steps,),
        in_specs=[
            full,
            full,
            pl.BlockSpec((each, 1, width, cols), lambda s: (s, 0, 0, at)),
            pl.BlockSpec((each, 1, width, cols), lambda s: (s, 1, 0, at)),
            pl.BlockSpec((each, 1, cols), lambda s: (s, 0, at)),
        ]
        + ([] if first else [pl.BlockSpec(memory_space=pl.ANY)] * 2),
        out_specs=[full, full, out_w, pl.BlockSpec((each, 1, cols), lambda s: (s, 0, 0))],
        out_shape=[acc_shape, acc_shape, w_shape, jax.ShapeDtypeStruct((shards, 1, cols), F32)],
        scratch_shapes=[
            pltpu.VMEM((rows, each * cols), LOW),
            pltpu.VMEM((rows, each * cols), LOW),
            pltpu.SemaphoreType.DMA((2,)),
            *extra,
        ],
        compiler_params=params(2 + part if pairwise else None),
        cost_estimate=cost(12 * rows * width * cols * shards, 24 * rows * width),
        name=f"mlp_{part}",
    )(normed, grad_two, w_mlp, w_mlp, bias, *([] if first else carried))


def turn_kernel(seq, pairwise, alive_ref, resid_ref, y_ref, gn_ref, g2_ref, att_ref, w_ref, vec_ref,
                out_ref, gr_ref, ga_ref, dw_ref, sums_ref, dw_scr, *exchange):
    i = pl.program_id(0)
    if pairwise:
        pl.when(i == 0)(greet_partner)
    shards, _, _, cols = w_ref.shape
    resid = resid_ref[...]
    out_ref[0] = ((resid + y_ref[...] + vec_ref[7:8]) * alive_ref[i]).astype(LOW)[0:seq]
    normal, inverse = centred(resid)
    upstream = gn_ref[...]
    grad_out = g2_ref[...].astype(F32)
    grad_resid = grad_out + norm_back(upstream, normal, inverse, vec_ref[2:3])
    gr_ref[...] = grad_resid
    low = grad_resid.astype(LOW)
    rows = [
        jnp.sum(upstream * normal, axis=0, keepdims=True),
        jnp.sum(upstream, axis=0, keepdims=True),
        jnp.sum(grad_resid, axis=0, keepdims=True),
        jnp.sum(grad_out, axis=0, keepdims=True),
    ]
    rows = jnp.concatenate(rows, axis=0)

    @pl.when(i == 0)
    def _():
        sums_ref[...] = rows

    @pl.when(i != 0)
    def _():
        sums_ref[...] += rows

    for t in range(shards):
        ga_ref[:, t * cols : (t + 1) * cols] = dot(low, w_ref[t, 0]).astype(LOW)
    part = dot(low, att_ref[...], TN)

    @pl.when(i == 0)
    def _():
        dw_scr[...] = part

    @pl.when(i != 0)
    def _():
        dw_scr[...] += part

    @pl.when(i == pl.num_programs(0) - 1)
    def _():
        if pairwise:
            sent, received, sends, receives = exchange
            ours, theirs = bands(dw_scr.shape[0] // 2)
            sent[0] = dw_scr[theirs, :].astype(LOW)
            copy = to_partner(sent, received, sends, receives, 0)
            copy.start()
            copy.wait()
            total = (dw_scr[ours, :] + received[0].astype(F32)).astype(LOW)
            for t in range(shards):
                dw_ref[t, 0] = total[:, t * cols : (t + 1) * cols]
            return
        depth = dw_ref.shape[3]
        for f in range(dw_ref.shape[0]):
            for t in range(shards):
                dw_ref[f, t, 0] = dw_scr[f * depth : (f + 1) * depth, t * cols : (t + 1) * cols].astype(LOW)


def turn(alive, resid, branch, grad_normed, grad_two, attended, w_attn, vec, images, seq, fsdp):
    rows, width = resid.shape
    span = rows // images
    shards, _, _, cols = w_attn.shape
    depth = width // fsdp
    pairwise = fsdp == 2
    lead = () if pairwise else (fsdp,)
    block = pl.BlockSpec((span, width), lambda i: (i, 0))
    return pl.pallas_call(
        functools.partial(turn_kernel, seq, pairwise),
        grid=(images,),
        in_specs=[
            pl.BlockSpec(memory_space=pltpu.SMEM),
            block, block, block, block, block,
            pl.BlockSpec((shards, 1, width, cols), lambda i: (0, 3, 0, 0)),
            pl.BlockSpec(vec.shape, lambda i: (0, 0)),
        ],
        out_specs=[
            pl.BlockSpec((1, seq, width), lambda i: (i, 0, 0)),
            block, block,
            pl.BlockSpec((*lead, shards, 1, depth, cols), lambda i: (0,) * (4 + len(lead))),
            pl.BlockSpec((4, width), lambda i: (0, 0)),
        ],
        out_shape=[
            jax.ShapeDtypeStruct((images, seq, width), LOW),
            jax.ShapeDtypeStruct((rows, width), F32),
            jax.ShapeDtypeStruct((rows, width), LOW),
            jax.ShapeDtypeStruct((*lead, shards, 1, depth, cols), LOW),
            jax.ShapeDtypeStruct((4, width), F32),
        ],
        scratch_shapes=[pltpu.VMEM((width, width), F32)] + (exchange_scratch(1, (depth, width))[1:] if pairwise else []),
        compiler_params=params(6 if pairwise else None),
        cost_estimate=cost(4 * rows * width * width, 24 * rows * width),
        name="turn",
    )(alive, resid, branch, grad_normed, grad_two, attended, w_attn, vec)


def unattend_kernel(seq, q_ref, k_ref, v_ref, g_ref, dq_ref, dk_ref, dv_ref):
    span = q_ref.shape[1]
    scale = HD**-0.5
    q, k, v, g = q_ref[0], k_ref[0], v_ref[0], g_ref[...]
    parts = []
    for h in range(2):
        scores = dot(half_lanes(k, h), q, NT)
        row = lax.broadcasted_iota(jnp.int32, scores.shape, 0)
        scores = jnp.where(row < seq, scores, -1e30)
        top = jnp.max(scores, axis=0, keepdims=True)
        raised = jnp.exp((scores - top) * scale)
        total = jnp.sum(raised, axis=0, keepdims=True)
        probs = raised * (1.0 / total)
        gp = dot(half_lanes(v, h), g, NT)
        delta = jnp.sum(probs * gp, axis=0, keepdims=True)
        gs = (probs * (gp - delta)).astype(LOW)
        dv = dot(probs.astype(LOW), g)
        dk = dot(gs, q)
        dq = dot(gs, k, TN)
        parts.append((dq, dk, dv))
    lane = lax.broadcasted_iota(jnp.int32, (span, 2 * HD), 1) < HD
    dq_ref[0] = (jnp.where(lane, parts[0][0], parts[1][0]) * scale).astype(LOW)
    dk_ref[0] = (jnp.where(lane, parts[0][1], parts[1][1]) * scale).astype(LOW)
    dv_ref[0] = jnp.where(lane, parts[0][2], parts[1][2]).astype(LOW)


def unattend(qkv, grad_attended, images, seq, part, parts, shards):
    _, rows, width = qkv.shape
    span = rows // images
    pair = 2 * HD
    each = width // shards // parts // pair

    def spot(h):
        return (h // each) * (each * parts) + part * each + h % each

    def take(j):
        return pl.BlockSpec((1, span, pair), lambda i, h: (j, i, spot(h)))

    out = pl.BlockSpec((1, span, pair), lambda i, h: (0, i, h))
    shape = jax.ShapeDtypeStruct((1, rows, width // parts), LOW)
    return pl.pallas_call(
        functools.partial(unattend_kernel, seq),
        grid=(images, width // pair // parts),
        in_specs=[take(0), take(1), take(2), pl.BlockSpec((span, pair), lambda i, h: (i, spot(h)))],
        out_specs=[out, out, out],
        out_shape=[shape, shape, shape],
        compiler_params=params(),
        cost_estimate=cost(
            40 * rows * span * width // parts, 14 * rows * width // parts, rows * span * (width // HD) // parts
        ),
        name=f"unattend_{part}",
    )(qkv, qkv, qkv, grad_attended)


def close_kernel(seq, images, pairwise, groups, first, final, n_ref, dq_ref, dk_ref, dv_ref, w_ref, *refs):
    if not first:
        carry_ref, *refs = refs
    elif pairwise:
        more_ref, *refs = refs
    if final:
        x_ref, gr_ref, vec_ref, *refs = refs
        if pairwise:
            diff_ref, *refs = refs
        out_ref, norm_ref, *refs = refs
        if pairwise:
            total_ref, *refs = refs
    else:
        acc_ref, *refs = refs
    dw_ref, sums_ref, acc_scr, *exchange = refs
    j = pl.program_id(0)
    shards, _, _, cols = w_ref.shape
    span = n_ref.shape[0] // images
    if pairwise:
        own, sent, received, sends, receives, *exchange = exchange
        if not final:
            pl.when(j == 0)(greet_partner)
    if pairwise and final:
        mine, landed, sends_two, receives_two, loaded = exchange
        g, f, t = lax.axis_index("group"), lax.axis_index("fsdp"), lax.axis_index("tensor")
        quarter = landed.shape[1]

        def rows(n):
            return pl.ds(pl.multiple_of(n * quarter, quarter), quarter)

        def other(k):
            return (lax.rem(g + k, groups), f, t)

        def part(k):
            return pltpu.make_async_remote_copy(
                src_ref=diff_ref.at[rows(lax.rem(g + k, groups)), :],
                dst_ref=landed.at[k],
                send_sem=sends_two.at[k],
                recv_sem=receives_two.at[k],
                device_id=other(k),
                device_id_type=MESH,
            )

        keep = pltpu.make_async_copy(diff_ref.at[rows(g), :], mine, loaded.at[0])

        @pl.when(j == 0)
        def _():
            barrier = pltpu.get_barrier_semaphore()
            pl.semaphore_signal(barrier, inc=1, device_id=partner(), device_id_type=MESH)
            for k in range(1, groups):
                pl.semaphore_signal(barrier, inc=1, device_id=other(k), device_id_type=MESH)
            pl.semaphore_wait(barrier, groups)
            for k in range(1, groups):
                part(k).start()
            keep.start()

    @pl.when(j == 0)
    def _():
        acc_scr[...] = jnp.zeros_like(acc_scr) if first else carry_ref[...]
        sums_ref[0:1, :] = jnp.sum(dq_ref[0].astype(F32), axis=0, keepdims=True)
        sums_ref[1:2, :] = jnp.sum(dv_ref[0].astype(F32), axis=0, keepdims=True)

    def spread(n, total, f=None):
        for t in range(shards):
            piece = total[:, t * cols : (t + 1) * cols]
            if f is None:
                dw_ref[t, n] = piece
            else:
                dw_ref[f, t, 0] = piece

    def step(ref):
        weight = jnp.concatenate([w_ref[t, 0] for t in range(shards)], axis=1)
        if pairwise:
            ours, theirs = bands(n_ref.shape[1] // 2)
            sent[j] = dot(n_ref[:, theirs], ref[0], TN).astype(LOW)
            to_partner(sent, received, sends, receives, j).start()
            own[j] = dot(n_ref[:, ours], ref[0], TN)
        else:
            depth = dw_ref.shape[3]
            dw = dot(n_ref[...], ref[0], TN).astype(LOW)
            for f in range(dw_ref.shape[0]):
                spread(0, dw[f * depth : (f + 1) * depth], f)
        acc_scr[...] += dot(ref[0], weight, NT)

    @pl.when(j == 0)
    def _():
        step(dq_ref)

    @pl.when(j == 1)
    def _():
        step(dk_ref)

    @pl.when(j == 2)
    def _():
        step(dv_ref)
        if pairwise:
            for n in range(own.shape[0]):
                to_partner(sent, received, sends, receives, n).wait()
                spread(n, (own[n] + received[n].astype(F32)).astype(LOW))
            if first:
                for t in range(shards):
                    for n in range(dw_ref.shape[1] - 3):
                        dw_ref[t, 3 + n] = more_ref[t, 0, :, n * cols : (n + 1) * cols]
        if not final:
            acc_ref[...] = acc_scr[...]
            return
        gain = jnp.zeros((1, vec_ref.shape[1]), F32)
        shift = jnp.zeros((1, vec_ref.shape[1]), F32)
        for i in range(images):
            normal, inverse = centred(x_ref[i].astype(F32))
            upstream = acc_scr[i * span : i * span + seq, :]
            out_ref[i] = gr_ref[i * span : i * span + seq, :] + norm_back(upstream, normal, inverse, vec_ref[0:1])
            gain += jnp.sum(upstream * normal, axis=0, keepdims=True)
            shift += jnp.sum(upstream, axis=0, keepdims=True)
        norm_ref[0:1, :] = gain
        norm_ref[1:2, :] = shift
        if pairwise:
            keep.wait()
            total = mine[...].astype(F32)
            for k in range(1, groups):
                part(k).wait()
                total = total + landed[k].astype(F32)
            total_ref[...] = total.astype(LOW)


def close(part, parts, normed, grads, w_attn, carry, more, ending, fsdp, groups, images, seq):
    rows, width = normed.shape
    shards, _, _, cols = w_attn.shape
    cols = cols // parts
    lanes = shards * cols
    depth = width // fsdp
    pairwise, first, final = fsdp == 2, carry is None, ending is not None
    single = pl.Buffered(1)
    stack = pl.BlockSpec((1, rows, lanes), lambda j: (0, 0, 0), pipeline_mode=single)
    full = pl.BlockSpec((rows, width), lambda j: (0, 0), pipeline_mode=single)
    image = pl.BlockSpec((images, seq, width), lambda j: (0, 0, 0), pipeline_mode=single)
    if pairwise:
        many = 3 + parts if first else 3
        dw_spec = pl.BlockSpec((shards, many, depth, cols), lambda j: (0, 0, 0, 0), pipeline_mode=single)
        dw_shape = jax.ShapeDtypeStruct((shards, many, depth, cols), LOW)
        extra = exchange_scratch(3, (depth, lanes))
    else:
        dw_spec = pl.BlockSpec((fsdp, shards, 1, depth, cols), lambda j: (0, 0, j, 0, 0))
        dw_shape = jax.ShapeDtypeStruct((fsdp, shards, 3, depth, cols), LOW)
        extra = []
    in_specs = [full, stack, stack, stack, pl.BlockSpec((shards, 1, width, cols), lambda j: (0, j, 0, part))]
    out_specs, out_shape = [], []
    if not first:
        in_specs.append(full)
    elif pairwise:
        in_specs.append(pl.BlockSpec(more.shape, lambda j: (0, 0, 0, 0), pipeline_mode=single))
    if final:
        in_specs += [image, full, pl.BlockSpec((12, width), lambda j: (0, 0))]
        out_specs += [image, pl.BlockSpec((2, width), lambda j: (0, 0))]
        out_shape += [jax.ShapeDtypeStruct((images, seq, width), F32), jax.ShapeDtypeStruct((2, width), F32)]
        if pairwise:
            quarter, lanes_two = ending[3].shape[0] // groups, ending[3].shape[1]
            in_specs.append(pl.BlockSpec(memory_space=pl.ANY))
            out_specs.append(pl.BlockSpec((quarter, lanes_two), lambda j: (0, 0), pipeline_mode=single))
            out_shape.append(jax.ShapeDtypeStruct((quarter, lanes_two), LOW))
            dma = pltpu.SemaphoreType.DMA
            extra = [
                *extra,
                pltpu.VMEM((quarter, lanes_two), LOW),
                pltpu.VMEM((groups, quarter, lanes_two), LOW),
                dma((groups,)),
                dma((groups,)),
                dma((1,)),
            ]
    else:
        out_specs.append(full)
        out_shape.append(jax.ShapeDtypeStruct((rows, width), F32))
    return pl.pallas_call(
        functools.partial(close_kernel, seq, images, pairwise, groups, first, final),
        grid=(3,),
        in_specs=in_specs,
        out_specs=[*out_specs, dw_spec, pl.BlockSpec((2, lanes), lambda j: (0, 0))],
        out_shape=[*out_shape, dw_shape, jax.ShapeDtypeStruct((2, lanes), F32)],
        scratch_shapes=[pltpu.VMEM((rows, width), F32), *extra],
        compiler_params=params(7 + part if pairwise else None),
        cost_estimate=cost(12 * rows * width * lanes, 20 * rows * width),
        name=f"close_{part}",
    )(normed, *grads, w_attn, *([carry] if not first else [more] if pairwise else []), *(ending if final else []))


def attend_pair(seq, q, k, v):
    scale = HD**-0.5
    parts = []
    for h in range(2):
        scores = dot(q, half_lanes(k, h), NT)
        lane = lax.broadcasted_iota(jnp.int32, scores.shape, 1)
        scores = jnp.where(lane < seq, scores, -1e30)
        top = jnp.max(scores, axis=1, keepdims=True)
        raised = jnp.exp((scores - top) * scale)
        total = jnp.sum(raised, axis=1, keepdims=True)
        probs = (raised * (1.0 / total)).astype(LOW)
        parts.append(dot(probs, v))
    lane = lax.broadcasted_iota(jnp.int32, parts[0].shape, 1)
    return jnp.where(lane < HD, parts[0], parts[1]).astype(LOW)


def front_kernel(
    images, seq, alive_ref, a_in, m_in, x_ref, g_ref, vec_ref,
    a_out, m_out, n_out, qkv_out, att_out, resid_out, n2_out, g2_out,
    a_wide, m_wide, a_hold, m_hold, n_scr, qkv_scr, att_scr, w_scr, o_scr, x_scr, resid_scr, n2_scr, g2_scr,
    zs, zr, xs, xr, ys, yr, xfs, xfr, yfs, yfr, cs, cr, ls, ws,
):
    g, f, z = lax.axis_index("group"), lax.axis_index("fsdp"), lax.axis_index("tensor")
    shards = lax.axis_size("tensor")
    last = shards - 1
    x_at, y_at = g % 2, g // 2
    east, north = y_at * 2 + (1 - x_at), (1 - y_at) * 2 + x_at
    depth, cols = a_in.shape[1:]
    band = depth // 4
    shared = band * 3 // 8
    rest = band - 2 * shared
    span = n_scr.shape[0] // images

    def place(column):
        cx, cy = column % 2, column // 2
        return 2 * (cx + cy - 2 * cx * cy) + cy

    mine, of_east, of_north = place(g), place(east), place(north)
    z_row = mine * band - shared * (mine % 2)
    lead_east = of_east * band + shared * (of_east % 2)
    lead_north = of_north * band + shared * (of_north % 2)
    chunks = ((a_out, 0, 3), (a_out, 3, 1), (m_out, 0, 1), (m_out, 1, 1))

    def tile(n):
        return pl.multiple_of(n, 16)

    def held(n, t, row, rows):
        out, j, many = chunks[n]
        return out.at[t, pl.ds(j, many), pl.ds(tile(f * depth + row), rows), :]

    def send(part, sems, semr, n, t, to):
        return pltpu.make_async_remote_copy(
            src_ref=part, dst_ref=part, send_sem=sems.at[n, t], recv_sem=semr.at[n, t], device_id=to, device_id_type=MESH
        )

    def along(n, t, up):
        part = held(n, t, z_row, band + shared)
        return pltpu.make_async_remote_copy(
            src_ref=part,
            dst_ref=part,
            send_sem=zs.at[n, t, 0 if up else 1],
            recv_sem=zr.at[n, t],
            device_id=(g, f, z + 1 if up else z - 1),
            device_id_type=MESH,
        )

    def to_east(n, t):
        return send(held(n, t, mine * band, band), xs, xr, n, t, (east, f, z))

    def to_north(n, t):
        return send(held(n, t, mine * band, band), ys, yr, n, t, (north, f, z))

    def north_to_east(n, t):
        return send(held(n, t, lead_north, shared), xfs, xfr, n, t, (east, f, z))

    def east_to_north(n, t):
        return send(held(n, t, lead_east + shared, rest), yfs, yfr, n, t, (north, f, z))

    def across(n, t):
        return send(held(n, t, 0, depth), cs, cr, n, t, (g, 1 - f, z))

    rows = pl.ds(tile(f * depth), depth)
    loads = (
        pltpu.make_async_copy(a_in, a_wide, ls.at[0]),
        pltpu.make_async_copy(m_in, m_wide, ls.at[1]),
    )
    keeps = (
        pltpu.make_async_copy(a_hold, a_out.at[z, :, rows, :], ls.at[2]),
        pltpu.make_async_copy(m_hold, m_out.at[z, :, rows, :], ls.at[3]),
    )
    loads[0].start()

    barrier = pltpu.get_barrier_semaphore()

    def greet(to):
        pl.semaphore_signal(barrier, inc=1, device_id=to, device_id_type=MESH)

    for to in ((east, f, z), (north, f, z), (g, 1 - f, z)):
        greet(to)

    @pl.when(z > 0)
    def _():
        greet((g, f, z - 1))

    @pl.when(z < last)
    def _():
        greet((g, f, z + 1))

    loads[0].wait()
    a_hold[...] = a_wide[...].astype(LOW)
    keeps[0].start()
    pl.semaphore_wait(barrier, 3 + jnp.minimum(z, 1) + jnp.minimum(last - z, 1))
    keeps[0].wait()

    count = len(chunks)

    def when_real(k, up, run):
        @pl.when(z - k >= 0 if up else z + k <= last)
        def _():
            run(z - k if up else z + k)

    def own(n):
        @pl.when(z < last)
        def _():
            along(n, z, True).start()

        @pl.when(z > 0)
        def _():
            along(n, z, False).start()

        across(n, z).start()

    def land(n, k, up):
        def run(t):
            along(n, t, up).wait_recv()

            @pl.when(z < last if up else z > 0)
            def _():
                along(n, t, up).start()

            to_east(n, t).start()
            to_north(n, t).start()

        when_real(k, up, run)

    def relay(n, k, up):
        def run(t):
            to_east(n, t).wait_recv()
            east_to_north(n, t).start()
            to_north(n, t).wait_recv()
            north_to_east(n, t).start()

        when_real(k, up, run)

    def finish(n, k, up):
        def run(t):
            east_to_north(n, t).wait_recv()
            north_to_east(n, t).wait_recv()
            across(n, t).start()

        when_real(k, up, run)

    def both(run, n, k):
        for up in (True, False):
            run(n, k, up)

    def fetch(t):
        return pltpu.make_async_copy(a_out.at[t, pl.ds(0, 3)], w_scr, ws.at[0])

    def maps(t):
        across(0, t).wait_recv()
        fetch(t).start()
        fetch(t).wait()
        here = pl.ds(pl.multiple_of(t * cols, cols), cols)
        for j in range(3):
            out = dot(n_scr[...], w_scr[j])
            if j != 1:
                out = out + vec_ref[4 + j // 2 : 5 + j // 2, here]
            qkv_scr[j, :, here] = out.astype(LOW)

    def project(n, k, up):
        when_real(k, up, maps)

    own(0)
    loads[1].start()
    n_scr[...] = jnp.zeros_like(n_scr)
    for i in range(images):
        normal, _ = centred(x_ref[i].astype(F32))
        n_scr[pl.ds(i * span, seq), :] = (normal * vec_ref[0:1] + vec_ref[1:2]).astype(LOW)
    puts = [pltpu.make_async_copy(n_scr, n_out, ws.at[1])]
    puts[0].start()
    both(land, 0, 1)
    loads[1].wait()
    m_hold[...] = m_wide[...].astype(LOW)
    keeps[1].start()
    maps(z)
    both(land, 0, 2)
    both(relay, 0, 1)
    keeps[1].wait()
    both(land, 0, 3)
    for n in range(1, count):
        own(n)
    both(relay, 0, 2)
    both(finish, 0, 1)
    both(relay, 0, 3)
    both(finish, 0, 2)
    both(project, 0, 1)
    both(finish, 0, 3)
    both(project, 0, 2)

    rest_items = [(n, k) for k in range(1, last + 1) for n in range(1, count)]
    total = len(rest_items) + 2

    def advance(at):
        if at < len(rest_items):
            both(land, *rest_items[at])
        if 0 <= at - 1 < len(rest_items):
            both(relay, *rest_items[at - 1])
        if 0 <= at - 2 < len(rest_items):
            both(finish, *rest_items[at - 2])

    advance(0)
    both(project, 0, 3)
    puts.append(pltpu.make_async_copy(qkv_scr, qkv_out, ws.at[2]))
    puts[-1].start()

    pair = 2 * HD
    pairs = qkv_scr.shape[2] // pair
    stretch = max(pairs // 4, 1)
    at = 1
    for i in range(images):
        for start in range(0, pairs, stretch):

            def body(h, carry):
                lanes = pl.ds(pl.multiple_of(h * pair, pair), pair)
                here = pl.ds(i * span, span)
                att_scr[here, lanes] = attend_pair(
                    seq, qkv_scr[0, here, lanes], qkv_scr[1, here, lanes], qkv_scr[2, here, lanes]
                )
                return carry

            lax.fori_loop(start, start + stretch, body, 0)
            if at < total:
                advance(at)
                at += 1
    puts.append(pltpu.make_async_copy(att_scr, att_out, ws.at[3]))
    puts[-1].start()
    while at < total - 2:
        advance(at)
        at += 1

    for t in range(shards):
        across(1, t).wait_recv()
    take = pltpu.make_async_copy(a_out.at[:, 3], o_scr, ws.at[0])
    take.start()
    take.wait()
    x_scr[...] = jnp.zeros_like(x_scr)
    for i in range(images):
        here = pl.ds(i * span, span)
        x_scr[0:seq, :] = x_ref[i].astype(F32)
        out = x_scr[...] + vec_ref[6:7]
        for t in range(shards):
            out = out + dot(att_scr[here, t * cols : (t + 1) * cols], o_scr[t], NT)
        resid_scr[here, :] = out
        normal, _ = centred(out)
        n2_scr[here, :] = (normal * vec_ref[2:3] + vec_ref[3:4]).astype(LOW)
        x_scr[0:seq, :] = g_ref[i].astype(F32) * alive_ref[i]
        g2_scr[here, :] = x_scr[...].astype(LOW)
        if at < total:
            advance(at)
            at += 1
    for n, (src, dst) in enumerate(((resid_scr, resid_out), (n2_scr, n2_out), (g2_scr, g2_out))):
        puts.append(pltpu.make_async_copy(src, dst, ws.at[4 + n]))
        puts[-1].start()
    while at < total:
        advance(at)
        at += 1
    for put in puts:
        put.wait()

    for n in range(count):
        @pl.when(z < last)
        def _():
            along(n, z, True).wait_send()

        @pl.when(z > 0)
        def _():
            along(n, z, False).wait_send()

        for t in range(shards):
            across(n, t).wait_send()
            if n > 1:
                across(n, t).wait_recv()

    def settle(n, k, up):
        def run(t):
            @pl.when(z < last if up else z > 0)
            def _():
                along(n, t, up).wait_send()

            to_east(n, t).wait_send()
            to_north(n, t).wait_send()
            east_to_north(n, t).wait_send()
            north_to_east(n, t).wait_send()

        when_real(k, up, run)

    for n in range(count):
        for k in range(1, last + 1):
            both(settle, n, k)


def front(alive, attn_master, mlp_master, patches, cotangent, vec, shards):
    _, depth, a_cols = attn_master.shape
    _, _, m_cols = mlp_master.shape
    images, seq, width = patches.shape
    rows = images * padded(seq)
    anywhere = pl.BlockSpec(memory_space=pl.ANY)
    inside = pl.BlockSpec(memory_space=pltpu.VMEM)
    dma = pltpu.SemaphoreType.DMA
    low = jax.ShapeDtypeStruct((rows, width), LOW)
    return pl.pallas_call(
        functools.partial(front_kernel, images, seq),
        in_specs=[pl.BlockSpec(memory_space=pltpu.SMEM), anywhere, anywhere, inside, inside, inside],
        out_specs=[anywhere] * 8,
        out_shape=[
            jax.ShapeDtypeStruct((shards, 4, width, a_cols), LOW),
            jax.ShapeDtypeStruct((shards, 2, width, m_cols), LOW),
            low,
            jax.ShapeDtypeStruct((3, rows, width), LOW),
            low,
            jax.ShapeDtypeStruct((rows, width), F32),
            low,
            low,
        ],
        scratch_shapes=[
            pltpu.VMEM(attn_master.shape, F32),
            pltpu.VMEM(mlp_master.shape, F32),
            pltpu.VMEM(attn_master.shape, LOW),
            pltpu.VMEM(mlp_master.shape, LOW),
            pltpu.VMEM((rows, width), LOW),
            pltpu.VMEM((3, rows, width), LOW),
            pltpu.VMEM((rows, width), LOW),
            pltpu.VMEM((3, width, a_cols), LOW),
            pltpu.VMEM((shards, width, a_cols), LOW),
            pltpu.VMEM((rows // images, width), F32),
            pltpu.VMEM((rows, width), F32),
            pltpu.VMEM((rows, width), LOW),
            pltpu.VMEM((rows, width), LOW),
            dma((4, shards, 2)),
        ]
        + [dma((4, shards))] * 11
        + [dma((4,)), dma((7,))],
        compiler_params=params(1),
        cost_estimate=cost(8 * rows * width * width, 30 * rows * width),
        name="front",
    )(alive, attn_master, mlp_master, patches, cotangent, vec)


def inner_adamw(master, gradient, first, second, step_rate, decay_rate):
    first_moment = 0.9 * first + 0.1 * gradient
    second_moment = 0.95 * second + 0.05 * gradient * gradient
    step_ratio = (
        first_moment / (1.0 - 0.9**STEP) / (jnp.sqrt(second_moment / (1.0 - 0.95**STEP)) + 1e-08)
    )
    return (master - step_rate * (step_ratio + decay_rate * master), second_moment)


def outer_nesterov(master, outer_old, difference):
    momentum = OUTER_MOMENTUM * outer_old + difference
    return momentum, master - OUTER_RATE * (difference + OUTER_MOMENTUM * momentum)


def inner_kernel(join, count, *refs):
    pieces, (master_ref, moment_ref, *_, inner_ref, diff_ref) = refs[:count], refs[count:]
    gradient = join(*[piece[0] for piece in pieces]).astype(F32)
    master = master_ref[0]
    new, second = inner_adamw(master, gradient, moment_ref[0, 0, 0], moment_ref[0, 1, 0], INNER_RATE, WEIGHT_DECAY)
    inner_ref[0, 0, 0] = gradient
    inner_ref[0, 1, 0] = second
    diff_ref[0] = (master - new).astype(LOW)


def inner_step(join, pieces, unit, units, cols, master, moments, into, name):
    depth = master.shape[1]
    rows = min(depth, 131072 // cols)
    block = pl.BlockSpec((1, rows, cols), lambda u, r: (unit(u)[0], r, unit(u)[1]))
    both = pl.BlockSpec((1, 2, 1, rows, cols), lambda u, r: (0, 0, unit(u)[0], r, unit(u)[1]))
    piece_specs = [pl.BlockSpec((1, rows, piece.shape[2]), lambda u, r: (u, r, 0)) for piece in pieces]
    count = len(pieces)
    return pl.pallas_call(
        functools.partial(inner_kernel, join, count),
        grid=(units, depth // rows),
        in_specs=[*piece_specs, block, both] + ([] if into is None else [pl.BlockSpec(memory_space=pl.ANY)]),
        out_specs=[both, pl.BlockSpec((1, rows, cols), lambda u, r: (u, r, 0))],
        out_shape=[
            jax.ShapeDtypeStruct(moments.shape, F32),
            jax.ShapeDtypeStruct((units, depth, cols), LOW),
        ],
        input_output_aliases={} if into is None else {count + 2: 0},
        compiler_params=params(),
        cost_estimate=cost(30 * units * depth * cols, 24 * units * depth * cols),
        name=name,
    )(*pieces, master, moments, *([] if into is None else [into]))


def outer_kernel(groups, g_ref, total_ref, master_ref, outer_ref, *refs):
    state_ref, copy_ref = refs[-2:]
    difference = total_ref[...].reshape(copy_ref.shape[1:]).astype(F32) / groups
    momentum, fresh = outer_nesterov(master_ref[0], outer_ref[0], difference)
    state_ref[0, 0] = difference
    state_ref[1, 0] = momentum
    state_ref[2, 0] = fresh
    copy_ref[0] = fresh.astype(LOW)


def outer_step(groups, me, total, slots, unit, units, cols, master, outer_old, into, name):
    depth = master.shape[1]
    rows = min(depth, 131072 // cols, total.shape[1])
    each = total.shape[1] // rows
    block = pl.BlockSpec((1, rows, cols), lambda u, r, g: (unit(u)[0], r, unit(u)[1]))
    state = pl.BlockSpec((3, 1, rows, cols), lambda u, r, g: (0, unit(u)[0], r, unit(u)[1]))

    def spot(u, r, g):
        at = u * (depth // rows) + r
        quarter = at // each
        return (lax.rem(g[0] + groups - quarter, groups) if slots else quarter), at % each, 0

    aliased = [] if into is None else [pl.BlockSpec(memory_space=pl.ANY)] * 2
    return pl.pallas_call(
        functools.partial(outer_kernel, groups),
        grid_spec=pltpu.PrefetchScalarGridSpec(
            num_scalar_prefetch=1,
            grid=(units, depth // rows),
            in_specs=[pl.BlockSpec((1, rows, cols), spot), block, block, *aliased],
            out_specs=[state, block],
        ),
        out_shape=[
            jax.ShapeDtypeStruct((3, *master.shape), F32),
            jax.ShapeDtypeStruct(master.shape, LOW),
        ],
        input_output_aliases={} if into is None else {4: 0, 5: 1},
        compiler_params=params(),
        cost_estimate=cost(10 * units * depth * cols, 24 * units * depth * cols),
        name=name,
    )(me, total, master, outer_old, *([] if into is None else into))


def group_kernel(groups, shards, fsdp, diff_ref, *refs):
    if fsdp:
        part_ref, master_ref, moment_ref, outer_ref, total_ref, inner_ref, state_ref, copy_ref, *refs = refs
    else:
        total_ref, *refs = refs
    landed, summed, sends, receives, sends_two, receives_two, *small = refs
    g, f, t = lax.axis_index("group"), lax.axis_index("fsdp"), lax.axis_index("tensor")
    span = landed.shape[1]

    def rows(n):
        return pl.ds(pl.multiple_of(n * span, span), span)

    def other(k):
        return lax.rem(g + k, groups)

    def back(k):
        return lax.rem(g + groups - k, groups)

    def copy(src, dst, sems, semr, k, to):
        return pltpu.make_async_remote_copy(
            src_ref=src, dst_ref=dst, send_sem=sems.at[k], recv_sem=semr.at[k], device_id=to, device_id_type=MESH
        )

    def part(k):
        return copy(diff_ref.at[rows(other(k)), :], landed.at[k], sends, receives, k, (other(k), f, t))

    def result(k):
        return copy(summed, landed.at[groups + k], sends_two, receives_two, k, (other(k), f, t))

    barrier = pltpu.get_barrier_semaphore()
    for k in range(1, groups):
        pl.semaphore_signal(barrier, inc=1, device_id=(other(k), f, t), device_id_type=MESH)
    members = shards * fsdp
    if fsdp:
        few, mine, one, two, three, four = small
        me = f * shards + t

        def place(k):
            at = lax.rem(me + k, members)
            return (g, at // shards, lax.rem(at, shards))

        def piece(k):
            return copy(part_ref, few.at[k], one, two, k, place(k))

        def share(k):
            return copy(mine, few.at[members + k], three, four, k, (other(k), f, t))

        for k in range(1, members):
            pl.semaphore_signal(barrier, inc=1, device_id=place(k), device_id_type=MESH)
    pl.semaphore_wait(barrier, groups - 1 + max(members - 1, 0))

    for k in range(1, groups):
        part(k).start()
    if fsdp:
        for k in range(1, members):
            piece(k).start()
        few[0] = part_ref[...]
        for k in range(1, members):
            piece(k).wait_recv()
        gradient = jnp.zeros(part_ref.shape, F32)
        for n in range(members):
            gradient = gradient + few[lax.rem(me + members - n, members)]
        master = master_ref[...]
        new, second = inner_adamw(master, gradient, moment_ref[0], moment_ref[1], VECTOR_RATE, 0.0)
        inner_ref[0] = gradient
        inner_ref[1] = second
        mine[...] = master - new
        for k in range(1, groups):
            share(k).start()
        few[members] = mine[...]
    total = diff_ref[rows(g), :].astype(F32)
    for k in range(1, groups):
        part(k).wait_recv()
        total = total + landed[k].astype(F32)
    summed[...] = total.astype(LOW)
    for k in range(1, groups):
        result(k).start()
    total_ref[rows(g), :] = summed[...]
    if fsdp:
        for k in range(1, groups):
            share(k).wait_recv()
        difference = jnp.zeros(part_ref.shape, F32)
        for n in range(groups):
            difference = difference + few[members + lax.rem(g + groups - n, groups)]
        difference = difference / groups
        momentum, fresh = outer_nesterov(master, outer_ref[...], difference)
        state_ref[0] = difference
        state_ref[1] = momentum
        state_ref[2] = fresh
        copy_ref[...] = fresh.astype(LOW)
    for k in range(1, groups):
        result(k).wait_recv()
        total_ref[rows(back(k)), :] = landed[groups + k]
    for k in range(1, groups):
        part(k).wait_send()
        result(k).wait_send()
    if fsdp:
        for k in range(1, members):
            piece(k).wait_send()
        for k in range(1, groups):
            share(k).wait_send()


def group_sum(diff, groups, identity, name, vectors=None, shards=0, fsdp=0):
    flat = diff.reshape(-1, diff.shape[-1])
    span, cols = flat.shape[0] // groups, flat.shape[1]
    dma = pltpu.SemaphoreType.DMA
    whole = pl.BlockSpec(memory_space=pltpu.VMEM)
    out_shape = [jax.ShapeDtypeStruct(flat.shape, LOW)]
    extra = []
    if fsdp:
        shape = vectors[0].shape
        out_shape += [
            jax.ShapeDtypeStruct((2, *shape), F32),
            jax.ShapeDtypeStruct((3, *shape), F32),
            jax.ShapeDtypeStruct(shape, LOW),
        ]
        extra = [
            pltpu.VMEM((fsdp * shards + groups, *shape), F32),
            pltpu.VMEM(shape, F32),
            dma((fsdp * shards,)),
            dma((fsdp * shards,)),
            dma((groups,)),
            dma((groups,)),
        ]
    total, *rest = pl.pallas_call(
        functools.partial(group_kernel, groups, shards, fsdp),
        in_specs=[whole] * (5 if fsdp else 1),
        out_specs=[whole] * len(out_shape),
        out_shape=out_shape,
        scratch_shapes=[
            pltpu.VMEM((2 * groups, span, cols), LOW),
            pltpu.VMEM((span, cols), LOW),
            *[dma((groups,))] * 4,
            *extra,
        ],
        compiler_params=params(identity),
        cost_estimate=cost(4 * flat.size, 8 * flat.size),
        name=name,
    )(flat, *(vectors or []))
    return total.reshape(diff.shape), *rest


def gather_weights(shard):
    whole = lax.all_gather(shard, "tensor", axis=0)
    return lax.all_gather(whole, "fsdp", axis=2, tiled=True)


def around(array, k, groups):
    return lax.ppermute(array, "group", [(i, (i + k) % groups) for i in range(groups)])


def exchange_parts(diff, groups):
    g = lax.axis_index("group")
    quarters = diff.reshape(groups, -1, diff.shape[-1])
    parts = [lax.dynamic_index_in_dim(quarters, lax.rem(g + k, groups), 0, keepdims=False) for k in range(groups)]
    total = sum([around(parts[k], k, groups).astype(F32) for k in range(1, groups)], parts[0].astype(F32))
    return total.astype(LOW)


def exchange_total(own, groups):
    return [own] + [around(own, k, groups) for k in range(1, groups)]


def scatter_gradient(gradient):
    half = gradient if gradient.ndim == 4 else lax.psum_scatter(gradient, "fsdp", scatter_dimension=0)
    return lax.psum_scatter(half, "tensor", scatter_dimension=0)


def local(
    patches,
    output_grad,
    live_counts,
    attn_master,
    mlp_master,
    vector_master,
    attn_moments,
    mlp_moments,
    vector_moments,
    attn_outer,
    mlp_outer,
    vector_outer,
):
    vec = vector_master
    tensor_size, fsdp = lax.axis_size("tensor"), lax.axis_size("fsdp")
    groups = lax.axis_size("group")
    local_images, seq, width = patches.shape[2:]
    slot = (lax.axis_index("fsdp") * tensor_size + lax.axis_index("tensor")) * local_images
    slot = slot + jnp.arange(local_images)
    counts = jnp.take(live_counts[0], slot // IMG_DEV, axis=1)
    alive = ((slot % IMG_DEV)[None, :] < counts).astype(F32).reshape(-1)
    x = patches.reshape(-1, seq, width)
    cotangent = output_grad.reshape(-1, seq, width)
    images = x.shape[0]

    if (groups, fsdp) == (4, 2):
        w_attn, w_mlp, normed_one, qkv, attended, resid, normed_two, grad_two = front(
            alive, attn_master, mlp_master, x, cotangent, vec, tensor_size
        )
    else:
        w_attn = gather_weights(attn_master.astype(LOW))
        w_mlp = gather_weights(mlp_master.astype(LOW))
        normed_one, qkv = project(x, w_attn, vec)
        attended = attend(qkv, images, seq)
        resid, normed_two, grad_two = mix(alive, attended, x, cotangent, w_attn, vec)
    bias = vec[8:].reshape(tensor_size, 1, -1)
    carried = None
    mlp_grads, bias_parts = [], []
    for part, (start, cols) in enumerate(PIECES):
        *carried, dw, db = mlp(part, start, cols, normed_two, grad_two, w_mlp, bias, carried, fsdp)
        mlp_grads.append(scatter_gradient(dw))
        bias_parts.append(db)
    branch, grad_normed = carried
    block_output, grad_resid, grad_attended, dw_out, sums_two = turn(
        alive, resid, branch, grad_normed, grad_two, attended, w_attn, vec, images, seq, fsdp
    )
    def beside(*parts):
        return jnp.concatenate(parts, axis=-1)

    pairwise = fsdp == 2
    me = lax.axis_index("group").astype(jnp.int32).reshape(1)
    half = attn_master.shape[2] // PARTS
    grads = unattend(qkv, grad_attended, images, seq, 0, PARTS, tensor_size)
    head_grad, mlp_grads[0] = lax.optimization_barrier((grads[0], mlp_grads[0]))
    carry, dw_early, head_sums = close(
        0, PARTS, normed_one, (head_grad, *grads[1:]), w_attn, None, dw_out, None, fsdp, groups, images, seq
    )
    if not pairwise:
        halves = jnp.moveaxis(dw_out.reshape(*dw_out.shape[:-1], PARTS, half), -2, 2)
        dw_early = jnp.concatenate([dw_early, halves[:, :, :, 0]], axis=2)
    early_grad = scatter_gradient(dw_early)
    head_sums = [head_sums]
    carry, mlp_grads[1] = lax.optimization_barrier((carry, mlp_grads[1]))
    grads = unattend(qkv, grad_attended, images, seq, 1, PARTS, tensor_size)

    mlp_grads[0], head_grad = lax.optimization_barrier((mlp_grads[0], grads[0]))
    mlp_inner, mlp_diff = inner_step(
        beside, mlp_grads, lambda u: (u, 0), 2, mlp_master.shape[2], mlp_master, mlp_moments, None, "inner_mlp"
    )
    carry, mlp_diff = lax.optimization_barrier((carry, mlp_diff))
    ending = [x, grad_resid, vec]
    if pairwise:
        ending.append(mlp_diff.reshape(-1, mlp_diff.shape[-1]))
    patches_grad, sums_one, *mlp_own, dw_late, sums = close(
        1, PARTS, normed_one, (head_grad, *grads[1:]), w_attn, carry, None, ending, fsdp, groups, images, seq
    )
    if not pairwise:
        mlp_own = [exchange_parts(mlp_diff, groups)]
    mlp_total = exchange_total(mlp_own[0], groups)
    late_grad = scatter_gradient(dw_late)
    head_sums.append(sums)

    def early(u):
        return jnp.minimum(u, 3), jnp.maximum(u - 3, 0)

    def late(u):
        return u, 1

    def first(piece):
        return piece

    attn_inner, early_diff = inner_step(
        first, [early_grad], early, 3 + PARTS, half, attn_master, attn_moments, None, "inner_early"
    )
    (early_total,) = group_sum(early_diff, groups, 10, "group_early")
    attn_state, attn_copy = outer_step(
        groups, me, early_total, False, early, 3 + PARTS, half, attn_master, attn_outer, None, "outer_early"
    )
    attn_copy, *mlp_total = lax.optimization_barrier((attn_copy, *mlp_total))
    mlp_state, mlp_copy = outer_step(
        groups,
        me,
        jnp.stack(mlp_total),
        True,
        lambda u: (u, 0),
        2,
        mlp_master.shape[2],
        mlp_master,
        mlp_outer,
        None,
        "outer_mlp",
    )
    head_rows = jnp.concatenate([v.reshape(2, tensor_size, -1) for v in head_sums], axis=-1).reshape(2, width)
    hidden_bias = jnp.concatenate(bias_parts, axis=-1).reshape(-1, width)
    vector_part = jnp.concatenate([sums_one, sums_two[:2], head_rows, sums_two[2:], hidden_bias])

    late_grad, mlp_state = lax.optimization_barrier((late_grad, mlp_state))
    attn_inner, late_diff = inner_step(
        first, [late_grad], late, 3, half, attn_master, attn_moments, attn_inner, "inner_late"
    )
    if pairwise:
        late_total, vector_inner, vector_state, vector_copy = group_sum(
            late_diff,
            groups,
            11,
            "group_late",
            [vector_part, vec, vector_moments[0], vector_outer],
            tensor_size,
            fsdp,
        )
    else:
        (late_total,) = group_sum(late_diff, groups, 11, "group_late")
        vector_grad = lax.psum(vector_part, ("fsdp", "tensor"))
        new_vector, second_vector = inner_adamw(
            vec, vector_grad, vector_moments[0, 0], vector_moments[0, 1], VECTOR_RATE, 0.0
        )
        diff_vector = lax.psum(vec - new_vector, "group") / groups
        momentum, fresh = outer_nesterov(vec, vector_outer, diff_vector)
        vector_inner = jnp.stack([vector_grad, second_vector])
        vector_state, vector_copy = jnp.stack([diff_vector, momentum, fresh]), fresh.astype(LOW)
    attn_state, attn_copy = outer_step(
        groups, me, late_total, False, late, 3, half, attn_master, attn_outer, (attn_state, attn_copy), "outer_late"
    )
    return (
        block_output.reshape(patches.shape),
        patches_grad.reshape(patches.shape),
        attn_inner,
        attn_state,
        attn_copy,
        mlp_inner,
        mlp_state,
        mlp_copy,
        vector_inner[None],
        vector_state,
        vector_copy,
    )


def solution(mesh):
    placed = (
        P("group", None, ("fsdp", "tensor"), None, None),
        P("group", None, ("fsdp", "tensor"), None, None),
        P("group", None, None),
        P(None, "fsdp", "tensor"),
        P(None, "fsdp", "tensor"),
        P(),
        P("group", None, None, "fsdp", "tensor"),
        P("group", None, None, "fsdp", "tensor"),
        P("group", None, None, None),
        P(None, "fsdp", "tensor"),
        P(None, "fsdp", "tensor"),
        P(),
    )
    return jax.shard_map(
        local,
        mesh=mesh,
        in_specs=placed,
        out_specs=(
            P("group", None, ("fsdp", "tensor"), None, None),
            P("group", None, ("fsdp", "tensor"), None, None),
            P("group", None, None, "fsdp", "tensor"),
            P(None, None, "fsdp", "tensor"),
            P(None, "fsdp", "tensor"),
            P("group", None, None, "fsdp", "tensor"),
            P(None, None, "fsdp", "tensor"),
            P(None, "fsdp", "tensor"),
            P("group", None, None, None),
            P(),
            P(),
        ),
        check_vma=False,
    )
```

```python
import functools

import jax
import jax.numpy as jnp
from jax import lax
from jax.experimental import pallas as pl
from jax.experimental.pallas import tpu as pltpu
from jax.sharding import PartitionSpec as P

HD = 64
STEP = 8
IMG_DEV = 4
EPSILON = 1e-06
INNER_RATE = 0.02
VECTOR_RATE = 0.2
WEIGHT_DECAY = 0.1
OUTER_RATE = 0.7
OUTER_MOMENTUM = 0.9
PIECES = ((0, 256), (256, 256), (512, 512))
PARTS = 2
LOW = jnp.bfloat16
F32 = jnp.float32
NN = (((1,), (0,)), ((), ()))
NT = (((1,), (1,)), ((), ()))
TN = (((0,), (0,)), ((), ()))


def dot(a, b, dims=NN):
    return lax.dot_general(a, b, dims, preferred_element_type=F32)


MESH = pl.DeviceIdType.MESH


def params(identity=None):
    if identity is None:
        return pltpu.CompilerParams(vmem_limit_bytes=60 * 2**20)
    return pltpu.CompilerParams(vmem_limit_bytes=60 * 2**20, collective_id=identity, has_side_effects=True)


def partner():
    return (lax.axis_index("group"), 1 - lax.axis_index("fsdp"), lax.axis_index("tensor"))


def greet_partner():
    barrier = pltpu.get_barrier_semaphore()
    pl.semaphore_signal(barrier, inc=1, device_id=partner(), device_id_type=MESH)
    pl.semaphore_wait(barrier, 1)


def to_partner(sent, received, sends, receives, n):
    return pltpu.make_async_remote_copy(
        src_ref=sent.at[n],
        dst_ref=received.at[n],
        send_sem=sends.at[n],
        recv_sem=receives.at[n],
        device_id=partner(),
        device_id_type=MESH,
    )


def bands(depth):
    f = lax.axis_index("fsdp")
    return pl.ds(pl.multiple_of(f * depth, depth), depth), pl.ds(pl.multiple_of((1 - f) * depth, depth), depth)


def exchange_scratch(steps, shape):
    dma = pltpu.SemaphoreType.DMA
    return [
        pltpu.VMEM((steps, *shape), F32),
        pltpu.VMEM((steps, *shape), LOW),
        pltpu.VMEM((steps, *shape), LOW),
        dma((steps,)),
        dma((steps,)),
    ]


def cost(flops, moved, special=0):
    return pl.CostEstimate(flops=int(flops), bytes_accessed=int(moved), transcendentals=int(special))


def padded(rows):
    return -(-rows // 16) * 16


def centred(source):
    centre = source - jnp.mean(source, axis=-1, keepdims=True)
    spread = jnp.mean(centre * centre, axis=-1, keepdims=True)
    inverse = lax.rsqrt(spread + EPSILON)
    return centre * inverse, inverse


def norm_back(upstream, normal, inverse, gain):
    pulled = upstream * gain
    mean_one = jnp.mean(pulled, axis=-1, keepdims=True)
    mean_two = jnp.mean(pulled * normal, axis=-1, keepdims=True)
    return inverse * (pulled - mean_one - normal * mean_two)


def project_kernel(images, seq, x_ref, w_ref, vec_ref, n_ref, out_ref, n_scr):
    j, t = pl.program_id(0), pl.program_id(1)
    span = n_scr.shape[0] // images

    @pl.when((j == 0) & (t == 0))
    def _():
        n_scr[...] = jnp.zeros_like(n_scr)
        for i in range(images):
            normal, _ = centred(x_ref[i].astype(F32))
            n_scr[pl.ds(i * span, seq), :] = (normal * vec_ref[0:1] + vec_ref[1:2]).astype(LOW)
        n_ref[...] = n_scr[...]

    cols = out_ref.shape[-1]
    out = dot(n_scr[...], w_ref[0, 0])
    at = pl.ds(pl.multiple_of(t * cols, cols), cols)
    bias = jnp.where(j == 0, vec_ref[4:5, at], jnp.where(j == 2, vec_ref[5:6, at], 0.0))
    out_ref[0] = (out + bias).astype(LOW)


def project(patches, w_attn, vec):
    images, seq, width = patches.shape
    shards, _, _, cols = w_attn.shape
    rows = images * padded(seq)
    return pl.pallas_call(
        functools.partial(project_kernel, images, seq),
        grid=(3, shards),
        in_specs=[
            pl.BlockSpec((images, seq, width), lambda j, t: (0, 0, 0)),
            pl.BlockSpec((1, 1, width, cols), lambda j, t: (t, j, 0, 0)),
            pl.BlockSpec(vec.shape, lambda j, t: (0, 0)),
        ],
        out_specs=[
            pl.BlockSpec((rows, width), lambda j, t: (0, 0)),
            pl.BlockSpec((1, rows, cols), lambda j, t: (j, 0, t)),
        ],
        out_shape=[
            jax.ShapeDtypeStruct((rows, width), LOW),
            jax.ShapeDtypeStruct((3, rows, width), LOW),
        ],
        scratch_shapes=[pltpu.VMEM((rows, width), LOW)],
        compiler_params=params(),
        cost_estimate=cost(6 * rows * width * width, 16 * rows * width),
        name="project",
    )(patches, w_attn, vec)


def half_lanes(value, which):
    lane = lax.broadcasted_iota(jnp.int32, value.shape, 1)
    return jnp.where((lane >= HD) == bool(which), value, jnp.zeros_like(value))


def attend_kernel(seq, q_ref, k_ref, v_ref, out_ref):
    span = q_ref.shape[1]
    scale = HD**-0.5
    q, k, v = q_ref[0], k_ref[0], v_ref[0]
    parts = []
    for h in range(2):
        scores = dot(q, half_lanes(k, h), NT)
        lane = lax.broadcasted_iota(jnp.int32, scores.shape, 1)
        scores = jnp.where(lane < seq, scores, -1e30)
        top = jnp.max(scores, axis=1, keepdims=True)
        raised = jnp.exp((scores - top) * scale)
        total = jnp.sum(raised, axis=1, keepdims=True)
        probs = (raised * (1.0 / total)).astype(LOW)
        parts.append(dot(probs, v))
    lane = lax.broadcasted_iota(jnp.int32, (span, 2 * HD), 1)
    out_ref[...] = jnp.where(lane < HD, parts[0], parts[1]).astype(LOW)


def attend(qkv, images, seq):
    _, rows, width = qkv.shape
    span = rows // images
    pair = 2 * HD

    def take(j):
        return pl.BlockSpec((1, span, pair), lambda i, h: (j, i, h))

    return pl.pallas_call(
        functools.partial(attend_kernel, seq),
        grid=(images, width // pair),
        in_specs=[take(0), take(1), take(2)],
        out_specs=pl.BlockSpec((span, pair), lambda i, h: (i, h)),
        out_shape=jax.ShapeDtypeStruct((rows, width), LOW),
        compiler_params=params(),
        cost_estimate=cost(16 * rows * span * width, 8 * rows * width, rows * span * (width // HD)),
        name="attend",
    )(qkv, qkv, qkv)


def mix_kernel(seq, alive_ref, att_ref, x_ref, g_ref, w_ref, vec_ref, resid_ref, n_ref, g2_ref, x_scr):
    i = pl.program_id(0)
    shards, _, _, cols = w_ref.shape
    x_scr[...] = jnp.zeros_like(x_scr)
    x_scr[0:seq, :] = x_ref[0].astype(F32)
    total = x_scr[...] + vec_ref[6:7]
    for t in range(shards):
        total = total + dot(att_ref[:, t * cols : (t + 1) * cols], w_ref[t, 0], NT)
    resid_ref[...] = total
    normal, _ = centred(total)
    n_ref[...] = (normal * vec_ref[2:3] + vec_ref[3:4]).astype(LOW)
    x_scr[0:seq, :] = g_ref[0].astype(F32) * alive_ref[i]
    g2_ref[...] = x_scr[...].astype(LOW)


def mix(alive, attended, patches, cotangent, w_attn, vec):
    images, seq, width = patches.shape
    rows = attended.shape[0]
    span = rows // images
    shards, _, _, cols = w_attn.shape
    block = pl.BlockSpec((span, width), lambda i: (i, 0))
    whole = jax.ShapeDtypeStruct((rows, width), LOW)
    return pl.pallas_call(
        functools.partial(mix_kernel, seq),
        grid=(images,),
        in_specs=[
            pl.BlockSpec(memory_space=pltpu.SMEM),
            block,
            pl.BlockSpec((1, seq, width), lambda i: (i, 0, 0)),
            pl.BlockSpec((1, seq, width), lambda i: (i, 0, 0)),
            pl.BlockSpec((shards, 1, width, cols), lambda i: (0, 3, 0, 0)),
            pl.BlockSpec(vec.shape, lambda i: (0, 0)),
        ],
        out_specs=[block, block, block],
        out_shape=[jax.ShapeDtypeStruct((rows, width), F32), whole, whole],
        scratch_shapes=[pltpu.VMEM((span, width), F32)],
        compiler_params=params(),
        cost_estimate=cost(2 * rows * width * width, 16 * rows * width),
        name="mix",
    )(alive, attended, patches, cotangent, w_attn, vec)


def mlp_kernel(first, pairwise, n_ref, g_ref, w1_ref, w2_ref, bias_ref, *refs):
    if not first:
        yi_ref, gi_ref, *refs = refs
    y_ref, gn_ref, dw_ref, db_ref, h_scr, p_scr, loaded, *exchange = refs
    step = pl.program_id(0)
    each, _, width, cols = w1_ref.shape
    if not first:
        loads = (
            pltpu.make_async_copy(yi_ref, y_ref, loaded.at[0]),
            pltpu.make_async_copy(gi_ref, gn_ref, loaded.at[1]),
        )

    @pl.when(step == 0)
    def _():
        if not first:
            for load in loads:
                load.start()
        else:
            y_ref[...] = jnp.zeros_like(y_ref)
            gn_ref[...] = jnp.zeros_like(gn_ref)
        if pairwise:
            greet_partner()

    w1 = jnp.concatenate([w1_ref[t, 0] for t in range(each)], axis=1)
    w2 = jnp.concatenate([w2_ref[t, 0] for t in range(each)], axis=1)
    bias = jnp.concatenate([bias_ref[t] for t in range(each)], axis=1)
    pre = dot(n_ref[...], w1) + bias
    cdf = 0.5 * (1.0 + lax.erf(pre * 0.7071067811865476))
    h_scr[...] = (pre * cdf).astype(LOW)
    slope = cdf + pre * jnp.exp(-0.5 * pre * pre) * 0.3989422804014327
    p_scr[...] = (dot(g_ref[...], w2) * slope).astype(LOW)
    sums = jnp.sum(p_scr[...].astype(F32), axis=0, keepdims=True)
    for t in range(each):
        db_ref[t] = sums[:, t * cols : (t + 1) * cols]

    if pairwise:
        own, sent, received, sends, receives = exchange
        ours, theirs = bands(width // 2)

        slot = lax.rem(step, 2)

        def collect(n):
            at = lax.rem(n, 2)
            to_partner(sent, received, sends, receives, at).wait()
            for which in range(2):
                total = (own[at, which] + received[at, which].astype(F32)).astype(LOW)
                for t in range(each):
                    dw_ref[n * each + t, which] = total[:, t * cols : (t + 1) * cols]

        @pl.when(step > 0)
        def _():
            collect(step - 1)

        sent[slot, 0] = dot(n_ref[:, theirs], p_scr[...], TN).astype(LOW)
        sent[slot, 1] = dot(g_ref[:, theirs], h_scr[...], TN).astype(LOW)
        to_partner(sent, received, sends, receives, slot).start()
        own[slot, 0] = dot(n_ref[:, ours], p_scr[...], TN)
        own[slot, 1] = dot(g_ref[:, ours], h_scr[...], TN)

    else:
        shards, depth = dw_ref.shape[0], dw_ref.shape[3]
        d1 = dot(n_ref[...], p_scr[...], TN).astype(LOW)
        d2 = dot(g_ref[...], h_scr[...], TN).astype(LOW)
        for f in range(shards):
            for t in range(each):
                dw_ref[f, t, 0] = d1[f * depth : (f + 1) * depth, t * cols : (t + 1) * cols]
                dw_ref[f, t, 1] = d2[f * depth : (f + 1) * depth, t * cols : (t + 1) * cols]

    if not first:

        @pl.when(step == 0)
        def _():
            for load in loads:
                load.wait()

    y_ref[...] += dot(h_scr[...], w2, NT)
    gn_ref[...] += dot(p_scr[...], w1, NT)
    if pairwise:

        @pl.when(step == pl.num_programs(0) - 1)
        def _():
            collect(step)


def mlp(part, start, cols, normed, grad_two, w_mlp, bias, carried, fsdp):
    rows, width = normed.shape
    shards = w_mlp.shape[0]
    each = max(512 // cols, 1)
    at = start // cols
    first, pairwise = carried is None, fsdp == 2
    single = pl.Buffered(1)
    full = pl.BlockSpec((rows, width), lambda s: (0, 0), pipeline_mode=single)
    depth = width // fsdp
    steps = shards // each
    acc_shape = jax.ShapeDtypeStruct((rows, width), F32)
    if pairwise:
        out_w = pl.BlockSpec((shards, 2, depth, cols), lambda s: (0, 0, 0, 0), pipeline_mode=single)
        w_shape = jax.ShapeDtypeStruct((shards, 2, depth, cols), LOW)
        extra = exchange_scratch(2, (2, depth, each * cols))
    else:
        out_w = pl.BlockSpec((fsdp, each, 2, depth, cols), lambda s: (0, s, 0, 0, 0))
        w_shape = jax.ShapeDtypeStruct((fsdp, shards, 2, depth, cols), LOW)
        extra = []
    return pl.pallas_call(
        functools.partial(mlp_kernel, first, pairwise),
        grid=(steps,),
        in_specs=[
            full,
            full,
            pl.BlockSpec((each, 1, width, cols), lambda s: (s, 0, 0, at)),
            pl.BlockSpec((each, 1, width, cols), lambda s: (s, 1, 0, at)),
            pl.BlockSpec((each, 1, cols), lambda s: (s, 0, at)),
        ]
        + ([] if first else [pl.BlockSpec(memory_space=pl.ANY)] * 2),
        out_specs=[full, full, out_w, pl.BlockSpec((each, 1, cols), lambda s: (s, 0, 0))],
        out_shape=[acc_shape, acc_shape, w_shape, jax.ShapeDtypeStruct((shards, 1, cols), F32)],
        scratch_shapes=[
            pltpu.VMEM((rows, each * cols), LOW),
            pltpu.VMEM((rows, each * cols), LOW),
            pltpu.SemaphoreType.DMA((2,)),
            *extra,
        ],
        compiler_params=params(2 + part if pairwise else None),
        cost_estimate=cost(12 * rows * width * cols * shards, 24 * rows * width),
        name=f"mlp_{part}",
    )(normed, grad_two, w_mlp, w_mlp, bias, *([] if first else carried))


def turn_kernel(seq, pairwise, alive_ref, resid_ref, y_ref, gn_ref, g2_ref, att_ref, w_ref, vec_ref,
                out_ref, gr_ref, ga_ref, dw_ref, sums_ref, dw_scr, *exchange):
    i = pl.program_id(0)
    if pairwise:
        pl.when(i == 0)(greet_partner)
    shards, _, _, cols = w_ref.shape
    resid = resid_ref[...]
    out_ref[0] = ((resid + y_ref[...] + vec_ref[7:8]) * alive_ref[i]).astype(LOW)[0:seq]
    normal, inverse = centred(resid)
    upstream = gn_ref[...]
    grad_out = g2_ref[...].astype(F32)
    grad_resid = grad_out + norm_back(upstream, normal, inverse, vec_ref[2:3])
    gr_ref[...] = grad_resid
    low = grad_resid.astype(LOW)
    rows = [
        jnp.sum(upstream * normal, axis=0, keepdims=True),
        jnp.sum(upstream, axis=0, keepdims=True),
        jnp.sum(grad_resid, axis=0, keepdims=True),
        jnp.sum(grad_out, axis=0, keepdims=True),
    ]
    rows = jnp.concatenate(rows, axis=0)

    @pl.when(i == 0)
    def _():
        sums_ref[...] = rows

    @pl.when(i != 0)
    def _():
        sums_ref[...] += rows

    for t in range(shards):
        ga_ref[:, t * cols : (t + 1) * cols] = dot(low, w_ref[t, 0]).astype(LOW)
    part = dot(low, att_ref[...], TN)

    @pl.when(i == 0)
    def _():
        dw_scr[...] = part

    @pl.when(i != 0)
    def _():
        dw_scr[...] += part

    @pl.when(i == pl.num_programs(0) - 1)
    def _():
        if pairwise:
            sent, received, sends, receives = exchange
            ours, theirs = bands(dw_scr.shape[0] // 2)
            sent[0] = dw_scr[theirs, :].astype(LOW)
            copy = to_partner(sent, received, sends, receives, 0)
            copy.start()
            copy.wait()
            total = (dw_scr[ours, :] + received[0].astype(F32)).astype(LOW)
            for t in range(shards):
                dw_ref[t, 0] = total[:, t * cols : (t + 1) * cols]
            return
        depth = dw_ref.shape[3]
        for f in range(dw_ref.shape[0]):
            for t in range(shards):
                dw_ref[f, t, 0] = dw_scr[f * depth : (f + 1) * depth, t * cols : (t + 1) * cols].astype(LOW)


def turn(alive, resid, branch, grad_normed, grad_two, attended, w_attn, vec, images, seq, fsdp):
    rows, width = resid.shape
    span = rows // images
    shards, _, _, cols = w_attn.shape
    depth = width // fsdp
    pairwise = fsdp == 2
    lead = () if pairwise else (fsdp,)
    block = pl.BlockSpec((span, width), lambda i: (i, 0))
    return pl.pallas_call(
        functools.partial(turn_kernel, seq, pairwise),
        grid=(images,),
        in_specs=[
            pl.BlockSpec(memory_space=pltpu.SMEM),
            block, block, block, block, block,
            pl.BlockSpec((shards, 1, width, cols), lambda i: (0, 3, 0, 0)),
            pl.BlockSpec(vec.shape, lambda i: (0, 0)),
        ],
        out_specs=[
            pl.BlockSpec((1, seq, width), lambda i: (i, 0, 0)),
            block, block,
            pl.BlockSpec((*lead, shards, 1, depth, cols), lambda i: (0,) * (4 + len(lead))),
            pl.BlockSpec((4, width), lambda i: (0, 0)),
        ],
        out_shape=[
            jax.ShapeDtypeStruct((images, seq, width), LOW),
            jax.ShapeDtypeStruct((rows, width), F32),
            jax.ShapeDtypeStruct((rows, width), LOW),
            jax.ShapeDtypeStruct((*lead, shards, 1, depth, cols), LOW),
            jax.ShapeDtypeStruct((4, width), F32),
        ],
        scratch_shapes=[pltpu.VMEM((width, width), F32)] + (exchange_scratch(1, (depth, width))[1:] if pairwise else []),
        compiler_params=params(6 if pairwise else None),
        cost_estimate=cost(4 * rows * width * width, 24 * rows * width),
        name="turn",
    )(alive, resid, branch, grad_normed, grad_two, attended, w_attn, vec)


def unattend_kernel(seq, q_ref, k_ref, v_ref, g_ref, dq_ref, dk_ref, dv_ref):
    span = q_ref.shape[1]
    scale = HD**-0.5
    q, k, v, g = q_ref[0], k_ref[0], v_ref[0], g_ref[...]
    parts = []
    for h in range(2):
        scores = dot(half_lanes(k, h), q, NT)
        row = lax.broadcasted_iota(jnp.int32, scores.shape, 0)
        scores = jnp.where(row < seq, scores, -1e30)
        top = jnp.max(scores, axis=0, keepdims=True)
        raised = jnp.exp((scores - top) * scale)
        total = jnp.sum(raised, axis=0, keepdims=True)
        probs = raised * (1.0 / total)
        gp = dot(half_lanes(v, h), g, NT)
        delta = jnp.sum(probs * gp, axis=0, keepdims=True)
        gs = (probs * (gp - delta)).astype(LOW)
        dv = dot(probs.astype(LOW), g)
        dk = dot(gs, q)
        dq = dot(gs, k, TN)
        parts.append((dq, dk, dv))
    lane = lax.broadcasted_iota(jnp.int32, (span, 2 * HD), 1) < HD
    dq_ref[0] = (jnp.where(lane, parts[0][0], parts[1][0]) * scale).astype(LOW)
    dk_ref[0] = (jnp.where(lane, parts[0][1], parts[1][1]) * scale).astype(LOW)
    dv_ref[0] = jnp.where(lane, parts[0][2], parts[1][2]).astype(LOW)


def unattend(qkv, grad_attended, images, seq, part, parts, shards):
    _, rows, width = qkv.shape
    span = rows // images
    pair = 2 * HD
    each = width // shards // parts // pair

    def spot(h):
        return (h // each) * (each * parts) + part * each + h % each

    def take(j):
        return pl.BlockSpec((1, span, pair), lambda i, h: (j, i, spot(h)))

    out = pl.BlockSpec((1, span, pair), lambda i, h: (0, i, h))
    shape = jax.ShapeDtypeStruct((1, rows, width // parts), LOW)
    return pl.pallas_call(
        functools.partial(unattend_kernel, seq),
        grid=(images, width // pair // parts),
        in_specs=[take(0), take(1), take(2), pl.BlockSpec((span, pair), lambda i, h: (i, spot(h)))],
        out_specs=[out, out, out],
        out_shape=[shape, shape, shape],
        compiler_params=params(),
        cost_estimate=cost(
            40 * rows * span * width // parts, 14 * rows * width // parts, rows * span * (width // HD) // parts
        ),
        name=f"unattend_{part}",
    )(qkv, qkv, qkv, grad_attended)


def close_kernel(seq, images, pairwise, groups, first, final, n_ref, dq_ref, dk_ref, dv_ref, w_ref, *refs):
    if not first:
        carry_ref, *refs = refs
    elif pairwise:
        more_ref, *refs = refs
    if final:
        x_ref, gr_ref, vec_ref, *refs = refs
        if pairwise:
            diff_ref, *refs = refs
        out_ref, norm_ref, *refs = refs
        if pairwise:
            total_ref, *refs = refs
    else:
        acc_ref, *refs = refs
    dw_ref, sums_ref, acc_scr, *exchange = refs
    j = pl.program_id(0)
    shards, _, _, cols = w_ref.shape
    span = n_ref.shape[0] // images
    if pairwise:
        own, sent, received, sends, receives, *exchange = exchange
        if not final:
            pl.when(j == 0)(greet_partner)
    if pairwise and final:
        mine, landed, sends_two, receives_two, loaded = exchange
        g, f, t = lax.axis_index("group"), lax.axis_index("fsdp"), lax.axis_index("tensor")
        quarter = landed.shape[1]

        def rows(n):
            return pl.ds(pl.multiple_of(n * quarter, quarter), quarter)

        def other(k):
            return (lax.rem(g + k, groups), f, t)

        def part(k):
            return pltpu.make_async_remote_copy(
                src_ref=diff_ref.at[rows(lax.rem(g + k, groups)), :],
                dst_ref=landed.at[k],
                send_sem=sends_two.at[k],
                recv_sem=receives_two.at[k],
                device_id=other(k),
                device_id_type=MESH,
            )

        keep = pltpu.make_async_copy(diff_ref.at[rows(g), :], mine, loaded.at[0])

        @pl.when(j == 0)
        def _():
            barrier = pltpu.get_barrier_semaphore()
            pl.semaphore_signal(barrier, inc=1, device_id=partner(), device_id_type=MESH)
            for k in range(1, groups):
                pl.semaphore_signal(barrier, inc=1, device_id=other(k), device_id_type=MESH)
            pl.semaphore_wait(barrier, groups)
            for k in range(1, groups):
                part(k).start()
            keep.start()

    @pl.when(j == 0)
    def _():
        acc_scr[...] = jnp.zeros_like(acc_scr) if first else carry_ref[...]
        sums_ref[0:1, :] = jnp.sum(dq_ref[0].astype(F32), axis=0, keepdims=True)
        sums_ref[1:2, :] = jnp.sum(dv_ref[0].astype(F32), axis=0, keepdims=True)

    def spread(n, total, f=None):
        for t in range(shards):
            piece = total[:, t * cols : (t + 1) * cols]
            if f is None:
                dw_ref[t, n] = piece
            else:
                dw_ref[f, t, 0] = piece

    def step(ref):
        weight = jnp.concatenate([w_ref[t, 0] for t in range(shards)], axis=1)
        if pairwise:
            ours, theirs = bands(n_ref.shape[1] // 2)
            sent[j] = dot(n_ref[:, theirs], ref[0], TN).astype(LOW)
            to_partner(sent, received, sends, receives, j).start()
            own[j] = dot(n_ref[:, ours], ref[0], TN)
        else:
            depth = dw_ref.shape[3]
            dw = dot(n_ref[...], ref[0], TN).astype(LOW)
            for f in range(dw_ref.shape[0]):
                spread(0, dw[f * depth : (f + 1) * depth], f)
        acc_scr[...] += dot(ref[0], weight, NT)

    @pl.when(j == 0)
    def _():
        step(dq_ref)

    @pl.when(j == 1)
    def _():
        step(dk_ref)

    @pl.when(j == 2)
    def _():
        step(dv_ref)
        if pairwise:
            for n in range(own.shape[0]):
                to_partner(sent, received, sends, receives, n).wait()
                spread(n, (own[n] + received[n].astype(F32)).astype(LOW))
            if first:
                for t in range(shards):
                    for n in range(dw_ref.shape[1] - 3):
                        dw_ref[t, 3 + n] = more_ref[t, 0, :, n * cols : (n + 1) * cols]
        if not final:
            acc_ref[...] = acc_scr[...]
            return
        gain = jnp.zeros((1, vec_ref.shape[1]), F32)
        shift = jnp.zeros((1, vec_ref.shape[1]), F32)
        for i in range(images):
            normal, inverse = centred(x_ref[i].astype(F32))
            upstream = acc_scr[i * span : i * span + seq, :]
            out_ref[i, :, 0, :] = gr_ref[i * span : i * span + seq, :] + norm_back(upstream, normal, inverse, vec_ref[0:1])
            gain += jnp.sum(upstream * normal, axis=0, keepdims=True)
            shift += jnp.sum(upstream, axis=0, keepdims=True)
        norm_ref[0:1, :] = gain
        norm_ref[1:2, :] = shift
        if pairwise:
            keep.wait()
            total = mine[...].astype(F32)
            for k in range(1, groups):
                part(k).wait()
                total = total + landed[k].astype(F32)
            total_ref[...] = total.astype(LOW)


def close(part, parts, normed, grads, w_attn, carry, more, ending, fsdp, groups, images, seq):
    rows, width = normed.shape
    shards, _, _, cols = w_attn.shape
    cols = cols // parts
    lanes = shards * cols
    depth = width // fsdp
    pairwise, first, final = fsdp == 2, carry is None, ending is not None
    single = pl.Buffered(1)
    stack = pl.BlockSpec((1, rows, lanes), lambda j: (0, 0, 0), pipeline_mode=single)
    full = pl.BlockSpec((rows, width), lambda j: (0, 0), pipeline_mode=single)
    image = pl.BlockSpec((images, seq, width), lambda j: (0, 0, 0), pipeline_mode=single)
    if pairwise:
        many = 3 + parts if first else 3
        dw_spec = pl.BlockSpec((shards, many, depth, cols), lambda j: (0, 0, 0, 0), pipeline_mode=single)
        dw_shape = jax.ShapeDtypeStruct((shards, many, depth, cols), LOW)
        extra = exchange_scratch(3, (depth, lanes))
    else:
        dw_spec = pl.BlockSpec((fsdp, shards, 1, depth, cols), lambda j: (0, 0, j, 0, 0))
        dw_shape = jax.ShapeDtypeStruct((fsdp, shards, 3, depth, cols), LOW)
        extra = []
    in_specs = [full, stack, stack, stack, pl.BlockSpec((shards, 1, width, cols), lambda j: (0, j, 0, part))]
    out_specs, out_shape = [], []
    if not first:
        in_specs.append(full)
    elif pairwise:
        in_specs.append(pl.BlockSpec(more.shape, lambda j: (0, 0, 0, 0), pipeline_mode=single))
    if final:
        in_specs += [image, full, pl.BlockSpec((12, width), lambda j: (0, 0))]
        flat = pl.BlockSpec((images, seq, 1, width), lambda j: (0, 0, 0, 0), pipeline_mode=single)
        out_specs += [flat, pl.BlockSpec((2, width), lambda j: (0, 0))]
        out_shape += [jax.ShapeDtypeStruct((images, seq, 1, width), F32), jax.ShapeDtypeStruct((2, width), F32)]
        if pairwise:
            quarter, lanes_two = ending[3].shape[0] // groups, ending[3].shape[1]
            in_specs.append(pl.BlockSpec(memory_space=pl.ANY))
            out_specs.append(pl.BlockSpec((quarter, lanes_two), lambda j: (0, 0), pipeline_mode=single))
            out_shape.append(jax.ShapeDtypeStruct((quarter, lanes_two), LOW))
            dma = pltpu.SemaphoreType.DMA
            extra = [
                *extra,
                pltpu.VMEM((quarter, lanes_two), LOW),
                pltpu.VMEM((groups, quarter, lanes_two), LOW),
                dma((groups,)),
                dma((groups,)),
                dma((1,)),
            ]
    else:
        out_specs.append(full)
        out_shape.append(jax.ShapeDtypeStruct((rows, width), F32))
    return pl.pallas_call(
        functools.partial(close_kernel, seq, images, pairwise, groups, first, final),
        grid=(3,),
        in_specs=in_specs,
        out_specs=[*out_specs, dw_spec, pl.BlockSpec((2, lanes), lambda j: (0, 0))],
        out_shape=[*out_shape, dw_shape, jax.ShapeDtypeStruct((2, lanes), F32)],
        scratch_shapes=[pltpu.VMEM((rows, width), F32), *extra],
        compiler_params=params(7 + part if pairwise else None),
        cost_estimate=cost(12 * rows * width * lanes, 20 * rows * width),
        name=f"close_{part}",
    )(normed, *grads, w_attn, *([carry] if not first else [more] if pairwise else []), *(ending if final else []))


def attend_pair(seq, q, k, v):
    scale = HD**-0.5
    parts = []
    for h in range(2):
        scores = dot(q, half_lanes(k, h), NT)
        lane = lax.broadcasted_iota(jnp.int32, scores.shape, 1)
        scores = jnp.where(lane < seq, scores, -1e30)
        top = jnp.max(scores, axis=1, keepdims=True)
        raised = jnp.exp((scores - top) * scale)
        total = jnp.sum(raised, axis=1, keepdims=True)
        probs = (raised * (1.0 / total)).astype(LOW)
        parts.append(dot(probs, v))
    lane = lax.broadcasted_iota(jnp.int32, parts[0].shape, 1)
    return jnp.where(lane < HD, parts[0], parts[1]).astype(LOW)


def front_kernel(
    images, seq, alive_ref, a_in, m_in, x_ref, g_ref, vec_ref,
    a_out, m_out, n_out, qkv_out, att_out, resid_out, n2_out, g2_out,
    a_wide, m_wide, a_hold, m_hold, n_scr, qkv_scr, att_scr, w_scr, o_scr, x_scr, resid_scr, n2_scr, g2_scr,
    zs, zr, xs, xr, ys, yr, xfs, xfr, yfs, yfr, cs, cr, ls, ws,
):
    g, f, z = lax.axis_index("group"), lax.axis_index("fsdp"), lax.axis_index("tensor")
    shards = lax.axis_size("tensor")
    last = shards - 1
    x_at, y_at = g % 2, g // 2
    east, north = y_at * 2 + (1 - x_at), (1 - y_at) * 2 + x_at
    depth, cols = a_in.shape[1:]
    band = depth // 4
    shared = band * 3 // 8
    rest = band - 2 * shared
    span = n_scr.shape[0] // images

    def place(column):
        cx, cy = column % 2, column // 2
        return 2 * (cx + cy - 2 * cx * cy) + cy

    mine, of_east, of_north = place(g), place(east), place(north)
    z_row = mine * band - shared * (mine % 2)
    lead_east = of_east * band + shared * (of_east % 2)
    lead_north = of_north * band + shared * (of_north % 2)
    chunks = ((a_out, 0, 3), (a_out, 3, 1), (m_out, 0, 1), (m_out, 1, 1))

    def tile(n):
        return pl.multiple_of(n, 16)

    def held(n, t, row, rows):
        out, j, many = chunks[n]
        return out.at[t, pl.ds(j, many), pl.ds(tile(f * depth + row), rows), :]

    def send(part, sems, semr, n, t, to):
        return pltpu.make_async_remote_copy(
            src_ref=part, dst_ref=part, send_sem=sems.at[n, t], recv_sem=semr.at[n, t], device_id=to, device_id_type=MESH
        )

    def along(n, t, up):
        part = held(n, t, z_row, band + shared)
        return pltpu.make_async_remote_copy(
            src_ref=part,
            dst_ref=part,
            send_sem=zs.at[n, t, 0 if up else 1],
            recv_sem=zr.at[n, t],
            device_id=(g, f, z + 1 if up else z - 1),
            device_id_type=MESH,
        )

    def to_east(n, t):
        return send(held(n, t, mine * band, band), xs, xr, n, t, (east, f, z))

    def to_north(n, t):
        return send(held(n, t, mine * band, band), ys, yr, n, t, (north, f, z))

    def north_to_east(n, t):
        return send(held(n, t, lead_north, shared), xfs, xfr, n, t, (east, f, z))

    def east_to_north(n, t):
        return send(held(n, t, lead_east + shared, rest), yfs, yfr, n, t, (north, f, z))

    def across(n, t):
        return send(held(n, t, 0, depth), cs, cr, n, t, (g, 1 - f, z))

    rows = pl.ds(tile(f * depth), depth)
    loads = (
        pltpu.make_async_copy(a_in, a_wide, ls.at[0]),
        pltpu.make_async_copy(m_in, m_wide, ls.at[1]),
    )
    keeps = (
        pltpu.make_async_copy(a_hold, a_out.at[z, :, rows, :], ls.at[2]),
        pltpu.make_async_copy(m_hold, m_out.at[z, :, rows, :], ls.at[3]),
    )
    loads[0].start()

    barrier = pltpu.get_barrier_semaphore()

    def greet(to):
        pl.semaphore_signal(barrier, inc=1, device_id=to, device_id_type=MESH)

    for to in ((east, f, z), (north, f, z), (g, 1 - f, z)):
        greet(to)

    @pl.when(z > 0)
    def _():
        greet((g, f, z - 1))

    @pl.when(z < last)
    def _():
        greet((g, f, z + 1))

    loads[0].wait()
    a_hold[...] = a_wide[...].astype(LOW)
    keeps[0].start()
    pl.semaphore_wait(barrier, 3 + jnp.minimum(z, 1) + jnp.minimum(last - z, 1))
    keeps[0].wait()

    count = len(chunks)

    def when_real(k, up, run):
        @pl.when(z - k >= 0 if up else z + k <= last)
        def _():
            run(z - k if up else z + k)

    def own(n):
        @pl.when(z < last)
        def _():
            along(n, z, True).start()

        @pl.when(z > 0)
        def _():
            along(n, z, False).start()

        across(n, z).start()

    def land(n, k, up):
        def run(t):
            along(n, t, up).wait_recv()

            @pl.when(z < last if up else z > 0)
            def _():
                along(n, t, up).start()

            to_east(n, t).start()
            to_north(n, t).start()

        when_real(k, up, run)

    def relay(n, k, up):
        def run(t):
            to_east(n, t).wait_recv()
            east_to_north(n, t).start()
            to_north(n, t).wait_recv()
            north_to_east(n, t).start()

        when_real(k, up, run)

    def finish(n, k, up):
        def run(t):
            east_to_north(n, t).wait_recv()
            north_to_east(n, t).wait_recv()
            across(n, t).start()

        when_real(k, up, run)

    def both(run, n, k):
        for up in (True, False):
            run(n, k, up)

    def fetch(t):
        return pltpu.make_async_copy(a_out.at[t, pl.ds(0, 3)], w_scr, ws.at[0])

    def maps(t):
        across(0, t).wait_recv()
        fetch(t).start()
        fetch(t).wait()
        here = pl.ds(pl.multiple_of(t * cols, cols), cols)

        def body(j, carry):
            bias = jnp.where(j == 0, vec_ref[4:5, here], jnp.where(j == 2, vec_ref[5:6, here], 0.0))
            qkv_scr[j, :, here] = (dot(n_scr[...], w_scr[j]) + bias).astype(LOW)
            return carry

        lax.fori_loop(0, 3, body, 0)

    def project(n, k, up):
        when_real(k, up, maps)

    own(0)
    loads[1].start()
    n_scr[...] = jnp.zeros_like(n_scr)
    for i in range(images):
        normal, _ = centred(x_ref[i].astype(F32))
        n_scr[pl.ds(i * span, seq), :] = (normal * vec_ref[0:1] + vec_ref[1:2]).astype(LOW)
    puts = [pltpu.make_async_copy(n_scr, n_out, ws.at[1])]
    puts[0].start()
    both(land, 0, 1)
    loads[1].wait()
    m_hold[...] = m_wide[...].astype(LOW)
    keeps[1].start()
    maps(z)
    both(land, 0, 2)
    both(relay, 0, 1)
    keeps[1].wait()
    both(land, 0, 3)
    for n in range(1, count):
        own(n)
    both(relay, 0, 2)
    both(finish, 0, 1)
    both(relay, 0, 3)
    both(finish, 0, 2)
    both(project, 0, 1)
    both(finish, 0, 3)
    both(project, 0, 2)

    rest_items = [(n, k) for k in range(1, last + 1) for n in range(1, count)]
    total = len(rest_items) + 2

    def advance(at):
        if at < len(rest_items):
            both(land, *rest_items[at])
        if 0 <= at - 1 < len(rest_items):
            both(relay, *rest_items[at - 1])
        if 0 <= at - 2 < len(rest_items):
            both(finish, *rest_items[at - 2])

    advance(0)
    both(project, 0, 3)
    puts.append(pltpu.make_async_copy(qkv_scr, qkv_out, ws.at[2]))
    puts[-1].start()

    pair = 2 * HD
    pairs = qkv_scr.shape[2] // pair
    stretch = max(pairs // 4, 1)
    at = 1
    for i in range(images):
        for start in range(0, pairs, stretch):

            def body(h, carry):
                lanes = pl.ds(pl.multiple_of(h * pair, pair), pair)
                here = pl.ds(i * span, span)
                att_scr[here, lanes] = attend_pair(
                    seq, qkv_scr[0, here, lanes], qkv_scr[1, here, lanes], qkv_scr[2, here, lanes]
                )
                return carry

            lax.fori_loop(start, start + stretch, body, 0)
            if at < total:
                advance(at)
                at += 1
    puts.append(pltpu.make_async_copy(att_scr, att_out, ws.at[3]))
    puts[-1].start()
    while at < total - 2:
        advance(at)
        at += 1

    for t in range(shards):
        across(1, t).wait_recv()
    take = pltpu.make_async_copy(a_out.at[:, 3], o_scr, ws.at[0])
    take.start()
    take.wait()
    x_scr[...] = jnp.zeros_like(x_scr)
    for i in range(images):
        here = pl.ds(i * span, span)
        x_scr[0:seq, :] = x_ref[i].astype(F32)
        out = x_scr[...] + vec_ref[6:7]
        for t in range(shards):
            out = out + dot(att_scr[here, t * cols : (t + 1) * cols], o_scr[t], NT)
        resid_scr[here, :] = out
        normal, _ = centred(out)
        n2_scr[here, :] = (normal * vec_ref[2:3] + vec_ref[3:4]).astype(LOW)
        x_scr[0:seq, :] = g_ref[i].astype(F32) * alive_ref[i]
        g2_scr[here, :] = x_scr[...].astype(LOW)
        if at < total:
            advance(at)
            at += 1
    for n, (src, dst) in enumerate(((resid_scr, resid_out), (n2_scr, n2_out), (g2_scr, g2_out))):
        puts.append(pltpu.make_async_copy(src, dst, ws.at[4 + n]))
        puts[-1].start()
    while at < total:
        advance(at)
        at += 1
    for put in puts:
        put.wait()

    for n in range(count):
        @pl.when(z < last)
        def _():
            along(n, z, True).wait_send()

        @pl.when(z > 0)
        def _():
            along(n, z, False).wait_send()

        for t in range(shards):
            across(n, t).wait_send()
            if n > 1:
                across(n, t).wait_recv()

    def settle(n, k, up):
        def run(t):
            @pl.when(z < last if up else z > 0)
            def _():
                along(n, t, up).wait_send()

            to_east(n, t).wait_send()
            to_north(n, t).wait_send()
            east_to_north(n, t).wait_send()
            north_to_east(n, t).wait_send()

        when_real(k, up, run)

    for n in range(count):
        for k in range(1, last + 1):
            both(settle, n, k)


def front(alive, attn_master, mlp_master, patches, cotangent, vec, shards):
    _, depth, a_cols = attn_master.shape
    _, _, m_cols = mlp_master.shape
    images, seq, width = patches.shape
    rows = images * padded(seq)
    anywhere = pl.BlockSpec(memory_space=pl.ANY)
    inside = pl.BlockSpec(memory_space=pltpu.VMEM)
    dma = pltpu.SemaphoreType.DMA
    low = jax.ShapeDtypeStruct((rows, width), LOW)
    return pl.pallas_call(
        functools.partial(front_kernel, images, seq),
        in_specs=[pl.BlockSpec(memory_space=pltpu.SMEM), anywhere, anywhere, inside, inside, inside],
        out_specs=[anywhere] * 8,
        out_shape=[
            jax.ShapeDtypeStruct((shards, 4, width, a_cols), LOW),
            jax.ShapeDtypeStruct((shards, 2, width, m_cols), LOW),
            low,
            jax.ShapeDtypeStruct((3, rows, width), LOW),
            low,
            jax.ShapeDtypeStruct((rows, width), F32),
            low,
            low,
        ],
        scratch_shapes=[
            pltpu.VMEM(attn_master.shape, F32),
            pltpu.VMEM(mlp_master.shape, F32),
            pltpu.VMEM(attn_master.shape, LOW),
            pltpu.VMEM(mlp_master.shape, LOW),
            pltpu.VMEM((rows, width), LOW),
            pltpu.VMEM((3, rows, width), LOW),
            pltpu.VMEM((rows, width), LOW),
            pltpu.VMEM((3, width, a_cols), LOW),
            pltpu.VMEM((shards, width, a_cols), LOW),
            pltpu.VMEM((rows // images, width), F32),
            pltpu.VMEM((rows, width), F32),
            pltpu.VMEM((rows, width), LOW),
            pltpu.VMEM((rows, width), LOW),
            dma((4, shards, 2)),
        ]
        + [dma((4, shards))] * 11
        + [dma((4,)), dma((7,))],
        compiler_params=params(1),
        cost_estimate=cost(8 * rows * width * width, 30 * rows * width),
        name="front",
    )(alive, attn_master, mlp_master, patches, cotangent, vec)


def inner_adamw(master, gradient, first, second, step_rate, decay_rate):
    first_moment = 0.9 * first + 0.1 * gradient
    second_moment = 0.95 * second + 0.05 * gradient * gradient
    step_ratio = (
        first_moment / (1.0 - 0.9**STEP) / (jnp.sqrt(second_moment / (1.0 - 0.95**STEP)) + 1e-08)
    )
    return (master - step_rate * (step_ratio + decay_rate * master), second_moment)


def outer_nesterov(master, outer_old, difference):
    momentum = OUTER_MOMENTUM * outer_old + difference
    return momentum, master - OUTER_RATE * (difference + OUTER_MOMENTUM * momentum)


def inner_kernel(join, count, *refs):
    pieces, (master_ref, moment_ref, *_, inner_ref, diff_ref) = refs[:count], refs[count:]
    gradient = join(*[piece[0] for piece in pieces]).astype(F32)
    master = master_ref[0]
    new, second = inner_adamw(master, gradient, moment_ref[0, 0, 0], moment_ref[0, 1, 0], INNER_RATE, WEIGHT_DECAY)
    inner_ref[0, 0, 0] = gradient
    inner_ref[0, 1, 0] = second
    diff_ref[0] = (master - new).astype(LOW)


def inner_step(join, pieces, unit, units, cols, master, moments, into, name):
    depth = master.shape[1]
    rows = min(depth, 524288 // cols)
    block = pl.BlockSpec((1, rows, cols), lambda u, r: (unit(u)[0], r, unit(u)[1]))
    both = pl.BlockSpec((1, 2, 1, rows, cols), lambda u, r: (0, 0, unit(u)[0], r, unit(u)[1]))
    piece_specs = [pl.BlockSpec((1, rows, piece.shape[2]), lambda u, r: (u, r, 0)) for piece in pieces]
    count = len(pieces)
    return pl.pallas_call(
        functools.partial(inner_kernel, join, count),
        grid=(units, depth // rows),
        in_specs=[*piece_specs, block, both] + ([] if into is None else [pl.BlockSpec(memory_space=pl.ANY)]),
        out_specs=[both, pl.BlockSpec((1, rows, cols), lambda u, r: (u, r, 0))],
        out_shape=[
            jax.ShapeDtypeStruct(moments.shape, F32),
            jax.ShapeDtypeStruct((units, depth, cols), LOW),
        ],
        input_output_aliases={} if into is None else {count + 2: 0},
        compiler_params=params(),
        cost_estimate=cost(30 * units * depth * cols, 24 * units * depth * cols),
        name=name,
    )(*pieces, master, moments, *([] if into is None else [into]))


def outer_kernel(groups, slots, each, g_ref, *refs):
    totals, (master_ref, outer_ref, *_, state_ref, copy_ref) = refs[:slots], refs[slots:]
    rows = copy_ref.shape[1]
    if slots == 1:
        total = totals[0][0]
    else:
        at = pl.program_id(0) * pl.num_programs(1) + pl.program_id(1)
        slot = lax.rem(g_ref[0] + groups - at // each, groups)
        here = pl.ds(pl.multiple_of(lax.rem(at, each) * rows, rows), rows)
        total = totals[0][here, :]
        for n in range(1, slots):
            total = jnp.where(slot == n, totals[n][here, :], total)
    difference = total.astype(F32) / groups
    momentum, fresh = outer_nesterov(master_ref[0], outer_ref[0], difference)
    state_ref[0, 0] = difference
    state_ref[1, 0] = momentum
    state_ref[2, 0] = fresh
    copy_ref[0] = fresh.astype(LOW)


def outer_step(groups, me, totals, unit, units, cols, master, outer_old, into, name):
    depth = master.shape[1]
    slots = len(totals)
    rows = min(depth, 524288 // cols, totals[0].shape[-2])
    each = totals[0].shape[-2] // rows
    block = pl.BlockSpec((1, rows, cols), lambda u, r, g: (unit(u)[0], r, unit(u)[1]))
    state = pl.BlockSpec((3, 1, rows, cols), lambda u, r, g: (0, unit(u)[0], r, unit(u)[1]))
    if slots == 1:
        total = pl.BlockSpec((1, rows, cols), lambda u, r, g: (u, r, 0))
    else:
        total = pl.BlockSpec(totals[0].shape, lambda u, r, g: (0, 0))
    aliased = [] if into is None else [pl.BlockSpec(memory_space=pl.ANY)] * 2
    return pl.pallas_call(
        functools.partial(outer_kernel, groups, slots, each),
        grid_spec=pltpu.PrefetchScalarGridSpec(
            num_scalar_prefetch=1,
            grid=(units, depth // rows),
            in_specs=[*[total] * slots, block, block, *aliased],
            out_specs=[state, block],
        ),
        out_shape=[
            jax.ShapeDtypeStruct((3, *master.shape), F32),
            jax.ShapeDtypeStruct(master.shape, LOW),
        ],
        input_output_aliases={} if into is None else {slots + 3: 0, slots + 4: 1},
        compiler_params=params(),
        cost_estimate=cost(10 * units * depth * cols, 24 * units * depth * cols),
        name=name,
    )(me, *totals, master, outer_old, *([] if into is None else into))


def group_kernel(groups, shards, fsdp, diff_ref, *refs):
    if fsdp:
        part_ref, master_ref, moment_ref, outer_ref, total_ref, inner_ref, state_ref, copy_ref, *refs = refs
    else:
        total_ref, *refs = refs
    landed, summed, sends, receives, sends_two, receives_two, *small = refs
    g, f, t = lax.axis_index("group"), lax.axis_index("fsdp"), lax.axis_index("tensor")
    span = landed.shape[1]

    def rows(n):
        return pl.ds(pl.multiple_of(n * span, span), span)

    def other(k):
        return lax.rem(g + k, groups)

    def back(k):
        return lax.rem(g + groups - k, groups)

    def copy(src, dst, sems, semr, k, to):
        return pltpu.make_async_remote_copy(
            src_ref=src, dst_ref=dst, send_sem=sems.at[k], recv_sem=semr.at[k], device_id=to, device_id_type=MESH
        )

    def part(k):
        return copy(diff_ref.at[rows(other(k)), :], landed.at[k], sends, receives, k, (other(k), f, t))

    def result(k):
        return copy(summed, landed.at[groups + k], sends_two, receives_two, k, (other(k), f, t))

    barrier = pltpu.get_barrier_semaphore()
    for k in range(1, groups):
        pl.semaphore_signal(barrier, inc=1, device_id=(other(k), f, t), device_id_type=MESH)
    members = shards * fsdp
    if fsdp:
        few, mine, one, two, three, four = small
        me = f * shards + t

        def place(k):
            at = lax.rem(me + k, members)
            return (g, at // shards, lax.rem(at, shards))

        def piece(k):
            return copy(part_ref, few.at[k], one, two, k, place(k))

        def share(k):
            return copy(mine, few.at[members + k], three, four, k, (other(k), f, t))

        for k in range(1, members):
            pl.semaphore_signal(barrier, inc=1, device_id=place(k), device_id_type=MESH)
    pl.semaphore_wait(barrier, groups - 1 + max(members - 1, 0))

    for k in range(1, groups):
        part(k).start()
    if fsdp:
        for k in range(1, members):
            piece(k).start()
        few[0] = part_ref[...]
        for k in range(1, members):
            piece(k).wait_recv()
        gradient = jnp.zeros(part_ref.shape, F32)
        for n in range(members):
            gradient = gradient + few[lax.rem(me + members - n, members)]
        master = master_ref[...]
        new, second = inner_adamw(master, gradient, moment_ref[0], moment_ref[1], VECTOR_RATE, 0.0)
        inner_ref[0] = gradient
        inner_ref[1] = second
        mine[...] = master - new
        for k in range(1, groups):
            share(k).start()
        few[members] = mine[...]
    total = diff_ref[rows(g), :].astype(F32)
    for k in range(1, groups):
        part(k).wait_recv()
        total = total + landed[k].astype(F32)
    summed[...] = total.astype(LOW)
    for k in range(1, groups):
        result(k).start()
    total_ref[rows(g), :] = summed[...]
    if fsdp:
        for k in range(1, groups):
            share(k).wait_recv()
        difference = jnp.zeros(part_ref.shape, F32)
        for n in range(groups):
            difference = difference + few[members + lax.rem(g + groups - n, groups)]
        difference = difference / groups
        momentum, fresh = outer_nesterov(master, outer_ref[...], difference)
        state_ref[0] = difference
        state_ref[1] = momentum
        state_ref[2] = fresh
        copy_ref[...] = fresh.astype(LOW)
    for k in range(1, groups):
        result(k).wait_recv()
        total_ref[rows(back(k)), :] = landed[groups + k]
    for k in range(1, groups):
        part(k).wait_send()
        result(k).wait_send()
    if fsdp:
        for k in range(1, members):
            piece(k).wait_send()
        for k in range(1, groups):
            share(k).wait_send()


def group_sum(diff, groups, identity, name, vectors=None, shards=0, fsdp=0):
    flat = diff.reshape(-1, diff.shape[-1])
    span, cols = flat.shape[0] // groups, flat.shape[1]
    dma = pltpu.SemaphoreType.DMA
    whole = pl.BlockSpec(memory_space=pltpu.VMEM)
    out_shape = [jax.ShapeDtypeStruct(flat.shape, LOW)]
    extra = []
    if fsdp:
        shape = vectors[0].shape
        out_shape += [
            jax.ShapeDtypeStruct((2, *shape), F32),
            jax.ShapeDtypeStruct((3, *shape), F32),
            jax.ShapeDtypeStruct(shape, LOW),
        ]
        extra = [
            pltpu.VMEM((fsdp * shards + groups, *shape), F32),
            pltpu.VMEM(shape, F32),
            dma((fsdp * shards,)),
            dma((fsdp * shards,)),
            dma((groups,)),
            dma((groups,)),
        ]
    total, *rest = pl.pallas_call(
        functools.partial(group_kernel, groups, shards, fsdp),
        in_specs=[whole] * (5 if fsdp else 1),
        out_specs=[whole] * len(out_shape),
        out_shape=out_shape,
        scratch_shapes=[
            pltpu.VMEM((2 * groups, span, cols), LOW),
            pltpu.VMEM((span, cols), LOW),
            *[dma((groups,))] * 4,
            *extra,
        ],
        compiler_params=params(identity),
        cost_estimate=cost(4 * flat.size, 8 * flat.size),
        name=name,
    )(flat, *(vectors or []))
    return total.reshape(diff.shape), *rest


def gather_weights(shard):
    whole = lax.all_gather(shard, "tensor", axis=0)
    return lax.all_gather(whole, "fsdp", axis=2, tiled=True)


def around(array, k, groups):
    return lax.ppermute(array, "group", [(i, (i + k) % groups) for i in range(groups)])


def exchange_parts(diff, groups):
    g = lax.axis_index("group")
    quarters = diff.reshape(groups, -1, diff.shape[-1])
    parts = [lax.dynamic_index_in_dim(quarters, lax.rem(g + k, groups), 0, keepdims=False) for k in range(groups)]
    total = sum([around(parts[k], k, groups).astype(F32) for k in range(1, groups)], parts[0].astype(F32))
    return total.astype(LOW)


def exchange_total(own, groups):
    return [own] + [around(own, k, groups) for k in range(1, groups)]


def scatter_gradient(gradient):
    half = gradient if gradient.ndim == 4 else lax.psum_scatter(gradient, "fsdp", scatter_dimension=0)
    return lax.psum_scatter(half, "tensor", scatter_dimension=0)


def local(
    patches,
    output_grad,
    live_counts,
    attn_master,
    mlp_master,
    vector_master,
    attn_moments,
    mlp_moments,
    vector_moments,
    attn_outer,
    mlp_outer,
    vector_outer,
):
    vec = vector_master
    tensor_size, fsdp = lax.axis_size("tensor"), lax.axis_size("fsdp")
    groups = lax.axis_size("group")
    local_images, seq, width = patches.shape[2:]
    slot = (lax.axis_index("fsdp") * tensor_size + lax.axis_index("tensor")) * local_images
    slot = slot + jnp.arange(local_images)
    counts = jnp.take(live_counts[0], slot // IMG_DEV, axis=1)
    alive = ((slot % IMG_DEV)[None, :] < counts).astype(F32).reshape(-1)
    x = patches.reshape(-1, seq, width)
    cotangent = output_grad.reshape(-1, seq, width)
    images = x.shape[0]

    if (groups, fsdp) == (4, 2):
        w_attn, w_mlp, normed_one, qkv, attended, resid, normed_two, grad_two = front(
            alive, attn_master, mlp_master, x, cotangent, vec, tensor_size
        )
    else:
        w_attn = gather_weights(attn_master.astype(LOW))
        w_mlp = gather_weights(mlp_master.astype(LOW))
        normed_one, qkv = project(x, w_attn, vec)
        attended = attend(qkv, images, seq)
        resid, normed_two, grad_two = mix(alive, attended, x, cotangent, w_attn, vec)
    bias = vec[8:].reshape(tensor_size, 1, -1)
    carried = None
    mlp_grads, bias_parts = [], []
    for part, (start, cols) in enumerate(PIECES):
        *carried, dw, db = mlp(part, start, cols, normed_two, grad_two, w_mlp, bias, carried, fsdp)
        mlp_grads.append(scatter_gradient(dw))
        bias_parts.append(db)
    branch, grad_normed = carried
    block_output, grad_resid, grad_attended, dw_out, sums_two = turn(
        alive, resid, branch, grad_normed, grad_two, attended, w_attn, vec, images, seq, fsdp
    )
    def beside(*parts):
        return jnp.concatenate(parts, axis=-1)

    pairwise = fsdp == 2
    me = lax.axis_index("group").astype(jnp.int32).reshape(1)
    half = attn_master.shape[2] // PARTS
    grads = unattend(qkv, grad_attended, images, seq, 0, PARTS, tensor_size)
    head_grad, mlp_grads[0] = lax.optimization_barrier((grads[0], mlp_grads[0]))
    carry, dw_early, head_sums = close(
        0, PARTS, normed_one, (head_grad, *grads[1:]), w_attn, None, dw_out, None, fsdp, groups, images, seq
    )
    if not pairwise:
        halves = jnp.moveaxis(dw_out.reshape(*dw_out.shape[:-1], PARTS, half), -2, 2)
        dw_early = jnp.concatenate([dw_early, halves[:, :, :, 0]], axis=2)
    early_grad = scatter_gradient(dw_early)
    head_sums = [head_sums]
    carry, mlp_grads[1] = lax.optimization_barrier((carry, mlp_grads[1]))
    grads = unattend(qkv, grad_attended, images, seq, 1, PARTS, tensor_size)

    mlp_grads[0], head_grad = lax.optimization_barrier((mlp_grads[0], grads[0]))
    mlp_inner, mlp_diff = inner_step(
        beside, mlp_grads, lambda u: (u, 0), 2, mlp_master.shape[2], mlp_master, mlp_moments, None, "inner_mlp"
    )
    carry, mlp_diff = lax.optimization_barrier((carry, mlp_diff))
    ending = [x, grad_resid, vec]
    if pairwise:
        ending.append(mlp_diff.reshape(-1, mlp_diff.shape[-1]))
    patches_grad, sums_one, *mlp_own, dw_late, sums = close(
        1, PARTS, normed_one, (head_grad, *grads[1:]), w_attn, carry, None, ending, fsdp, groups, images, seq
    )
    if not pairwise:
        mlp_own = [exchange_parts(mlp_diff, groups)]
    mlp_total = exchange_total(mlp_own[0], groups)
    late_grad = scatter_gradient(dw_late)
    head_sums.append(sums)

    def early(u):
        return jnp.minimum(u, 3), jnp.maximum(u - 3, 0)

    def late(u):
        return u, 1

    def first(piece):
        return piece

    attn_inner, early_diff = inner_step(
        first, [early_grad], early, 3 + PARTS, half, attn_master, attn_moments, None, "inner_early"
    )
    head_rows = jnp.concatenate([v.reshape(2, tensor_size, -1) for v in head_sums], axis=-1).reshape(2, width)
    hidden_bias = jnp.concatenate(bias_parts, axis=-1).reshape(-1, width)
    vector_part = jnp.concatenate([sums_one, sums_two[:2], head_rows, sums_two[2:], hidden_bias])

    if pairwise:
        early_total, vector_inner, vector_state, vector_copy = group_sum(
            early_diff,
            groups,
            10,
            "group_early",
            [vector_part, vec, vector_moments[0], vector_outer],
            tensor_size,
            fsdp,
        )
    else:
        (early_total,) = group_sum(early_diff, groups, 10, "group_early")
        vector_grad = lax.psum(vector_part, ("fsdp", "tensor"))
        new_vector, second_vector = inner_adamw(
            vec, vector_grad, vector_moments[0, 0], vector_moments[0, 1], VECTOR_RATE, 0.0
        )
        diff_vector = lax.psum(vec - new_vector, "group") / groups
        momentum, fresh = outer_nesterov(vec, vector_outer, diff_vector)
        vector_inner = jnp.stack([vector_grad, second_vector])
        vector_state, vector_copy = jnp.stack([diff_vector, momentum, fresh]), fresh.astype(LOW)
    attn_state, attn_copy = outer_step(
        groups, me, [early_total], early, 3 + PARTS, half, attn_master, attn_outer, None, "outer_early"
    )
    attn_copy, *mlp_total = lax.optimization_barrier((attn_copy, *mlp_total))
    mlp_state, mlp_copy = outer_step(
        groups,
        me,
        mlp_total,
        lambda u: (u, 0),
        2,
        mlp_master.shape[2],
        mlp_master,
        mlp_outer,
        None,
        "outer_mlp",
    )
    late_grad, mlp_state = lax.optimization_barrier((late_grad, mlp_state))
    attn_inner, late_diff = inner_step(
        first, [late_grad], late, 3, half, attn_master, attn_moments, attn_inner, "inner_late"
    )
    (late_total,) = group_sum(late_diff, groups, 11, "group_late")
    attn_state, attn_copy = outer_step(
        groups, me, [late_total], late, 3, half, attn_master, attn_outer, (attn_state, attn_copy), "outer_late"
    )
    return (
        block_output.reshape(patches.shape),
        patches_grad.reshape(patches.shape),
        attn_inner,
        attn_state,
        attn_copy,
        mlp_inner,
        mlp_state,
        mlp_copy,
        vector_inner[None],
        vector_state,
        vector_copy,
    )


def solution(mesh):
    placed = (
        P("group", None, ("fsdp", "tensor"), None, None),
        P("group", None, ("fsdp", "tensor"), None, None),
        P("group", None, None),
        P(None, "fsdp", "tensor"),
        P(None, "fsdp", "tensor"),
        P(),
        P("group", None, None, "fsdp", "tensor"),
        P("group", None, None, "fsdp", "tensor"),
        P("group", None, None, None),
        P(None, "fsdp", "tensor"),
        P(None, "fsdp", "tensor"),
        P(),
    )
    return jax.shard_map(
        local,
        mesh=mesh,
        in_specs=placed,
        out_specs=(
            P("group", None, ("fsdp", "tensor"), None, None),
            P("group", None, ("fsdp", "tensor"), None, None),
            P("group", None, None, "fsdp", "tensor"),
            P(None, None, "fsdp", "tensor"),
            P(None, "fsdp", "tensor"),
            P("group", None, None, "fsdp", "tensor"),
            P(None, None, "fsdp", "tensor"),
            P(None, "fsdp", "tensor"),
            P("group", None, None, None),
            P(),
            P(),
        ),
        check_vma=False,
    )
```

```python
import functools

import jax
import jax.numpy as jnp
from jax import lax
from jax.experimental import pallas as pl
from jax.experimental.pallas import tpu as pltpu
from jax.sharding import PartitionSpec as P

HD = 64
STEP = 8
IMG_DEV = 4
EPSILON = 1e-06
INNER_RATE = 0.02
VECTOR_RATE = 0.2
WEIGHT_DECAY = 0.1
OUTER_RATE = 0.7
OUTER_MOMENTUM = 0.9
PIECES = ((0, 256), (256, 256), (512, 512))
PARTS = 2
LOW = jnp.bfloat16
F32 = jnp.float32
NN = (((1,), (0,)), ((), ()))
NT = (((1,), (1,)), ((), ()))
TN = (((0,), (0,)), ((), ()))


def dot(a, b, dims=NN):
    return lax.dot_general(a, b, dims, preferred_element_type=F32)


MESH = pl.DeviceIdType.MESH


def params(identity=None):
    if identity is None:
        return pltpu.CompilerParams(vmem_limit_bytes=60 * 2**20)
    return pltpu.CompilerParams(vmem_limit_bytes=60 * 2**20, collective_id=identity, has_side_effects=True)


def partner():
    return (lax.axis_index("group"), 1 - lax.axis_index("fsdp"), lax.axis_index("tensor"))


def greet_partner():
    barrier = pltpu.get_barrier_semaphore()
    pl.semaphore_signal(barrier, inc=1, device_id=partner(), device_id_type=MESH)
    pl.semaphore_wait(barrier, 1)


def to_partner(sent, received, sends, receives, n):
    return pltpu.make_async_remote_copy(
        src_ref=sent.at[n],
        dst_ref=received.at[n],
        send_sem=sends.at[n],
        recv_sem=receives.at[n],
        device_id=partner(),
        device_id_type=MESH,
    )


def bands(depth):
    f = lax.axis_index("fsdp")
    return pl.ds(pl.multiple_of(f * depth, depth), depth), pl.ds(pl.multiple_of((1 - f) * depth, depth), depth)


def exchange_scratch(steps, shape):
    dma = pltpu.SemaphoreType.DMA
    return [
        pltpu.VMEM((steps, *shape), F32),
        pltpu.VMEM((steps, *shape), LOW),
        pltpu.VMEM((steps, *shape), LOW),
        dma((steps,)),
        dma((steps,)),
    ]


def cost(flops, moved, special=0):
    return pl.CostEstimate(flops=int(flops), bytes_accessed=int(moved), transcendentals=int(special))


def padded(rows):
    return -(-rows // 16) * 16


def centred(source):
    centre = source - jnp.mean(source, axis=-1, keepdims=True)
    spread = jnp.mean(centre * centre, axis=-1, keepdims=True)
    inverse = lax.rsqrt(spread + EPSILON)
    return centre * inverse, inverse


def norm_back(upstream, normal, inverse, gain):
    pulled = upstream * gain
    mean_one = jnp.mean(pulled, axis=-1, keepdims=True)
    mean_two = jnp.mean(pulled * normal, axis=-1, keepdims=True)
    return inverse * (pulled - mean_one - normal * mean_two)


def project_kernel(images, seq, x_ref, w_ref, vec_ref, n_ref, out_ref, n_scr):
    j, t = pl.program_id(0), pl.program_id(1)
    span = n_scr.shape[0] // images

    @pl.when((j == 0) & (t == 0))
    def _():
        n_scr[...] = jnp.zeros_like(n_scr)
        for i in range(images):
            normal, _ = centred(x_ref[i].astype(F32))
            n_scr[pl.ds(i * span, seq), :] = (normal * vec_ref[0:1] + vec_ref[1:2]).astype(LOW)
        n_ref[...] = n_scr[...]

    cols = out_ref.shape[-1]
    out = dot(n_scr[...], w_ref[0, 0])
    at = pl.ds(pl.multiple_of(t * cols, cols), cols)
    bias = jnp.where(j == 0, vec_ref[4:5, at], jnp.where(j == 2, vec_ref[5:6, at], 0.0))
    out_ref[0] = (out + bias).astype(LOW)


def project(patches, w_attn, vec):
    images, seq, width = patches.shape
    shards, _, _, cols = w_attn.shape
    rows = images * padded(seq)
    return pl.pallas_call(
        functools.partial(project_kernel, images, seq),
        grid=(3, shards),
        in_specs=[
            pl.BlockSpec((images, seq, width), lambda j, t: (0, 0, 0)),
            pl.BlockSpec((1, 1, width, cols), lambda j, t: (t, j, 0, 0)),
            pl.BlockSpec(vec.shape, lambda j, t: (0, 0)),
        ],
        out_specs=[
            pl.BlockSpec((rows, width), lambda j, t: (0, 0)),
            pl.BlockSpec((1, rows, cols), lambda j, t: (j, 0, t)),
        ],
        out_shape=[
            jax.ShapeDtypeStruct((rows, width), LOW),
            jax.ShapeDtypeStruct((3, rows, width), LOW),
        ],
        scratch_shapes=[pltpu.VMEM((rows, width), LOW)],
        compiler_params=params(),
        cost_estimate=cost(6 * rows * width * width, 16 * rows * width),
        name="project",
    )(patches, w_attn, vec)


def half_lanes(value, which):
    lane = lax.broadcasted_iota(jnp.int32, value.shape, 1)
    return jnp.where((lane >= HD) == bool(which), value, jnp.zeros_like(value))


def attend_kernel(seq, q_ref, k_ref, v_ref, out_ref):
    span = q_ref.shape[1]
    scale = HD**-0.5
    q, k, v = q_ref[0], k_ref[0], v_ref[0]
    parts = []
    for h in range(2):
        scores = dot(q, half_lanes(k, h), NT)
        lane = lax.broadcasted_iota(jnp.int32, scores.shape, 1)
        scores = jnp.where(lane < seq, scores, -1e30)
        top = jnp.max(scores, axis=1, keepdims=True)
        raised = jnp.exp((scores - top) * scale)
        total = jnp.sum(raised, axis=1, keepdims=True)
        probs = (raised * (1.0 / total)).astype(LOW)
        parts.append(dot(probs, v))
    lane = lax.broadcasted_iota(jnp.int32, (span, 2 * HD), 1)
    out_ref[...] = jnp.where(lane < HD, parts[0], parts[1]).astype(LOW)


def attend(qkv, images, seq):
    _, rows, width = qkv.shape
    span = rows // images
    pair = 2 * HD

    def take(j):
        return pl.BlockSpec((1, span, pair), lambda i, h: (j, i, h))

    return pl.pallas_call(
        functools.partial(attend_kernel, seq),
        grid=(images, width // pair),
        in_specs=[take(0), take(1), take(2)],
        out_specs=pl.BlockSpec((span, pair), lambda i, h: (i, h)),
        out_shape=jax.ShapeDtypeStruct((rows, width), LOW),
        compiler_params=params(),
        cost_estimate=cost(16 * rows * span * width, 8 * rows * width, rows * span * (width // HD)),
        name="attend",
    )(qkv, qkv, qkv)


def mix_kernel(seq, alive_ref, att_ref, x_ref, g_ref, w_ref, vec_ref, resid_ref, n_ref, g2_ref, x_scr):
    i = pl.program_id(0)
    shards, _, _, cols = w_ref.shape
    x_scr[...] = jnp.zeros_like(x_scr)
    x_scr[0:seq, :] = x_ref[0].astype(F32)
    total = x_scr[...] + vec_ref[6:7]
    for t in range(shards):
        total = total + dot(att_ref[:, t * cols : (t + 1) * cols], w_ref[t, 0], NT)
    resid_ref[...] = total
    normal, _ = centred(total)
    n_ref[...] = (normal * vec_ref[2:3] + vec_ref[3:4]).astype(LOW)
    x_scr[0:seq, :] = g_ref[0].astype(F32) * alive_ref[i]
    g2_ref[...] = x_scr[...].astype(LOW)


def mix(alive, attended, patches, cotangent, w_attn, vec):
    images, seq, width = patches.shape
    rows = attended.shape[0]
    span = rows // images
    shards, _, _, cols = w_attn.shape
    block = pl.BlockSpec((span, width), lambda i: (i, 0))
    whole = jax.ShapeDtypeStruct((rows, width), LOW)
    return pl.pallas_call(
        functools.partial(mix_kernel, seq),
        grid=(images,),
        in_specs=[
            pl.BlockSpec(memory_space=pltpu.SMEM),
            block,
            pl.BlockSpec((1, seq, width), lambda i: (i, 0, 0)),
            pl.BlockSpec((1, seq, width), lambda i: (i, 0, 0)),
            pl.BlockSpec((shards, 1, width, cols), lambda i: (0, 3, 0, 0)),
            pl.BlockSpec(vec.shape, lambda i: (0, 0)),
        ],
        out_specs=[block, block, block],
        out_shape=[jax.ShapeDtypeStruct((rows, width), F32), whole, whole],
        scratch_shapes=[pltpu.VMEM((span, width), F32)],
        compiler_params=params(),
        cost_estimate=cost(2 * rows * width * width, 16 * rows * width),
        name="mix",
    )(alive, attended, patches, cotangent, w_attn, vec)


def mlp_kernel(first, pairwise, n_ref, g_ref, w1_ref, w2_ref, bias_ref, *refs):
    if not first:
        yi_ref, gi_ref, *refs = refs
    y_ref, gn_ref, dw_ref, db_ref, h_scr, p_scr, loaded, *exchange = refs
    step = pl.program_id(0)
    each, _, width, cols = w1_ref.shape
    if not first:
        loads = (
            pltpu.make_async_copy(yi_ref, y_ref, loaded.at[0]),
            pltpu.make_async_copy(gi_ref, gn_ref, loaded.at[1]),
        )

    @pl.when(step == 0)
    def _():
        if not first:
            for load in loads:
                load.start()
        else:
            y_ref[...] = jnp.zeros_like(y_ref)
            gn_ref[...] = jnp.zeros_like(gn_ref)
        if pairwise:
            greet_partner()

    w1 = jnp.concatenate([w1_ref[t, 0] for t in range(each)], axis=1)
    w2 = jnp.concatenate([w2_ref[t, 0] for t in range(each)], axis=1)
    bias = jnp.concatenate([bias_ref[t] for t in range(each)], axis=1)
    pre = dot(n_ref[...], w1) + bias
    cdf = 0.5 * (1.0 + lax.erf(pre * 0.7071067811865476))
    h_scr[...] = (pre * cdf).astype(LOW)
    slope = cdf + pre * jnp.exp(-0.5 * pre * pre) * 0.3989422804014327
    p_scr[...] = (dot(g_ref[...], w2) * slope).astype(LOW)
    sums = jnp.sum(p_scr[...].astype(F32), axis=0, keepdims=True)
    for t in range(each):
        db_ref[t] = sums[:, t * cols : (t + 1) * cols]

    if pairwise:
        own, sent, received, sends, receives = exchange
        ours, theirs = bands(width // 2)

        slot = lax.rem(step, 2)

        def collect(n):
            at = lax.rem(n, 2)
            to_partner(sent, received, sends, receives, at).wait()
            for which in range(2):
                total = (own[at, which] + received[at, which].astype(F32)).astype(LOW)
                for t in range(each):
                    dw_ref[n * each + t, which] = total[:, t * cols : (t + 1) * cols]

        @pl.when(step > 0)
        def _():
            collect(step - 1)

        sent[slot, 0] = dot(n_ref[:, theirs], p_scr[...], TN).astype(LOW)
        sent[slot, 1] = dot(g_ref[:, theirs], h_scr[...], TN).astype(LOW)
        to_partner(sent, received, sends, receives, slot).start()
        own[slot, 0] = dot(n_ref[:, ours], p_scr[...], TN)
        own[slot, 1] = dot(g_ref[:, ours], h_scr[...], TN)

    else:
        shards, depth = dw_ref.shape[0], dw_ref.shape[3]
        d1 = dot(n_ref[...], p_scr[...], TN).astype(LOW)
        d2 = dot(g_ref[...], h_scr[...], TN).astype(LOW)
        for f in range(shards):
            for t in range(each):
                dw_ref[f, t, 0] = d1[f * depth : (f + 1) * depth, t * cols : (t + 1) * cols]
                dw_ref[f, t, 1] = d2[f * depth : (f + 1) * depth, t * cols : (t + 1) * cols]

    if not first:

        @pl.when(step == 0)
        def _():
            for load in loads:
                load.wait()

    y_ref[...] += dot(h_scr[...], w2, NT)
    gn_ref[...] += dot(p_scr[...], w1, NT)
    if pairwise:

        @pl.when(step == pl.num_programs(0) - 1)
        def _():
            collect(step)


def mlp(part, start, cols, normed, grad_two, w_mlp, bias, carried, fsdp):
    rows, width = normed.shape
    shards = w_mlp.shape[0]
    each = max(512 // cols, 1)
    at = start // cols
    first, pairwise = carried is None, fsdp == 2
    single = pl.Buffered(1)
    full = pl.BlockSpec((rows, width), lambda s: (0, 0), pipeline_mode=single)
    depth = width // fsdp
    steps = shards // each
    acc_shape = jax.ShapeDtypeStruct((rows, width), F32)
    if pairwise:
        out_w = pl.BlockSpec((shards, 2, depth, cols), lambda s: (0, 0, 0, 0), pipeline_mode=single)
        w_shape = jax.ShapeDtypeStruct((shards, 2, depth, cols), LOW)
        extra = exchange_scratch(2, (2, depth, each * cols))
    else:
        out_w = pl.BlockSpec((fsdp, each, 2, depth, cols), lambda s: (0, s, 0, 0, 0))
        w_shape = jax.ShapeDtypeStruct((fsdp, shards, 2, depth, cols), LOW)
        extra = []
    return pl.pallas_call(
        functools.partial(mlp_kernel, first, pairwise),
        grid=(steps,),
        in_specs=[
            full,
            full,
            pl.BlockSpec((each, 1, width, cols), lambda s: (s, 0, 0, at)),
            pl.BlockSpec((each, 1, width, cols), lambda s: (s, 1, 0, at)),
            pl.BlockSpec((each, 1, cols), lambda s: (s, 0, at)),
        ]
        + ([] if first else [pl.BlockSpec(memory_space=pl.ANY)] * 2),
        out_specs=[full, full, out_w, pl.BlockSpec((each, 1, cols), lambda s: (s, 0, 0))],
        out_shape=[acc_shape, acc_shape, w_shape, jax.ShapeDtypeStruct((shards, 1, cols), F32)],
        scratch_shapes=[
            pltpu.VMEM((rows, each * cols), LOW),
            pltpu.VMEM((rows, each * cols), LOW),
            pltpu.SemaphoreType.DMA((2,)),
            *extra,
        ],
        compiler_params=params(2 + part if pairwise else None),
        cost_estimate=cost(12 * rows * width * cols * shards, 24 * rows * width),
        name=f"mlp_{part}",
    )(normed, grad_two, w_mlp, w_mlp, bias, *([] if first else carried))


def turn_kernel(seq, pairwise, alive_ref, resid_ref, y_ref, gn_ref, g2_ref, att_ref, w_ref, vec_ref,
                out_ref, gr_ref, ga_ref, dw_ref, sums_ref, dw_scr, *exchange):
    i = pl.program_id(0)
    if pairwise:
        pl.when(i == 0)(greet_partner)
    shards, _, _, cols = w_ref.shape
    resid = resid_ref[...]
    out_ref[0] = ((resid + y_ref[...] + vec_ref[7:8]) * alive_ref[i]).astype(LOW)[0:seq]
    normal, inverse = centred(resid)
    upstream = gn_ref[...]
    grad_out = g2_ref[...].astype(F32)
    grad_resid = grad_out + norm_back(upstream, normal, inverse, vec_ref[2:3])
    gr_ref[...] = grad_resid
    low = grad_resid.astype(LOW)
    rows = [
        jnp.sum(upstream * normal, axis=0, keepdims=True),
        jnp.sum(upstream, axis=0, keepdims=True),
        jnp.sum(grad_resid, axis=0, keepdims=True),
        jnp.sum(grad_out, axis=0, keepdims=True),
    ]
    rows = jnp.concatenate(rows, axis=0)

    @pl.when(i == 0)
    def _():
        sums_ref[...] = rows

    @pl.when(i != 0)
    def _():
        sums_ref[...] += rows

    for t in range(shards):
        ga_ref[:, t * cols : (t + 1) * cols] = dot(low, w_ref[t, 0]).astype(LOW)
    part = dot(low, att_ref[...], TN)

    @pl.when(i == 0)
    def _():
        dw_scr[...] = part

    @pl.when(i != 0)
    def _():
        dw_scr[...] += part

    @pl.when(i == pl.num_programs(0) - 1)
    def _():
        if pairwise:
            sent, received, sends, receives = exchange
            ours, theirs = bands(dw_scr.shape[0] // 2)
            sent[0] = dw_scr[theirs, :].astype(LOW)
            copy = to_partner(sent, received, sends, receives, 0)
            copy.start()
            copy.wait()
            total = (dw_scr[ours, :] + received[0].astype(F32)).astype(LOW)
            for t in range(shards):
                dw_ref[t, 0] = total[:, t * cols : (t + 1) * cols]
            return
        depth = dw_ref.shape[3]
        for f in range(dw_ref.shape[0]):
            for t in range(shards):
                dw_ref[f, t, 0] = dw_scr[f * depth : (f + 1) * depth, t * cols : (t + 1) * cols].astype(LOW)


def turn(alive, resid, branch, grad_normed, grad_two, attended, w_attn, vec, images, seq, fsdp):
    rows, width = resid.shape
    span = rows // images
    shards, _, _, cols = w_attn.shape
    depth = width // fsdp
    pairwise = fsdp == 2
    lead = () if pairwise else (fsdp,)
    block = pl.BlockSpec((span, width), lambda i: (i, 0))
    return pl.pallas_call(
        functools.partial(turn_kernel, seq, pairwise),
        grid=(images,),
        in_specs=[
            pl.BlockSpec(memory_space=pltpu.SMEM),
            block, block, block, block, block,
            pl.BlockSpec((shards, 1, width, cols), lambda i: (0, 3, 0, 0)),
            pl.BlockSpec(vec.shape, lambda i: (0, 0)),
        ],
        out_specs=[
            pl.BlockSpec((1, seq, width), lambda i: (i, 0, 0)),
            block, block,
            pl.BlockSpec((*lead, shards, 1, depth, cols), lambda i: (0,) * (4 + len(lead))),
            pl.BlockSpec((4, width), lambda i: (0, 0)),
        ],
        out_shape=[
            jax.ShapeDtypeStruct((images, seq, width), LOW),
            jax.ShapeDtypeStruct((rows, width), F32),
            jax.ShapeDtypeStruct((rows, width), LOW),
            jax.ShapeDtypeStruct((*lead, shards, 1, depth, cols), LOW),
            jax.ShapeDtypeStruct((4, width), F32),
        ],
        scratch_shapes=[pltpu.VMEM((width, width), F32)] + (exchange_scratch(1, (depth, width))[1:] if pairwise else []),
        compiler_params=params(6 if pairwise else None),
        cost_estimate=cost(4 * rows * width * width, 24 * rows * width),
        name="turn",
    )(alive, resid, branch, grad_normed, grad_two, attended, w_attn, vec)


def unattend_kernel(seq, q_ref, k_ref, v_ref, g_ref, out_ref):
    span = q_ref.shape[1]
    scale = HD**-0.5
    q, k, v, g = q_ref[0], k_ref[0], v_ref[0], g_ref[...]
    parts = []
    for h in range(2):
        scores = dot(half_lanes(k, h), q, NT)
        row = lax.broadcasted_iota(jnp.int32, scores.shape, 0)
        scores = jnp.where(row < seq, scores, -1e30)
        top = jnp.max(scores, axis=0, keepdims=True)
        raised = jnp.exp((scores - top) * scale)
        total = jnp.sum(raised, axis=0, keepdims=True)
        probs = raised * (1.0 / total)
        gp = dot(half_lanes(v, h), g, NT)
        delta = jnp.sum(probs * gp, axis=0, keepdims=True)
        gs = (probs * (gp - delta)).astype(LOW)
        dv = dot(probs.astype(LOW), g)
        dk = dot(gs, q)
        dq = dot(gs, k, TN)
        parts.append((dq, dk, dv))
    lane = lax.broadcasted_iota(jnp.int32, (span, 2 * HD), 1) < HD
    out_ref[0] = (jnp.where(lane, parts[0][0], parts[1][0]) * scale).astype(LOW)
    out_ref[1] = (jnp.where(lane, parts[0][1], parts[1][1]) * scale).astype(LOW)
    out_ref[2] = jnp.where(lane, parts[0][2], parts[1][2]).astype(LOW)


def unattend(qkv, grad_attended, images, seq, part, parts, shards):
    _, rows, width = qkv.shape
    span = rows // images
    pair = 2 * HD
    each = width // shards // parts // pair

    def spot(h):
        return (h // each) * (each * parts) + part * each + h % each

    def take(j):
        return pl.BlockSpec((1, span, pair), lambda i, h: (j, i, spot(h)))

    return pl.pallas_call(
        functools.partial(unattend_kernel, seq),
        grid=(images, width // pair // parts),
        in_specs=[take(0), take(1), take(2), pl.BlockSpec((span, pair), lambda i, h: (i, spot(h)))],
        out_specs=pl.BlockSpec((3, span, pair), lambda i, h: (0, i, h)),
        out_shape=jax.ShapeDtypeStruct((3, rows, width // parts), LOW),
        compiler_params=params(),
        cost_estimate=cost(
            40 * rows * span * width // parts, 14 * rows * width // parts, rows * span * (width // HD) // parts
        ),
        name=f"unattend_{part}",
    )(qkv, qkv, qkv, grad_attended)


def close_kernel(seq, images, pairwise, groups, first, final, n_ref, grad_ref, w_ref, *refs):
    if not first:
        carry_ref, *refs = refs
    elif pairwise:
        more_ref, *refs = refs
    if final:
        x_ref, gr_ref, vec_ref, *refs = refs
        if pairwise:
            diff_ref, *refs = refs
        out_ref, norm_ref, *refs = refs
        if pairwise:
            total_ref, *refs = refs
    else:
        acc_ref, *refs = refs
    dw_ref, sums_ref, acc_scr, *exchange = refs
    j = pl.program_id(0)
    shards, _, _, cols = w_ref.shape
    span = n_ref.shape[0] // images
    if pairwise:
        own, sent, received, sends, receives, *exchange = exchange
        if not final:
            pl.when(j == 0)(greet_partner)
    if pairwise and final:
        mine, landed, sends_two, receives_two, loaded = exchange
        g, f, t = lax.axis_index("group"), lax.axis_index("fsdp"), lax.axis_index("tensor")
        quarter = landed.shape[1]

        def rows(n):
            return pl.ds(pl.multiple_of(n * quarter, quarter), quarter)

        def other(k):
            return (lax.rem(g + k, groups), f, t)

        def part(k):
            return pltpu.make_async_remote_copy(
                src_ref=diff_ref.at[rows(lax.rem(g + k, groups)), :],
                dst_ref=landed.at[k],
                send_sem=sends_two.at[k],
                recv_sem=receives_two.at[k],
                device_id=other(k),
                device_id_type=MESH,
            )

        keep = pltpu.make_async_copy(diff_ref.at[rows(g), :], mine, loaded.at[0])

        @pl.when(j == 0)
        def _():
            barrier = pltpu.get_barrier_semaphore()
            pl.semaphore_signal(barrier, inc=1, device_id=partner(), device_id_type=MESH)
            for k in range(1, groups):
                pl.semaphore_signal(barrier, inc=1, device_id=other(k), device_id_type=MESH)
            pl.semaphore_wait(barrier, groups)
            for k in range(1, groups):
                part(k).start()
            keep.start()

    @pl.when(j == 0)
    def _():
        acc_scr[...] = jnp.zeros_like(acc_scr) if first else carry_ref[...]

    sums = jnp.sum(grad_ref[0].astype(F32), axis=0, keepdims=True)
    for n, matrix in enumerate((0, 2)):

        @pl.when(j == matrix)
        def _():
            sums_ref[n : n + 1, :] = sums

    def spread(n, total, f=None):
        for t in range(shards):
            piece = total[:, t * cols : (t + 1) * cols]
            if f is None:
                dw_ref[t, n] = piece
            else:
                dw_ref[f, t, 0] = piece

    weight = jnp.concatenate([w_ref[t, 0] for t in range(shards)], axis=1)
    if pairwise:
        ours, theirs = bands(n_ref.shape[1] // 2)
        sent[j] = dot(n_ref[:, theirs], grad_ref[0], TN).astype(LOW)
        to_partner(sent, received, sends, receives, j).start()
        own[j] = dot(n_ref[:, ours], grad_ref[0], TN)
    else:
        depth = dw_ref.shape[3]
        dw = dot(n_ref[...], grad_ref[0], TN).astype(LOW)
        for f in range(dw_ref.shape[0]):
            spread(0, dw[f * depth : (f + 1) * depth], f)
    acc_scr[...] += dot(grad_ref[0], weight, NT)

    @pl.when(j == 2)
    def _():
        if pairwise:
            for n in range(own.shape[0]):
                to_partner(sent, received, sends, receives, n).wait()
                spread(n, (own[n] + received[n].astype(F32)).astype(LOW))
            if first:
                for t in range(shards):
                    for n in range(dw_ref.shape[1] - 3):
                        dw_ref[t, 3 + n] = more_ref[t, 0, :, n * cols : (n + 1) * cols]
        if not final:
            acc_ref[...] = acc_scr[...]
            return
        gain = jnp.zeros((1, vec_ref.shape[1]), F32)
        shift = jnp.zeros((1, vec_ref.shape[1]), F32)
        for i in range(images):
            normal, inverse = centred(x_ref[i].astype(F32))
            upstream = acc_scr[i * span : i * span + seq, :]
            out_ref[i, :, 0, :] = gr_ref[i * span : i * span + seq, :] + norm_back(upstream, normal, inverse, vec_ref[0:1])
            gain += jnp.sum(upstream * normal, axis=0, keepdims=True)
            shift += jnp.sum(upstream, axis=0, keepdims=True)
        norm_ref[0:1, :] = gain
        norm_ref[1:2, :] = shift
        if pairwise:
            keep.wait()
            total = mine[...].astype(F32)
            for k in range(1, groups):
                part(k).wait()
                total = total + landed[k].astype(F32)
            total_ref[...] = total.astype(LOW)


def close(part, parts, normed, grads, w_attn, carry, more, ending, fsdp, groups, images, seq):
    rows, width = normed.shape
    shards, _, _, cols = w_attn.shape
    cols = cols // parts
    lanes = shards * cols
    depth = width // fsdp
    pairwise, first, final = fsdp == 2, carry is None, ending is not None
    single = pl.Buffered(1)
    stack = pl.BlockSpec((1, rows, lanes), lambda j: (j, 0, 0))
    full = pl.BlockSpec((rows, width), lambda j: (0, 0), pipeline_mode=single)
    image = pl.BlockSpec((images, seq, width), lambda j: (0, 0, 0), pipeline_mode=single)
    if pairwise:
        many = 3 + parts if first else 3
        dw_spec = pl.BlockSpec((shards, many, depth, cols), lambda j: (0, 0, 0, 0), pipeline_mode=single)
        dw_shape = jax.ShapeDtypeStruct((shards, many, depth, cols), LOW)
        extra = exchange_scratch(3, (depth, lanes))
    else:
        dw_spec = pl.BlockSpec((fsdp, shards, 1, depth, cols), lambda j: (0, 0, j, 0, 0))
        dw_shape = jax.ShapeDtypeStruct((fsdp, shards, 3, depth, cols), LOW)
        extra = []
    in_specs = [full, stack, pl.BlockSpec((shards, 1, width, cols), lambda j: (0, j, 0, part))]
    out_specs, out_shape = [], []
    if not first:
        in_specs.append(full)
    elif pairwise:
        in_specs.append(pl.BlockSpec(more.shape, lambda j: (0, 0, 0, 0), pipeline_mode=single))
    if final:
        in_specs += [image, full, pl.BlockSpec((12, width), lambda j: (0, 0))]
        flat = pl.BlockSpec((images, seq, 1, width), lambda j: (0, 0, 0, 0), pipeline_mode=single)
        out_specs += [flat, pl.BlockSpec((2, width), lambda j: (0, 0))]
        out_shape += [jax.ShapeDtypeStruct((images, seq, 1, width), F32), jax.ShapeDtypeStruct((2, width), F32)]
        if pairwise:
            quarter, lanes_two = ending[3].shape[0] // groups, ending[3].shape[1]
            in_specs.append(pl.BlockSpec(memory_space=pl.ANY))
            out_specs.append(pl.BlockSpec((quarter, lanes_two), lambda j: (0, 0), pipeline_mode=single))
            out_shape.append(jax.ShapeDtypeStruct((quarter, lanes_two), LOW))
            dma = pltpu.SemaphoreType.DMA
            extra = [
                *extra,
                pltpu.VMEM((quarter, lanes_two), LOW),
                pltpu.VMEM((groups, quarter, lanes_two), LOW),
                dma((groups,)),
                dma((groups,)),
                dma((1,)),
            ]
    else:
        out_specs.append(full)
        out_shape.append(jax.ShapeDtypeStruct((rows, width), F32))
    return pl.pallas_call(
        functools.partial(close_kernel, seq, images, pairwise, groups, first, final),
        grid=(3,),
        in_specs=in_specs,
        out_specs=[*out_specs, dw_spec, pl.BlockSpec((2, lanes), lambda j: (0, 0))],
        out_shape=[*out_shape, dw_shape, jax.ShapeDtypeStruct((2, lanes), F32)],
        scratch_shapes=[pltpu.VMEM((rows, width), F32), *extra],
        compiler_params=params(7 + part if pairwise else None),
        cost_estimate=cost(12 * rows * width * lanes, 20 * rows * width),
        name=f"close_{part}",
    )(normed, grads, w_attn, *([carry] if not first else [more] if pairwise else []), *(ending if final else []))


def attend_pair(seq, q, k, v):
    scale = HD**-0.5
    parts = []
    for h in range(2):
        scores = dot(q, half_lanes(k, h), NT)
        lane = lax.broadcasted_iota(jnp.int32, scores.shape, 1)
        scores = jnp.where(lane < seq, scores, -1e30)
        top = jnp.max(scores, axis=1, keepdims=True)
        raised = jnp.exp((scores - top) * scale)
        total = jnp.sum(raised, axis=1, keepdims=True)
        probs = (raised * (1.0 / total)).astype(LOW)
        parts.append(dot(probs, v))
    lane = lax.broadcasted_iota(jnp.int32, parts[0].shape, 1)
    return jnp.where(lane < HD, parts[0], parts[1]).astype(LOW)


def front_kernel(
    images, seq, alive_ref, a_in, m_in, x_ref, g_ref, vec_ref,
    a_out, m_out, n_out, qkv_out, att_out, resid_out, n2_out, g2_out,
    a_wide, m_wide, a_hold, m_hold, n_scr, qkv_scr, att_scr, w_scr, o_scr, x_scr, resid_scr, n2_scr, g2_scr,
    zs, zr, xs, xr, ys, yr, xfs, xfr, yfs, yfr, cs, cr, ls, ws,
):
    g, f, z = lax.axis_index("group"), lax.axis_index("fsdp"), lax.axis_index("tensor")
    shards = lax.axis_size("tensor")
    last = shards - 1
    x_at, y_at = g % 2, g // 2
    east, north = y_at * 2 + (1 - x_at), (1 - y_at) * 2 + x_at
    depth, cols = a_in.shape[1:]
    band = depth // 4
    shared = band * 3 // 8
    rest = band - 2 * shared
    span = n_scr.shape[0] // images

    def place(column):
        cx, cy = column % 2, column // 2
        return 2 * (cx + cy - 2 * cx * cy) + cy

    mine, of_east, of_north = place(g), place(east), place(north)
    z_row = mine * band - shared * (mine % 2)
    lead_east = of_east * band + shared * (of_east % 2)
    lead_north = of_north * band + shared * (of_north % 2)
    chunks = ((a_out, 0, 3), (a_out, 3, 1), (m_out, 0, 1), (m_out, 1, 1))

    def tile(n):
        return pl.multiple_of(n, 16)

    def held(n, t, row, rows):
        out, j, many = chunks[n]
        return out.at[t, pl.ds(j, many), pl.ds(tile(f * depth + row), rows), :]

    def send(part, sems, semr, n, t, to):
        return pltpu.make_async_remote_copy(
            src_ref=part, dst_ref=part, send_sem=sems.at[n, t], recv_sem=semr.at[n, t], device_id=to, device_id_type=MESH
        )

    def along(n, t, up):
        part = held(n, t, z_row, band + shared)
        return pltpu.make_async_remote_copy(
            src_ref=part,
            dst_ref=part,
            send_sem=zs.at[n, t, 0 if up else 1],
            recv_sem=zr.at[n, t],
            device_id=(g, f, z + 1 if up else z - 1),
            device_id_type=MESH,
        )

    def to_east(n, t):
        return send(held(n, t, mine * band, band), xs, xr, n, t, (east, f, z))

    def to_north(n, t):
        return send(held(n, t, mine * band, band), ys, yr, n, t, (north, f, z))

    def north_to_east(n, t):
        return send(held(n, t, lead_north, shared), xfs, xfr, n, t, (east, f, z))

    def east_to_north(n, t):
        return send(held(n, t, lead_east + shared, rest), yfs, yfr, n, t, (north, f, z))

    def across(n, t):
        return send(held(n, t, 0, depth), cs, cr, n, t, (g, 1 - f, z))

    rows = pl.ds(tile(f * depth), depth)
    loads = (
        pltpu.make_async_copy(a_in, a_wide, ls.at[0]),
        pltpu.make_async_copy(m_in, m_wide, ls.at[1]),
    )
    keeps = (
        pltpu.make_async_copy(a_hold, a_out.at[z, :, rows, :], ls.at[2]),
        pltpu.make_async_copy(m_hold, m_out.at[z, :, rows, :], ls.at[3]),
    )
    loads[0].start()

    barrier = pltpu.get_barrier_semaphore()

    def greet(to):
        pl.semaphore_signal(barrier, inc=1, device_id=to, device_id_type=MESH)

    for to in ((east, f, z), (north, f, z), (g, 1 - f, z)):
        greet(to)

    @pl.when(z > 0)
    def _():
        greet((g, f, z - 1))

    @pl.when(z < last)
    def _():
        greet((g, f, z + 1))

    loads[0].wait()
    a_hold[...] = a_wide[...].astype(LOW)
    keeps[0].start()
    pl.semaphore_wait(barrier, 3 + jnp.minimum(z, 1) + jnp.minimum(last - z, 1))
    keeps[0].wait()

    count = len(chunks)

    def when_real(k, up, run):
        @pl.when(z - k >= 0 if up else z + k <= last)
        def _():
            run(z - k if up else z + k)

    def own(n):
        @pl.when(z < last)
        def _():
            along(n, z, True).start()

        @pl.when(z > 0)
        def _():
            along(n, z, False).start()

        across(n, z).start()

    def land(n, k, up):
        def run(t):
            along(n, t, up).wait_recv()

            @pl.when(z < last if up else z > 0)
            def _():
                along(n, t, up).start()

            to_east(n, t).start()
            to_north(n, t).start()

        when_real(k, up, run)

    def relay(n, k, up):
        def run(t):
            to_east(n, t).wait_recv()
            east_to_north(n, t).start()
            to_north(n, t).wait_recv()
            north_to_east(n, t).start()

        when_real(k, up, run)

    def finish(n, k, up):
        def run(t):
            east_to_north(n, t).wait_recv()
            north_to_east(n, t).wait_recv()
            across(n, t).start()

        when_real(k, up, run)

    def both(run, n, k):
        for up in (True, False):
            run(n, k, up)

    def fetch(t):
        return pltpu.make_async_copy(a_out.at[t, pl.ds(0, 3)], w_scr, ws.at[0])

    def maps(t):
        across(0, t).wait_recv()
        fetch(t).start()
        fetch(t).wait()
        here = pl.ds(pl.multiple_of(t * cols, cols), cols)

        def body(j, carry):
            bias = jnp.where(j == 0, vec_ref[4:5, here], jnp.where(j == 2, vec_ref[5:6, here], 0.0))
            qkv_scr[j, :, here] = (dot(n_scr[...], w_scr[j]) + bias).astype(LOW)
            return carry

        lax.fori_loop(0, 3, body, 0)

    def project(k):
        def body(d, carry):
            t = z - k + 2 * k * d

            @pl.when((t >= 0) & (t <= last))
            def _():
                maps(t)

            return carry

        lax.fori_loop(0, 2, body, 0)

    own(0)
    loads[1].start()
    n_scr[...] = jnp.zeros_like(n_scr)

    def norm_image(i, carry):
        normal, _ = centred(x_ref[i].astype(F32))
        n_scr[pl.ds(pl.multiple_of(i * span, 16), seq), :] = (normal * vec_ref[0:1] + vec_ref[1:2]).astype(LOW)
        return carry

    lax.fori_loop(0, images, norm_image, 0)
    puts = [pltpu.make_async_copy(n_scr, n_out, ws.at[1])]
    puts[0].start()
    both(land, 0, 1)
    loads[1].wait()
    m_hold[...] = m_wide[...].astype(LOW)
    keeps[1].start()
    maps(z)
    both(land, 0, 2)
    both(relay, 0, 1)
    keeps[1].wait()
    both(land, 0, 3)
    for n in range(1, count):
        own(n)
    both(relay, 0, 2)
    both(finish, 0, 1)
    both(relay, 0, 3)
    both(finish, 0, 2)
    project(1)
    both(finish, 0, 3)
    project(2)

    rest_items = [(n, k) for k in range(1, last + 1) for n in range(1, count)]
    total = len(rest_items) + 2

    def advance(at):
        if at < len(rest_items):
            both(land, *rest_items[at])
        if 0 <= at - 1 < len(rest_items):
            both(relay, *rest_items[at - 1])
        if 0 <= at - 2 < len(rest_items):
            both(finish, *rest_items[at - 2])

    advance(0)
    project(3)
    puts.append(pltpu.make_async_copy(qkv_scr, qkv_out, ws.at[2]))
    puts[-1].start()

    pair = 2 * HD
    pairs = qkv_scr.shape[2] // pair
    stretch = max(pairs // 4, 1)
    segments = images * pairs // stretch

    def segment(n, carry):
        def body(m, carry):
            at = n * stretch + m
            lanes = pl.ds(pl.multiple_of(lax.rem(at, pairs) * pair, pair), pair)
            here = pl.ds(pl.multiple_of(at // pairs * span, 16), span)
            att_scr[here, lanes] = attend_pair(
                seq, qkv_scr[0, here, lanes], qkv_scr[1, here, lanes], qkv_scr[2, here, lanes]
            )
            return carry

        lax.fori_loop(0, stretch, body, 0)
        for c in range(min(segments, total - 3)):
            pl.when(n == c)(functools.partial(advance, 1 + c))
        return carry

    lax.fori_loop(0, segments, segment, 0)
    at = 1 + min(segments, total - 3)
    puts.append(pltpu.make_async_copy(att_scr, att_out, ws.at[3]))
    puts[-1].start()
    while at < total - 2:
        advance(at)
        at += 1

    for t in range(shards):
        across(1, t).wait_recv()
    take = pltpu.make_async_copy(a_out.at[:, 3], o_scr, ws.at[0])
    take.start()
    take.wait()
    x_scr[...] = jnp.zeros_like(x_scr)

    def mix_image(i, carry):
        here = pl.ds(pl.multiple_of(i * span, 16), span)
        x_scr[0:seq, :] = x_ref[i].astype(F32)
        out = x_scr[...] + vec_ref[6:7]
        for t in range(shards):
            out = out + dot(att_scr[here, t * cols : (t + 1) * cols], o_scr[t], NT)
        resid_scr[here, :] = out
        normal, _ = centred(out)
        n2_scr[here, :] = (normal * vec_ref[2:3] + vec_ref[3:4]).astype(LOW)
        x_scr[0:seq, :] = g_ref[i].astype(F32) * alive_ref[i]
        g2_scr[here, :] = x_scr[...].astype(LOW)
        for c in range(min(images, total - at)):
            pl.when(i == c)(functools.partial(advance, at + c))
        return carry

    lax.fori_loop(0, images, mix_image, 0)
    at += min(images, total - at)
    for n, (src, dst) in enumerate(((resid_scr, resid_out), (n2_scr, n2_out), (g2_scr, g2_out))):
        puts.append(pltpu.make_async_copy(src, dst, ws.at[4 + n]))
        puts[-1].start()
    while at < total:
        advance(at)
        at += 1
    for put in puts:
        put.wait()

    for n in range(count):
        @pl.when(z < last)
        def _():
            along(n, z, True).wait_send()

        @pl.when(z > 0)
        def _():
            along(n, z, False).wait_send()

        for t in range(shards):
            across(n, t).wait_send()
            if n > 1:
                across(n, t).wait_recv()

    def settle(n, k, up):
        def run(t):
            @pl.when(z < last if up else z > 0)
            def _():
                along(n, t, up).wait_send()

            to_east(n, t).wait_send()
            to_north(n, t).wait_send()
            east_to_north(n, t).wait_send()
            north_to_east(n, t).wait_send()

        when_real(k, up, run)

    for n in range(count):
        for k in range(1, last + 1):
            both(settle, n, k)


def front(alive, attn_master, mlp_master, patches, cotangent, vec, shards):
    _, depth, a_cols = attn_master.shape
    _, _, m_cols = mlp_master.shape
    images, seq, width = patches.shape
    rows = images * padded(seq)
    anywhere = pl.BlockSpec(memory_space=pl.ANY)
    inside = pl.BlockSpec(memory_space=pltpu.VMEM)
    dma = pltpu.SemaphoreType.DMA
    low = jax.ShapeDtypeStruct((rows, width), LOW)
    return pl.pallas_call(
        functools.partial(front_kernel, images, seq),
        in_specs=[pl.BlockSpec(memory_space=pltpu.SMEM), anywhere, anywhere, inside, inside, inside],
        out_specs=[anywhere] * 8,
        out_shape=[
            jax.ShapeDtypeStruct((shards, 4, width, a_cols), LOW),
            jax.ShapeDtypeStruct((shards, 2, width, m_cols), LOW),
            low,
            jax.ShapeDtypeStruct((3, rows, width), LOW),
            low,
            jax.ShapeDtypeStruct((rows, width), F32),
            low,
            low,
        ],
        scratch_shapes=[
            pltpu.VMEM(attn_master.shape, F32),
            pltpu.VMEM(mlp_master.shape, F32),
            pltpu.VMEM(attn_master.shape, LOW),
            pltpu.VMEM(mlp_master.shape, LOW),
            pltpu.VMEM((rows, width), LOW),
            pltpu.VMEM((3, rows, width), LOW),
            pltpu.VMEM((rows, width), LOW),
            pltpu.VMEM((3, width, a_cols), LOW),
            pltpu.VMEM((shards, width, a_cols), LOW),
            pltpu.VMEM((rows // images, width), F32),
            pltpu.VMEM((rows, width), F32),
            pltpu.VMEM((rows, width), LOW),
            pltpu.VMEM((rows, width), LOW),
            dma((4, shards, 2)),
        ]
        + [dma((4, shards))] * 11
        + [dma((4,)), dma((7,))],
        compiler_params=params(1),
        cost_estimate=cost(8 * rows * width * width, 30 * rows * width),
        name="front",
    )(alive, attn_master, mlp_master, patches, cotangent, vec)


def inner_adamw(master, gradient, first, second, step_rate, decay_rate):
    first_moment = 0.9 * first + 0.1 * gradient
    second_moment = 0.95 * second + 0.05 * gradient * gradient
    step_ratio = (
        first_moment / (1.0 - 0.9**STEP) / (jnp.sqrt(second_moment / (1.0 - 0.95**STEP)) + 1e-08)
    )
    return (master - step_rate * (step_ratio + decay_rate * master), second_moment)


def outer_nesterov(master, outer_old, difference):
    momentum = OUTER_MOMENTUM * outer_old + difference
    return momentum, master - OUTER_RATE * (difference + OUTER_MOMENTUM * momentum)


def inner_kernel(join, count, *refs):
    pieces, (master_ref, moment_ref, *_, inner_ref, diff_ref) = refs[:count], refs[count:]
    gradient = join(*[piece[0] for piece in pieces]).astype(F32)
    master = master_ref[0]
    new, second = inner_adamw(master, gradient, moment_ref[0, 0, 0], moment_ref[0, 1, 0], INNER_RATE, WEIGHT_DECAY)
    inner_ref[0, 0, 0] = gradient
    inner_ref[0, 1, 0] = second
    diff_ref[0] = (master - new).astype(LOW)


def inner_step(join, pieces, unit, units, cols, master, moments, into, name):
    depth = master.shape[1]
    rows = min(depth, 524288 // cols)
    block = pl.BlockSpec((1, rows, cols), lambda u, r: (unit(u)[0], r, unit(u)[1]))
    both = pl.BlockSpec((1, 2, 1, rows, cols), lambda u, r: (0, 0, unit(u)[0], r, unit(u)[1]))
    piece_specs = [pl.BlockSpec((1, rows, piece.shape[2]), lambda u, r: (u, r, 0)) for piece in pieces]
    count = len(pieces)
    return pl.pallas_call(
        functools.partial(inner_kernel, join, count),
        grid=(units, depth // rows),
        in_specs=[*piece_specs, block, both] + ([] if into is None else [pl.BlockSpec(memory_space=pl.ANY)]),
        out_specs=[both, pl.BlockSpec((1, rows, cols), lambda u, r: (u, r, 0))],
        out_shape=[
            jax.ShapeDtypeStruct(moments.shape, F32),
            jax.ShapeDtypeStruct((units, depth, cols), LOW),
        ],
        input_output_aliases={} if into is None else {count + 2: 0},
        compiler_params=params(),
        cost_estimate=cost(30 * units * depth * cols, 24 * units * depth * cols),
        name=name,
    )(*pieces, master, moments, *([] if into is None else [into]))


def outer_kernel(groups, slots, each, g_ref, *refs):
    totals, (master_ref, outer_ref, *_, state_ref, copy_ref) = refs[:slots], refs[slots:]
    rows = copy_ref.shape[1]
    if slots == 1:
        total = totals[0][0]
    else:
        at = pl.program_id(0) * pl.num_programs(1) + pl.program_id(1)
        slot = lax.rem(g_ref[0] + groups - at // each, groups)
        here = pl.ds(pl.multiple_of(lax.rem(at, each) * rows, rows), rows)
        total = totals[0][here, :]
        for n in range(1, slots):
            total = jnp.where(slot == n, totals[n][here, :], total)
    difference = total.astype(F32) / groups
    momentum, fresh = outer_nesterov(master_ref[0], outer_ref[0], difference)
    state_ref[0, 0] = difference
    state_ref[1, 0] = momentum
    state_ref[2, 0] = fresh
    copy_ref[0] = fresh.astype(LOW)


def outer_step(groups, me, totals, unit, units, cols, master, outer_old, into, name):
    depth = master.shape[1]
    slots = len(totals)
    rows = min(depth, 524288 // cols, totals[0].shape[-2])
    each = totals[0].shape[-2] // rows
    block = pl.BlockSpec((1, rows, cols), lambda u, r, g: (unit(u)[0], r, unit(u)[1]))
    state = pl.BlockSpec((3, 1, rows, cols), lambda u, r, g: (0, unit(u)[0], r, unit(u)[1]))
    if slots == 1:
        total = pl.BlockSpec((1, rows, cols), lambda u, r, g: (u, r, 0))
    else:
        total = pl.BlockSpec(totals[0].shape, lambda u, r, g: (0, 0))
    aliased = [] if into is None else [pl.BlockSpec(memory_space=pl.ANY)] * 2
    return pl.pallas_call(
        functools.partial(outer_kernel, groups, slots, each),
        grid_spec=pltpu.PrefetchScalarGridSpec(
            num_scalar_prefetch=1,
            grid=(units, depth // rows),
            in_specs=[*[total] * slots, block, block, *aliased],
            out_specs=[state, block],
        ),
        out_shape=[
            jax.ShapeDtypeStruct((3, *master.shape), F32),
            jax.ShapeDtypeStruct(master.shape, LOW),
        ],
        input_output_aliases={} if into is None else {slots + 3: 0, slots + 4: 1},
        compiler_params=params(),
        cost_estimate=cost(10 * units * depth * cols, 24 * units * depth * cols),
        name=name,
    )(me, *totals, master, outer_old, *([] if into is None else into))


def group_kernel(groups, shards, vectors, diff_ref, *refs):
    if vectors:
        part_ref, master_ref, moment_ref, outer_ref, total_ref, inner_ref, state_ref, copy_ref, *refs = refs
    else:
        total_ref, *refs = refs
    landed, summed, sends, receives, sends_two, receives_two, *small = refs
    g, f, t = lax.axis_index("group"), lax.axis_index("fsdp"), lax.axis_index("tensor")
    span = landed.shape[1]

    def rows(n):
        return pl.ds(pl.multiple_of(n * span, span), span)

    def other(k):
        return lax.rem(g + k, groups)

    def back(k):
        return lax.rem(g + groups - k, groups)

    def copy(src, dst, sems, semr, k, to):
        return pltpu.make_async_remote_copy(
            src_ref=src, dst_ref=dst, send_sem=sems.at[k], recv_sem=semr.at[k], device_id=to, device_id_type=MESH
        )

    def part(k):
        return copy(diff_ref.at[rows(other(k)), :], landed.at[k], sends, receives, k, (other(k), f, t))

    def result(k):
        return copy(summed, landed.at[groups + k], sends_two, receives_two, k, (other(k), f, t))

    barrier = pltpu.get_barrier_semaphore()
    for k in range(1, groups):
        pl.semaphore_signal(barrier, inc=1, device_id=(other(k), f, t), device_id_type=MESH)
    if vectors:
        stage, pair, mine, line, whole, few, diffs, ss, rs, ls, lr, gs, gr = small
        half = part_ref.shape[0] // 2
        halves = (pl.ds(0, half), pl.ds(half, half))

        def pick(ref):
            return jnp.where(f == 0, ref[halves[0], :], ref[halves[1], :])

        def line_copy(k):
            return copy(mine, line.at[k], ls, lr, k, (g, f, lax.rem(t + k, shards)))

        def few_copy(k):
            return copy(diffs.at[f], few.at[k], gs, gr, k, (other(k), f, t))

        pair_copy = copy(stage.at[1 - f], pair, ss, rs, 0, partner())
        whole_copy = copy(whole.at[f], whole.at[f], ss, rs, 1, partner())
        final_copy = copy(mine, stage.at[f], ss, rs, 2, partner())
        pl.semaphore_signal(barrier, inc=1, device_id=partner(), device_id_type=MESH)
        for k in range(1, shards):
            pl.semaphore_signal(barrier, inc=1, device_id=(g, f, lax.rem(t + k, shards)), device_id_type=MESH)
        stage[...] = jnp.zeros_like(stage)
        diffs[...] = jnp.zeros_like(diffs)
        for n in range(2):
            stage[n, 0:half] = part_ref[halves[n], :]
    pl.semaphore_wait(barrier, groups - 1 + (shards if vectors else 0))

    for k in range(1, groups):
        part(k).start()
    if vectors:
        pair_copy.start()
        pair_copy.wait()
        mine[...] = stage[f] + pair[...]
        for k in range(1, shards):
            line_copy(k).start()
        line[0] = mine[...]
        for k in range(1, shards):
            line_copy(k).wait()
        gradient = jnp.zeros(mine.shape, F32)
        for n in range(shards):
            gradient = gradient + line[lax.rem(t + shards - n, shards)]
        whole[f] = gradient
        whole_copy.start()
        new, _ = inner_adamw(
            pick(master_ref), gradient[0:half], pick(moment_ref.at[0]), pick(moment_ref.at[1]), VECTOR_RATE, 0.0
        )
        diffs[f, 0:half] = pick(master_ref) - new
        for k in range(1, groups):
            few_copy(k).start()
        few[0] = diffs[f]
        whole_copy.wait()
        for n in range(2):
            own = whole[n, 0:half]
            _, second = inner_adamw(
                master_ref[halves[n], :], own, moment_ref[0, halves[n], :], moment_ref[1, halves[n], :], VECTOR_RATE, 0.0
            )
            inner_ref[0, halves[n], :] = own
            inner_ref[1, halves[n], :] = second
    total = diff_ref[rows(g), :].astype(F32)
    for k in range(1, groups):
        part(k).wait_recv()
        total = total + landed[k].astype(F32)
    summed[...] = total.astype(LOW)
    for k in range(1, groups):
        result(k).start()
    total_ref[rows(g), :] = summed[...]
    if vectors:
        for k in range(1, groups):
            few_copy(k).wait()
        difference = jnp.zeros(mine.shape, F32)
        for n in range(groups):
            difference = difference + few[lax.rem(g + groups - n, groups)]
        mine[...] = difference / groups
        stage[f] = mine[...]
        final_copy.start()
        final_copy.wait()
        for n in range(2):
            difference = stage[n, 0:half]
            momentum, fresh = outer_nesterov(master_ref[halves[n], :], outer_ref[halves[n], :], difference)
            state_ref[0, halves[n], :] = difference
            state_ref[1, halves[n], :] = momentum
            state_ref[2, halves[n], :] = fresh
            copy_ref[halves[n], :] = fresh.astype(LOW)
    for k in range(1, groups):
        result(k).wait_recv()
        total_ref[rows(back(k)), :] = landed[groups + k]
    for k in range(1, groups):
        part(k).wait_send()
        result(k).wait_send()


def group_sum(diff, groups, identity, name, vectors=None, shards=0):
    flat = diff.reshape(-1, diff.shape[-1])
    span, cols = flat.shape[0] // groups, flat.shape[1]
    dma = pltpu.SemaphoreType.DMA
    whole = pl.BlockSpec(memory_space=pltpu.VMEM)
    out_shape = [jax.ShapeDtypeStruct(flat.shape, LOW)]
    extra = []
    if vectors:
        shape = vectors[0].shape
        half = (-(-shape[0] // 16) * 8, shape[1])
        out_shape += [
            jax.ShapeDtypeStruct((2, *shape), F32),
            jax.ShapeDtypeStruct((3, *shape), F32),
            jax.ShapeDtypeStruct(shape, LOW),
        ]
        extra = [
            pltpu.VMEM((2, *half), F32),
            pltpu.VMEM(half, F32),
            pltpu.VMEM(half, F32),
            pltpu.VMEM((shards, *half), F32),
            pltpu.VMEM((2, *half), F32),
            pltpu.VMEM((groups, *half), F32),
            pltpu.VMEM((2, *half), F32),
            dma((3,)),
            dma((3,)),
            dma((shards,)),
            dma((shards,)),
            dma((groups,)),
            dma((groups,)),
        ]
    total, *rest = pl.pallas_call(
        functools.partial(group_kernel, groups, shards, bool(vectors)),
        in_specs=[whole] * (5 if vectors else 1),
        out_specs=[whole] * len(out_shape),
        out_shape=out_shape,
        scratch_shapes=[
            pltpu.VMEM((2 * groups, span, cols), LOW),
            pltpu.VMEM((span, cols), LOW),
            *[dma((groups,))] * 4,
            *extra,
        ],
        compiler_params=params(identity),
        cost_estimate=cost(4 * flat.size, 8 * flat.size),
        name=name,
    )(flat, *(vectors or []))
    return total.reshape(diff.shape), *rest


def gather_weights(shard):
    whole = lax.all_gather(shard, "tensor", axis=0)
    return lax.all_gather(whole, "fsdp", axis=2, tiled=True)


def around(array, k, groups):
    return lax.ppermute(array, "group", [(i, (i + k) % groups) for i in range(groups)])


def exchange_parts(diff, groups):
    g = lax.axis_index("group")
    quarters = diff.reshape(groups, -1, diff.shape[-1])
    parts = [lax.dynamic_index_in_dim(quarters, lax.rem(g + k, groups), 0, keepdims=False) for k in range(groups)]
    total = sum([around(parts[k], k, groups).astype(F32) for k in range(1, groups)], parts[0].astype(F32))
    return total.astype(LOW)


def exchange_total(own, groups):
    return [own] + [around(own, k, groups) for k in range(1, groups)]


def scatter_gradient(gradient):
    half = gradient if gradient.ndim == 4 else lax.psum_scatter(gradient, "fsdp", scatter_dimension=0)
    return lax.psum_scatter(half, "tensor", scatter_dimension=0)


def local(
    patches,
    output_grad,
    live_counts,
    attn_master,
    mlp_master,
    vector_master,
    attn_moments,
    mlp_moments,
    vector_moments,
    attn_outer,
    mlp_outer,
    vector_outer,
):
    vec = vector_master
    tensor_size, fsdp = lax.axis_size("tensor"), lax.axis_size("fsdp")
    groups = lax.axis_size("group")
    local_images, seq, width = patches.shape[2:]
    slot = (lax.axis_index("fsdp") * tensor_size + lax.axis_index("tensor")) * local_images
    slot = slot + jnp.arange(local_images)
    counts = jnp.take(live_counts[0], slot // IMG_DEV, axis=1)
    alive = ((slot % IMG_DEV)[None, :] < counts).astype(F32).reshape(-1)
    x = patches.reshape(-1, seq, width)
    cotangent = output_grad.reshape(-1, seq, width)
    images = x.shape[0]

    if (groups, fsdp) == (4, 2):
        w_attn, w_mlp, normed_one, qkv, attended, resid, normed_two, grad_two = front(
            alive, attn_master, mlp_master, x, cotangent, vec, tensor_size
        )
    else:
        w_attn = gather_weights(attn_master.astype(LOW))
        w_mlp = gather_weights(mlp_master.astype(LOW))
        normed_one, qkv = project(x, w_attn, vec)
        attended = attend(qkv, images, seq)
        resid, normed_two, grad_two = mix(alive, attended, x, cotangent, w_attn, vec)
    bias = vec[8:].reshape(tensor_size, 1, -1)
    carried = None
    mlp_grads, bias_parts = [], []
    for part, (start, cols) in enumerate(PIECES):
        *carried, dw, db = mlp(part, start, cols, normed_two, grad_two, w_mlp, bias, carried, fsdp)
        mlp_grads.append(scatter_gradient(dw))
        bias_parts.append(db)
    branch, grad_normed = carried
    block_output, grad_resid, grad_attended, dw_out, sums_two = turn(
        alive, resid, branch, grad_normed, grad_two, attended, w_attn, vec, images, seq, fsdp
    )
    def beside(*parts):
        return jnp.concatenate(parts, axis=-1)

    pairwise = fsdp == 2
    me = lax.axis_index("group").astype(jnp.int32).reshape(1)
    half = attn_master.shape[2] // PARTS
    grads = unattend(qkv, grad_attended, images, seq, 0, PARTS, tensor_size)
    grads, mlp_grads[0] = lax.optimization_barrier((grads, mlp_grads[0]))
    carry, dw_early, head_sums = close(
        0, PARTS, normed_one, grads, w_attn, None, dw_out, None, fsdp, groups, images, seq
    )
    if not pairwise:
        halves = jnp.moveaxis(dw_out.reshape(*dw_out.shape[:-1], PARTS, half), -2, 2)
        dw_early = jnp.concatenate([dw_early, halves[:, :, :, 0]], axis=2)
    early_grad = scatter_gradient(dw_early)
    head_sums = [head_sums]
    carry, mlp_grads[1] = lax.optimization_barrier((carry, mlp_grads[1]))
    grads = unattend(qkv, grad_attended, images, seq, 1, PARTS, tensor_size)

    mlp_grads[0], grads = lax.optimization_barrier((mlp_grads[0], grads))
    mlp_inner, mlp_diff = inner_step(
        beside, mlp_grads, lambda u: (u, 0), 2, mlp_master.shape[2], mlp_master, mlp_moments, None, "inner_mlp"
    )
    carry, mlp_diff = lax.optimization_barrier((carry, mlp_diff))
    ending = [x, grad_resid, vec]
    if pairwise:
        ending.append(mlp_diff.reshape(-1, mlp_diff.shape[-1]))
    patches_grad, sums_one, *mlp_own, dw_late, sums = close(
        1, PARTS, normed_one, grads, w_attn, carry, None, ending, fsdp, groups, images, seq
    )
    if not pairwise:
        mlp_own = [exchange_parts(mlp_diff, groups)]
    mlp_total = exchange_total(mlp_own[0], groups)
    late_grad = scatter_gradient(dw_late)
    head_sums.append(sums)

    def early(u):
        return jnp.minimum(u, 3), jnp.maximum(u - 3, 0)

    def late(u):
        return u, 1

    def first(piece):
        return piece

    attn_inner, early_diff = inner_step(
        first, [early_grad], early, 3 + PARTS, half, attn_master, attn_moments, None, "inner_early"
    )
    head_rows = jnp.concatenate([v.reshape(2, tensor_size, -1) for v in head_sums], axis=-1).reshape(2, width)
    hidden_bias = jnp.concatenate(bias_parts, axis=-1).reshape(-1, width)
    vector_part = jnp.concatenate([sums_one, sums_two[:2], head_rows, sums_two[2:], hidden_bias])

    if pairwise:
        early_total, vector_inner, vector_state, vector_copy = group_sum(
            early_diff,
            groups,
            10,
            "group_early",
            [vector_part, vec, vector_moments[0], vector_outer],
            tensor_size,
        )
    else:
        (early_total,) = group_sum(early_diff, groups, 10, "group_early")
        vector_grad = lax.psum(vector_part, ("fsdp", "tensor"))
        new_vector, second_vector = inner_adamw(
            vec, vector_grad, vector_moments[0, 0], vector_moments[0, 1], VECTOR_RATE, 0.0
        )
        diff_vector = lax.psum(vec - new_vector, "group") / groups
        momentum, fresh = outer_nesterov(vec, vector_outer, diff_vector)
        vector_inner = jnp.stack([vector_grad, second_vector])
        vector_state, vector_copy = jnp.stack([diff_vector, momentum, fresh]), fresh.astype(LOW)
    attn_state, attn_copy = outer_step(
        groups, me, [early_total], early, 3 + PARTS, half, attn_master, attn_outer, None, "outer_early"
    )
    attn_copy, *mlp_total = lax.optimization_barrier((attn_copy, *mlp_total))
    mlp_state, mlp_copy = outer_step(
        groups,
        me,
        mlp_total,
        lambda u: (u, 0),
        2,
        mlp_master.shape[2],
        mlp_master,
        mlp_outer,
        None,
        "outer_mlp",
    )
    late_grad, mlp_state = lax.optimization_barrier((late_grad, mlp_state))
    attn_inner, late_diff = inner_step(
        first, [late_grad], late, 3, half, attn_master, attn_moments, attn_inner, "inner_late"
    )
    (late_total,) = group_sum(late_diff, groups, 11, "group_late")
    attn_state, attn_copy = outer_step(
        groups, me, [late_total], late, 3, half, attn_master, attn_outer, (attn_state, attn_copy), "outer_late"
    )
    return (
        block_output.reshape(patches.shape),
        patches_grad.reshape(patches.shape),
        attn_inner,
        attn_state,
        attn_copy,
        mlp_inner,
        mlp_state,
        mlp_copy,
        vector_inner[None],
        vector_state,
        vector_copy,
    )


def solution(mesh):
    placed = (
        P("group", None, ("fsdp", "tensor"), None, None),
        P("group", None, ("fsdp", "tensor"), None, None),
        P("group", None, None),
        P(None, "fsdp", "tensor"),
        P(None, "fsdp", "tensor"),
        P(),
        P("group", None, None, "fsdp", "tensor"),
        P("group", None, None, "fsdp", "tensor"),
        P("group", None, None, None),
        P(None, "fsdp", "tensor"),
        P(None, "fsdp", "tensor"),
        P(),
    )
    return jax.shard_map(
        local,
        mesh=mesh,
        in_specs=placed,
        out_specs=(
            P("group", None, ("fsdp", "tensor"), None, None),
            P("group", None, ("fsdp", "tensor"), None, None),
            P("group", None, None, "fsdp", "tensor"),
            P(None, None, "fsdp", "tensor"),
            P(None, "fsdp", "tensor"),
            P("group", None, None, "fsdp", "tensor"),
            P(None, None, "fsdp", "tensor"),
            P(None, "fsdp", "tensor"),
            P("group", None, None, None),
            P(),
            P(),
        ),
        check_vma=False,
    )
```

```python
import functools

import jax
import jax.numpy as jnp
from jax import lax
from jax.experimental import pallas as pl
from jax.experimental.pallas import tpu as pltpu
from jax.sharding import PartitionSpec as P

HD = 64
STEP = 8
IMG_DEV = 4
EPSILON = 1e-06
INNER_RATE = 0.02
VECTOR_RATE = 0.2
WEIGHT_DECAY = 0.1
OUTER_RATE = 0.7
OUTER_MOMENTUM = 0.9
PIECES = ((0, 256), (256, 256), (512, 512))
PARTS = 2
LOW = jnp.bfloat16
F32 = jnp.float32
NN = (((1,), (0,)), ((), ()))
NT = (((1,), (1,)), ((), ()))
TN = (((0,), (0,)), ((), ()))


def dot(a, b, dims=NN):
    return lax.dot_general(a, b, dims, preferred_element_type=F32)


MESH = pl.DeviceIdType.MESH


def params(identity=None):
    if identity is None:
        return pltpu.CompilerParams(vmem_limit_bytes=60 * 2**20)
    return pltpu.CompilerParams(vmem_limit_bytes=60 * 2**20, collective_id=identity, has_side_effects=True)


def partner():
    return (lax.axis_index("group"), 1 - lax.axis_index("fsdp"), lax.axis_index("tensor"))


def greet_partner():
    barrier = pltpu.get_barrier_semaphore()
    pl.semaphore_signal(barrier, inc=1, device_id=partner(), device_id_type=MESH)
    pl.semaphore_wait(barrier, 1)


def to_partner(sent, received, sends, receives, n):
    return pltpu.make_async_remote_copy(
        src_ref=sent.at[n],
        dst_ref=received.at[n],
        send_sem=sends.at[n],
        recv_sem=receives.at[n],
        device_id=partner(),
        device_id_type=MESH,
    )


def bands(depth):
    f = lax.axis_index("fsdp")
    return pl.ds(pl.multiple_of(f * depth, depth), depth), pl.ds(pl.multiple_of((1 - f) * depth, depth), depth)


def exchange_scratch(steps, shape):
    dma = pltpu.SemaphoreType.DMA
    return [
        pltpu.VMEM((steps, *shape), F32),
        pltpu.VMEM((steps, *shape), LOW),
        pltpu.VMEM((steps, *shape), LOW),
        dma((steps,)),
        dma((steps,)),
    ]


def cost(flops, moved, special=0):
    return pl.CostEstimate(flops=int(flops), bytes_accessed=int(moved), transcendentals=int(special))


def padded(rows):
    return -(-rows // 16) * 16


def centred(source):
    centre = source - jnp.mean(source, axis=-1, keepdims=True)
    spread = jnp.mean(centre * centre, axis=-1, keepdims=True)
    inverse = lax.rsqrt(spread + EPSILON)
    return centre * inverse, inverse


def norm_back(upstream, normal, inverse, gain):
    pulled = upstream * gain
    mean_one = jnp.mean(pulled, axis=-1, keepdims=True)
    mean_two = jnp.mean(pulled * normal, axis=-1, keepdims=True)
    return inverse * (pulled - mean_one - normal * mean_two)


def project_kernel(images, seq, x_ref, w_ref, vec_ref, n_ref, out_ref, n_scr):
    j, t = pl.program_id(0), pl.program_id(1)
    span = n_scr.shape[0] // images

    @pl.when((j == 0) & (t == 0))
    def _():
        n_scr[...] = jnp.zeros_like(n_scr)
        for i in range(images):
            normal, _ = centred(x_ref[i].astype(F32))
            n_scr[pl.ds(i * span, seq), :] = (normal * vec_ref[0:1] + vec_ref[1:2]).astype(LOW)
        n_ref[...] = n_scr[...]

    cols = out_ref.shape[-1]
    out = dot(n_scr[...], w_ref[0, 0])
    at = pl.ds(pl.multiple_of(t * cols, cols), cols)
    bias = jnp.where(j == 0, vec_ref[4:5, at], jnp.where(j == 2, vec_ref[5:6, at], 0.0))
    out_ref[0] = (out + bias).astype(LOW)


def project(patches, w_attn, vec):
    images, seq, width = patches.shape
    shards, _, _, cols = w_attn.shape
    rows = images * padded(seq)
    return pl.pallas_call(
        functools.partial(project_kernel, images, seq),
        grid=(3, shards),
        in_specs=[
            pl.BlockSpec((images, seq, width), lambda j, t: (0, 0, 0)),
            pl.BlockSpec((1, 1, width, cols), lambda j, t: (t, j, 0, 0)),
            pl.BlockSpec(vec.shape, lambda j, t: (0, 0)),
        ],
        out_specs=[
            pl.BlockSpec((rows, width), lambda j, t: (0, 0)),
            pl.BlockSpec((1, rows, cols), lambda j, t: (j, 0, t)),
        ],
        out_shape=[
            jax.ShapeDtypeStruct((rows, width), LOW),
            jax.ShapeDtypeStruct((3, rows, width), LOW),
        ],
        scratch_shapes=[pltpu.VMEM((rows, width), LOW)],
        compiler_params=params(),
        cost_estimate=cost(6 * rows * width * width, 16 * rows * width),
        name="project",
    )(patches, w_attn, vec)


def half_lanes(value, which):
    lane = lax.broadcasted_iota(jnp.int32, value.shape, 1)
    return jnp.where((lane >= HD) == bool(which), value, jnp.zeros_like(value))


def attend_kernel(seq, q_ref, k_ref, v_ref, out_ref):
    span = q_ref.shape[1]
    scale = HD**-0.5
    q, k, v = q_ref[0], k_ref[0], v_ref[0]
    parts = []
    for h in range(2):
        scores = dot(q, half_lanes(k, h), NT)
        lane = lax.broadcasted_iota(jnp.int32, scores.shape, 1)
        scores = jnp.where(lane < seq, scores, -1e30)
        top = jnp.max(scores, axis=1, keepdims=True)
        raised = jnp.exp((scores - top) * scale)
        total = jnp.sum(raised, axis=1, keepdims=True)
        probs = (raised * (1.0 / total)).astype(LOW)
        parts.append(dot(probs, v))
    lane = lax.broadcasted_iota(jnp.int32, (span, 2 * HD), 1)
    out_ref[...] = jnp.where(lane < HD, parts[0], parts[1]).astype(LOW)


def attend(qkv, images, seq):
    _, rows, width = qkv.shape
    span = rows // images
    pair = 2 * HD

    def take(j):
        return pl.BlockSpec((1, span, pair), lambda i, h: (j, i, h))

    return pl.pallas_call(
        functools.partial(attend_kernel, seq),
        grid=(images, width // pair),
        in_specs=[take(0), take(1), take(2)],
        out_specs=pl.BlockSpec((span, pair), lambda i, h: (i, h)),
        out_shape=jax.ShapeDtypeStruct((rows, width), LOW),
        compiler_params=params(),
        cost_estimate=cost(16 * rows * span * width, 8 * rows * width, rows * span * (width // HD)),
        name="attend",
    )(qkv, qkv, qkv)


def mix_kernel(seq, alive_ref, att_ref, x_ref, g_ref, w_ref, vec_ref, resid_ref, n_ref, g2_ref, x_scr):
    i = pl.program_id(0)
    shards, _, _, cols = w_ref.shape
    x_scr[...] = jnp.zeros_like(x_scr)
    x_scr[0:seq, :] = x_ref[0].astype(F32)
    total = x_scr[...] + vec_ref[6:7]
    for t in range(shards):
        total = total + dot(att_ref[:, t * cols : (t + 1) * cols], w_ref[t, 0], NT)
    resid_ref[...] = total
    normal, _ = centred(total)
    n_ref[...] = (normal * vec_ref[2:3] + vec_ref[3:4]).astype(LOW)
    x_scr[0:seq, :] = g_ref[0].astype(F32) * alive_ref[i]
    g2_ref[...] = x_scr[...].astype(LOW)


def mix(alive, attended, patches, cotangent, w_attn, vec):
    images, seq, width = patches.shape
    rows = attended.shape[0]
    span = rows // images
    shards, _, _, cols = w_attn.shape
    block = pl.BlockSpec((span, width), lambda i: (i, 0))
    whole = jax.ShapeDtypeStruct((rows, width), LOW)
    return pl.pallas_call(
        functools.partial(mix_kernel, seq),
        grid=(images,),
        in_specs=[
            pl.BlockSpec(memory_space=pltpu.SMEM),
            block,
            pl.BlockSpec((1, seq, width), lambda i: (i, 0, 0)),
            pl.BlockSpec((1, seq, width), lambda i: (i, 0, 0)),
            pl.BlockSpec((shards, 1, width, cols), lambda i: (0, 3, 0, 0)),
            pl.BlockSpec(vec.shape, lambda i: (0, 0)),
        ],
        out_specs=[block, block, block],
        out_shape=[jax.ShapeDtypeStruct((rows, width), F32), whole, whole],
        scratch_shapes=[pltpu.VMEM((span, width), F32)],
        compiler_params=params(),
        cost_estimate=cost(2 * rows * width * width, 16 * rows * width),
        name="mix",
    )(alive, attended, patches, cotangent, w_attn, vec)


def mlp_kernel(first, pairwise, n_ref, g_ref, w1_ref, w2_ref, bias_ref, *refs):
    if not first:
        yi_ref, gi_ref, *refs = refs
    y_ref, gn_ref, dw_ref, db_ref, h_scr, p_scr, loaded, *exchange = refs
    step = pl.program_id(0)
    each, _, width, cols = w1_ref.shape
    if not first:
        loads = (
            pltpu.make_async_copy(yi_ref, y_ref, loaded.at[0]),
            pltpu.make_async_copy(gi_ref, gn_ref, loaded.at[1]),
        )

    @pl.when(step == 0)
    def _():
        if not first:
            for load in loads:
                load.start()
        else:
            y_ref[...] = jnp.zeros_like(y_ref)
            gn_ref[...] = jnp.zeros_like(gn_ref)
        if pairwise:
            greet_partner()

    w1 = jnp.concatenate([w1_ref[t, 0] for t in range(each)], axis=1)
    w2 = jnp.concatenate([w2_ref[t, 0] for t in range(each)], axis=1)
    bias = jnp.concatenate([bias_ref[t] for t in range(each)], axis=1)
    pre = dot(n_ref[...], w1) + bias
    cdf = 0.5 * (1.0 + lax.erf(pre * 0.7071067811865476))
    h_scr[...] = (pre * cdf).astype(LOW)
    slope = cdf + pre * jnp.exp(-0.5 * pre * pre) * 0.3989422804014327
    p_scr[...] = (dot(g_ref[...], w2) * slope).astype(LOW)
    sums = jnp.sum(p_scr[...].astype(F32), axis=0, keepdims=True)
    for t in range(each):
        db_ref[t] = sums[:, t * cols : (t + 1) * cols]

    if pairwise:
        own, sent, received, sends, receives = exchange
        ours, theirs = bands(width // 2)

        slot = lax.rem(step, 2)

        def collect(n):
            at = lax.rem(n, 2)
            to_partner(sent, received, sends, receives, at).wait()
            for which in range(2):
                total = (own[at, which] + received[at, which].astype(F32)).astype(LOW)
                for t in range(each):
                    dw_ref[n * each + t, which] = total[:, t * cols : (t + 1) * cols]

        @pl.when(step > 0)
        def _():
            collect(step - 1)

        sent[slot, 0] = dot(n_ref[:, theirs], p_scr[...], TN).astype(LOW)
        sent[slot, 1] = dot(g_ref[:, theirs], h_scr[...], TN).astype(LOW)
        to_partner(sent, received, sends, receives, slot).start()
        own[slot, 0] = dot(n_ref[:, ours], p_scr[...], TN)
        own[slot, 1] = dot(g_ref[:, ours], h_scr[...], TN)

    else:
        shards, depth = dw_ref.shape[0], dw_ref.shape[3]
        d1 = dot(n_ref[...], p_scr[...], TN).astype(LOW)
        d2 = dot(g_ref[...], h_scr[...], TN).astype(LOW)
        for f in range(shards):
            for t in range(each):
                dw_ref[f, t, 0] = d1[f * depth : (f + 1) * depth, t * cols : (t + 1) * cols]
                dw_ref[f, t, 1] = d2[f * depth : (f + 1) * depth, t * cols : (t + 1) * cols]

    if not first:

        @pl.when(step == 0)
        def _():
            for load in loads:
                load.wait()

    y_ref[...] += dot(h_scr[...], w2, NT)
    gn_ref[...] += dot(p_scr[...], w1, NT)
    if pairwise:

        @pl.when(step == pl.num_programs(0) - 1)
        def _():
            collect(step)


def mlp(part, start, cols, normed, grad_two, w_mlp, bias, carried, fsdp):
    rows, width = normed.shape
    shards = w_mlp.shape[0]
    each = max(512 // cols, 1)
    at = start // cols
    first, pairwise = carried is None, fsdp == 2
    single = pl.Buffered(1)
    full = pl.BlockSpec((rows, width), lambda s: (0, 0), pipeline_mode=single)
    depth = width // fsdp
    steps = shards // each
    acc_shape = jax.ShapeDtypeStruct((rows, width), F32)
    if pairwise:
        out_w = pl.BlockSpec((shards, 2, depth, cols), lambda s: (0, 0, 0, 0), pipeline_mode=single)
        w_shape = jax.ShapeDtypeStruct((shards, 2, depth, cols), LOW)
        extra = exchange_scratch(2, (2, depth, each * cols))
    else:
        out_w = pl.BlockSpec((fsdp, each, 2, depth, cols), lambda s: (0, s, 0, 0, 0))
        w_shape = jax.ShapeDtypeStruct((fsdp, shards, 2, depth, cols), LOW)
        extra = []
    return pl.pallas_call(
        functools.partial(mlp_kernel, first, pairwise),
        grid=(steps,),
        in_specs=[
            full,
            full,
            pl.BlockSpec((each, 1, width, cols), lambda s: (s, 0, 0, at)),
            pl.BlockSpec((each, 1, width, cols), lambda s: (s, 1, 0, at)),
            pl.BlockSpec((each, 1, cols), lambda s: (s, 0, at)),
        ]
        + ([] if first else [pl.BlockSpec(memory_space=pl.ANY)] * 2),
        out_specs=[full, full, out_w, pl.BlockSpec((each, 1, cols), lambda s: (s, 0, 0))],
        out_shape=[acc_shape, acc_shape, w_shape, jax.ShapeDtypeStruct((shards, 1, cols), F32)],
        scratch_shapes=[
            pltpu.VMEM((rows, each * cols), LOW),
            pltpu.VMEM((rows, each * cols), LOW),
            pltpu.SemaphoreType.DMA((2,)),
            *extra,
        ],
        compiler_params=params(2 + part if pairwise else None),
        cost_estimate=cost(12 * rows * width * cols * shards, 24 * rows * width),
        name=f"mlp_{part}",
    )(normed, grad_two, w_mlp, w_mlp, bias, *([] if first else carried))


def turn_kernel(seq, pairwise, alive_ref, resid_ref, y_ref, gn_ref, g2_ref, att_ref, w_ref, vec_ref,
                out_ref, gr_ref, ga_ref, dw_ref, sums_ref, dw_scr, *exchange):
    i = pl.program_id(0)
    if pairwise:
        pl.when(i == 0)(greet_partner)
    shards, _, _, cols = w_ref.shape
    resid = resid_ref[...]
    out_ref[0] = ((resid + y_ref[...] + vec_ref[7:8]) * alive_ref[i]).astype(LOW)[0:seq]
    normal, inverse = centred(resid)
    upstream = gn_ref[...]
    grad_out = g2_ref[...].astype(F32)
    grad_resid = grad_out + norm_back(upstream, normal, inverse, vec_ref[2:3])
    gr_ref[...] = grad_resid
    low = grad_resid.astype(LOW)
    rows = [
        jnp.sum(upstream * normal, axis=0, keepdims=True),
        jnp.sum(upstream, axis=0, keepdims=True),
        jnp.sum(grad_resid, axis=0, keepdims=True),
        jnp.sum(grad_out, axis=0, keepdims=True),
    ]
    rows = jnp.concatenate(rows, axis=0)

    @pl.when(i == 0)
    def _():
        sums_ref[...] = rows

    @pl.when(i != 0)
    def _():
        sums_ref[...] += rows

    for t in range(shards):
        ga_ref[:, t * cols : (t + 1) * cols] = dot(low, w_ref[t, 0]).astype(LOW)
    part = dot(low, att_ref[...], TN)

    @pl.when(i == 0)
    def _():
        dw_scr[...] = part

    @pl.when(i != 0)
    def _():
        dw_scr[...] += part

    @pl.when(i == pl.num_programs(0) - 1)
    def _():
        if pairwise:
            sent, received, sends, receives = exchange
            ours, theirs = bands(dw_scr.shape[0] // 2)
            sent[0] = dw_scr[theirs, :].astype(LOW)
            copy = to_partner(sent, received, sends, receives, 0)
            copy.start()
            copy.wait()
            total = (dw_scr[ours, :] + received[0].astype(F32)).astype(LOW)
            for t in range(shards):
                dw_ref[t, 0] = total[:, t * cols : (t + 1) * cols]
            return
        depth = dw_ref.shape[3]
        for f in range(dw_ref.shape[0]):
            for t in range(shards):
                dw_ref[f, t, 0] = dw_scr[f * depth : (f + 1) * depth, t * cols : (t + 1) * cols].astype(LOW)


def turn(alive, resid, branch, grad_normed, grad_two, attended, w_attn, vec, images, seq, fsdp):
    rows, width = resid.shape
    span = rows // images
    shards, _, _, cols = w_attn.shape
    depth = width // fsdp
    pairwise = fsdp == 2
    lead = () if pairwise else (fsdp,)
    block = pl.BlockSpec((span, width), lambda i: (i, 0))
    return pl.pallas_call(
        functools.partial(turn_kernel, seq, pairwise),
        grid=(images,),
        in_specs=[
            pl.BlockSpec(memory_space=pltpu.SMEM),
            block, block, block, block, block,
            pl.BlockSpec((shards, 1, width, cols), lambda i: (0, 3, 0, 0)),
            pl.BlockSpec(vec.shape, lambda i: (0, 0)),
        ],
        out_specs=[
            pl.BlockSpec((1, seq, width), lambda i: (i, 0, 0)),
            block, block,
            pl.BlockSpec((*lead, shards, 1, depth, cols), lambda i: (0,) * (4 + len(lead))),
            pl.BlockSpec((4, width), lambda i: (0, 0)),
        ],
        out_shape=[
            jax.ShapeDtypeStruct((images, seq, width), LOW),
            jax.ShapeDtypeStruct((rows, width), F32),
            jax.ShapeDtypeStruct((rows, width), LOW),
            jax.ShapeDtypeStruct((*lead, shards, 1, depth, cols), LOW),
            jax.ShapeDtypeStruct((4, width), F32),
        ],
        scratch_shapes=[pltpu.VMEM((width, width), F32)] + (exchange_scratch(1, (depth, width))[1:] if pairwise else []),
        compiler_params=params(6 if pairwise else None),
        cost_estimate=cost(4 * rows * width * width, 24 * rows * width),
        name="turn",
    )(alive, resid, branch, grad_normed, grad_two, attended, w_attn, vec)


def unattend_kernel(seq, q_ref, k_ref, v_ref, g_ref, out_ref):
    span = q_ref.shape[1]
    scale = HD**-0.5
    q, k, v, g = q_ref[0], k_ref[0], v_ref[0], g_ref[...]
    parts = []
    for h in range(2):
        scores = dot(half_lanes(k, h), q, NT)
        row = lax.broadcasted_iota(jnp.int32, scores.shape, 0)
        scores = jnp.where(row < seq, scores, -1e30)
        top = jnp.max(scores, axis=0, keepdims=True)
        raised = jnp.exp((scores - top) * scale)
        total = jnp.sum(raised, axis=0, keepdims=True)
        probs = raised * (1.0 / total)
        gp = dot(half_lanes(v, h), g, NT)
        delta = jnp.sum(probs * gp, axis=0, keepdims=True)
        gs = (probs * (gp - delta)).astype(LOW)
        dv = dot(probs.astype(LOW), g)
        dk = dot(gs, q)
        dq = dot(gs, k, TN)
        parts.append((dq, dk, dv))
    lane = lax.broadcasted_iota(jnp.int32, (span, 2 * HD), 1) < HD
    out_ref[0] = (jnp.where(lane, parts[0][0], parts[1][0]) * scale).astype(LOW)
    out_ref[1] = (jnp.where(lane, parts[0][1], parts[1][1]) * scale).astype(LOW)
    out_ref[2] = jnp.where(lane, parts[0][2], parts[1][2]).astype(LOW)


def unattend(qkv, grad_attended, images, seq, part, parts, shards):
    _, rows, width = qkv.shape
    span = rows // images
    pair = 2 * HD
    each = width // shards // parts // pair

    def spot(h):
        return (h // each) * (each * parts) + part * each + h % each

    def take(j):
        return pl.BlockSpec((1, span, pair), lambda i, h: (j, i, spot(h)))

    return pl.pallas_call(
        functools.partial(unattend_kernel, seq),
        grid=(images, width // pair // parts),
        in_specs=[take(0), take(1), take(2), pl.BlockSpec((span, pair), lambda i, h: (i, spot(h)))],
        out_specs=pl.BlockSpec((3, span, pair), lambda i, h: (0, i, h)),
        out_shape=jax.ShapeDtypeStruct((3, rows, width // parts), LOW),
        compiler_params=params(),
        cost_estimate=cost(
            40 * rows * span * width // parts, 14 * rows * width // parts, rows * span * (width // HD) // parts
        ),
        name=f"unattend_{part}",
    )(qkv, qkv, qkv, grad_attended)


def close_kernel(pairwise, groups, first, final, n_ref, grad_ref, w_ref, *refs):
    if not first:
        carry_ref, *refs = refs
    elif pairwise:
        more_ref, *refs = refs
    if pairwise and final:
        diff_ref, acc_ref, total_ref, *refs = refs
    else:
        acc_ref, *refs = refs
    dw_ref, sums_ref, acc_scr, *exchange = refs
    j = pl.program_id(0)
    shards, _, _, cols = w_ref.shape
    if pairwise:
        own, sent, received, sends, receives, *exchange = exchange
        if not final:
            pl.when(j == 0)(greet_partner)
    if pairwise and final:
        mine, landed, sends_two, receives_two, loaded = exchange
        g, f, t = lax.axis_index("group"), lax.axis_index("fsdp"), lax.axis_index("tensor")
        quarter = landed.shape[1]

        def rows(n):
            return pl.ds(pl.multiple_of(n * quarter, quarter), quarter)

        def other(k):
            return (lax.rem(g + k, groups), f, t)

        def part(k):
            return pltpu.make_async_remote_copy(
                src_ref=diff_ref.at[rows(lax.rem(g + k, groups)), :],
                dst_ref=landed.at[k],
                send_sem=sends_two.at[k],
                recv_sem=receives_two.at[k],
                device_id=other(k),
                device_id_type=MESH,
            )

        keep = pltpu.make_async_copy(diff_ref.at[rows(g), :], mine, loaded.at[0])

        @pl.when(j == 0)
        def _():
            barrier = pltpu.get_barrier_semaphore()
            pl.semaphore_signal(barrier, inc=1, device_id=partner(), device_id_type=MESH)
            for k in range(1, groups):
                pl.semaphore_signal(barrier, inc=1, device_id=other(k), device_id_type=MESH)
            pl.semaphore_wait(barrier, groups)
            for k in range(1, groups):
                part(k).start()
            keep.start()

    @pl.when(j == 0)
    def _():
        acc_scr[...] = jnp.zeros_like(acc_scr) if first else carry_ref[...]

    sums = jnp.sum(grad_ref[0].astype(F32), axis=0, keepdims=True)
    for n, matrix in enumerate((0, 2)):

        @pl.when(j == matrix)
        def _():
            sums_ref[n : n + 1, :] = sums

    def spread(n, total, f=None):
        for t in range(shards):
            piece = total[:, t * cols : (t + 1) * cols]
            if f is None:
                dw_ref[t, n] = piece
            else:
                dw_ref[f, t, 0] = piece

    weight = jnp.concatenate([w_ref[t, 0] for t in range(shards)], axis=1)
    if pairwise:
        ours, theirs = bands(n_ref.shape[1] // 2)
        sent[j] = dot(n_ref[:, theirs], grad_ref[0], TN).astype(LOW)
        to_partner(sent, received, sends, receives, j).start()
        own[j] = dot(n_ref[:, ours], grad_ref[0], TN)
    else:
        depth = dw_ref.shape[3]
        dw = dot(n_ref[...], grad_ref[0], TN).astype(LOW)
        for f in range(dw_ref.shape[0]):
            spread(0, dw[f * depth : (f + 1) * depth], f)
    acc_scr[...] += dot(grad_ref[0], weight, NT)

    @pl.when(j == 2)
    def _():
        if pairwise:
            for n in range(own.shape[0]):
                to_partner(sent, received, sends, receives, n).wait()
                spread(n, (own[n] + received[n].astype(F32)).astype(LOW))
            if first:
                for t in range(shards):
                    for n in range(dw_ref.shape[1] - 3):
                        dw_ref[t, 3 + n] = more_ref[t, 0, :, n * cols : (n + 1) * cols]
        acc_ref[...] = acc_scr[...]
        if pairwise and final:
            keep.wait()
            total = mine[...].astype(F32)
            for k in range(1, groups):
                part(k).wait()
                total = total + landed[k].astype(F32)
            total_ref[...] = total.astype(LOW)


def close(part, parts, normed, grads, w_attn, carry, more, ending, fsdp, groups):
    rows, width = normed.shape
    shards, _, _, cols = w_attn.shape
    cols = cols // parts
    lanes = shards * cols
    depth = width // fsdp
    pairwise, first, final = fsdp == 2, carry is None, ending is not None
    single = pl.Buffered(1)
    stack = pl.BlockSpec((1, rows, lanes), lambda j: (j, 0, 0))
    full = pl.BlockSpec((rows, width), lambda j: (0, 0), pipeline_mode=single)
    if pairwise:
        many = 3 + parts if first else 3
        dw_spec = pl.BlockSpec((shards, many, depth, cols), lambda j: (0, 0, 0, 0), pipeline_mode=single)
        dw_shape = jax.ShapeDtypeStruct((shards, many, depth, cols), LOW)
        extra = exchange_scratch(3, (depth, lanes))
    else:
        dw_spec = pl.BlockSpec((fsdp, shards, 1, depth, cols), lambda j: (0, 0, j, 0, 0))
        dw_shape = jax.ShapeDtypeStruct((fsdp, shards, 3, depth, cols), LOW)
        extra = []
    in_specs = [full, stack, pl.BlockSpec((shards, 1, width, cols), lambda j: (0, j, 0, part))]
    out_specs, out_shape = [], []
    if not first:
        in_specs.append(full)
    elif pairwise:
        in_specs.append(pl.BlockSpec(more.shape, lambda j: (0, 0, 0, 0), pipeline_mode=single))
    out_specs.append(full)
    out_shape.append(jax.ShapeDtypeStruct((rows, width), F32))
    if pairwise and final:
        quarter, lanes_two = ending.shape[0] // groups, ending.shape[1]
        in_specs.append(pl.BlockSpec(memory_space=pl.ANY))
        out_specs.append(pl.BlockSpec((quarter, lanes_two), lambda j: (0, 0), pipeline_mode=single))
        out_shape.append(jax.ShapeDtypeStruct((quarter, lanes_two), LOW))
        dma = pltpu.SemaphoreType.DMA
        extra = [
            *extra,
            pltpu.VMEM((quarter, lanes_two), LOW),
            pltpu.VMEM((groups, quarter, lanes_two), LOW),
            dma((groups,)),
            dma((groups,)),
            dma((1,)),
        ]
    return pl.pallas_call(
        functools.partial(close_kernel, pairwise, groups, first, final),
        grid=(3,),
        in_specs=in_specs,
        out_specs=[*out_specs, dw_spec, pl.BlockSpec((2, lanes), lambda j: (0, 0))],
        out_shape=[*out_shape, dw_shape, jax.ShapeDtypeStruct((2, lanes), F32)],
        scratch_shapes=[pltpu.VMEM((rows, width), F32), *extra],
        compiler_params=params(7 + part if pairwise else None),
        cost_estimate=cost(12 * rows * width * lanes, 20 * rows * width),
        name=f"close_{part}",
    )(normed, grads, w_attn, *([carry] if not first else [more] if pairwise else []), *([ending] if pairwise and final else []))


def finish_kernel(acc_ref, gr_ref, x_ref, vec_ref, out_ref, norm_ref):
    i = pl.program_id(0)
    seq = out_ref.shape[1]
    normal, inverse = centred(x_ref[...].astype(F32))
    upstream = acc_ref[...]
    grad = gr_ref[...] + norm_back(upstream, normal, inverse, vec_ref[0:1])
    out_ref[0, :, 0, :] = grad[0:seq]
    sums = [jnp.sum(upstream * normal, axis=0, keepdims=True), jnp.sum(upstream, axis=0, keepdims=True)]
    sums = jnp.concatenate(sums, axis=0)

    @pl.when(i == 0)
    def _():
        norm_ref[...] = sums

    @pl.when(i != 0)
    def _():
        norm_ref[...] += sums


def finish(acc, grad_resid, x_rows, vec, images, seq):
    rows, width = acc.shape
    block = pl.BlockSpec((rows // images, width), lambda i: (i, 0))
    return pl.pallas_call(
        finish_kernel,
        grid=(images,),
        in_specs=[block, block, block, pl.BlockSpec(vec.shape, lambda i: (0, 0))],
        out_specs=[pl.BlockSpec((1, seq, 1, width), lambda i: (i, 0, 0, 0)), pl.BlockSpec((2, width), lambda i: (0, 0))],
        out_shape=[
            jax.ShapeDtypeStruct((images, seq, 1, width), F32),
            jax.ShapeDtypeStruct((2, width), F32),
        ],
        compiler_params=params(),
        cost_estimate=cost(20 * rows * width, 14 * rows * width),
        name="finish",
    )(acc, grad_resid, x_rows, vec)


def attend_pair(seq, q, k, v):
    scale = HD**-0.5
    parts = []
    for h in range(2):
        scores = dot(q, half_lanes(k, h), NT)
        lane = lax.broadcasted_iota(jnp.int32, scores.shape, 1)
        scores = jnp.where(lane < seq, scores, -1e30)
        top = jnp.max(scores, axis=1, keepdims=True)
        raised = jnp.exp((scores - top) * scale)
        total = jnp.sum(raised, axis=1, keepdims=True)
        probs = (raised * (1.0 / total)).astype(LOW)
        parts.append(dot(probs, v))
    lane = lax.broadcasted_iota(jnp.int32, parts[0].shape, 1)
    return jnp.where(lane < HD, parts[0], parts[1]).astype(LOW)


def front_kernel(
    images, seq, alive_ref, a_in, m_in, x_ref, g_ref, vec_ref,
    a_out, m_out, n_out, qkv_out, att_out, resid_out, n2_out, g2_out, x_out,
    a_wide, m_wide, a_hold, m_hold, n_scr, qkv_scr, att_scr, w_scr, o_scr, resid_scr, n2_scr, g2_scr, x_all,
    zs, zr, xs, xr, ys, yr, xfs, xfr, yfs, yfr, cs, cr, ls, ws,
):
    g, f, z = lax.axis_index("group"), lax.axis_index("fsdp"), lax.axis_index("tensor")
    shards = lax.axis_size("tensor")
    last = shards - 1
    x_at, y_at = g % 2, g // 2
    east, north = y_at * 2 + (1 - x_at), (1 - y_at) * 2 + x_at
    depth, cols = a_in.shape[1:]
    band = depth // 4
    shared = band * 3 // 8
    rest = band - 2 * shared
    span = n_scr.shape[0] // images

    def place(column):
        cx, cy = column % 2, column // 2
        return 2 * (cx + cy - 2 * cx * cy) + cy

    mine, of_east, of_north = place(g), place(east), place(north)
    z_row = mine * band - shared * (mine % 2)
    lead_east = of_east * band + shared * (of_east % 2)
    lead_north = of_north * band + shared * (of_north % 2)
    chunks = ((a_out, 0, 3), (a_out, 3, 1), (m_out, 0, 1), (m_out, 1, 1))

    def tile(n):
        return pl.multiple_of(n, 16)

    def held(n, t, row, rows):
        out, j, many = chunks[n]
        return out.at[t, pl.ds(j, many), pl.ds(tile(f * depth + row), rows), :]

    def send(part, sems, semr, n, t, to):
        return pltpu.make_async_remote_copy(
            src_ref=part, dst_ref=part, send_sem=sems.at[n, t], recv_sem=semr.at[n, t], device_id=to, device_id_type=MESH
        )

    def along(n, t, up):
        part = held(n, t, z_row, band + shared)
        return pltpu.make_async_remote_copy(
            src_ref=part,
            dst_ref=part,
            send_sem=zs.at[n, t, 0 if up else 1],
            recv_sem=zr.at[n, t],
            device_id=(g, f, z + 1 if up else z - 1),
            device_id_type=MESH,
        )

    def to_east(n, t):
        return send(held(n, t, mine * band, band), xs, xr, n, t, (east, f, z))

    def to_north(n, t):
        return send(held(n, t, mine * band, band), ys, yr, n, t, (north, f, z))

    def north_to_east(n, t):
        return send(held(n, t, lead_north, shared), xfs, xfr, n, t, (east, f, z))

    def east_to_north(n, t):
        return send(held(n, t, lead_east + shared, rest), yfs, yfr, n, t, (north, f, z))

    def across(n, t):
        return send(held(n, t, 0, depth), cs, cr, n, t, (g, 1 - f, z))

    rows = pl.ds(tile(f * depth), depth)
    loads = (
        pltpu.make_async_copy(a_in, a_wide, ls.at[0]),
        pltpu.make_async_copy(m_in, m_wide, ls.at[1]),
    )
    keeps = (
        pltpu.make_async_copy(a_hold, a_out.at[z, :, rows, :], ls.at[2]),
        pltpu.make_async_copy(m_hold, m_out.at[z, :, rows, :], ls.at[3]),
    )
    loads[0].start()

    barrier = pltpu.get_barrier_semaphore()

    def greet(to):
        pl.semaphore_signal(barrier, inc=1, device_id=to, device_id_type=MESH)

    for to in ((east, f, z), (north, f, z), (g, 1 - f, z)):
        greet(to)

    @pl.when(z > 0)
    def _():
        greet((g, f, z - 1))

    @pl.when(z < last)
    def _():
        greet((g, f, z + 1))

    loads[0].wait()
    a_hold[...] = a_wide[...].astype(LOW)
    keeps[0].start()
    pl.semaphore_wait(barrier, 3 + jnp.minimum(z, 1) + jnp.minimum(last - z, 1))
    keeps[0].wait()

    count = len(chunks)

    def when_real(k, up, run):
        @pl.when(z - k >= 0 if up else z + k <= last)
        def _():
            run(z - k if up else z + k)

    def own(n):
        @pl.when(z < last)
        def _():
            along(n, z, True).start()

        @pl.when(z > 0)
        def _():
            along(n, z, False).start()

        across(n, z).start()

    def land(n, k, up):
        def run(t):
            along(n, t, up).wait_recv()

            @pl.when(z < last if up else z > 0)
            def _():
                along(n, t, up).start()

            to_east(n, t).start()
            to_north(n, t).start()

        when_real(k, up, run)

    def relay(n, k, up):
        def run(t):
            to_east(n, t).wait_recv()
            east_to_north(n, t).start()
            to_north(n, t).wait_recv()
            north_to_east(n, t).start()

        when_real(k, up, run)

    def finish(n, k, up):
        def run(t):
            east_to_north(n, t).wait_recv()
            north_to_east(n, t).wait_recv()
            across(n, t).start()

        when_real(k, up, run)

    def both(run, n, k):
        for up in (True, False):
            run(n, k, up)

    def fetch(t):
        return pltpu.make_async_copy(a_out.at[t, pl.ds(0, 3)], w_scr, ws.at[0])

    def maps(t):
        across(0, t).wait_recv()
        fetch(t).start()
        fetch(t).wait()
        here = pl.ds(pl.multiple_of(t * cols, cols), cols)

        def body(j, carry):
            bias = jnp.where(j == 0, vec_ref[4:5, here], jnp.where(j == 2, vec_ref[5:6, here], 0.0))
            qkv_scr[j, :, here] = (dot(n_scr[...], w_scr[j]) + bias).astype(LOW)
            return carry

        lax.fori_loop(0, 3, body, 0)

    def project(k):
        def body(d, carry):
            t = z - k + 2 * k * d

            @pl.when((t >= 0) & (t <= last))
            def _():
                maps(t)

            return carry

        lax.fori_loop(0, 2, body, 0)

    own(0)
    loads[1].start()
    n_scr[...] = jnp.zeros_like(n_scr)
    x_all[...] = jnp.zeros_like(x_all)
    g2_scr[...] = jnp.zeros_like(g2_scr)
    for i in range(images):
        here = pl.ds(i * span, seq)
        image = x_ref[:, i, :]
        x_all[here, :] = image
        normal, _ = centred(image.astype(F32))
        n_scr[here, :] = (normal * vec_ref[0:1] + vec_ref[1:2]).astype(LOW)
    puts = [pltpu.make_async_copy(n_scr, n_out, ws.at[1])]
    puts[0].start()
    puts.append(pltpu.make_async_copy(x_all, x_out, ws.at[7]))
    puts[-1].start()
    both(land, 0, 1)
    loads[1].wait()
    m_hold[...] = m_wide[...].astype(LOW)
    keeps[1].start()
    maps(z)
    for i in range(images):
        g2_scr[pl.ds(i * span, seq), :] = (g_ref[:, i, :].astype(F32) * alive_ref[i]).astype(LOW)
    both(land, 0, 2)
    both(relay, 0, 1)
    keeps[1].wait()
    both(land, 0, 3)
    for n in range(1, count):
        own(n)
    both(relay, 0, 2)
    both(finish, 0, 1)
    both(relay, 0, 3)
    both(finish, 0, 2)
    project(1)
    both(finish, 0, 3)
    project(2)

    rest_items = [(n, k) for k in range(1, last + 1) for n in range(1, count)]
    total = len(rest_items) + 2

    def advance(at):
        if at < len(rest_items):
            both(land, *rest_items[at])
        if 0 <= at - 1 < len(rest_items):
            both(relay, *rest_items[at - 1])
        if 0 <= at - 2 < len(rest_items):
            both(finish, *rest_items[at - 2])

    advance(0)
    project(3)
    puts.append(pltpu.make_async_copy(qkv_scr, qkv_out, ws.at[2]))
    puts[-1].start()

    pair = 2 * HD
    pairs = qkv_scr.shape[2] // pair
    stretch = max(pairs // 4, 1)
    segments = images * pairs // stretch

    def segment(n, carry):
        def body(m, carry):
            at = n * stretch + m
            lanes = pl.ds(pl.multiple_of(lax.rem(at, pairs) * pair, pair), pair)
            here = pl.ds(pl.multiple_of(at // pairs * span, 16), span)
            att_scr[here, lanes] = attend_pair(
                seq, qkv_scr[0, here, lanes], qkv_scr[1, here, lanes], qkv_scr[2, here, lanes]
            )
            return carry

        lax.fori_loop(0, stretch, body, 0)
        for c in range(min(segments, total - 3)):
            pl.when(n == c)(functools.partial(advance, 1 + c))
        return carry

    lax.fori_loop(0, segments, segment, 0)
    at = 1 + min(segments, total - 3)
    puts.append(pltpu.make_async_copy(att_scr, att_out, ws.at[3]))
    puts[-1].start()
    while at < total - 2:
        advance(at)
        at += 1

    for t in range(shards):
        across(1, t).wait_recv()
    take = pltpu.make_async_copy(a_out.at[:, 3], o_scr, ws.at[0])
    take.start()
    take.wait()

    def mix_image(i, carry):
        here = pl.ds(pl.multiple_of(i * span, 16), span)
        out = x_all[here, :].astype(F32) + vec_ref[6:7]
        for t in range(shards):
            out = out + dot(att_scr[here, t * cols : (t + 1) * cols], o_scr[t], NT)
        resid_scr[here, :] = out
        normal, _ = centred(out)
        n2_scr[here, :] = (normal * vec_ref[2:3] + vec_ref[3:4]).astype(LOW)
        for c in range(min(images, total - at)):
            pl.when(i == c)(functools.partial(advance, at + c))
        return carry

    lax.fori_loop(0, images, mix_image, 0)
    at += min(images, total - at)
    for n, (src, dst) in enumerate(((resid_scr, resid_out), (n2_scr, n2_out), (g2_scr, g2_out))):
        puts.append(pltpu.make_async_copy(src, dst, ws.at[4 + n]))
        puts[-1].start()
    while at < total:
        advance(at)
        at += 1
    for put in puts:
        put.wait()

    for n in range(count):
        @pl.when(z < last)
        def _():
            along(n, z, True).wait_send()

        @pl.when(z > 0)
        def _():
            along(n, z, False).wait_send()

        for t in range(shards):
            across(n, t).wait_send()
            if n > 1:
                across(n, t).wait_recv()

    def settle(n, k, up):
        def run(t):
            @pl.when(z < last if up else z > 0)
            def _():
                along(n, t, up).wait_send()

            to_east(n, t).wait_send()
            to_north(n, t).wait_send()
            east_to_north(n, t).wait_send()
            north_to_east(n, t).wait_send()

        when_real(k, up, run)

    for n in range(count):
        for k in range(1, last + 1):
            both(settle, n, k)


def front(alive, attn_master, mlp_master, patches, cotangent, vec, shards):
    _, depth, a_cols = attn_master.shape
    _, _, m_cols = mlp_master.shape
    seq, images, width = patches.shape
    rows = images * padded(seq)
    anywhere = pl.BlockSpec(memory_space=pl.ANY)
    inside = pl.BlockSpec(memory_space=pltpu.VMEM)
    dma = pltpu.SemaphoreType.DMA
    low = jax.ShapeDtypeStruct((rows, width), LOW)
    return pl.pallas_call(
        functools.partial(front_kernel, images, seq),
        in_specs=[pl.BlockSpec(memory_space=pltpu.SMEM), anywhere, anywhere, inside, inside, inside],
        out_specs=[anywhere] * 9,
        out_shape=[
            jax.ShapeDtypeStruct((shards, 4, width, a_cols), LOW),
            jax.ShapeDtypeStruct((shards, 2, width, m_cols), LOW),
            low,
            jax.ShapeDtypeStruct((3, rows, width), LOW),
            low,
            jax.ShapeDtypeStruct((rows, width), F32),
            low,
            low,
            low,
        ],
        scratch_shapes=[
            pltpu.VMEM(attn_master.shape, F32),
            pltpu.VMEM(mlp_master.shape, F32),
            pltpu.VMEM(attn_master.shape, LOW),
            pltpu.VMEM(mlp_master.shape, LOW),
            pltpu.VMEM((rows, width), LOW),
            pltpu.VMEM((3, rows, width), LOW),
            pltpu.VMEM((rows, width), LOW),
            pltpu.VMEM((3, width, a_cols), LOW),
            pltpu.VMEM((shards, width, a_cols), LOW),
            pltpu.VMEM((rows, width), F32),
            pltpu.VMEM((rows, width), LOW),
            pltpu.VMEM((rows, width), LOW),
            pltpu.VMEM((rows, width), LOW),
            dma((4, shards, 2)),
        ]
        + [dma((4, shards))] * 11
        + [dma((4,)), dma((8,))],
        compiler_params=params(1),
        cost_estimate=cost(8 * rows * width * width, 30 * rows * width),
        name="front",
    )(alive, attn_master, mlp_master, patches, cotangent, vec)


def inner_adamw(master, gradient, first, second, step_rate, decay_rate):
    first_moment = 0.9 * first + 0.1 * gradient
    second_moment = 0.95 * second + 0.05 * gradient * gradient
    step_ratio = (
        first_moment / (1.0 - 0.9**STEP) / (jnp.sqrt(second_moment / (1.0 - 0.95**STEP)) + 1e-08)
    )
    return (master - step_rate * (step_ratio + decay_rate * master), second_moment)


def outer_nesterov(master, outer_old, difference):
    momentum = OUTER_MOMENTUM * outer_old + difference
    return momentum, master - OUTER_RATE * (difference + OUTER_MOMENTUM * momentum)


def inner_kernel(join, count, *refs):
    pieces, (master_ref, moment_ref, *_, inner_ref, diff_ref) = refs[:count], refs[count:]
    gradient = join(*[piece[0] for piece in pieces]).astype(F32)
    master = master_ref[0]
    new, second = inner_adamw(master, gradient, moment_ref[0, 0, 0], moment_ref[0, 1, 0], INNER_RATE, WEIGHT_DECAY)
    inner_ref[0, 0, 0] = gradient
    inner_ref[0, 1, 0] = second
    diff_ref[0] = (master - new).astype(LOW)


def inner_step(join, pieces, unit, units, cols, master, moments, into, name):
    depth = master.shape[1]
    rows = min(depth, 524288 // cols)
    block = pl.BlockSpec((1, rows, cols), lambda u, r: (unit(u)[0], r, unit(u)[1]))
    both = pl.BlockSpec((1, 2, 1, rows, cols), lambda u, r: (0, 0, unit(u)[0], r, unit(u)[1]))
    piece_specs = [pl.BlockSpec((1, rows, piece.shape[2]), lambda u, r: (u, r, 0)) for piece in pieces]
    count = len(pieces)
    return pl.pallas_call(
        functools.partial(inner_kernel, join, count),
        grid=(units, depth // rows),
        in_specs=[*piece_specs, block, both] + ([] if into is None else [pl.BlockSpec(memory_space=pl.ANY)]),
        out_specs=[both, pl.BlockSpec((1, rows, cols), lambda u, r: (u, r, 0))],
        out_shape=[
            jax.ShapeDtypeStruct(moments.shape, F32),
            jax.ShapeDtypeStruct((units, depth, cols), LOW),
        ],
        input_output_aliases={} if into is None else {count + 2: 0},
        compiler_params=params(),
        cost_estimate=cost(30 * units * depth * cols, 24 * units * depth * cols),
        name=name,
    )(*pieces, master, moments, *([] if into is None else [into]))


def outer_kernel(groups, slots, each, g_ref, *refs):
    totals, (master_ref, outer_ref, *_, state_ref, copy_ref) = refs[:slots], refs[slots:]
    rows = copy_ref.shape[1]
    if slots == 1:
        total = totals[0][0]
    else:
        at = pl.program_id(0) * pl.num_programs(1) + pl.program_id(1)
        slot = lax.rem(g_ref[0] + groups - at // each, groups)
        here = pl.ds(pl.multiple_of(lax.rem(at, each) * rows, rows), rows)
        total = totals[0][here, :]
        for n in range(1, slots):
            total = jnp.where(slot == n, totals[n][here, :], total)
    difference = total.astype(F32) / groups
    momentum, fresh = outer_nesterov(master_ref[0], outer_ref[0], difference)
    state_ref[0, 0] = difference
    state_ref[1, 0] = momentum
    state_ref[2, 0] = fresh
    copy_ref[0] = fresh.astype(LOW)


def outer_step(groups, me, totals, unit, units, cols, master, outer_old, into, name):
    depth = master.shape[1]
    slots = len(totals)
    rows = min(depth, 524288 // cols, totals[0].shape[-2])
    each = totals[0].shape[-2] // rows
    block = pl.BlockSpec((1, rows, cols), lambda u, r, g: (unit(u)[0], r, unit(u)[1]))
    state = pl.BlockSpec((3, 1, rows, cols), lambda u, r, g: (0, unit(u)[0], r, unit(u)[1]))
    if slots == 1:
        total = pl.BlockSpec((1, rows, cols), lambda u, r, g: (u, r, 0))
    else:
        total = pl.BlockSpec(totals[0].shape, lambda u, r, g: (0, 0))
    aliased = [] if into is None else [pl.BlockSpec(memory_space=pl.ANY)] * 2
    return pl.pallas_call(
        functools.partial(outer_kernel, groups, slots, each),
        grid_spec=pltpu.PrefetchScalarGridSpec(
            num_scalar_prefetch=1,
            grid=(units, depth // rows),
            in_specs=[*[total] * slots, block, block, *aliased],
            out_specs=[state, block],
        ),
        out_shape=[
            jax.ShapeDtypeStruct((3, *master.shape), F32),
            jax.ShapeDtypeStruct(master.shape, LOW),
        ],
        input_output_aliases={} if into is None else {slots + 3: 0, slots + 4: 1},
        compiler_params=params(),
        cost_estimate=cost(10 * units * depth * cols, 24 * units * depth * cols),
        name=name,
    )(me, *totals, master, outer_old, *([] if into is None else into))


def group_kernel(groups, shards, vectors, diff_ref, *refs):
    if vectors:
        part_ref, master_ref, moment_ref, outer_ref, total_ref, inner_ref, state_ref, copy_ref, *refs = refs
    else:
        total_ref, *refs = refs
    landed, summed, sends, receives, sends_two, receives_two, *small = refs
    g, f, t = lax.axis_index("group"), lax.axis_index("fsdp"), lax.axis_index("tensor")
    span = landed.shape[1]

    def rows(n):
        return pl.ds(pl.multiple_of(n * span, span), span)

    def other(k):
        return lax.rem(g + k, groups)

    def back(k):
        return lax.rem(g + groups - k, groups)

    def copy(src, dst, sems, semr, k, to):
        return pltpu.make_async_remote_copy(
            src_ref=src, dst_ref=dst, send_sem=sems.at[k], recv_sem=semr.at[k], device_id=to, device_id_type=MESH
        )

    def part(k):
        return copy(diff_ref.at[rows(other(k)), :], landed.at[k], sends, receives, k, (other(k), f, t))

    def result(k):
        return copy(summed, landed.at[groups + k], sends_two, receives_two, k, (other(k), f, t))

    barrier = pltpu.get_barrier_semaphore()
    for k in range(1, groups):
        pl.semaphore_signal(barrier, inc=1, device_id=(other(k), f, t), device_id_type=MESH)
    if vectors:
        stage, pair, mine, line, whole, few, diffs, ss, rs, ls, lr, gs, gr = small
        half = part_ref.shape[0] // 2
        halves = (pl.ds(0, half), pl.ds(half, half))

        def pick(ref):
            return jnp.where(f == 0, ref[halves[0], :], ref[halves[1], :])

        def line_copy(k):
            return copy(mine, line.at[k], ls, lr, k, (g, f, lax.rem(t + k, shards)))

        def few_copy(k):
            return copy(diffs.at[f], few.at[k], gs, gr, k, (other(k), f, t))

        pair_copy = copy(stage.at[1 - f], pair, ss, rs, 0, partner())
        whole_copy = copy(whole.at[f], whole.at[f], ss, rs, 1, partner())
        final_copy = copy(mine, stage.at[f], ss, rs, 2, partner())
        pl.semaphore_signal(barrier, inc=1, device_id=partner(), device_id_type=MESH)
        for k in range(1, shards):
            pl.semaphore_signal(barrier, inc=1, device_id=(g, f, lax.rem(t + k, shards)), device_id_type=MESH)
        stage[...] = jnp.zeros_like(stage)
        diffs[...] = jnp.zeros_like(diffs)
        for n in range(2):
            stage[n, 0:half] = part_ref[halves[n], :]
    pl.semaphore_wait(barrier, groups - 1 + (shards if vectors else 0))

    for k in range(1, groups):
        part(k).start()
    if vectors:
        pair_copy.start()
        pair_copy.wait()
        mine[...] = stage[f] + pair[...]
        for k in range(1, shards):
            line_copy(k).start()
        line[0] = mine[...]
        for k in range(1, shards):
            line_copy(k).wait()
        gradient = jnp.zeros(mine.shape, F32)
        for n in range(shards):
            gradient = gradient + line[lax.rem(t + shards - n, shards)]
        whole[f] = gradient
        whole_copy.start()
        new, _ = inner_adamw(
            pick(master_ref), gradient[0:half], pick(moment_ref.at[0]), pick(moment_ref.at[1]), VECTOR_RATE, 0.0
        )
        diffs[f, 0:half] = pick(master_ref) - new
        for k in range(1, groups):
            few_copy(k).start()
        few[0] = diffs[f]
        whole_copy.wait()
        for n in range(2):
            own = whole[n, 0:half]
            _, second = inner_adamw(
                master_ref[halves[n], :], own, moment_ref[0, halves[n], :], moment_ref[1, halves[n], :], VECTOR_RATE, 0.0
            )
            inner_ref[0, halves[n], :] = own
            inner_ref[1, halves[n], :] = second
    total = diff_ref[rows(g), :].astype(F32)
    for k in range(1, groups):
        part(k).wait_recv()
        total = total + landed[k].astype(F32)
    summed[...] = total.astype(LOW)
    for k in range(1, groups):
        result(k).start()
    total_ref[rows(g), :] = summed[...]
    if vectors:
        for k in range(1, groups):
            few_copy(k).wait()
        difference = jnp.zeros(mine.shape, F32)
        for n in range(groups):
            difference = difference + few[lax.rem(g + groups - n, groups)]
        mine[...] = difference / groups
        stage[f] = mine[...]
        final_copy.start()
        final_copy.wait()
        for n in range(2):
            difference = stage[n, 0:half]
            momentum, fresh = outer_nesterov(master_ref[halves[n], :], outer_ref[halves[n], :], difference)
            state_ref[0, halves[n], :] = difference
            state_ref[1, halves[n], :] = momentum
            state_ref[2, halves[n], :] = fresh
            copy_ref[halves[n], :] = fresh.astype(LOW)
    for k in range(1, groups):
        result(k).wait_recv()
        total_ref[rows(back(k)), :] = landed[groups + k]
    for k in range(1, groups):
        part(k).wait_send()
        result(k).wait_send()


def group_sum(diff, groups, identity, name, vectors=None, shards=0):
    flat = diff.reshape(-1, diff.shape[-1])
    span, cols = flat.shape[0] // groups, flat.shape[1]
    dma = pltpu.SemaphoreType.DMA
    whole = pl.BlockSpec(memory_space=pltpu.VMEM)
    out_shape = [jax.ShapeDtypeStruct(flat.shape, LOW)]
    extra = []
    if vectors:
        shape = vectors[0].shape
        half = (-(-shape[0] // 16) * 8, shape[1])
        out_shape += [
            jax.ShapeDtypeStruct((2, *shape), F32),
            jax.ShapeDtypeStruct((3, *shape), F32),
            jax.ShapeDtypeStruct(shape, LOW),
        ]
        extra = [
            pltpu.VMEM((2, *half), F32),
            pltpu.VMEM(half, F32),
            pltpu.VMEM(half, F32),
            pltpu.VMEM((shards, *half), F32),
            pltpu.VMEM((2, *half), F32),
            pltpu.VMEM((groups, *half), F32),
            pltpu.VMEM((2, *half), F32),
            dma((3,)),
            dma((3,)),
            dma((shards,)),
            dma((shards,)),
            dma((groups,)),
            dma((groups,)),
        ]
    total, *rest = pl.pallas_call(
        functools.partial(group_kernel, groups, shards, bool(vectors)),
        in_specs=[whole] * (5 if vectors else 1),
        out_specs=[whole] * len(out_shape),
        out_shape=out_shape,
        scratch_shapes=[
            pltpu.VMEM((2 * groups, span, cols), LOW),
            pltpu.VMEM((span, cols), LOW),
            *[dma((groups,))] * 4,
            *extra,
        ],
        compiler_params=params(identity),
        cost_estimate=cost(4 * flat.size, 8 * flat.size),
        name=name,
    )(flat, *(vectors or []))
    return total.reshape(diff.shape), *rest


def gather_weights(shard):
    whole = lax.all_gather(shard, "tensor", axis=0)
    return lax.all_gather(whole, "fsdp", axis=2, tiled=True)


def around(array, k, groups):
    return lax.ppermute(array, "group", [(i, (i + k) % groups) for i in range(groups)])


def exchange_parts(diff, groups):
    g = lax.axis_index("group")
    quarters = diff.reshape(groups, -1, diff.shape[-1])
    parts = [lax.dynamic_index_in_dim(quarters, lax.rem(g + k, groups), 0, keepdims=False) for k in range(groups)]
    total = sum([around(parts[k], k, groups).astype(F32) for k in range(1, groups)], parts[0].astype(F32))
    return total.astype(LOW)


def exchange_total(own, groups):
    return [own] + [around(own, k, groups) for k in range(1, groups)]


def scatter_gradient(gradient):
    half = gradient if gradient.ndim == 4 else lax.psum_scatter(gradient, "fsdp", scatter_dimension=0)
    return lax.psum_scatter(half, "tensor", scatter_dimension=0)


def local(
    patches,
    output_grad,
    live_counts,
    attn_master,
    mlp_master,
    vector_master,
    attn_moments,
    mlp_moments,
    vector_moments,
    attn_outer,
    mlp_outer,
    vector_outer,
):
    vec = vector_master
    tensor_size, fsdp = lax.axis_size("tensor"), lax.axis_size("fsdp")
    groups = lax.axis_size("group")
    local_images, seq, width = patches.shape[2:]
    slot = (lax.axis_index("fsdp") * tensor_size + lax.axis_index("tensor")) * local_images
    slot = slot + jnp.arange(local_images)
    counts = jnp.take(live_counts[0], slot // IMG_DEV, axis=1)
    alive = ((slot % IMG_DEV)[None, :] < counts).astype(F32).reshape(-1)
    x = patches.reshape(-1, seq, width)
    cotangent = output_grad.reshape(-1, seq, width)
    images = x.shape[0]

    if (groups, fsdp) == (4, 2):
        beside_images = [
            jnp.moveaxis(v.reshape(images, seq, width), 0, 1) for v in (patches, output_grad)
        ]
        w_attn, w_mlp, normed_one, qkv, attended, resid, normed_two, grad_two, x_rows = front(
            alive, attn_master, mlp_master, *beside_images, vec, tensor_size
        )
    else:
        w_attn = gather_weights(attn_master.astype(LOW))
        w_mlp = gather_weights(mlp_master.astype(LOW))
        normed_one, qkv = project(x, w_attn, vec)
        attended = attend(qkv, images, seq)
        resid, normed_two, grad_two = mix(alive, attended, x, cotangent, w_attn, vec)
        x_rows = jnp.pad(x, ((0, 0), (0, padded(seq) - seq), (0, 0))).reshape(-1, width)
    bias = vec[8:].reshape(tensor_size, 1, -1)
    carried = None
    mlp_grads, bias_parts = [], []
    for part, (start, cols) in enumerate(PIECES):
        *carried, dw, db = mlp(part, start, cols, normed_two, grad_two, w_mlp, bias, carried, fsdp)
        mlp_grads.append(scatter_gradient(dw))
        bias_parts.append(db)
    branch, grad_normed = carried
    block_output, grad_resid, grad_attended, dw_out, sums_two = turn(
        alive, resid, branch, grad_normed, grad_two, attended, w_attn, vec, images, seq, fsdp
    )
    def beside(*parts):
        return jnp.concatenate(parts, axis=-1)

    pairwise = fsdp == 2
    me = lax.axis_index("group").astype(jnp.int32).reshape(1)
    half = attn_master.shape[2] // PARTS
    grads = unattend(qkv, grad_attended, images, seq, 0, PARTS, tensor_size)
    grads, mlp_grads[0] = lax.optimization_barrier((grads, mlp_grads[0]))
    carry, dw_early, head_sums = close(
        0, PARTS, normed_one, grads, w_attn, None, dw_out, None, fsdp, groups
    )
    if not pairwise:
        halves = jnp.moveaxis(dw_out.reshape(*dw_out.shape[:-1], PARTS, half), -2, 2)
        dw_early = jnp.concatenate([dw_early, halves[:, :, :, 0]], axis=2)
    early_grad = scatter_gradient(dw_early)
    head_sums = [head_sums]
    carry, mlp_grads[1] = lax.optimization_barrier((carry, mlp_grads[1]))
    grads = unattend(qkv, grad_attended, images, seq, 1, PARTS, tensor_size)

    mlp_grads[0], grads = lax.optimization_barrier((mlp_grads[0], grads))
    mlp_inner, mlp_diff = inner_step(
        beside, mlp_grads, lambda u: (u, 0), 2, mlp_master.shape[2], mlp_master, mlp_moments, None, "inner_mlp"
    )
    carry, mlp_diff = lax.optimization_barrier((carry, mlp_diff))
    ending = mlp_diff.reshape(-1, mlp_diff.shape[-1])
    carry, *mlp_own, dw_late, sums = close(
        1, PARTS, normed_one, grads, w_attn, carry, None, ending, fsdp, groups
    )
    patches_grad, sums_one = finish(carry, grad_resid, x_rows, vec, images, seq)
    if not pairwise:
        mlp_own = [exchange_parts(mlp_diff, groups)]
    mlp_total = exchange_total(mlp_own[0], groups)
    late_grad = scatter_gradient(dw_late)
    head_sums.append(sums)

    def early(u):
        return jnp.minimum(u, 3), jnp.maximum(u - 3, 0)

    def late(u):
        return u, 1

    def first(piece):
        return piece

    attn_inner, early_diff = inner_step(
        first, [early_grad], early, 3 + PARTS, half, attn_master, attn_moments, None, "inner_early"
    )
    head_rows = jnp.concatenate([v.reshape(2, tensor_size, -1) for v in head_sums], axis=-1).reshape(2, width)
    hidden_bias = jnp.concatenate(bias_parts, axis=-1).reshape(-1, width)
    vector_part = jnp.concatenate([sums_one, sums_two[:2], head_rows, sums_two[2:], hidden_bias])

    if pairwise:
        early_total, vector_inner, vector_state, vector_copy = group_sum(
            early_diff,
            groups,
            10,
            "group_early",
            [vector_part, vec, vector_moments[0], vector_outer],
            tensor_size,
        )
    else:
        (early_total,) = group_sum(early_diff, groups, 10, "group_early")
        vector_grad = lax.psum(vector_part, ("fsdp", "tensor"))
        new_vector, second_vector = inner_adamw(
            vec, vector_grad, vector_moments[0, 0], vector_moments[0, 1], VECTOR_RATE, 0.0
        )
        diff_vector = lax.psum(vec - new_vector, "group") / groups
        momentum, fresh = outer_nesterov(vec, vector_outer, diff_vector)
        vector_inner = jnp.stack([vector_grad, second_vector])
        vector_state, vector_copy = jnp.stack([diff_vector, momentum, fresh]), fresh.astype(LOW)
    attn_state, attn_copy = outer_step(
        groups, me, [early_total], early, 3 + PARTS, half, attn_master, attn_outer, None, "outer_early"
    )
    attn_copy, *mlp_total = lax.optimization_barrier((attn_copy, *mlp_total))
    mlp_state, mlp_copy = outer_step(
        groups,
        me,
        mlp_total,
        lambda u: (u, 0),
        2,
        mlp_master.shape[2],
        mlp_master,
        mlp_outer,
        None,
        "outer_mlp",
    )
    late_grad, mlp_state = lax.optimization_barrier((late_grad, mlp_state))
    attn_inner, late_diff = inner_step(
        first, [late_grad], late, 3, half, attn_master, attn_moments, attn_inner, "inner_late"
    )
    (late_total,) = group_sum(late_diff, groups, 11, "group_late")
    attn_state, attn_copy = outer_step(
        groups, me, [late_total], late, 3, half, attn_master, attn_outer, (attn_state, attn_copy), "outer_late"
    )
    return (
        block_output.reshape(patches.shape),
        patches_grad.reshape(patches.shape),
        attn_inner,
        attn_state,
        attn_copy,
        mlp_inner,
        mlp_state,
        mlp_copy,
        vector_inner[None],
        vector_state,
        vector_copy,
    )


def solution(mesh):
    placed = (
        P("group", None, ("fsdp", "tensor"), None, None),
        P("group", None, ("fsdp", "tensor"), None, None),
        P("group", None, None),
        P(None, "fsdp", "tensor"),
        P(None, "fsdp", "tensor"),
        P(),
        P("group", None, None, "fsdp", "tensor"),
        P("group", None, None, "fsdp", "tensor"),
        P("group", None, None, None),
        P(None, "fsdp", "tensor"),
        P(None, "fsdp", "tensor"),
        P(),
    )
    return jax.shard_map(
        local,
        mesh=mesh,
        in_specs=placed,
        out_specs=(
            P("group", None, ("fsdp", "tensor"), None, None),
            P("group", None, ("fsdp", "tensor"), None, None),
            P("group", None, None, "fsdp", "tensor"),
            P(None, None, "fsdp", "tensor"),
            P(None, "fsdp", "tensor"),
            P("group", None, None, "fsdp", "tensor"),
            P(None, None, "fsdp", "tensor"),
            P(None, "fsdp", "tensor"),
            P("group", None, None, None),
            P(),
            P(),
        ),
        check_vma=False,
    )
```

```python
import functools

import jax
import jax.numpy as jnp
from jax import lax
from jax.experimental import pallas as pl
from jax.experimental.pallas import tpu as pltpu
from jax.sharding import PartitionSpec as P

HD = 64
STEP = 8
IMG_DEV = 4
EPSILON = 1e-06
INNER_RATE = 0.02
VECTOR_RATE = 0.2
WEIGHT_DECAY = 0.1
OUTER_RATE = 0.7
OUTER_MOMENTUM = 0.9
PIECES = ((0, 256), (256, 256), (512, 512))
PARTS = 2
LOW = jnp.bfloat16
F32 = jnp.float32
NN = (((1,), (0,)), ((), ()))
NT = (((1,), (1,)), ((), ()))
TN = (((0,), (0,)), ((), ()))


def dot(a, b, dims=NN):
    return lax.dot_general(a, b, dims, preferred_element_type=F32)


MESH = pl.DeviceIdType.MESH


def params(identity=None):
    if identity is None:
        return pltpu.CompilerParams(vmem_limit_bytes=60 * 2**20)
    return pltpu.CompilerParams(vmem_limit_bytes=60 * 2**20, collective_id=identity, has_side_effects=True)


def partner():
    return (lax.axis_index("group"), 1 - lax.axis_index("fsdp"), lax.axis_index("tensor"))


def greet_partner():
    barrier = pltpu.get_barrier_semaphore()
    pl.semaphore_signal(barrier, inc=1, device_id=partner(), device_id_type=MESH)
    pl.semaphore_wait(barrier, 1)


def to_partner(sent, received, sends, receives, n):
    return pltpu.make_async_remote_copy(
        src_ref=sent.at[n],
        dst_ref=received.at[n],
        send_sem=sends.at[n],
        recv_sem=receives.at[n],
        device_id=partner(),
        device_id_type=MESH,
    )


def bands(depth):
    f = lax.axis_index("fsdp")
    return pl.ds(pl.multiple_of(f * depth, depth), depth), pl.ds(pl.multiple_of((1 - f) * depth, depth), depth)


def exchange_scratch(steps, shape):
    dma = pltpu.SemaphoreType.DMA
    return [
        pltpu.VMEM((steps, *shape), F32),
        pltpu.VMEM((steps, *shape), LOW),
        pltpu.VMEM((steps, *shape), LOW),
        dma((steps,)),
        dma((steps,)),
    ]


def cost(flops, moved, special=0):
    return pl.CostEstimate(flops=int(flops), bytes_accessed=int(moved), transcendentals=int(special))


def padded(rows):
    return -(-rows // 16) * 16


def centred(source):
    centre = source - jnp.mean(source, axis=-1, keepdims=True)
    spread = jnp.mean(centre * centre, axis=-1, keepdims=True)
    inverse = lax.rsqrt(spread + EPSILON)
    return centre * inverse, inverse


def norm_back(upstream, normal, inverse, gain):
    pulled = upstream * gain
    mean_one = jnp.mean(pulled, axis=-1, keepdims=True)
    mean_two = jnp.mean(pulled * normal, axis=-1, keepdims=True)
    return inverse * (pulled - mean_one - normal * mean_two)


def project_kernel(images, seq, x_ref, w_ref, vec_ref, n_ref, out_ref, n_scr):
    j, t = pl.program_id(0), pl.program_id(1)
    span = n_scr.shape[0] // images

    @pl.when((j == 0) & (t == 0))
    def _():
        n_scr[...] = jnp.zeros_like(n_scr)
        for i in range(images):
            normal, _ = centred(x_ref[i].astype(F32))
            n_scr[pl.ds(i * span, seq), :] = (normal * vec_ref[0:1] + vec_ref[1:2]).astype(LOW)
        n_ref[...] = n_scr[...]

    cols = out_ref.shape[-1]
    out = dot(n_scr[...], w_ref[0, 0])
    at = pl.ds(pl.multiple_of(t * cols, cols), cols)
    bias = jnp.where(j == 0, vec_ref[4:5, at], jnp.where(j == 2, vec_ref[5:6, at], 0.0))
    out_ref[0] = (out + bias).astype(LOW)


def project(patches, w_attn, vec):
    images, seq, width = patches.shape
    shards, _, _, cols = w_attn.shape
    rows = images * padded(seq)
    return pl.pallas_call(
        functools.partial(project_kernel, images, seq),
        grid=(3, shards),
        in_specs=[
            pl.BlockSpec((images, seq, width), lambda j, t: (0, 0, 0)),
            pl.BlockSpec((1, 1, width, cols), lambda j, t: (t, j, 0, 0)),
            pl.BlockSpec(vec.shape, lambda j, t: (0, 0)),
        ],
        out_specs=[
            pl.BlockSpec((rows, width), lambda j, t: (0, 0)),
            pl.BlockSpec((1, rows, cols), lambda j, t: (j, 0, t)),
        ],
        out_shape=[
            jax.ShapeDtypeStruct((rows, width), LOW),
            jax.ShapeDtypeStruct((3, rows, width), LOW),
        ],
        scratch_shapes=[pltpu.VMEM((rows, width), LOW)],
        compiler_params=params(),
        cost_estimate=cost(6 * rows * width * width, 16 * rows * width),
        name="project",
    )(patches, w_attn, vec)


def half_lanes(value, which):
    lane = lax.broadcasted_iota(jnp.int32, value.shape, 1)
    return jnp.where((lane >= HD) == bool(which), value, jnp.zeros_like(value))


def attend_kernel(seq, q_ref, k_ref, v_ref, out_ref):
    span = q_ref.shape[1]
    scale = HD**-0.5
    q, k, v = q_ref[0], k_ref[0], v_ref[0]
    parts = []
    for h in range(2):
        scores = dot(q, half_lanes(k, h), NT)
        lane = lax.broadcasted_iota(jnp.int32, scores.shape, 1)
        scores = jnp.where(lane < seq, scores, -1e30)
        top = jnp.max(scores, axis=1, keepdims=True)
        raised = jnp.exp((scores - top) * scale)
        total = jnp.sum(raised, axis=1, keepdims=True)
        probs = (raised * (1.0 / total)).astype(LOW)
        parts.append(dot(probs, v))
    lane = lax.broadcasted_iota(jnp.int32, (span, 2 * HD), 1)
    out_ref[...] = jnp.where(lane < HD, parts[0], parts[1]).astype(LOW)


def attend(qkv, images, seq):
    _, rows, width = qkv.shape
    span = rows // images
    pair = 2 * HD

    def take(j):
        return pl.BlockSpec((1, span, pair), lambda i, h: (j, i, h))

    return pl.pallas_call(
        functools.partial(attend_kernel, seq),
        grid=(images, width // pair),
        in_specs=[take(0), take(1), take(2)],
        out_specs=pl.BlockSpec((span, pair), lambda i, h: (i, h)),
        out_shape=jax.ShapeDtypeStruct((rows, width), LOW),
        compiler_params=params(),
        cost_estimate=cost(16 * rows * span * width, 8 * rows * width, rows * span * (width // HD)),
        name="attend",
    )(qkv, qkv, qkv)


def mix_kernel(seq, alive_ref, att_ref, x_ref, g_ref, w_ref, vec_ref, resid_ref, n_ref, g2_ref, x_scr):
    i = pl.program_id(0)
    shards, _, _, cols = w_ref.shape
    x_scr[...] = jnp.zeros_like(x_scr)
    x_scr[0:seq, :] = x_ref[0].astype(F32)
    total = x_scr[...] + vec_ref[6:7]
    for t in range(shards):
        total = total + dot(att_ref[:, t * cols : (t + 1) * cols], w_ref[t, 0], NT)
    resid_ref[...] = total
    normal, _ = centred(total)
    n_ref[...] = (normal * vec_ref[2:3] + vec_ref[3:4]).astype(LOW)
    x_scr[0:seq, :] = g_ref[0].astype(F32) * alive_ref[i]
    g2_ref[...] = x_scr[...].astype(LOW)


def mix(alive, attended, patches, cotangent, w_attn, vec):
    images, seq, width = patches.shape
    rows = attended.shape[0]
    span = rows // images
    shards, _, _, cols = w_attn.shape
    block = pl.BlockSpec((span, width), lambda i: (i, 0))
    whole = jax.ShapeDtypeStruct((rows, width), LOW)
    return pl.pallas_call(
        functools.partial(mix_kernel, seq),
        grid=(images,),
        in_specs=[
            pl.BlockSpec(memory_space=pltpu.SMEM),
            block,
            pl.BlockSpec((1, seq, width), lambda i: (i, 0, 0)),
            pl.BlockSpec((1, seq, width), lambda i: (i, 0, 0)),
            pl.BlockSpec((shards, 1, width, cols), lambda i: (0, 3, 0, 0)),
            pl.BlockSpec(vec.shape, lambda i: (0, 0)),
        ],
        out_specs=[block, block, block],
        out_shape=[jax.ShapeDtypeStruct((rows, width), F32), whole, whole],
        scratch_shapes=[pltpu.VMEM((span, width), F32)],
        compiler_params=params(),
        cost_estimate=cost(2 * rows * width * width, 16 * rows * width),
        name="mix",
    )(alive, attended, patches, cotangent, w_attn, vec)


def mlp_kernel(first, pairwise, n_ref, g_ref, w1_ref, w2_ref, bias_ref, *refs):
    if not first:
        yi_ref, gi_ref, *refs = refs
    y_ref, gn_ref, dw_ref, db_ref, h_scr, p_scr, loaded, *exchange = refs
    step = pl.program_id(0)
    each, _, width, cols = w1_ref.shape
    if not first:
        loads = (
            pltpu.make_async_copy(yi_ref, y_ref, loaded.at[0]),
            pltpu.make_async_copy(gi_ref, gn_ref, loaded.at[1]),
        )

    @pl.when(step == 0)
    def _():
        if not first:
            for load in loads:
                load.start()
        else:
            y_ref[...] = jnp.zeros_like(y_ref)
            gn_ref[...] = jnp.zeros_like(gn_ref)
        if pairwise:
            greet_partner()

    w1 = jnp.concatenate([w1_ref[t, 0] for t in range(each)], axis=1)
    w2 = jnp.concatenate([w2_ref[t, 0] for t in range(each)], axis=1)
    bias = jnp.concatenate([bias_ref[t] for t in range(each)], axis=1)
    pre = dot(n_ref[...], w1) + bias
    cdf = 0.5 * (1.0 + lax.erf(pre * 0.7071067811865476))
    h_scr[...] = (pre * cdf).astype(LOW)
    slope = cdf + pre * jnp.exp(-0.5 * pre * pre) * 0.3989422804014327
    p_scr[...] = (dot(g_ref[...], w2) * slope).astype(LOW)
    sums = jnp.sum(p_scr[...].astype(F32), axis=0, keepdims=True)
    for t in range(each):
        db_ref[t] = sums[:, t * cols : (t + 1) * cols]

    if pairwise:
        own, sent, received, sends, receives = exchange
        ours, theirs = bands(width // 2)

        slot = lax.rem(step, 2)

        def collect(n):
            at = lax.rem(n, 2)
            to_partner(sent, received, sends, receives, at).wait()
            for which in range(2):
                total = (own[at, which] + received[at, which].astype(F32)).astype(LOW)
                for t in range(each):
                    dw_ref[n * each + t, which] = total[:, t * cols : (t + 1) * cols]

        @pl.when(step > 0)
        def _():
            collect(step - 1)

        sent[slot, 0] = dot(n_ref[:, theirs], p_scr[...], TN).astype(LOW)
        sent[slot, 1] = dot(g_ref[:, theirs], h_scr[...], TN).astype(LOW)
        to_partner(sent, received, sends, receives, slot).start()
        own[slot, 0] = dot(n_ref[:, ours], p_scr[...], TN)
        own[slot, 1] = dot(g_ref[:, ours], h_scr[...], TN)

    else:
        shards, depth = dw_ref.shape[0], dw_ref.shape[3]
        d1 = dot(n_ref[...], p_scr[...], TN).astype(LOW)
        d2 = dot(g_ref[...], h_scr[...], TN).astype(LOW)
        for f in range(shards):
            for t in range(each):
                dw_ref[f, t, 0] = d1[f * depth : (f + 1) * depth, t * cols : (t + 1) * cols]
                dw_ref[f, t, 1] = d2[f * depth : (f + 1) * depth, t * cols : (t + 1) * cols]

    if not first:

        @pl.when(step == 0)
        def _():
            for load in loads:
                load.wait()

    y_ref[...] += dot(h_scr[...], w2, NT)
    gn_ref[...] += dot(p_scr[...], w1, NT)
    if pairwise:

        @pl.when(step == pl.num_programs(0) - 1)
        def _():
            collect(step)


def mlp(part, start, cols, normed, grad_two, w_mlp, bias, carried, fsdp):
    rows, width = normed.shape
    shards = w_mlp.shape[0]
    each = max(512 // cols, 1)
    at = start // cols
    first, pairwise = carried is None, fsdp == 2
    single = pl.Buffered(1)
    full = pl.BlockSpec((rows, width), lambda s: (0, 0), pipeline_mode=single)
    depth = width // fsdp
    steps = shards // each
    acc_shape = jax.ShapeDtypeStruct((rows, width), F32)
    if pairwise:
        out_w = pl.BlockSpec((shards, 2, depth, cols), lambda s: (0, 0, 0, 0), pipeline_mode=single)
        w_shape = jax.ShapeDtypeStruct((shards, 2, depth, cols), LOW)
        extra = exchange_scratch(2, (2, depth, each * cols))
    else:
        out_w = pl.BlockSpec((fsdp, each, 2, depth, cols), lambda s: (0, s, 0, 0, 0))
        w_shape = jax.ShapeDtypeStruct((fsdp, shards, 2, depth, cols), LOW)
        extra = []
    return pl.pallas_call(
        functools.partial(mlp_kernel, first, pairwise),
        grid=(steps,),
        in_specs=[
            full,
            full,
            pl.BlockSpec((each, 1, width, cols), lambda s: (s, 0, 0, at)),
            pl.BlockSpec((each, 1, width, cols), lambda s: (s, 1, 0, at)),
            pl.BlockSpec((each, 1, cols), lambda s: (s, 0, at)),
        ]
        + ([] if first else [pl.BlockSpec(memory_space=pl.ANY)] * 2),
        out_specs=[full, full, out_w, pl.BlockSpec((each, 1, cols), lambda s: (s, 0, 0))],
        out_shape=[acc_shape, acc_shape, w_shape, jax.ShapeDtypeStruct((shards, 1, cols), F32)],
        scratch_shapes=[
            pltpu.VMEM((rows, each * cols), LOW),
            pltpu.VMEM((rows, each * cols), LOW),
            pltpu.SemaphoreType.DMA((2,)),
            *extra,
        ],
        compiler_params=params(2 + part if pairwise else None),
        cost_estimate=cost(12 * rows * width * cols * shards, 24 * rows * width),
        name=f"mlp_{part}",
    )(normed, grad_two, w_mlp, w_mlp, bias, *([] if first else carried))


def turn_kernel(seq, pairwise, alive_ref, resid_ref, y_ref, gn_ref, g2_ref, att_ref, w_ref, vec_ref,
                out_ref, gr_ref, ga_ref, dw_ref, sums_ref, dw_scr, *exchange):
    i = pl.program_id(0)
    if pairwise:
        pl.when(i == 0)(greet_partner)
    shards, _, _, cols = w_ref.shape
    resid = resid_ref[...]
    out_ref[0] = ((resid + y_ref[...] + vec_ref[7:8]) * alive_ref[i]).astype(LOW)[0:seq]
    normal, inverse = centred(resid)
    upstream = gn_ref[...]
    grad_out = g2_ref[...].astype(F32)
    grad_resid = grad_out + norm_back(upstream, normal, inverse, vec_ref[2:3])
    gr_ref[...] = grad_resid
    low = grad_resid.astype(LOW)
    rows = [
        jnp.sum(upstream * normal, axis=0, keepdims=True),
        jnp.sum(upstream, axis=0, keepdims=True),
        jnp.sum(grad_resid, axis=0, keepdims=True),
        jnp.sum(grad_out, axis=0, keepdims=True),
    ]
    rows = jnp.concatenate(rows, axis=0)

    @pl.when(i == 0)
    def _():
        sums_ref[...] = rows

    @pl.when(i != 0)
    def _():
        sums_ref[...] += rows

    for t in range(shards):
        ga_ref[:, t * cols : (t + 1) * cols] = dot(low, w_ref[t, 0]).astype(LOW)
    part = dot(low, att_ref[...], TN)

    @pl.when(i == 0)
    def _():
        dw_scr[...] = part

    @pl.when(i != 0)
    def _():
        dw_scr[...] += part

    @pl.when(i == pl.num_programs(0) - 1)
    def _():
        if pairwise:
            sent, received, sends, receives = exchange
            ours, theirs = bands(dw_scr.shape[0] // 2)
            sent[0] = dw_scr[theirs, :].astype(LOW)
            copy = to_partner(sent, received, sends, receives, 0)
            copy.start()
            copy.wait()
            total = (dw_scr[ours, :] + received[0].astype(F32)).astype(LOW)
            for t in range(shards):
                dw_ref[t, 0] = total[:, t * cols : (t + 1) * cols]
            return
        depth = dw_ref.shape[3]
        for f in range(dw_ref.shape[0]):
            for t in range(shards):
                dw_ref[f, t, 0] = dw_scr[f * depth : (f + 1) * depth, t * cols : (t + 1) * cols].astype(LOW)


def turn(alive, resid, branch, grad_normed, grad_two, attended, w_attn, vec, images, seq, fsdp):
    rows, width = resid.shape
    span = rows // images
    shards, _, _, cols = w_attn.shape
    depth = width // fsdp
    pairwise = fsdp == 2
    lead = () if pairwise else (fsdp,)
    block = pl.BlockSpec((span, width), lambda i: (i, 0))
    return pl.pallas_call(
        functools.partial(turn_kernel, seq, pairwise),
        grid=(images,),
        in_specs=[
            pl.BlockSpec(memory_space=pltpu.SMEM),
            block, block, block, block, block,
            pl.BlockSpec((shards, 1, width, cols), lambda i: (0, 3, 0, 0)),
            pl.BlockSpec(vec.shape, lambda i: (0, 0)),
        ],
        out_specs=[
            pl.BlockSpec((1, seq, width), lambda i: (i, 0, 0)),
            block, block,
            pl.BlockSpec((*lead, shards, 1, depth, cols), lambda i: (0,) * (4 + len(lead))),
            pl.BlockSpec((4, width), lambda i: (0, 0)),
        ],
        out_shape=[
            jax.ShapeDtypeStruct((images, seq, width), LOW),
            jax.ShapeDtypeStruct((rows, width), F32),
            jax.ShapeDtypeStruct((rows, width), LOW),
            jax.ShapeDtypeStruct((*lead, shards, 1, depth, cols), LOW),
            jax.ShapeDtypeStruct((4, width), F32),
        ],
        scratch_shapes=[pltpu.VMEM((width, width), F32)] + (exchange_scratch(1, (depth, width))[1:] if pairwise else []),
        compiler_params=params(6 if pairwise else None),
        cost_estimate=cost(4 * rows * width * width, 24 * rows * width),
        name="turn",
    )(alive, resid, branch, grad_normed, grad_two, attended, w_attn, vec)


def unattend_kernel(seq, q_ref, k_ref, v_ref, g_ref, out_ref):
    span = q_ref.shape[1]
    scale = HD**-0.5
    q, k, v, g = q_ref[0], k_ref[0], v_ref[0], g_ref[...]
    parts = []
    for h in range(2):
        scores = dot(half_lanes(k, h), q, NT)
        row = lax.broadcasted_iota(jnp.int32, scores.shape, 0)
        scores = jnp.where(row < seq, scores, -1e30)
        top = jnp.max(scores, axis=0, keepdims=True)
        raised = jnp.exp((scores - top) * scale)
        total = jnp.sum(raised, axis=0, keepdims=True)
        probs = raised * (1.0 / total)
        gp = dot(half_lanes(v, h), g, NT)
        delta = jnp.sum(probs * gp, axis=0, keepdims=True)
        gs = (probs * (gp - delta)).astype(LOW)
        dv = dot(probs.astype(LOW), g)
        dk = dot(gs, q)
        dq = dot(gs, k, TN)
        parts.append((dq, dk, dv))
    lane = lax.broadcasted_iota(jnp.int32, (span, 2 * HD), 1) < HD
    out_ref[0] = (jnp.where(lane, parts[0][0], parts[1][0]) * scale).astype(LOW)
    out_ref[1] = (jnp.where(lane, parts[0][1], parts[1][1]) * scale).astype(LOW)
    out_ref[2] = jnp.where(lane, parts[0][2], parts[1][2]).astype(LOW)


def unattend(qkv, grad_attended, images, seq, part, parts, shards):
    _, rows, width = qkv.shape
    span = rows // images
    pair = 2 * HD
    each = width // shards // parts // pair

    def spot(h):
        return (h // each) * (each * parts) + part * each + h % each

    def take(j):
        return pl.BlockSpec((1, span, pair), lambda i, h: (j, i, spot(h)))

    return pl.pallas_call(
        functools.partial(unattend_kernel, seq),
        grid=(images, width // pair // parts),
        in_specs=[take(0), take(1), take(2), pl.BlockSpec((span, pair), lambda i, h: (i, spot(h)))],
        out_specs=pl.BlockSpec((3, span, pair), lambda i, h: (0, i, h)),
        out_shape=jax.ShapeDtypeStruct((3, rows, width // parts), LOW),
        compiler_params=params(),
        cost_estimate=cost(
            40 * rows * span * width // parts, 14 * rows * width // parts, rows * span * (width // HD) // parts
        ),
        name=f"unattend_{part}",
    )(qkv, qkv, qkv, grad_attended)


def close_kernel(pairwise, first, n_ref, grad_ref, w_ref, *refs):
    if not first:
        carry_ref, *refs = refs
    elif pairwise:
        more_ref, *refs = refs
    acc_ref, dw_ref, sums_ref, acc_scr, *exchange = refs
    j = pl.program_id(0)
    shards, _, _, cols = w_ref.shape
    if pairwise:
        own, sent, received, sends, receives = exchange
        pl.when(j == 0)(greet_partner)
    @pl.when(j == 0)
    def _():
        acc_scr[...] = jnp.zeros_like(acc_scr) if first else carry_ref[...]

    sums = jnp.sum(grad_ref[0].astype(F32), axis=0, keepdims=True)
    for n, matrix in enumerate((0, 2)):

        @pl.when(j == matrix)
        def _():
            sums_ref[n : n + 1, :] = sums

    def spread(n, total, f=None):
        for t in range(shards):
            piece = total[:, t * cols : (t + 1) * cols]
            if f is None:
                dw_ref[t, n] = piece
            else:
                dw_ref[f, t, 0] = piece

    weight = jnp.concatenate([w_ref[t, 0] for t in range(shards)], axis=1)
    if pairwise:
        ours, theirs = bands(n_ref.shape[1] // 2)
        sent[j] = dot(n_ref[:, theirs], grad_ref[0], TN).astype(LOW)
        to_partner(sent, received, sends, receives, j).start()
        own[j] = dot(n_ref[:, ours], grad_ref[0], TN)
    else:
        depth = dw_ref.shape[3]
        dw = dot(n_ref[...], grad_ref[0], TN).astype(LOW)
        for f in range(dw_ref.shape[0]):
            spread(0, dw[f * depth : (f + 1) * depth], f)
    acc_scr[...] += dot(grad_ref[0], weight, NT)

    @pl.when(j == 2)
    def _():
        if pairwise:
            for n in range(own.shape[0]):
                to_partner(sent, received, sends, receives, n).wait()
                spread(n, (own[n] + received[n].astype(F32)).astype(LOW))
            if first:
                for t in range(shards):
                    for n in range(dw_ref.shape[1] - 3):
                        dw_ref[t, 3 + n] = more_ref[t, 0, :, n * cols : (n + 1) * cols]
        acc_ref[...] = acc_scr[...]


def close(part, parts, normed, grads, w_attn, carry, more, fsdp):
    rows, width = normed.shape
    shards, _, _, cols = w_attn.shape
    cols = cols // parts
    lanes = shards * cols
    depth = width // fsdp
    pairwise, first = fsdp == 2, carry is None
    single = pl.Buffered(1)
    stack = pl.BlockSpec((1, rows, lanes), lambda j: (j, 0, 0))
    full = pl.BlockSpec((rows, width), lambda j: (0, 0), pipeline_mode=single)
    if pairwise:
        many = 3 + parts if first else 3
        dw_spec = pl.BlockSpec((shards, many, depth, cols), lambda j: (0, 0, 0, 0), pipeline_mode=single)
        dw_shape = jax.ShapeDtypeStruct((shards, many, depth, cols), LOW)
        extra = exchange_scratch(3, (depth, lanes))
    else:
        dw_spec = pl.BlockSpec((fsdp, shards, 1, depth, cols), lambda j: (0, 0, j, 0, 0))
        dw_shape = jax.ShapeDtypeStruct((fsdp, shards, 3, depth, cols), LOW)
        extra = []
    in_specs = [full, stack, pl.BlockSpec((shards, 1, width, cols), lambda j: (0, j, 0, part))]
    out_specs, out_shape = [], []
    if not first:
        in_specs.append(full)
    elif pairwise:
        in_specs.append(pl.BlockSpec(more.shape, lambda j: (0, 0, 0, 0), pipeline_mode=single))
    out_specs.append(full)
    out_shape.append(jax.ShapeDtypeStruct((rows, width), F32))
    return pl.pallas_call(
        functools.partial(close_kernel, pairwise, first),
        grid=(3,),
        in_specs=in_specs,
        out_specs=[*out_specs, dw_spec, pl.BlockSpec((2, lanes), lambda j: (0, 0))],
        out_shape=[*out_shape, dw_shape, jax.ShapeDtypeStruct((2, lanes), F32)],
        scratch_shapes=[pltpu.VMEM((rows, width), F32), *extra],
        compiler_params=params(7 + part if pairwise else None),
        cost_estimate=cost(12 * rows * width * lanes, 20 * rows * width),
        name=f"close_{part}",
    )(normed, grads, w_attn, *([carry] if not first else [more] if pairwise else []))


def finish_kernel(acc_ref, gr_ref, x_ref, vec_ref, out_ref, norm_ref):
    i = pl.program_id(0)
    seq = out_ref.shape[1]
    normal, inverse = centred(x_ref[...].astype(F32))
    upstream = acc_ref[...]
    grad = gr_ref[...] + norm_back(upstream, normal, inverse, vec_ref[0:1])
    out_ref[0, :, 0, :] = grad[0:seq]
    sums = [jnp.sum(upstream * normal, axis=0, keepdims=True), jnp.sum(upstream, axis=0, keepdims=True)]
    sums = jnp.concatenate(sums, axis=0)

    @pl.when(i == 0)
    def _():
        norm_ref[...] = sums

    @pl.when(i != 0)
    def _():
        norm_ref[...] += sums


def finish(acc, grad_resid, x_rows, vec, images, seq):
    rows, width = acc.shape
    block = pl.BlockSpec((rows // images, width), lambda i: (i, 0))
    return pl.pallas_call(
        finish_kernel,
        grid=(images,),
        in_specs=[block, block, block, pl.BlockSpec(vec.shape, lambda i: (0, 0))],
        out_specs=[pl.BlockSpec((1, seq, 1, width), lambda i: (i, 0, 0, 0)), pl.BlockSpec((2, width), lambda i: (0, 0))],
        out_shape=[
            jax.ShapeDtypeStruct((images, seq, 1, width), F32),
            jax.ShapeDtypeStruct((2, width), F32),
        ],
        compiler_params=params(),
        cost_estimate=cost(20 * rows * width, 14 * rows * width),
        name="finish",
    )(acc, grad_resid, x_rows, vec)


def attend_pair(seq, q, k, v):
    scale = HD**-0.5
    parts = []
    for h in range(2):
        scores = dot(q, half_lanes(k, h), NT)
        lane = lax.broadcasted_iota(jnp.int32, scores.shape, 1)
        scores = jnp.where(lane < seq, scores, -1e30)
        top = jnp.max(scores, axis=1, keepdims=True)
        raised = jnp.exp((scores - top) * scale)
        total = jnp.sum(raised, axis=1, keepdims=True)
        probs = (raised * (1.0 / total)).astype(LOW)
        parts.append(dot(probs, v))
    lane = lax.broadcasted_iota(jnp.int32, parts[0].shape, 1)
    return jnp.where(lane < HD, parts[0], parts[1]).astype(LOW)


def front_kernel(
    images, seq, alive_ref, a_in, m_in, x_ref, g_ref, vec_ref,
    a_out, m_out, n_out, qkv_out, att_out, resid_out, n2_out, g2_out, x_out,
    a_wide, m_wide, a_hold, m_hold, n_scr, qkv_scr, att_scr, w_scr, o_scr, resid_scr, n2_scr, g2_scr, x_all,
    zs, zr, xs, xr, ys, yr, xfs, xfr, yfs, yfr, cs, cr, ls, ws,
):
    g, f, z = lax.axis_index("group"), lax.axis_index("fsdp"), lax.axis_index("tensor")
    shards = lax.axis_size("tensor")
    last = shards - 1
    x_at, y_at = g % 2, g // 2
    east, north = y_at * 2 + (1 - x_at), (1 - y_at) * 2 + x_at
    depth, cols = a_in.shape[1:]
    band = depth // 4
    shared = band * 3 // 8
    rest = band - 2 * shared
    span = n_scr.shape[0] // images

    def place(column):
        cx, cy = column % 2, column // 2
        return 2 * (cx + cy - 2 * cx * cy) + cy

    mine, of_east, of_north = place(g), place(east), place(north)
    z_row = mine * band - shared * (mine % 2)
    lead_east = of_east * band + shared * (of_east % 2)
    lead_north = of_north * band + shared * (of_north % 2)
    chunks = ((a_out, 0, 3), (a_out, 3, 1), (m_out, 0, 1), (m_out, 1, 1))

    def tile(n):
        return pl.multiple_of(n, 16)

    def held(n, t, row, rows):
        out, j, many = chunks[n]
        return out.at[t, pl.ds(j, many), pl.ds(tile(f * depth + row), rows), :]

    def send(part, sems, semr, n, t, to):
        return pltpu.make_async_remote_copy(
            src_ref=part, dst_ref=part, send_sem=sems.at[n, t], recv_sem=semr.at[n, t], device_id=to, device_id_type=MESH
        )

    def along(n, t, up):
        part = held(n, t, z_row, band + shared)
        return pltpu.make_async_remote_copy(
            src_ref=part,
            dst_ref=part,
            send_sem=zs.at[n, t, 0 if up else 1],
            recv_sem=zr.at[n, t],
            device_id=(g, f, z + 1 if up else z - 1),
            device_id_type=MESH,
        )

    def to_east(n, t):
        return send(held(n, t, mine * band, band), xs, xr, n, t, (east, f, z))

    def to_north(n, t):
        return send(held(n, t, mine * band, band), ys, yr, n, t, (north, f, z))

    def north_to_east(n, t):
        return send(held(n, t, lead_north, shared), xfs, xfr, n, t, (east, f, z))

    def east_to_north(n, t):
        return send(held(n, t, lead_east + shared, rest), yfs, yfr, n, t, (north, f, z))

    def across(n, t):
        return send(held(n, t, 0, depth), cs, cr, n, t, (g, 1 - f, z))

    rows = pl.ds(tile(f * depth), depth)
    loads = (
        pltpu.make_async_copy(a_in, a_wide, ls.at[0]),
        pltpu.make_async_copy(m_in, m_wide, ls.at[1]),
    )
    keeps = (
        pltpu.make_async_copy(a_hold, a_out.at[z, :, rows, :], ls.at[2]),
        pltpu.make_async_copy(m_hold, m_out.at[z, :, rows, :], ls.at[3]),
    )
    loads[0].start()

    barrier = pltpu.get_barrier_semaphore()

    def greet(to):
        pl.semaphore_signal(barrier, inc=1, device_id=to, device_id_type=MESH)

    for to in ((east, f, z), (north, f, z), (g, 1 - f, z)):
        greet(to)

    @pl.when(z > 0)
    def _():
        greet((g, f, z - 1))

    @pl.when(z < last)
    def _():
        greet((g, f, z + 1))

    loads[0].wait()
    a_hold[...] = a_wide[...].astype(LOW)
    keeps[0].start()
    pl.semaphore_wait(barrier, 3 + jnp.minimum(z, 1) + jnp.minimum(last - z, 1))
    keeps[0].wait()

    count = len(chunks)

    def when_real(k, up, run):
        @pl.when(z - k >= 0 if up else z + k <= last)
        def _():
            run(z - k if up else z + k)

    def own(n):
        @pl.when(z < last)
        def _():
            along(n, z, True).start()

        @pl.when(z > 0)
        def _():
            along(n, z, False).start()

        across(n, z).start()

    def land(n, k, up):
        def run(t):
            along(n, t, up).wait_recv()

            @pl.when(z < last if up else z > 0)
            def _():
                along(n, t, up).start()

            to_east(n, t).start()
            to_north(n, t).start()

        when_real(k, up, run)

    def relay(n, k, up):
        def run(t):
            to_east(n, t).wait_recv()
            east_to_north(n, t).start()
            to_north(n, t).wait_recv()
            north_to_east(n, t).start()

        when_real(k, up, run)

    def finish(n, k, up):
        def run(t):
            east_to_north(n, t).wait_recv()
            north_to_east(n, t).wait_recv()
            across(n, t).start()

        when_real(k, up, run)

    def both(run, n, k):
        for up in (True, False):
            run(n, k, up)

    def fetch(t):
        return pltpu.make_async_copy(a_out.at[t, pl.ds(0, 3)], w_scr, ws.at[0])

    def maps(t):
        across(0, t).wait_recv()
        fetch(t).start()
        fetch(t).wait()
        here = pl.ds(pl.multiple_of(t * cols, cols), cols)

        def body(j, carry):
            bias = jnp.where(j == 0, vec_ref[4:5, here], jnp.where(j == 2, vec_ref[5:6, here], 0.0))
            qkv_scr[j, :, here] = (dot(n_scr[...], w_scr[j]) + bias).astype(LOW)
            return carry

        lax.fori_loop(0, 3, body, 0)

    def project(k):
        def body(d, carry):
            t = z - k + 2 * k * d

            @pl.when((t >= 0) & (t <= last))
            def _():
                maps(t)

            return carry

        lax.fori_loop(0, 2, body, 0)

    own(0)
    loads[1].start()
    n_scr[...] = jnp.zeros_like(n_scr)
    x_all[...] = jnp.zeros_like(x_all)
    g2_scr[...] = jnp.zeros_like(g2_scr)
    for i in range(images):
        here = pl.ds(i * span, seq)
        image = x_ref[:, i, :]
        x_all[here, :] = image
        normal, _ = centred(image.astype(F32))
        n_scr[here, :] = (normal * vec_ref[0:1] + vec_ref[1:2]).astype(LOW)
    puts = [pltpu.make_async_copy(n_scr, n_out, ws.at[1])]
    puts[0].start()
    puts.append(pltpu.make_async_copy(x_all, x_out, ws.at[7]))
    puts[-1].start()
    both(land, 0, 1)
    loads[1].wait()
    m_hold[...] = m_wide[...].astype(LOW)
    keeps[1].start()
    maps(z)
    both(land, 0, 2)
    both(relay, 0, 1)
    keeps[1].wait()
    both(land, 0, 3)
    for n in range(1, count):
        own(n)
    both(relay, 0, 2)
    both(finish, 0, 1)
    both(relay, 0, 3)
    both(finish, 0, 2)
    project(1)
    both(finish, 0, 3)
    project(2)

    rest_items = [(n, k) for k in range(1, last + 1) for n in range(1, count)]
    total = len(rest_items) + 2

    def advance(at):
        if at < len(rest_items):
            both(land, *rest_items[at])
        if 0 <= at - 1 < len(rest_items):
            both(relay, *rest_items[at - 1])
        if 0 <= at - 2 < len(rest_items):
            both(finish, *rest_items[at - 2])

    advance(0)
    project(3)
    puts.append(pltpu.make_async_copy(qkv_scr, qkv_out, ws.at[2]))
    puts[-1].start()

    pair = 2 * HD
    pairs = qkv_scr.shape[2] // pair
    stretch = max(pairs // 4, 1)
    segments = images * pairs // stretch

    def segment(n, carry):
        def body(m, carry):
            at = n * stretch + m
            lanes = pl.ds(pl.multiple_of(lax.rem(at, pairs) * pair, pair), pair)
            here = pl.ds(pl.multiple_of(at // pairs * span, 16), span)
            att_scr[here, lanes] = attend_pair(
                seq, qkv_scr[0, here, lanes], qkv_scr[1, here, lanes], qkv_scr[2, here, lanes]
            )
            return carry

        lax.fori_loop(0, stretch, body, 0)
        for c in range(min(segments, total - 3)):
            pl.when(n == c)(functools.partial(advance, 1 + c))
        return carry

    lax.fori_loop(0, segments, segment, 0)
    at = 1 + min(segments, total - 3)
    puts.append(pltpu.make_async_copy(att_scr, att_out, ws.at[3]))
    puts[-1].start()
    for i in range(images):
        g2_scr[pl.ds(i * span, seq), :] = (g_ref[:, i, :].astype(F32) * alive_ref[i]).astype(LOW)
    while at < total - 2:
        advance(at)
        at += 1

    for t in range(shards):
        across(1, t).wait_recv()
    take = pltpu.make_async_copy(a_out.at[:, 3], o_scr, ws.at[0])
    take.start()
    take.wait()

    def mix_image(i, carry):
        here = pl.ds(pl.multiple_of(i * span, 16), span)
        out = x_all[here, :].astype(F32) + vec_ref[6:7]
        for t in range(shards):
            out = out + dot(att_scr[here, t * cols : (t + 1) * cols], o_scr[t], NT)
        resid_scr[here, :] = out
        normal, _ = centred(out)
        n2_scr[here, :] = (normal * vec_ref[2:3] + vec_ref[3:4]).astype(LOW)
        for c in range(min(images, total - at)):
            pl.when(i == c)(functools.partial(advance, at + c))
        return carry

    lax.fori_loop(0, images, mix_image, 0)
    at += min(images, total - at)
    for n, (src, dst) in enumerate(((resid_scr, resid_out), (n2_scr, n2_out), (g2_scr, g2_out))):
        puts.append(pltpu.make_async_copy(src, dst, ws.at[4 + n]))
        puts[-1].start()
    while at < total:
        advance(at)
        at += 1
    for put in puts:
        put.wait()

    for n in range(count):
        @pl.when(z < last)
        def _():
            along(n, z, True).wait_send()

        @pl.when(z > 0)
        def _():
            along(n, z, False).wait_send()

        for t in range(shards):
            across(n, t).wait_send()
            if n > 1:
                across(n, t).wait_recv()

    def settle(n, k, up):
        def run(t):
            @pl.when(z < last if up else z > 0)
            def _():
                along(n, t, up).wait_send()

            to_east(n, t).wait_send()
            to_north(n, t).wait_send()
            east_to_north(n, t).wait_send()
            north_to_east(n, t).wait_send()

        when_real(k, up, run)

    for n in range(count):
        for k in range(1, last + 1):
            both(settle, n, k)


def front(alive, attn_master, mlp_master, patches, cotangent, vec, shards):
    _, depth, a_cols = attn_master.shape
    _, _, m_cols = mlp_master.shape
    seq, images, width = patches.shape
    rows = images * padded(seq)
    anywhere = pl.BlockSpec(memory_space=pl.ANY)
    inside = pl.BlockSpec(memory_space=pltpu.VMEM)
    dma = pltpu.SemaphoreType.DMA
    low = jax.ShapeDtypeStruct((rows, width), LOW)
    return pl.pallas_call(
        functools.partial(front_kernel, images, seq),
        in_specs=[pl.BlockSpec(memory_space=pltpu.SMEM), anywhere, anywhere, inside, inside, inside],
        out_specs=[anywhere] * 9,
        out_shape=[
            jax.ShapeDtypeStruct((shards, 4, width, a_cols), LOW),
            jax.ShapeDtypeStruct((shards, 2, width, m_cols), LOW),
            low,
            jax.ShapeDtypeStruct((3, rows, width), LOW),
            low,
            jax.ShapeDtypeStruct((rows, width), F32),
            low,
            low,
            low,
        ],
        scratch_shapes=[
            pltpu.VMEM(attn_master.shape, F32),
            pltpu.VMEM(mlp_master.shape, F32),
            pltpu.VMEM(attn_master.shape, LOW),
            pltpu.VMEM(mlp_master.shape, LOW),
            pltpu.VMEM((rows, width), LOW),
            pltpu.VMEM((3, rows, width), LOW),
            pltpu.VMEM((rows, width), LOW),
            pltpu.VMEM((3, width, a_cols), LOW),
            pltpu.VMEM((shards, width, a_cols), LOW),
            pltpu.VMEM((rows, width), F32),
            pltpu.VMEM((rows, width), LOW),
            pltpu.VMEM((rows, width), LOW),
            pltpu.VMEM((rows, width), LOW),
            dma((4, shards, 2)),
        ]
        + [dma((4, shards))] * 11
        + [dma((4,)), dma((8,))],
        compiler_params=params(1),
        cost_estimate=cost(8 * rows * width * width, 30 * rows * width),
        name="front",
    )(alive, attn_master, mlp_master, patches, cotangent, vec)


def inner_adamw(master, gradient, first, second, step_rate, decay_rate):
    first_moment = 0.9 * first + 0.1 * gradient
    second_moment = 0.95 * second + 0.05 * gradient * gradient
    step_ratio = (
        first_moment / (1.0 - 0.9**STEP) / (jnp.sqrt(second_moment / (1.0 - 0.95**STEP)) + 1e-08)
    )
    return (master - step_rate * (step_ratio + decay_rate * master), second_moment)


def outer_nesterov(master, outer_old, difference):
    momentum = OUTER_MOMENTUM * outer_old + difference
    return momentum, master - OUTER_RATE * (difference + OUTER_MOMENTUM * momentum)


def inner_kernel(join, count, *refs):
    pieces, (master_ref, moment_ref, *_, inner_ref, diff_ref) = refs[:count], refs[count:]
    gradient = join(*[piece[0] for piece in pieces]).astype(F32)
    master = master_ref[0]
    new, second = inner_adamw(master, gradient, moment_ref[0, 0, 0], moment_ref[0, 1, 0], INNER_RATE, WEIGHT_DECAY)
    inner_ref[0, 0, 0] = gradient
    inner_ref[0, 1, 0] = second
    diff_ref[0] = (master - new).astype(LOW)


def inner_step(join, pieces, unit, units, cols, master, moments, into, name):
    depth = master.shape[1]
    rows = min(depth, 524288 // cols)
    block = pl.BlockSpec((1, rows, cols), lambda u, r: (unit(u)[0], r, unit(u)[1]))
    both = pl.BlockSpec((1, 2, 1, rows, cols), lambda u, r: (0, 0, unit(u)[0], r, unit(u)[1]))
    piece_specs = [pl.BlockSpec((1, rows, piece.shape[2]), lambda u, r: (u, r, 0)) for piece in pieces]
    count = len(pieces)
    return pl.pallas_call(
        functools.partial(inner_kernel, join, count),
        grid=(units, depth // rows),
        in_specs=[*piece_specs, block, both] + ([] if into is None else [pl.BlockSpec(memory_space=pl.ANY)]),
        out_specs=[both, pl.BlockSpec((1, rows, cols), lambda u, r: (u, r, 0))],
        out_shape=[
            jax.ShapeDtypeStruct(moments.shape, F32),
            jax.ShapeDtypeStruct((units, depth, cols), LOW),
        ],
        input_output_aliases={} if into is None else {count + 2: 0},
        compiler_params=params(),
        cost_estimate=cost(30 * units * depth * cols, 24 * units * depth * cols),
        name=name,
    )(*pieces, master, moments, *([] if into is None else [into]))


def outer_kernel(groups, slots, each, g_ref, *refs):
    totals, (master_ref, outer_ref, *_, state_ref, copy_ref) = refs[:slots], refs[slots:]
    rows = copy_ref.shape[1]
    if slots == 1:
        total = totals[0][0]
    else:
        at = pl.program_id(0) * pl.num_programs(1) + pl.program_id(1)
        slot = lax.rem(g_ref[0] + groups - at // each, groups)
        here = pl.ds(pl.multiple_of(lax.rem(at, each) * rows, rows), rows)
        total = totals[0][here, :]
        for n in range(1, slots):
            total = jnp.where(slot == n, totals[n][here, :], total)
    difference = total.astype(F32) / groups
    momentum, fresh = outer_nesterov(master_ref[0], outer_ref[0], difference)
    state_ref[0, 0] = difference
    state_ref[1, 0] = momentum
    state_ref[2, 0] = fresh
    copy_ref[0] = fresh.astype(LOW)


def outer_step(groups, me, totals, unit, units, cols, master, outer_old, into, name):
    depth = master.shape[1]
    slots = len(totals)
    rows = min(depth, 524288 // cols, totals[0].shape[-2])
    each = totals[0].shape[-2] // rows
    block = pl.BlockSpec((1, rows, cols), lambda u, r, g: (unit(u)[0], r, unit(u)[1]))
    state = pl.BlockSpec((3, 1, rows, cols), lambda u, r, g: (0, unit(u)[0], r, unit(u)[1]))
    if slots == 1:
        total = pl.BlockSpec((1, rows, cols), lambda u, r, g: (u, r, 0))
    else:
        total = pl.BlockSpec(totals[0].shape, lambda u, r, g: (0, 0))
    aliased = [] if into is None else [pl.BlockSpec(memory_space=pl.ANY)] * 2
    return pl.pallas_call(
        functools.partial(outer_kernel, groups, slots, each),
        grid_spec=pltpu.PrefetchScalarGridSpec(
            num_scalar_prefetch=1,
            grid=(units, depth // rows),
            in_specs=[*[total] * slots, block, block, *aliased],
            out_specs=[state, block],
        ),
        out_shape=[
            jax.ShapeDtypeStruct((3, *master.shape), F32),
            jax.ShapeDtypeStruct(master.shape, LOW),
        ],
        input_output_aliases={} if into is None else {slots + 3: 0, slots + 4: 1},
        compiler_params=params(),
        cost_estimate=cost(10 * units * depth * cols, 24 * units * depth * cols),
        name=name,
    )(me, *totals, master, outer_old, *([] if into is None else into))


def group_kernel(groups, shards, vectors, diff_ref, *refs):
    if vectors:
        part_ref, master_ref, moment_ref, outer_ref, total_ref, inner_ref, state_ref, copy_ref, *refs = refs
    else:
        total_ref, *refs = refs
    landed, summed, sends, receives, sends_two, receives_two, *small = refs
    g, f, t = lax.axis_index("group"), lax.axis_index("fsdp"), lax.axis_index("tensor")
    span = landed.shape[1]

    def rows(n):
        return pl.ds(pl.multiple_of(n * span, span), span)

    def other(k):
        return lax.rem(g + k, groups)

    def back(k):
        return lax.rem(g + groups - k, groups)

    def copy(src, dst, sems, semr, k, to):
        return pltpu.make_async_remote_copy(
            src_ref=src, dst_ref=dst, send_sem=sems.at[k], recv_sem=semr.at[k], device_id=to, device_id_type=MESH
        )

    def part(k):
        return copy(diff_ref.at[rows(other(k)), :], landed.at[k], sends, receives, k, (other(k), f, t))

    def result(k):
        return copy(summed, landed.at[groups + k], sends_two, receives_two, k, (other(k), f, t))

    barrier = pltpu.get_barrier_semaphore()
    for k in range(1, groups):
        pl.semaphore_signal(barrier, inc=1, device_id=(other(k), f, t), device_id_type=MESH)
    if vectors:
        stage, pair, mine, line, whole, few, diffs, ss, rs, ls, lr, gs, gr = small
        half = part_ref.shape[0] // 2
        halves = (pl.ds(0, half), pl.ds(half, half))

        def pick(ref):
            return jnp.where(f == 0, ref[halves[0], :], ref[halves[1], :])

        def line_copy(k):
            return copy(mine, line.at[k], ls, lr, k, (g, f, lax.rem(t + k, shards)))

        def few_copy(k):
            return copy(diffs.at[f], few.at[k], gs, gr, k, (other(k), f, t))

        pair_copy = copy(stage.at[1 - f], pair, ss, rs, 0, partner())
        whole_copy = copy(whole.at[f], whole.at[f], ss, rs, 1, partner())
        final_copy = copy(mine, stage.at[f], ss, rs, 2, partner())
        pl.semaphore_signal(barrier, inc=1, device_id=partner(), device_id_type=MESH)
        for k in range(1, shards):
            pl.semaphore_signal(barrier, inc=1, device_id=(g, f, lax.rem(t + k, shards)), device_id_type=MESH)
        stage[...] = jnp.zeros_like(stage)
        diffs[...] = jnp.zeros_like(diffs)
        for n in range(2):
            stage[n, 0:half] = part_ref[halves[n], :]
    pl.semaphore_wait(barrier, groups - 1 + (shards if vectors else 0))

    for k in range(1, groups):
        part(k).start()
    if vectors:
        pair_copy.start()
        pair_copy.wait()
        mine[...] = stage[f] + pair[...]
        for k in range(1, shards):
            line_copy(k).start()
        line[0] = mine[...]
        for k in range(1, shards):
            line_copy(k).wait()
        gradient = jnp.zeros(mine.shape, F32)
        for n in range(shards):
            gradient = gradient + line[lax.rem(t + shards - n, shards)]
        whole[f] = gradient
        whole_copy.start()
        new, _ = inner_adamw(
            pick(master_ref), gradient[0:half], pick(moment_ref.at[0]), pick(moment_ref.at[1]), VECTOR_RATE, 0.0
        )
        diffs[f, 0:half] = pick(master_ref) - new
        for k in range(1, groups):
            few_copy(k).start()
        few[0] = diffs[f]
        whole_copy.wait()
        for n in range(2):
            own = whole[n, 0:half]
            _, second = inner_adamw(
                master_ref[halves[n], :], own, moment_ref[0, halves[n], :], moment_ref[1, halves[n], :], VECTOR_RATE, 0.0
            )
            inner_ref[0, halves[n], :] = own
            inner_ref[1, halves[n], :] = second
    total = diff_ref[rows(g), :].astype(F32)
    for k in range(1, groups):
        part(k).wait_recv()
        total = total + landed[k].astype(F32)
    summed[...] = total.astype(LOW)
    for k in range(1, groups):
        result(k).start()
    total_ref[rows(g), :] = summed[...]
    if vectors:
        for k in range(1, groups):
            few_copy(k).wait()
        difference = jnp.zeros(mine.shape, F32)
        for n in range(groups):
            difference = difference + few[lax.rem(g + groups - n, groups)]
        mine[...] = difference / groups
        stage[f] = mine[...]
        final_copy.start()
        final_copy.wait()
        for n in range(2):
            difference = stage[n, 0:half]
            momentum, fresh = outer_nesterov(master_ref[halves[n], :], outer_ref[halves[n], :], difference)
            state_ref[0, halves[n], :] = difference
            state_ref[1, halves[n], :] = momentum
            state_ref[2, halves[n], :] = fresh
            copy_ref[halves[n], :] = fresh.astype(LOW)
    for k in range(1, groups):
        result(k).wait_recv()
        total_ref[rows(back(k)), :] = landed[groups + k]
    for k in range(1, groups):
        part(k).wait_send()
        result(k).wait_send()


def group_sum(diff, groups, identity, name, vectors=None, shards=0):
    flat = diff.reshape(-1, diff.shape[-1])
    span, cols = flat.shape[0] // groups, flat.shape[1]
    dma = pltpu.SemaphoreType.DMA
    whole = pl.BlockSpec(memory_space=pltpu.VMEM)
    out_shape = [jax.ShapeDtypeStruct(flat.shape, LOW)]
    extra = []
    if vectors:
        shape = vectors[0].shape
        half = (-(-shape[0] // 16) * 8, shape[1])
        out_shape += [
            jax.ShapeDtypeStruct((2, *shape), F32),
            jax.ShapeDtypeStruct((3, *shape), F32),
            jax.ShapeDtypeStruct(shape, LOW),
        ]
        extra = [
            pltpu.VMEM((2, *half), F32),
            pltpu.VMEM(half, F32),
            pltpu.VMEM(half, F32),
            pltpu.VMEM((shards, *half), F32),
            pltpu.VMEM((2, *half), F32),
            pltpu.VMEM((groups, *half), F32),
            pltpu.VMEM((2, *half), F32),
            dma((3,)),
            dma((3,)),
            dma((shards,)),
            dma((shards,)),
            dma((groups,)),
            dma((groups,)),
        ]
    total, *rest = pl.pallas_call(
        functools.partial(group_kernel, groups, shards, bool(vectors)),
        in_specs=[whole] * (5 if vectors else 1),
        out_specs=[whole] * len(out_shape),
        out_shape=out_shape,
        scratch_shapes=[
            pltpu.VMEM((2 * groups, span, cols), LOW),
            pltpu.VMEM((span, cols), LOW),
            *[dma((groups,))] * 4,
            *extra,
        ],
        compiler_params=params(identity),
        cost_estimate=cost(4 * flat.size, 8 * flat.size),
        name=name,
    )(flat, *(vectors or []))
    return total.reshape(diff.shape), *rest


def gather_weights(shard):
    whole = lax.all_gather(shard, "tensor", axis=0)
    return lax.all_gather(whole, "fsdp", axis=2, tiled=True)


def around(array, k, groups):
    return lax.ppermute(array, "group", [(i, (i + k) % groups) for i in range(groups)])


def exchange_parts(diff, groups):
    g = lax.axis_index("group")
    quarters = diff.reshape(groups, -1, diff.shape[-1])
    parts = [lax.dynamic_index_in_dim(quarters, lax.rem(g + k, groups), 0, keepdims=False) for k in range(groups)]
    return parts[0], [around(parts[k], k, groups) for k in range(1, groups)]


def exchange_total(own, parts, groups):
    own = sum([part.astype(F32) for part in parts], own.astype(F32)).astype(LOW)
    return [own] + [around(own, k, groups) for k in range(1, groups)]


def scatter_gradient(gradient):
    half = gradient if gradient.ndim == 4 else lax.psum_scatter(gradient, "fsdp", scatter_dimension=0)
    return lax.psum_scatter(half, "tensor", scatter_dimension=0)


def local(
    patches,
    output_grad,
    live_counts,
    attn_master,
    mlp_master,
    vector_master,
    attn_moments,
    mlp_moments,
    vector_moments,
    attn_outer,
    mlp_outer,
    vector_outer,
):
    vec = vector_master
    tensor_size, fsdp = lax.axis_size("tensor"), lax.axis_size("fsdp")
    groups = lax.axis_size("group")
    local_images, seq, width = patches.shape[2:]
    slot = (lax.axis_index("fsdp") * tensor_size + lax.axis_index("tensor")) * local_images
    slot = slot + jnp.arange(local_images)
    counts = jnp.take(live_counts[0], slot // IMG_DEV, axis=1)
    alive = ((slot % IMG_DEV)[None, :] < counts).astype(F32).reshape(-1)
    x = patches.reshape(-1, seq, width)
    cotangent = output_grad.reshape(-1, seq, width)
    images = x.shape[0]

    if (groups, fsdp) == (4, 2):
        beside_images = [
            jnp.moveaxis(v.reshape(images, seq, width), 0, 1) for v in (patches, output_grad)
        ]
        w_attn, w_mlp, normed_one, qkv, attended, resid, normed_two, grad_two, x_rows = front(
            alive, attn_master, mlp_master, *beside_images, vec, tensor_size
        )
    else:
        w_attn = gather_weights(attn_master.astype(LOW))
        w_mlp = gather_weights(mlp_master.astype(LOW))
        normed_one, qkv = project(x, w_attn, vec)
        attended = attend(qkv, images, seq)
        resid, normed_two, grad_two = mix(alive, attended, x, cotangent, w_attn, vec)
        x_rows = jnp.pad(x, ((0, 0), (0, padded(seq) - seq), (0, 0))).reshape(-1, width)
    bias = vec[8:].reshape(tensor_size, 1, -1)
    carried = None
    mlp_grads, bias_parts = [], []
    for part, (start, cols) in enumerate(PIECES):
        *carried, dw, db = mlp(part, start, cols, normed_two, grad_two, w_mlp, bias, carried, fsdp)
        mlp_grads.append(scatter_gradient(dw))
        bias_parts.append(db)
    branch, grad_normed = carried
    block_output, grad_resid, grad_attended, dw_out, sums_two = turn(
        alive, resid, branch, grad_normed, grad_two, attended, w_attn, vec, images, seq, fsdp
    )
    def beside(*parts):
        return jnp.concatenate(parts, axis=-1)

    pairwise = fsdp == 2
    me = lax.axis_index("group").astype(jnp.int32).reshape(1)
    half = attn_master.shape[2] // PARTS
    grads = unattend(qkv, grad_attended, images, seq, 0, PARTS, tensor_size)
    grads, mlp_grads[0] = lax.optimization_barrier((grads, mlp_grads[0]))
    carry, dw_early, head_sums = close(
        0, PARTS, normed_one, grads, w_attn, None, dw_out, fsdp
    )
    if not pairwise:
        halves = jnp.moveaxis(dw_out.reshape(*dw_out.shape[:-1], PARTS, half), -2, 2)
        dw_early = jnp.concatenate([dw_early, halves[:, :, :, 0]], axis=2)
    early_grad = scatter_gradient(dw_early)
    head_sums = [head_sums]
    carry, mlp_grads[1] = lax.optimization_barrier((carry, mlp_grads[1]))
    grads = unattend(qkv, grad_attended, images, seq, 1, PARTS, tensor_size)

    carry, dw_late, sums = close(1, PARTS, normed_one, grads, w_attn, carry, None, fsdp)

    mlp_grads[0], carry = lax.optimization_barrier((mlp_grads[0], carry))
    mlp_inner, mlp_diff = inner_step(
        beside, mlp_grads, lambda u: (u, 0), 2, mlp_master.shape[2], mlp_master, mlp_moments, None, "inner_mlp"
    )
    own, parts = exchange_parts(mlp_diff, groups)
    carry, own = lax.optimization_barrier((carry, own))
    patches_grad, sums_one = finish(carry, grad_resid, x_rows, vec, images, seq)
    late_grad = scatter_gradient(dw_late)
    head_sums.append(sums)

    def early(u):
        return jnp.minimum(u, 3), jnp.maximum(u - 3, 0)

    def late(u):
        return u, 1

    def first(piece):
        return piece

    head_rows = jnp.concatenate([v.reshape(2, tensor_size, -1) for v in head_sums], axis=-1).reshape(2, width)
    hidden_bias = jnp.concatenate(bias_parts, axis=-1).reshape(-1, width)
    vector_part = jnp.concatenate([sums_one, sums_two[:2], head_rows, sums_two[2:], hidden_bias])
    early_grad, vector_part = lax.optimization_barrier((early_grad, vector_part))
    attn_inner, early_diff = inner_step(
        first, [early_grad], early, 3 + PARTS, half, attn_master, attn_moments, None, "inner_early"
    )

    own, *parts, early_diff = lax.optimization_barrier((own, *parts, early_diff))
    mlp_total = exchange_total(own, parts, groups)
    if pairwise:
        early_total, vector_inner, vector_state, vector_copy = group_sum(
            early_diff,
            groups,
            10,
            "group_early",
            [vector_part, vec, vector_moments[0], vector_outer],
            tensor_size,
        )
    else:
        (early_total,) = group_sum(early_diff, groups, 10, "group_early")
        vector_grad = lax.psum(vector_part, ("fsdp", "tensor"))
        new_vector, second_vector = inner_adamw(
            vec, vector_grad, vector_moments[0, 0], vector_moments[0, 1], VECTOR_RATE, 0.0
        )
        diff_vector = lax.psum(vec - new_vector, "group") / groups
        momentum, fresh = outer_nesterov(vec, vector_outer, diff_vector)
        vector_inner = jnp.stack([vector_grad, second_vector])
        vector_state, vector_copy = jnp.stack([diff_vector, momentum, fresh]), fresh.astype(LOW)
    attn_state, attn_copy = outer_step(
        groups, me, [early_total], early, 3 + PARTS, half, attn_master, attn_outer, None, "outer_early"
    )
    attn_copy, *mlp_total = lax.optimization_barrier((attn_copy, *mlp_total))
    mlp_state, mlp_copy = outer_step(
        groups,
        me,
        mlp_total,
        lambda u: (u, 0),
        2,
        mlp_master.shape[2],
        mlp_master,
        mlp_outer,
        None,
        "outer_mlp",
    )
    late_grad, mlp_state = lax.optimization_barrier((late_grad, mlp_state))
    attn_inner, late_diff = inner_step(
        first, [late_grad], late, 3, half, attn_master, attn_moments, attn_inner, "inner_late"
    )
    (late_total,) = group_sum(late_diff, groups, 11, "group_late")
    attn_state, attn_copy = outer_step(
        groups, me, [late_total], late, 3, half, attn_master, attn_outer, (attn_state, attn_copy), "outer_late"
    )
    return (
        block_output.reshape(patches.shape),
        patches_grad.reshape(patches.shape),
        attn_inner,
        attn_state,
        attn_copy,
        mlp_inner,
        mlp_state,
        mlp_copy,
        vector_inner[None],
        vector_state,
        vector_copy,
    )


def solution(mesh):
    placed = (
        P("group", None, ("fsdp", "tensor"), None, None),
        P("group", None, ("fsdp", "tensor"), None, None),
        P("group", None, None),
        P(None, "fsdp", "tensor"),
        P(None, "fsdp", "tensor"),
        P(),
        P("group", None, None, "fsdp", "tensor"),
        P("group", None, None, "fsdp", "tensor"),
        P("group", None, None, None),
        P(None, "fsdp", "tensor"),
        P(None, "fsdp", "tensor"),
        P(),
    )
    return jax.shard_map(
        local,
        mesh=mesh,
        in_specs=placed,
        out_specs=(
            P("group", None, ("fsdp", "tensor"), None, None),
            P("group", None, ("fsdp", "tensor"), None, None),
            P("group", None, None, "fsdp", "tensor"),
            P(None, None, "fsdp", "tensor"),
            P(None, "fsdp", "tensor"),
            P("group", None, None, "fsdp", "tensor"),
            P(None, None, "fsdp", "tensor"),
            P(None, "fsdp", "tensor"),
            P("group", None, None, None),
            P(),
            P(),
        ),
        check_vma=False,
    )
```

```python
import functools

import jax
import jax.numpy as jnp
from jax import lax
from jax.experimental import pallas as pl
from jax.experimental.pallas import tpu as pltpu
from jax.sharding import PartitionSpec as P

HD = 64
STEP = 8
IMG_DEV = 4
EPSILON = 1e-06
INNER_RATE = 0.02
VECTOR_RATE = 0.2
WEIGHT_DECAY = 0.1
OUTER_RATE = 0.7
OUTER_MOMENTUM = 0.9
PIECES = ((0, 256), (256, 256), (512, 512))
PARTS = 2
LOW = jnp.bfloat16
F32 = jnp.float32
NN = (((1,), (0,)), ((), ()))
NT = (((1,), (1,)), ((), ()))
TN = (((0,), (0,)), ((), ()))


def dot(a, b, dims=NN):
    return lax.dot_general(a, b, dims, preferred_element_type=F32)


MESH = pl.DeviceIdType.MESH


def params(identity=None):
    if identity is None:
        return pltpu.CompilerParams(vmem_limit_bytes=60 * 2**20)
    return pltpu.CompilerParams(vmem_limit_bytes=60 * 2**20, collective_id=identity, has_side_effects=True)


def partner():
    return (lax.axis_index("group"), 1 - lax.axis_index("fsdp"), lax.axis_index("tensor"))


def greet_partner():
    barrier = pltpu.get_barrier_semaphore()
    pl.semaphore_signal(barrier, inc=1, device_id=partner(), device_id_type=MESH)
    pl.semaphore_wait(barrier, 1)


def to_partner(sent, received, sends, receives, n):
    return pltpu.make_async_remote_copy(
        src_ref=sent.at[n],
        dst_ref=received.at[n],
        send_sem=sends.at[n],
        recv_sem=receives.at[n],
        device_id=partner(),
        device_id_type=MESH,
    )


def bands(depth):
    f = lax.axis_index("fsdp")
    return pl.ds(pl.multiple_of(f * depth, depth), depth), pl.ds(pl.multiple_of((1 - f) * depth, depth), depth)


def exchange_scratch(steps, shape):
    dma = pltpu.SemaphoreType.DMA
    return [
        pltpu.VMEM((steps, *shape), F32),
        pltpu.VMEM((steps, *shape), LOW),
        pltpu.VMEM((steps, *shape), LOW),
        dma((steps,)),
        dma((steps,)),
    ]


def cost(flops, moved, special=0):
    return pl.CostEstimate(flops=int(flops), bytes_accessed=int(moved), transcendentals=int(special))


def padded(rows):
    return -(-rows // 16) * 16


def centred(source):
    centre = source - jnp.mean(source, axis=-1, keepdims=True)
    spread = jnp.mean(centre * centre, axis=-1, keepdims=True)
    inverse = lax.rsqrt(spread + EPSILON)
    return centre * inverse, inverse


def norm_back(upstream, normal, inverse, gain):
    pulled = upstream * gain
    mean_one = jnp.mean(pulled, axis=-1, keepdims=True)
    mean_two = jnp.mean(pulled * normal, axis=-1, keepdims=True)
    return inverse * (pulled - mean_one - normal * mean_two)


def project_kernel(images, seq, x_ref, w_ref, vec_ref, n_ref, out_ref, n_scr):
    j, t = pl.program_id(0), pl.program_id(1)
    span = n_scr.shape[0] // images

    @pl.when((j == 0) & (t == 0))
    def _():
        n_scr[...] = jnp.zeros_like(n_scr)
        for i in range(images):
            normal, _ = centred(x_ref[i].astype(F32))
            n_scr[pl.ds(i * span, seq), :] = (normal * vec_ref[0:1] + vec_ref[1:2]).astype(LOW)
        n_ref[...] = n_scr[...]

    cols = out_ref.shape[-1]
    out = dot(n_scr[...], w_ref[0, 0])
    at = pl.ds(pl.multiple_of(t * cols, cols), cols)
    bias = jnp.where(j == 0, vec_ref[4:5, at], jnp.where(j == 2, vec_ref[5:6, at], 0.0))
    out_ref[0] = (out + bias).astype(LOW)


def project(patches, w_attn, vec):
    images, seq, width = patches.shape
    shards, _, _, cols = w_attn.shape
    rows = images * padded(seq)
    return pl.pallas_call(
        functools.partial(project_kernel, images, seq),
        grid=(3, shards),
        in_specs=[
            pl.BlockSpec((images, seq, width), lambda j, t: (0, 0, 0)),
            pl.BlockSpec((1, 1, width, cols), lambda j, t: (t, j, 0, 0)),
            pl.BlockSpec(vec.shape, lambda j, t: (0, 0)),
        ],
        out_specs=[
            pl.BlockSpec((rows, width), lambda j, t: (0, 0)),
            pl.BlockSpec((1, rows, cols), lambda j, t: (j, 0, t)),
        ],
        out_shape=[
            jax.ShapeDtypeStruct((rows, width), LOW),
            jax.ShapeDtypeStruct((3, rows, width), LOW),
        ],
        scratch_shapes=[pltpu.VMEM((rows, width), LOW)],
        compiler_params=params(),
        cost_estimate=cost(6 * rows * width * width, 16 * rows * width),
        name="project",
    )(patches, w_attn, vec)


def half_lanes(value, which):
    lane = lax.broadcasted_iota(jnp.int32, value.shape, 1)
    return jnp.where((lane >= HD) == bool(which), value, jnp.zeros_like(value))


def attend_kernel(seq, q_ref, k_ref, v_ref, out_ref):
    span = q_ref.shape[1]
    scale = HD**-0.5
    q, k, v = q_ref[0], k_ref[0], v_ref[0]
    parts = []
    for h in range(2):
        scores = dot(q, half_lanes(k, h), NT)
        lane = lax.broadcasted_iota(jnp.int32, scores.shape, 1)
        scores = jnp.where(lane < seq, scores, -1e30)
        top = jnp.max(scores, axis=1, keepdims=True)
        raised = jnp.exp((scores - top) * scale)
        total = jnp.sum(raised, axis=1, keepdims=True)
        probs = (raised * (1.0 / total)).astype(LOW)
        parts.append(dot(probs, v))
    lane = lax.broadcasted_iota(jnp.int32, (span, 2 * HD), 1)
    out_ref[...] = jnp.where(lane < HD, parts[0], parts[1]).astype(LOW)


def attend(qkv, images, seq):
    _, rows, width = qkv.shape
    span = rows // images
    pair = 2 * HD

    def take(j):
        return pl.BlockSpec((1, span, pair), lambda i, h: (j, i, h))

    return pl.pallas_call(
        functools.partial(attend_kernel, seq),
        grid=(images, width // pair),
        in_specs=[take(0), take(1), take(2)],
        out_specs=pl.BlockSpec((span, pair), lambda i, h: (i, h)),
        out_shape=jax.ShapeDtypeStruct((rows, width), LOW),
        compiler_params=params(),
        cost_estimate=cost(16 * rows * span * width, 8 * rows * width, rows * span * (width // HD)),
        name="attend",
    )(qkv, qkv, qkv)


def mix_kernel(seq, alive_ref, att_ref, x_ref, g_ref, w_ref, vec_ref, resid_ref, n_ref, g2_ref, x_scr):
    i = pl.program_id(0)
    shards, _, _, cols = w_ref.shape
    x_scr[...] = jnp.zeros_like(x_scr)
    x_scr[0:seq, :] = x_ref[0].astype(F32)
    total = x_scr[...] + vec_ref[6:7]
    for t in range(shards):
        total = total + dot(att_ref[:, t * cols : (t + 1) * cols], w_ref[t, 0], NT)
    resid_ref[...] = total
    normal, _ = centred(total)
    n_ref[...] = (normal * vec_ref[2:3] + vec_ref[3:4]).astype(LOW)
    x_scr[0:seq, :] = g_ref[0].astype(F32) * alive_ref[i]
    g2_ref[...] = x_scr[...].astype(LOW)


def mix(alive, attended, patches, cotangent, w_attn, vec):
    images, seq, width = patches.shape
    rows = attended.shape[0]
    span = rows // images
    shards, _, _, cols = w_attn.shape
    block = pl.BlockSpec((span, width), lambda i: (i, 0))
    whole = jax.ShapeDtypeStruct((rows, width), LOW)
    return pl.pallas_call(
        functools.partial(mix_kernel, seq),
        grid=(images,),
        in_specs=[
            pl.BlockSpec(memory_space=pltpu.SMEM),
            block,
            pl.BlockSpec((1, seq, width), lambda i: (i, 0, 0)),
            pl.BlockSpec((1, seq, width), lambda i: (i, 0, 0)),
            pl.BlockSpec((shards, 1, width, cols), lambda i: (0, 3, 0, 0)),
            pl.BlockSpec(vec.shape, lambda i: (0, 0)),
        ],
        out_specs=[block, block, block],
        out_shape=[jax.ShapeDtypeStruct((rows, width), F32), whole, whole],
        scratch_shapes=[pltpu.VMEM((span, width), F32)],
        compiler_params=params(),
        cost_estimate=cost(2 * rows * width * width, 16 * rows * width),
        name="mix",
    )(alive, attended, patches, cotangent, w_attn, vec)


def mlp_kernel(first, pairwise, n_ref, g_ref, w1_ref, w2_ref, bias_ref, *refs):
    if not first:
        yi_ref, gi_ref, *refs = refs
    y_ref, gn_ref, dw_ref, db_ref, h_scr, p_scr, loaded, *exchange = refs
    step = pl.program_id(0)
    each, _, width, cols = w1_ref.shape
    if not first:
        loads = (
            pltpu.make_async_copy(yi_ref, y_ref, loaded.at[0]),
            pltpu.make_async_copy(gi_ref, gn_ref, loaded.at[1]),
        )

    @pl.when(step == 0)
    def _():
        if not first:
            for load in loads:
                load.start()
        else:
            y_ref[...] = jnp.zeros_like(y_ref)
            gn_ref[...] = jnp.zeros_like(gn_ref)
        if pairwise:
            greet_partner()

    w1 = jnp.concatenate([w1_ref[t, 0] for t in range(each)], axis=1)
    w2 = jnp.concatenate([w2_ref[t, 0] for t in range(each)], axis=1)
    bias = jnp.concatenate([bias_ref[t] for t in range(each)], axis=1)
    pre = dot(n_ref[...], w1) + bias
    cdf = 0.5 * (1.0 + lax.erf(pre * 0.7071067811865476))
    h_scr[...] = (pre * cdf).astype(LOW)
    slope = cdf + pre * jnp.exp(-0.5 * pre * pre) * 0.3989422804014327
    p_scr[...] = (dot(g_ref[...], w2) * slope).astype(LOW)
    sums = jnp.sum(p_scr[...].astype(F32), axis=0, keepdims=True)
    for t in range(each):
        db_ref[t] = sums[:, t * cols : (t + 1) * cols]

    if pairwise:
        own, sent, received, sends, receives = exchange
        ours, theirs = bands(width // 2)

        slot = lax.rem(step, 2)

        def collect(n):
            at = lax.rem(n, 2)
            to_partner(sent, received, sends, receives, at).wait()
            for which in range(2):
                total = (own[at, which] + received[at, which].astype(F32)).astype(LOW)
                for t in range(each):
                    dw_ref[n * each + t, which] = total[:, t * cols : (t + 1) * cols]

        @pl.when(step > 0)
        def _():
            collect(step - 1)

        sent[slot, 0] = dot(n_ref[:, theirs], p_scr[...], TN).astype(LOW)
        sent[slot, 1] = dot(g_ref[:, theirs], h_scr[...], TN).astype(LOW)
        to_partner(sent, received, sends, receives, slot).start()
        own[slot, 0] = dot(n_ref[:, ours], p_scr[...], TN)
        own[slot, 1] = dot(g_ref[:, ours], h_scr[...], TN)

    else:
        shards, depth = dw_ref.shape[0], dw_ref.shape[3]
        d1 = dot(n_ref[...], p_scr[...], TN).astype(LOW)
        d2 = dot(g_ref[...], h_scr[...], TN).astype(LOW)
        for f in range(shards):
            for t in range(each):
                dw_ref[f, t, 0] = d1[f * depth : (f + 1) * depth, t * cols : (t + 1) * cols]
                dw_ref[f, t, 1] = d2[f * depth : (f + 1) * depth, t * cols : (t + 1) * cols]

    if not first:

        @pl.when(step == 0)
        def _():
            for load in loads:
                load.wait()

    y_ref[...] += dot(h_scr[...], w2, NT)
    gn_ref[...] += dot(p_scr[...], w1, NT)
    if pairwise:

        @pl.when(step == pl.num_programs(0) - 1)
        def _():
            collect(step)


def mlp(part, start, cols, normed, grad_two, w_mlp, bias, carried, fsdp):
    rows, width = normed.shape
    shards = w_mlp.shape[0]
    each = max(512 // cols, 1)
    at = start // cols
    first, pairwise = carried is None, fsdp == 2
    single = pl.Buffered(1)
    full = pl.BlockSpec((rows, width), lambda s: (0, 0), pipeline_mode=single)
    depth = width // fsdp
    steps = shards // each
    acc_shape = jax.ShapeDtypeStruct((rows, width), F32)
    if pairwise:
        out_w = pl.BlockSpec((shards, 2, depth, cols), lambda s: (0, 0, 0, 0), pipeline_mode=single)
        w_shape = jax.ShapeDtypeStruct((shards, 2, depth, cols), LOW)
        extra = exchange_scratch(2, (2, depth, each * cols))
    else:
        out_w = pl.BlockSpec((fsdp, each, 2, depth, cols), lambda s: (0, s, 0, 0, 0))
        w_shape = jax.ShapeDtypeStruct((fsdp, shards, 2, depth, cols), LOW)
        extra = []
    return pl.pallas_call(
        functools.partial(mlp_kernel, first, pairwise),
        grid=(steps,),
        in_specs=[
            full,
            full,
            pl.BlockSpec((each, 1, width, cols), lambda s: (s, 0, 0, at)),
            pl.BlockSpec((each, 1, width, cols), lambda s: (s, 1, 0, at)),
            pl.BlockSpec((each, 1, cols), lambda s: (s, 0, at)),
        ]
        + ([] if first else [pl.BlockSpec(memory_space=pl.ANY)] * 2),
        out_specs=[full, full, out_w, pl.BlockSpec((each, 1, cols), lambda s: (s, 0, 0))],
        out_shape=[acc_shape, acc_shape, w_shape, jax.ShapeDtypeStruct((shards, 1, cols), F32)],
        scratch_shapes=[
            pltpu.VMEM((rows, each * cols), LOW),
            pltpu.VMEM((rows, each * cols), LOW),
            pltpu.SemaphoreType.DMA((2,)),
            *extra,
        ],
        compiler_params=params(2 + part if pairwise else None),
        cost_estimate=cost(12 * rows * width * cols * shards, 24 * rows * width),
        name=f"mlp_{part}",
    )(normed, grad_two, w_mlp, w_mlp, bias, *([] if first else carried))


def turn_kernel(seq, pairwise, alive_ref, resid_ref, y_ref, gn_ref, g2_ref, att_ref, w_ref, vec_ref,
                out_ref, gr_ref, ga_ref, dw_ref, sums_ref, dw_scr, *exchange):
    i = pl.program_id(0)
    if pairwise:
        pl.when(i == 0)(greet_partner)
    shards, _, _, cols = w_ref.shape
    resid = resid_ref[...]
    out_ref[0] = ((resid + y_ref[...] + vec_ref[7:8]) * alive_ref[i]).astype(LOW)[0:seq]
    normal, inverse = centred(resid)
    upstream = gn_ref[...]
    grad_out = g2_ref[...].astype(F32)
    grad_resid = grad_out + norm_back(upstream, normal, inverse, vec_ref[2:3])
    gr_ref[...] = grad_resid
    low = grad_resid.astype(LOW)
    rows = [
        jnp.sum(upstream * normal, axis=0, keepdims=True),
        jnp.sum(upstream, axis=0, keepdims=True),
        jnp.sum(grad_resid, axis=0, keepdims=True),
        jnp.sum(grad_out, axis=0, keepdims=True),
    ]
    rows = jnp.concatenate(rows, axis=0)

    @pl.when(i == 0)
    def _():
        sums_ref[...] = rows

    @pl.when(i != 0)
    def _():
        sums_ref[...] += rows

    for t in range(shards):
        ga_ref[:, t * cols : (t + 1) * cols] = dot(low, w_ref[t, 0]).astype(LOW)
    part = dot(low, att_ref[...], TN)

    @pl.when(i == 0)
    def _():
        dw_scr[...] = part

    @pl.when(i != 0)
    def _():
        dw_scr[...] += part

    @pl.when(i == pl.num_programs(0) - 1)
    def _():
        if pairwise:
            sent, received, sends, receives = exchange
            ours, theirs = bands(dw_scr.shape[0] // 2)
            sent[0] = dw_scr[theirs, :].astype(LOW)
            copy = to_partner(sent, received, sends, receives, 0)
            copy.start()
            copy.wait()
            total = (dw_scr[ours, :] + received[0].astype(F32)).astype(LOW)
            for t in range(shards):
                dw_ref[t, 0] = total[:, t * cols : (t + 1) * cols]
            return
        depth = dw_ref.shape[3]
        for f in range(dw_ref.shape[0]):
            for t in range(shards):
                dw_ref[f, t, 0] = dw_scr[f * depth : (f + 1) * depth, t * cols : (t + 1) * cols].astype(LOW)


def turn(alive, resid, branch, grad_normed, grad_two, attended, w_attn, vec, images, seq, fsdp):
    rows, width = resid.shape
    span = rows // images
    shards, _, _, cols = w_attn.shape
    depth = width // fsdp
    pairwise = fsdp == 2
    lead = () if pairwise else (fsdp,)
    block = pl.BlockSpec((span, width), lambda i: (i, 0))
    return pl.pallas_call(
        functools.partial(turn_kernel, seq, pairwise),
        grid=(images,),
        in_specs=[
            pl.BlockSpec(memory_space=pltpu.SMEM),
            block, block, block, block, block,
            pl.BlockSpec((shards, 1, width, cols), lambda i: (0, 3, 0, 0)),
            pl.BlockSpec(vec.shape, lambda i: (0, 0)),
        ],
        out_specs=[
            pl.BlockSpec((1, seq, width), lambda i: (i, 0, 0)),
            block, block,
            pl.BlockSpec((*lead, shards, 1, depth, cols), lambda i: (0,) * (4 + len(lead))),
            pl.BlockSpec((4, width), lambda i: (0, 0)),
        ],
        out_shape=[
            jax.ShapeDtypeStruct((images, seq, width), LOW),
            jax.ShapeDtypeStruct((rows, width), F32),
            jax.ShapeDtypeStruct((rows, width), LOW),
            jax.ShapeDtypeStruct((*lead, shards, 1, depth, cols), LOW),
            jax.ShapeDtypeStruct((4, width), F32),
        ],
        scratch_shapes=[pltpu.VMEM((width, width), F32)] + (exchange_scratch(1, (depth, width))[1:] if pairwise else []),
        compiler_params=params(6 if pairwise else None),
        cost_estimate=cost(4 * rows * width * width, 24 * rows * width),
        name="turn",
    )(alive, resid, branch, grad_normed, grad_two, attended, w_attn, vec)


def carrier(groups, paired, diff_ref, total_ref, mine, landed, sends, receives, loaded):
    g, f, t = lax.axis_index("group"), lax.axis_index("fsdp"), lax.axis_index("tensor")
    quarter = landed.shape[1]

    def rows(n):
        return pl.ds(pl.multiple_of(n * quarter, quarter), quarter)

    def other(k):
        return (lax.rem(g + k, groups), f, t)

    def part(k):
        return pltpu.make_async_remote_copy(
            src_ref=diff_ref.at[rows(lax.rem(g + k, groups)), :],
            dst_ref=landed.at[k],
            send_sem=sends.at[k],
            recv_sem=receives.at[k],
            device_id=other(k),
            device_id_type=MESH,
        )

    keep = pltpu.make_async_copy(diff_ref.at[rows(g), :], mine, loaded.at[0])

    def begin():
        barrier = pltpu.get_barrier_semaphore()
        if paired:
            pl.semaphore_signal(barrier, inc=1, device_id=partner(), device_id_type=MESH)
        for k in range(1, groups):
            pl.semaphore_signal(barrier, inc=1, device_id=other(k), device_id_type=MESH)
        pl.semaphore_wait(barrier, groups - 1 + int(paired))
        for k in range(1, groups):
            part(k).start()
        keep.start()

    def end():
        keep.wait()
        total = mine[...].astype(F32)
        for k in range(1, groups):
            part(k).wait()
            total = total + landed[k].astype(F32)
        total_ref[...] = total.astype(LOW)

    return begin, end


def carrier_scratch(groups, quarter, lanes):
    dma = pltpu.SemaphoreType.DMA
    return [
        pltpu.VMEM((quarter, lanes), LOW),
        pltpu.VMEM((groups, quarter, lanes), LOW),
        dma((groups,)),
        dma((groups,)),
        dma((1,)),
    ]


def unattend_kernel(seq, groups, q_ref, k_ref, v_ref, g_ref, *refs):
    if groups:
        diff_ref, out_ref, total_ref, *scratch = refs
        begin, end = carrier(groups, False, diff_ref, total_ref, *scratch)
        pl.when((pl.program_id(0) == 0) & (pl.program_id(1) == 0))(begin)
    else:
        (out_ref,) = refs
    span = q_ref.shape[1]
    scale = HD**-0.5
    q, k, v, g = q_ref[0], k_ref[0], v_ref[0], g_ref[...]
    parts = []
    for h in range(2):
        scores = dot(half_lanes(k, h), q, NT)
        row = lax.broadcasted_iota(jnp.int32, scores.shape, 0)
        scores = jnp.where(row < seq, scores, -1e30)
        top = jnp.max(scores, axis=0, keepdims=True)
        raised = jnp.exp((scores - top) * scale)
        total = jnp.sum(raised, axis=0, keepdims=True)
        probs = raised * (1.0 / total)
        gp = dot(half_lanes(v, h), g, NT)
        delta = jnp.sum(probs * gp, axis=0, keepdims=True)
        gs = (probs * (gp - delta)).astype(LOW)
        dv = dot(probs.astype(LOW), g)
        dk = dot(gs, q)
        dq = dot(gs, k, TN)
        parts.append((dq, dk, dv))
    lane = lax.broadcasted_iota(jnp.int32, (span, 2 * HD), 1) < HD
    out_ref[0] = (jnp.where(lane, parts[0][0], parts[1][0]) * scale).astype(LOW)
    out_ref[1] = (jnp.where(lane, parts[0][1], parts[1][1]) * scale).astype(LOW)
    out_ref[2] = jnp.where(lane, parts[0][2], parts[1][2]).astype(LOW)
    if groups:
        at_end = (pl.program_id(0) == pl.num_programs(0) - 1) & (pl.program_id(1) == pl.num_programs(1) - 1)
        pl.when(at_end)(end)


def unattend(qkv, grad_attended, images, seq, part, parts, shards, diff=None, groups=0):
    _, rows, width = qkv.shape
    span = rows // images
    pair = 2 * HD
    each = width // shards // parts // pair

    def spot(h):
        return (h // each) * (each * parts) + part * each + h % each

    def take(j):
        return pl.BlockSpec((1, span, pair), lambda i, h: (j, i, spot(h)))

    in_specs = [take(0), take(1), take(2), pl.BlockSpec((span, pair), lambda i, h: (i, spot(h)))]
    out_specs = [pl.BlockSpec((3, span, pair), lambda i, h: (0, i, h))]
    out_shape = [jax.ShapeDtypeStruct((3, rows, width // parts), LOW)]
    scratch = []
    if groups:
        quarter, lanes = diff.shape[0] // groups, diff.shape[1]
        in_specs.append(pl.BlockSpec(memory_space=pl.ANY))
        out_specs.append(pl.BlockSpec((quarter, lanes), lambda i, h: (0, 0)))
        out_shape.append(jax.ShapeDtypeStruct((quarter, lanes), LOW))
        scratch = carrier_scratch(groups, quarter, lanes)
    return pl.pallas_call(
        functools.partial(unattend_kernel, seq, groups),
        grid=(images, width // pair // parts),
        in_specs=in_specs,
        out_specs=out_specs,
        out_shape=out_shape,
        scratch_shapes=scratch,
        compiler_params=params(9 if groups else None),
        cost_estimate=cost(
            40 * rows * span * width // parts, 14 * rows * width // parts, rows * span * (width // HD) // parts
        ),
        name=f"unattend_{part}",
    )(qkv, qkv, qkv, grad_attended, *([diff] if groups else []))


def close_kernel(pairwise, groups, first, final, n_ref, grad_ref, w_ref, *refs):
    if not first:
        carry_ref, *refs = refs
    elif pairwise:
        more_ref, *refs = refs
    if pairwise and final:
        diff_ref, acc_ref, total_ref, *refs = refs
    else:
        acc_ref, *refs = refs
    dw_ref, sums_ref, acc_scr, *exchange = refs
    j = pl.program_id(0)
    shards, _, _, cols = w_ref.shape
    if pairwise:
        own, sent, received, sends, receives, *exchange = exchange
        if not final:
            pl.when(j == 0)(greet_partner)
    if pairwise and final:
        begin, end = carrier(groups, True, diff_ref, total_ref, *exchange)
        pl.when(j == 0)(begin)

    @pl.when(j == 0)
    def _():
        acc_scr[...] = jnp.zeros_like(acc_scr) if first else carry_ref[...]

    sums = jnp.sum(grad_ref[0].astype(F32), axis=0, keepdims=True)
    for n, matrix in enumerate((0, 2)):

        @pl.when(j == matrix)
        def _():
            sums_ref[n : n + 1, :] = sums

    def spread(n, total, f=None):
        for t in range(shards):
            piece = total[:, t * cols : (t + 1) * cols]
            if f is None:
                dw_ref[t, n] = piece
            else:
                dw_ref[f, t, 0] = piece

    weight = jnp.concatenate([w_ref[t, 0] for t in range(shards)], axis=1)
    if pairwise:
        ours, theirs = bands(n_ref.shape[1] // 2)
        sent[j] = dot(n_ref[:, theirs], grad_ref[0], TN).astype(LOW)
        to_partner(sent, received, sends, receives, j).start()
        own[j] = dot(n_ref[:, ours], grad_ref[0], TN)
    else:
        depth = dw_ref.shape[3]
        dw = dot(n_ref[...], grad_ref[0], TN).astype(LOW)
        for f in range(dw_ref.shape[0]):
            spread(0, dw[f * depth : (f + 1) * depth], f)
    acc_scr[...] += dot(grad_ref[0], weight, NT)

    @pl.when(j == 2)
    def _():
        if pairwise:
            for n in range(own.shape[0]):
                to_partner(sent, received, sends, receives, n).wait()
                spread(n, (own[n] + received[n].astype(F32)).astype(LOW))
            if first:
                for t in range(shards):
                    for n in range(dw_ref.shape[1] - 3):
                        dw_ref[t, 3 + n] = more_ref[t, 0, :, n * cols : (n + 1) * cols]
        acc_ref[...] = acc_scr[...]
        if pairwise and final:
            end()


def close(part, parts, normed, grads, w_attn, carry, more, ending, fsdp, groups):
    rows, width = normed.shape
    shards, _, _, cols = w_attn.shape
    cols = cols // parts
    lanes = shards * cols
    depth = width // fsdp
    pairwise, first, final = fsdp == 2, carry is None, ending is not None
    single = pl.Buffered(1)
    stack = pl.BlockSpec((1, rows, lanes), lambda j: (j, 0, 0))
    full = pl.BlockSpec((rows, width), lambda j: (0, 0), pipeline_mode=single)
    if pairwise:
        many = 3 + parts if first else 3
        dw_spec = pl.BlockSpec((shards, many, depth, cols), lambda j: (0, 0, 0, 0), pipeline_mode=single)
        dw_shape = jax.ShapeDtypeStruct((shards, many, depth, cols), LOW)
        extra = exchange_scratch(3, (depth, lanes))
    else:
        dw_spec = pl.BlockSpec((fsdp, shards, 1, depth, cols), lambda j: (0, 0, j, 0, 0))
        dw_shape = jax.ShapeDtypeStruct((fsdp, shards, 3, depth, cols), LOW)
        extra = []
    in_specs = [full, stack, pl.BlockSpec((shards, 1, width, cols), lambda j: (0, j, 0, part))]
    out_specs, out_shape = [], []
    if not first:
        in_specs.append(full)
    elif pairwise:
        in_specs.append(pl.BlockSpec(more.shape, lambda j: (0, 0, 0, 0), pipeline_mode=single))
    out_specs.append(full)
    out_shape.append(jax.ShapeDtypeStruct((rows, width), F32))
    if pairwise and final:
        quarter, lanes_two = ending.shape[0] // groups, ending.shape[1]
        in_specs.append(pl.BlockSpec(memory_space=pl.ANY))
        out_specs.append(pl.BlockSpec((quarter, lanes_two), lambda j: (0, 0), pipeline_mode=single))
        out_shape.append(jax.ShapeDtypeStruct((quarter, lanes_two), LOW))
        extra = [*extra, *carrier_scratch(groups, quarter, lanes_two)]
    return pl.pallas_call(
        functools.partial(close_kernel, pairwise, groups, first, final),
        grid=(3,),
        in_specs=in_specs,
        out_specs=[*out_specs, dw_spec, pl.BlockSpec((2, lanes), lambda j: (0, 0))],
        out_shape=[*out_shape, dw_shape, jax.ShapeDtypeStruct((2, lanes), F32)],
        scratch_shapes=[pltpu.VMEM((rows, width), F32), *extra],
        compiler_params=params(7 + part if pairwise else None),
        cost_estimate=cost(12 * rows * width * lanes, 20 * rows * width),
        name=f"close_{part}",
    )(normed, grads, w_attn, *([carry] if not first else [more] if pairwise else []), *([ending] if pairwise and final else []))


def finish_kernel(acc_ref, gr_ref, x_ref, vec_ref, out_ref, norm_ref):
    i = pl.program_id(0)
    seq = out_ref.shape[1]
    normal, inverse = centred(x_ref[...].astype(F32))
    upstream = acc_ref[...]
    grad = gr_ref[...] + norm_back(upstream, normal, inverse, vec_ref[0:1])
    out_ref[0, :, 0, :] = grad[0:seq]
    sums = [jnp.sum(upstream * normal, axis=0, keepdims=True), jnp.sum(upstream, axis=0, keepdims=True)]
    sums = jnp.concatenate(sums, axis=0)

    @pl.when(i == 0)
    def _():
        norm_ref[...] = sums

    @pl.when(i != 0)
    def _():
        norm_ref[...] += sums


def finish(acc, grad_resid, x_rows, vec, images, seq):
    rows, width = acc.shape
    block = pl.BlockSpec((rows // images, width), lambda i: (i, 0))
    return pl.pallas_call(
        finish_kernel,
        grid=(images,),
        in_specs=[block, block, block, pl.BlockSpec(vec.shape, lambda i: (0, 0))],
        out_specs=[pl.BlockSpec((1, seq, 1, width), lambda i: (i, 0, 0, 0)), pl.BlockSpec((2, width), lambda i: (0, 0))],
        out_shape=[
            jax.ShapeDtypeStruct((images, seq, 1, width), F32),
            jax.ShapeDtypeStruct((2, width), F32),
        ],
        compiler_params=params(),
        cost_estimate=cost(20 * rows * width, 14 * rows * width),
        name="finish",
    )(acc, grad_resid, x_rows, vec)


def attend_pair(seq, q, k, v):
    scale = HD**-0.5
    parts = []
    for h in range(2):
        scores = dot(q, half_lanes(k, h), NT)
        lane = lax.broadcasted_iota(jnp.int32, scores.shape, 1)
        scores = jnp.where(lane < seq, scores, -1e30)
        top = jnp.max(scores, axis=1, keepdims=True)
        raised = jnp.exp((scores - top) * scale)
        total = jnp.sum(raised, axis=1, keepdims=True)
        probs = (raised * (1.0 / total)).astype(LOW)
        parts.append(dot(probs, v))
    lane = lax.broadcasted_iota(jnp.int32, parts[0].shape, 1)
    return jnp.where(lane < HD, parts[0], parts[1]).astype(LOW)


def front_kernel(
    images, seq, alive_ref, a_in, m_in, x_ref, g_ref, vec_ref,
    a_out, m_out, n_out, qkv_out, att_out, resid_out, n2_out, g2_out, x_out,
    a_wide, m_wide, a_hold, m_hold, n_scr, qkv_scr, att_scr, w_scr, o_scr, resid_scr, n2_scr, g2_scr, x_all,
    zs, zr, xs, xr, ys, yr, xfs, xfr, yfs, yfr, cs, cr, ls, ws,
):
    g, f, z = lax.axis_index("group"), lax.axis_index("fsdp"), lax.axis_index("tensor")
    shards = lax.axis_size("tensor")
    last = shards - 1
    x_at, y_at = g % 2, g // 2
    east, north = y_at * 2 + (1 - x_at), (1 - y_at) * 2 + x_at
    depth, cols = a_in.shape[1:]
    band = depth // 4
    shared = band * 3 // 8
    rest = band - 2 * shared
    span = n_scr.shape[0] // images

    def place(column):
        cx, cy = column % 2, column // 2
        return 2 * (cx + cy - 2 * cx * cy) + cy

    mine, of_east, of_north = place(g), place(east), place(north)
    z_row = mine * band - shared * (mine % 2)
    lead_east = of_east * band + shared * (of_east % 2)
    lead_north = of_north * band + shared * (of_north % 2)
    chunks = ((a_out, 0, 3), (a_out, 3, 1), (m_out, 0, 1), (m_out, 1, 1))

    def tile(n):
        return pl.multiple_of(n, 16)

    def held(n, t, row, rows):
        out, j, many = chunks[n]
        return out.at[t, pl.ds(j, many), pl.ds(tile(f * depth + row), rows), :]

    def send(part, sems, semr, n, t, to):
        return pltpu.make_async_remote_copy(
            src_ref=part, dst_ref=part, send_sem=sems.at[n, t], recv_sem=semr.at[n, t], device_id=to, device_id_type=MESH
        )

    def along(n, t, up):
        part = held(n, t, z_row, band + shared)
        return pltpu.make_async_remote_copy(
            src_ref=part,
            dst_ref=part,
            send_sem=zs.at[n, t, 0 if up else 1],
            recv_sem=zr.at[n, t],
            device_id=(g, f, z + 1 if up else z - 1),
            device_id_type=MESH,
        )

    def to_east(n, t):
        return send(held(n, t, mine * band, band), xs, xr, n, t, (east, f, z))

    def to_north(n, t):
        return send(held(n, t, mine * band, band), ys, yr, n, t, (north, f, z))

    def north_to_east(n, t):
        return send(held(n, t, lead_north, shared), xfs, xfr, n, t, (east, f, z))

    def east_to_north(n, t):
        return send(held(n, t, lead_east + shared, rest), yfs, yfr, n, t, (north, f, z))

    def across(n, t):
        return send(held(n, t, 0, depth), cs, cr, n, t, (g, 1 - f, z))

    rows = pl.ds(tile(f * depth), depth)
    loads = (
        pltpu.make_async_copy(a_in, a_wide, ls.at[0]),
        pltpu.make_async_copy(m_in, m_wide, ls.at[1]),
    )
    keeps = (
        pltpu.make_async_copy(a_hold, a_out.at[z, :, rows, :], ls.at[2]),
        pltpu.make_async_copy(m_hold, m_out.at[z, :, rows, :], ls.at[3]),
    )
    loads[0].start()

    barrier = pltpu.get_barrier_semaphore()

    def greet(to):
        pl.semaphore_signal(barrier, inc=1, device_id=to, device_id_type=MESH)

    for to in ((east, f, z), (north, f, z), (g, 1 - f, z)):
        greet(to)

    @pl.when(z > 0)
    def _():
        greet((g, f, z - 1))

    @pl.when(z < last)
    def _():
        greet((g, f, z + 1))

    loads[0].wait()
    a_hold[...] = a_wide[...].astype(LOW)
    keeps[0].start()
    pl.semaphore_wait(barrier, 3 + jnp.minimum(z, 1) + jnp.minimum(last - z, 1))
    keeps[0].wait()

    count = len(chunks)

    def when_real(k, up, run):
        @pl.when(z - k >= 0 if up else z + k <= last)
        def _():
            run(z - k if up else z + k)

    def own(n):
        @pl.when(z < last)
        def _():
            along(n, z, True).start()

        @pl.when(z > 0)
        def _():
            along(n, z, False).start()

        across(n, z).start()

    def land(n, k, up):
        def run(t):
            along(n, t, up).wait_recv()

            @pl.when(z < last if up else z > 0)
            def _():
                along(n, t, up).start()

            to_east(n, t).start()
            to_north(n, t).start()

        when_real(k, up, run)

    def relay(n, k, up):
        def run(t):
            to_east(n, t).wait_recv()
            east_to_north(n, t).start()
            to_north(n, t).wait_recv()
            north_to_east(n, t).start()

        when_real(k, up, run)

    def finish(n, k, up):
        def run(t):
            east_to_north(n, t).wait_recv()
            north_to_east(n, t).wait_recv()
            across(n, t).start()

        when_real(k, up, run)

    def both(run, n, k):
        for up in (True, False):
            run(n, k, up)

    def fetch(t):
        return pltpu.make_async_copy(a_out.at[t, pl.ds(0, 3)], w_scr, ws.at[0])

    def maps(t):
        across(0, t).wait_recv()
        fetch(t).start()
        fetch(t).wait()
        here = pl.ds(pl.multiple_of(t * cols, cols), cols)

        def body(j, carry):
            bias = jnp.where(j == 0, vec_ref[4:5, here], jnp.where(j == 2, vec_ref[5:6, here], 0.0))
            qkv_scr[j, :, here] = (dot(n_scr[...], w_scr[j]) + bias).astype(LOW)
            return carry

        lax.fori_loop(0, 3, body, 0)

    def project(k):
        def body(d, carry):
            t = z - k + 2 * k * d

            @pl.when((t >= 0) & (t <= last))
            def _():
                maps(t)

            return carry

        lax.fori_loop(0, 2, body, 0)

    own(0)
    loads[1].start()
    n_scr[...] = jnp.zeros_like(n_scr)
    x_all[...] = jnp.zeros_like(x_all)
    g2_scr[...] = jnp.zeros_like(g2_scr)
    for i in range(images):
        here = pl.ds(i * span, seq)
        image = x_ref[:, i, :]
        x_all[here, :] = image
        normal, _ = centred(image.astype(F32))
        n_scr[here, :] = (normal * vec_ref[0:1] + vec_ref[1:2]).astype(LOW)
    puts = [pltpu.make_async_copy(n_scr, n_out, ws.at[1])]
    puts[0].start()
    puts.append(pltpu.make_async_copy(x_all, x_out, ws.at[7]))
    puts[-1].start()
    both(land, 0, 1)
    loads[1].wait()
    m_hold[...] = m_wide[...].astype(LOW)
    keeps[1].start()
    maps(z)
    both(land, 0, 2)
    both(relay, 0, 1)
    keeps[1].wait()
    both(land, 0, 3)
    for n in range(1, count):
        own(n)
    both(relay, 0, 2)
    both(finish, 0, 1)
    both(relay, 0, 3)
    both(finish, 0, 2)
    project(1)
    both(finish, 0, 3)
    project(2)

    rest_items = [(n, k) for k in range(1, last + 1) for n in range(1, count)]
    total = len(rest_items) + 2

    def advance(at):
        if at < len(rest_items):
            both(land, *rest_items[at])
        if 0 <= at - 1 < len(rest_items):
            both(relay, *rest_items[at - 1])
        if 0 <= at - 2 < len(rest_items):
            both(finish, *rest_items[at - 2])

    advance(0)
    project(3)
    puts.append(pltpu.make_async_copy(qkv_scr, qkv_out, ws.at[2]))
    puts[-1].start()

    pair = 2 * HD
    pairs = qkv_scr.shape[2] // pair
    stretch = max(pairs // 4, 1)
    segments = images * pairs // stretch

    def segment(n, carry):
        def body(m, carry):
            at = n * stretch + m
            lanes = pl.ds(pl.multiple_of(lax.rem(at, pairs) * pair, pair), pair)
            here = pl.ds(pl.multiple_of(at // pairs * span, 16), span)
            att_scr[here, lanes] = attend_pair(
                seq, qkv_scr[0, here, lanes], qkv_scr[1, here, lanes], qkv_scr[2, here, lanes]
            )
            return carry

        lax.fori_loop(0, stretch, body, 0)
        for c in range(min(segments, total - 3)):
            pl.when(n == c)(functools.partial(advance, 1 + c))
        return carry

    lax.fori_loop(0, segments, segment, 0)
    at = 1 + min(segments, total - 3)
    puts.append(pltpu.make_async_copy(att_scr, att_out, ws.at[3]))
    puts[-1].start()
    for i in range(images):
        g2_scr[pl.ds(i * span, seq), :] = (g_ref[:, i, :].astype(F32) * alive_ref[i]).astype(LOW)
    while at < total - 2:
        advance(at)
        at += 1

    for t in range(shards):
        across(1, t).wait_recv()
    take = pltpu.make_async_copy(a_out.at[:, 3], o_scr, ws.at[0])
    take.start()
    take.wait()

    def mix_image(i, carry):
        here = pl.ds(pl.multiple_of(i * span, 16), span)
        out = x_all[here, :].astype(F32) + vec_ref[6:7]
        for t in range(shards):
            out = out + dot(att_scr[here, t * cols : (t + 1) * cols], o_scr[t], NT)
        resid_scr[here, :] = out
        normal, _ = centred(out)
        n2_scr[here, :] = (normal * vec_ref[2:3] + vec_ref[3:4]).astype(LOW)
        for c in range(min(images, total - at)):
            pl.when(i == c)(functools.partial(advance, at + c))
        return carry

    lax.fori_loop(0, images, mix_image, 0)
    at += min(images, total - at)
    for n, (src, dst) in enumerate(((resid_scr, resid_out), (n2_scr, n2_out), (g2_scr, g2_out))):
        puts.append(pltpu.make_async_copy(src, dst, ws.at[4 + n]))
        puts[-1].start()
    while at < total:
        advance(at)
        at += 1
    for put in puts:
        put.wait()

    for n in range(count):
        @pl.when(z < last)
        def _():
            along(n, z, True).wait_send()

        @pl.when(z > 0)
        def _():
            along(n, z, False).wait_send()

        for t in range(shards):
            across(n, t).wait_send()
            if n > 1:
                across(n, t).wait_recv()

    def settle(n, k, up):
        def run(t):
            @pl.when(z < last if up else z > 0)
            def _():
                along(n, t, up).wait_send()

            to_east(n, t).wait_send()
            to_north(n, t).wait_send()
            east_to_north(n, t).wait_send()
            north_to_east(n, t).wait_send()

        when_real(k, up, run)

    for n in range(count):
        for k in range(1, last + 1):
            both(settle, n, k)


def front(alive, attn_master, mlp_master, patches, cotangent, vec, shards):
    _, depth, a_cols = attn_master.shape
    _, _, m_cols = mlp_master.shape
    seq, images, width = patches.shape
    rows = images * padded(seq)
    anywhere = pl.BlockSpec(memory_space=pl.ANY)
    inside = pl.BlockSpec(memory_space=pltpu.VMEM)
    dma = pltpu.SemaphoreType.DMA
    low = jax.ShapeDtypeStruct((rows, width), LOW)
    return pl.pallas_call(
        functools.partial(front_kernel, images, seq),
        in_specs=[pl.BlockSpec(memory_space=pltpu.SMEM), anywhere, anywhere, inside, inside, inside],
        out_specs=[anywhere] * 9,
        out_shape=[
            jax.ShapeDtypeStruct((shards, 4, width, a_cols), LOW),
            jax.ShapeDtypeStruct((shards, 2, width, m_cols), LOW),
            low,
            jax.ShapeDtypeStruct((3, rows, width), LOW),
            low,
            jax.ShapeDtypeStruct((rows, width), F32),
            low,
            low,
            low,
        ],
        scratch_shapes=[
            pltpu.VMEM(attn_master.shape, F32),
            pltpu.VMEM(mlp_master.shape, F32),
            pltpu.VMEM(attn_master.shape, LOW),
            pltpu.VMEM(mlp_master.shape, LOW),
            pltpu.VMEM((rows, width), LOW),
            pltpu.VMEM((3, rows, width), LOW),
            pltpu.VMEM((rows, width), LOW),
            pltpu.VMEM((3, width, a_cols), LOW),
            pltpu.VMEM((shards, width, a_cols), LOW),
            pltpu.VMEM((rows, width), F32),
            pltpu.VMEM((rows, width), LOW),
            pltpu.VMEM((rows, width), LOW),
            pltpu.VMEM((rows, width), LOW),
            dma((4, shards, 2)),
        ]
        + [dma((4, shards))] * 11
        + [dma((4,)), dma((8,))],
        compiler_params=params(1),
        cost_estimate=cost(8 * rows * width * width, 30 * rows * width),
        name="front",
    )(alive, attn_master, mlp_master, patches, cotangent, vec)


def inner_adamw(master, gradient, first, second, step_rate, decay_rate):
    first_moment = 0.9 * first + 0.1 * gradient
    second_moment = 0.95 * second + 0.05 * gradient * gradient
    step_ratio = (
        first_moment / (1.0 - 0.9**STEP) / (jnp.sqrt(second_moment / (1.0 - 0.95**STEP)) + 1e-08)
    )
    return (master - step_rate * (step_ratio + decay_rate * master), second_moment)


def outer_nesterov(master, outer_old, difference):
    momentum = OUTER_MOMENTUM * outer_old + difference
    return momentum, master - OUTER_RATE * (difference + OUTER_MOMENTUM * momentum)


def inner_kernel(join, count, *refs):
    pieces, (master_ref, moment_ref, *_, inner_ref, diff_ref) = refs[:count], refs[count:]
    gradient = join(*[piece[0] for piece in pieces]).astype(F32)
    master = master_ref[0]
    new, second = inner_adamw(master, gradient, moment_ref[0, 0, 0], moment_ref[0, 1, 0], INNER_RATE, WEIGHT_DECAY)
    inner_ref[0, 0, 0] = gradient
    inner_ref[0, 1, 0] = second
    diff_ref[0] = (master - new).astype(LOW)


def inner_step(join, pieces, unit, units, cols, master, moments, into, name):
    depth = master.shape[1]
    rows = min(depth, 524288 // cols)
    block = pl.BlockSpec((1, rows, cols), lambda u, r: (unit(u)[0], r, unit(u)[1]))
    both = pl.BlockSpec((1, 2, 1, rows, cols), lambda u, r: (0, 0, unit(u)[0], r, unit(u)[1]))
    piece_specs = [pl.BlockSpec((1, rows, piece.shape[2]), lambda u, r: (u, r, 0)) for piece in pieces]
    count = len(pieces)
    return pl.pallas_call(
        functools.partial(inner_kernel, join, count),
        grid=(units, depth // rows),
        in_specs=[*piece_specs, block, both] + ([] if into is None else [pl.BlockSpec(memory_space=pl.ANY)]),
        out_specs=[both, pl.BlockSpec((1, rows, cols), lambda u, r: (u, r, 0))],
        out_shape=[
            jax.ShapeDtypeStruct(moments.shape, F32),
            jax.ShapeDtypeStruct((units, depth, cols), LOW),
        ],
        input_output_aliases={} if into is None else {count + 2: 0},
        compiler_params=params(),
        cost_estimate=cost(30 * units * depth * cols, 24 * units * depth * cols),
        name=name,
    )(*pieces, master, moments, *([] if into is None else [into]))


def outer_kernel(groups, slots, each, g_ref, *refs):
    totals, (master_ref, outer_ref, *_, state_ref, copy_ref) = refs[:slots], refs[slots:]
    rows = copy_ref.shape[1]
    if slots == 1:
        total = totals[0][0]
    else:
        at = pl.program_id(0) * pl.num_programs(1) + pl.program_id(1)
        slot = lax.rem(g_ref[0] + groups - at // each, groups)
        here = pl.ds(pl.multiple_of(lax.rem(at, each) * rows, rows), rows)
        total = totals[0][here, :]
        for n in range(1, slots):
            total = jnp.where(slot == n, totals[n][here, :], total)
    difference = total.astype(F32) / groups
    momentum, fresh = outer_nesterov(master_ref[0], outer_ref[0], difference)
    state_ref[0, 0] = difference
    state_ref[1, 0] = momentum
    state_ref[2, 0] = fresh
    copy_ref[0] = fresh.astype(LOW)


def outer_step(groups, me, totals, unit, units, cols, master, outer_old, into, name):
    depth = master.shape[1]
    slots = len(totals)
    rows = min(depth, 524288 // cols, totals[0].shape[-2])
    each = totals[0].shape[-2] // rows
    block = pl.BlockSpec((1, rows, cols), lambda u, r, g: (unit(u)[0], r, unit(u)[1]))
    state = pl.BlockSpec((3, 1, rows, cols), lambda u, r, g: (0, unit(u)[0], r, unit(u)[1]))
    if slots == 1:
        total = pl.BlockSpec((1, rows, cols), lambda u, r, g: (u, r, 0))
    else:
        total = pl.BlockSpec(totals[0].shape, lambda u, r, g: (0, 0))
    aliased = [] if into is None else [pl.BlockSpec(memory_space=pl.ANY)] * 2
    return pl.pallas_call(
        functools.partial(outer_kernel, groups, slots, each),
        grid_spec=pltpu.PrefetchScalarGridSpec(
            num_scalar_prefetch=1,
            grid=(units, depth // rows),
            in_specs=[*[total] * slots, block, block, *aliased],
            out_specs=[state, block],
        ),
        out_shape=[
            jax.ShapeDtypeStruct((3, *master.shape), F32),
            jax.ShapeDtypeStruct(master.shape, LOW),
        ],
        input_output_aliases={} if into is None else {slots + 3: 0, slots + 4: 1},
        compiler_params=params(),
        cost_estimate=cost(10 * units * depth * cols, 24 * units * depth * cols),
        name=name,
    )(me, *totals, master, outer_old, *([] if into is None else into))


def group_kernel(groups, shards, vectors, diff_ref, *refs):
    if vectors:
        part_ref, master_ref, moment_ref, outer_ref, total_ref, inner_ref, state_ref, copy_ref, *refs = refs
    else:
        total_ref, *refs = refs
    landed, summed, sends, receives, sends_two, receives_two, *small = refs
    g, f, t = lax.axis_index("group"), lax.axis_index("fsdp"), lax.axis_index("tensor")
    span = landed.shape[1]

    def rows(n):
        return pl.ds(pl.multiple_of(n * span, span), span)

    def other(k):
        return lax.rem(g + k, groups)

    def back(k):
        return lax.rem(g + groups - k, groups)

    def copy(src, dst, sems, semr, k, to):
        return pltpu.make_async_remote_copy(
            src_ref=src, dst_ref=dst, send_sem=sems.at[k], recv_sem=semr.at[k], device_id=to, device_id_type=MESH
        )

    def part(k):
        return copy(diff_ref.at[rows(other(k)), :], landed.at[k], sends, receives, k, (other(k), f, t))

    def result(k):
        return copy(summed, landed.at[groups + k], sends_two, receives_two, k, (other(k), f, t))

    barrier = pltpu.get_barrier_semaphore()
    for k in range(1, groups):
        pl.semaphore_signal(barrier, inc=1, device_id=(other(k), f, t), device_id_type=MESH)
    if vectors:
        stage, pair, mine, line, whole, few, diffs, ss, rs, ls, lr, gs, gr = small
        half = part_ref.shape[0] // 2
        halves = (pl.ds(0, half), pl.ds(half, half))

        def pick(ref):
            return jnp.where(f == 0, ref[halves[0], :], ref[halves[1], :])

        def line_copy(k):
            return copy(mine, line.at[k], ls, lr, k, (g, f, lax.rem(t + k, shards)))

        def few_copy(k):
            return copy(diffs.at[f], few.at[k], gs, gr, k, (other(k), f, t))

        pair_copy = copy(stage.at[1 - f], pair, ss, rs, 0, partner())
        whole_copy = copy(whole.at[f], whole.at[f], ss, rs, 1, partner())
        final_copy = copy(mine, stage.at[f], ss, rs, 2, partner())
        pl.semaphore_signal(barrier, inc=1, device_id=partner(), device_id_type=MESH)
        for k in range(1, shards):
            pl.semaphore_signal(barrier, inc=1, device_id=(g, f, lax.rem(t + k, shards)), device_id_type=MESH)
        stage[...] = jnp.zeros_like(stage)
        diffs[...] = jnp.zeros_like(diffs)
        for n in range(2):
            stage[n, 0:half] = part_ref[halves[n], :]
    pl.semaphore_wait(barrier, groups - 1 + (shards if vectors else 0))

    for k in range(1, groups):
        part(k).start()
    if vectors:
        pair_copy.start()
        pair_copy.wait()
        mine[...] = stage[f] + pair[...]
        for k in range(1, shards):
            line_copy(k).start()
        line[0] = mine[...]
        for k in range(1, shards):
            line_copy(k).wait()
        gradient = jnp.zeros(mine.shape, F32)
        for n in range(shards):
            gradient = gradient + line[lax.rem(t + shards - n, shards)]
        whole[f] = gradient
        whole_copy.start()
        new, _ = inner_adamw(
            pick(master_ref), gradient[0:half], pick(moment_ref.at[0]), pick(moment_ref.at[1]), VECTOR_RATE, 0.0
        )
        diffs[f, 0:half] = pick(master_ref) - new
        for k in range(1, groups):
            few_copy(k).start()
        few[0] = diffs[f]
        whole_copy.wait()
        for n in range(2):
            own = whole[n, 0:half]
            _, second = inner_adamw(
                master_ref[halves[n], :], own, moment_ref[0, halves[n], :], moment_ref[1, halves[n], :], VECTOR_RATE, 0.0
            )
            inner_ref[0, halves[n], :] = own
            inner_ref[1, halves[n], :] = second
    total = diff_ref[rows(g), :].astype(F32)
    for k in range(1, groups):
        part(k).wait_recv()
        total = total + landed[k].astype(F32)
    summed[...] = total.astype(LOW)
    for k in range(1, groups):
        result(k).start()
    total_ref[rows(g), :] = summed[...]
    if vectors:
        for k in range(1, groups):
            few_copy(k).wait()
        difference = jnp.zeros(mine.shape, F32)
        for n in range(groups):
            difference = difference + few[lax.rem(g + groups - n, groups)]
        mine[...] = difference / groups
        stage[f] = mine[...]
        final_copy.start()
        final_copy.wait()
        for n in range(2):
            difference = stage[n, 0:half]
            momentum, fresh = outer_nesterov(master_ref[halves[n], :], outer_ref[halves[n], :], difference)
            state_ref[0, halves[n], :] = difference
            state_ref[1, halves[n], :] = momentum
            state_ref[2, halves[n], :] = fresh
            copy_ref[halves[n], :] = fresh.astype(LOW)
    for k in range(1, groups):
        result(k).wait_recv()
        total_ref[rows(back(k)), :] = landed[groups + k]
    for k in range(1, groups):
        part(k).wait_send()
        result(k).wait_send()


def group_sum(diff, groups, identity, name, vectors=None, shards=0):
    flat = diff.reshape(-1, diff.shape[-1])
    span, cols = flat.shape[0] // groups, flat.shape[1]
    dma = pltpu.SemaphoreType.DMA
    whole = pl.BlockSpec(memory_space=pltpu.VMEM)
    out_shape = [jax.ShapeDtypeStruct(flat.shape, LOW)]
    extra = []
    if vectors:
        shape = vectors[0].shape
        half = (-(-shape[0] // 16) * 8, shape[1])
        out_shape += [
            jax.ShapeDtypeStruct((2, *shape), F32),
            jax.ShapeDtypeStruct((3, *shape), F32),
            jax.ShapeDtypeStruct(shape, LOW),
        ]
        extra = [
            pltpu.VMEM((2, *half), F32),
            pltpu.VMEM(half, F32),
            pltpu.VMEM(half, F32),
            pltpu.VMEM((shards, *half), F32),
            pltpu.VMEM((2, *half), F32),
            pltpu.VMEM((groups, *half), F32),
            pltpu.VMEM((2, *half), F32),
            dma((3,)),
            dma((3,)),
            dma((shards,)),
            dma((shards,)),
            dma((groups,)),
            dma((groups,)),
        ]
    total, *rest = pl.pallas_call(
        functools.partial(group_kernel, groups, shards, bool(vectors)),
        in_specs=[whole] * (5 if vectors else 1),
        out_specs=[whole] * len(out_shape),
        out_shape=out_shape,
        scratch_shapes=[
            pltpu.VMEM((2 * groups, span, cols), LOW),
            pltpu.VMEM((span, cols), LOW),
            *[dma((groups,))] * 4,
            *extra,
        ],
        compiler_params=params(identity),
        cost_estimate=cost(4 * flat.size, 8 * flat.size),
        name=name,
    )(flat, *(vectors or []))
    return total.reshape(diff.shape), *rest


def gather_weights(shard):
    whole = lax.all_gather(shard, "tensor", axis=0)
    return lax.all_gather(whole, "fsdp", axis=2, tiled=True)


def around(array, k, groups):
    return lax.ppermute(array, "group", [(i, (i + k) % groups) for i in range(groups)])


def exchange_parts(diff, groups):
    g = lax.axis_index("group")
    quarters = diff.reshape(groups, -1, diff.shape[-1])
    parts = [lax.dynamic_index_in_dim(quarters, lax.rem(g + k, groups), 0, keepdims=False) for k in range(groups)]
    total = sum([around(parts[k], k, groups).astype(F32) for k in range(1, groups)], parts[0].astype(F32))
    return total.astype(LOW)


def exchange_total(own, groups):
    return [own] + [around(own, k, groups) for k in range(1, groups)]


def scatter_gradient(gradient):
    half = gradient if gradient.ndim == 4 else lax.psum_scatter(gradient, "fsdp", scatter_dimension=0)
    return lax.psum_scatter(half, "tensor", scatter_dimension=0)


def local(
    patches,
    output_grad,
    live_counts,
    attn_master,
    mlp_master,
    vector_master,
    attn_moments,
    mlp_moments,
    vector_moments,
    attn_outer,
    mlp_outer,
    vector_outer,
):
    vec = vector_master
    tensor_size, fsdp = lax.axis_size("tensor"), lax.axis_size("fsdp")
    groups = lax.axis_size("group")
    local_images, seq, width = patches.shape[2:]
    slot = (lax.axis_index("fsdp") * tensor_size + lax.axis_index("tensor")) * local_images
    slot = slot + jnp.arange(local_images)
    counts = jnp.take(live_counts[0], slot // IMG_DEV, axis=1)
    alive = ((slot % IMG_DEV)[None, :] < counts).astype(F32).reshape(-1)
    x = patches.reshape(-1, seq, width)
    cotangent = output_grad.reshape(-1, seq, width)
    images = x.shape[0]

    if (groups, fsdp) == (4, 2):
        beside_images = [
            jnp.moveaxis(v.reshape(images, seq, width), 0, 1) for v in (patches, output_grad)
        ]
        w_attn, w_mlp, normed_one, qkv, attended, resid, normed_two, grad_two, x_rows = front(
            alive, attn_master, mlp_master, *beside_images, vec, tensor_size
        )
    else:
        w_attn = gather_weights(attn_master.astype(LOW))
        w_mlp = gather_weights(mlp_master.astype(LOW))
        normed_one, qkv = project(x, w_attn, vec)
        attended = attend(qkv, images, seq)
        resid, normed_two, grad_two = mix(alive, attended, x, cotangent, w_attn, vec)
        x_rows = jnp.pad(x, ((0, 0), (0, padded(seq) - seq), (0, 0))).reshape(-1, width)
    bias = vec[8:].reshape(tensor_size, 1, -1)
    carried = None
    mlp_grads, bias_parts = [], []
    for part, (start, cols) in enumerate(PIECES):
        *carried, dw, db = mlp(part, start, cols, normed_two, grad_two, w_mlp, bias, carried, fsdp)
        mlp_grads.append(scatter_gradient(dw))
        bias_parts.append(db)
    branch, grad_normed = carried
    block_output, grad_resid, grad_attended, dw_out, sums_two = turn(
        alive, resid, branch, grad_normed, grad_two, attended, w_attn, vec, images, seq, fsdp
    )
    def beside(*parts):
        return jnp.concatenate(parts, axis=-1)

    pairwise = fsdp == 2
    me = lax.axis_index("group").astype(jnp.int32).reshape(1)
    half = attn_master.shape[2] // PARTS
    (grads,) = unattend(qkv, grad_attended, images, seq, 0, PARTS, tensor_size)
    grads, mlp_grads[0] = lax.optimization_barrier((grads, mlp_grads[0]))
    carry, dw_early, head_sums = close(
        0, PARTS, normed_one, grads, w_attn, None, dw_out, None, fsdp, groups
    )
    if not pairwise:
        halves = jnp.moveaxis(dw_out.reshape(*dw_out.shape[:-1], PARTS, half), -2, 2)
        dw_early = jnp.concatenate([dw_early, halves[:, :, :, 0]], axis=2)
    early_grad = scatter_gradient(dw_early)
    head_sums = [head_sums]
    carry, mlp_grads[1] = lax.optimization_barrier((carry, mlp_grads[1]))
    hidden = mlp_master.shape[2] // 2
    mlp_inner, diff_one = inner_step(
        beside, mlp_grads[:2], lambda u: (u, 0), 2, hidden, mlp_master, mlp_moments, None, "inner_mlp_0"
    )
    riding = groups if pairwise else 0
    grads, *own_one = unattend(
        qkv, grad_attended, images, seq, 1, PARTS, tensor_size, diff_one.reshape(-1, hidden), riding
    )
    mlp_grads[2], grads = lax.optimization_barrier((mlp_grads[2], grads))
    mlp_inner, diff_two = inner_step(
        beside, mlp_grads[2:], lambda u: (u, 1), 2, hidden, mlp_master, mlp_moments, mlp_inner, "inner_mlp_1"
    )
    carry, diff_two = lax.optimization_barrier((carry, diff_two))
    carry, *own_two, dw_late, sums = close(
        1, PARTS, normed_one, grads, w_attn, carry, None, diff_two.reshape(-1, hidden), fsdp, groups
    )
    mlp_own = [beside(*own_one, *own_two)] if pairwise else []
    mlp_diff = beside(diff_one, diff_two)
    patches_grad, sums_one = finish(carry, grad_resid, x_rows, vec, images, seq)
    if not pairwise:
        mlp_own = [exchange_parts(mlp_diff, groups)]
    mlp_total = exchange_total(mlp_own[0], groups)
    late_grad = scatter_gradient(dw_late)
    head_sums.append(sums)

    def early(u):
        return jnp.minimum(u, 3), jnp.maximum(u - 3, 0)

    def late(u):
        return u, 1

    def first(piece):
        return piece

    attn_inner, early_diff = inner_step(
        first, [early_grad], early, 3 + PARTS, half, attn_master, attn_moments, None, "inner_early"
    )
    head_rows = jnp.concatenate([v.reshape(2, tensor_size, -1) for v in head_sums], axis=-1).reshape(2, width)
    hidden_bias = jnp.concatenate(bias_parts, axis=-1).reshape(-1, width)
    vector_part = jnp.concatenate([sums_one, sums_two[:2], head_rows, sums_two[2:], hidden_bias])

    if pairwise:
        early_total, vector_inner, vector_state, vector_copy = group_sum(
            early_diff,
            groups,
            10,
            "group_early",
            [vector_part, vec, vector_moments[0], vector_outer],
            tensor_size,
        )
    else:
        (early_total,) = group_sum(early_diff, groups, 10, "group_early")
        vector_grad = lax.psum(vector_part, ("fsdp", "tensor"))
        new_vector, second_vector = inner_adamw(
            vec, vector_grad, vector_moments[0, 0], vector_moments[0, 1], VECTOR_RATE, 0.0
        )
        diff_vector = lax.psum(vec - new_vector, "group") / groups
        momentum, fresh = outer_nesterov(vec, vector_outer, diff_vector)
        vector_inner = jnp.stack([vector_grad, second_vector])
        vector_state, vector_copy = jnp.stack([diff_vector, momentum, fresh]), fresh.astype(LOW)
    attn_state, attn_copy = outer_step(
        groups, me, [early_total], early, 3 + PARTS, half, attn_master, attn_outer, None, "outer_early"
    )
    attn_copy, *mlp_total = lax.optimization_barrier((attn_copy, *mlp_total))
    mlp_state, mlp_copy = outer_step(
        groups,
        me,
        mlp_total,
        lambda u: (u, 0),
        2,
        mlp_master.shape[2],
        mlp_master,
        mlp_outer,
        None,
        "outer_mlp",
    )
    late_grad, mlp_state = lax.optimization_barrier((late_grad, mlp_state))
    attn_inner, late_diff = inner_step(
        first, [late_grad], late, 3, half, attn_master, attn_moments, attn_inner, "inner_late"
    )
    (late_total,) = group_sum(late_diff, groups, 11, "group_late")
    attn_state, attn_copy = outer_step(
        groups, me, [late_total], late, 3, half, attn_master, attn_outer, (attn_state, attn_copy), "outer_late"
    )
    return (
        block_output.reshape(patches.shape),
        patches_grad.reshape(patches.shape),
        attn_inner,
        attn_state,
        attn_copy,
        mlp_inner,
        mlp_state,
        mlp_copy,
        vector_inner[None],
        vector_state,
        vector_copy,
    )


def solution(mesh):
    placed = (
        P("group", None, ("fsdp", "tensor"), None, None),
        P("group", None, ("fsdp", "tensor"), None, None),
        P("group", None, None),
        P(None, "fsdp", "tensor"),
        P(None, "fsdp", "tensor"),
        P(),
        P("group", None, None, "fsdp", "tensor"),
        P("group", None, None, "fsdp", "tensor"),
        P("group", None, None, None),
        P(None, "fsdp", "tensor"),
        P(None, "fsdp", "tensor"),
        P(),
    )
    return jax.shard_map(
        local,
        mesh=mesh,
        in_specs=placed,
        out_specs=(
            P("group", None, ("fsdp", "tensor"), None, None),
            P("group", None, ("fsdp", "tensor"), None, None),
            P("group", None, None, "fsdp", "tensor"),
            P(None, None, "fsdp", "tensor"),
            P(None, "fsdp", "tensor"),
            P("group", None, None, "fsdp", "tensor"),
            P(None, None, "fsdp", "tensor"),
            P(None, "fsdp", "tensor"),
            P("group", None, None, None),
            P(),
            P(),
        ),
        check_vma=False,
    )
```

```python
import functools

import jax
import jax.numpy as jnp
from jax import lax
from jax.experimental import pallas as pl
from jax.experimental.pallas import tpu as pltpu
from jax.sharding import PartitionSpec as P

HD = 64
STEP = 8
IMG_DEV = 4
EPSILON = 1e-06
INNER_RATE = 0.02
VECTOR_RATE = 0.2
WEIGHT_DECAY = 0.1
OUTER_RATE = 0.7
OUTER_MOMENTUM = 0.9
PIECES = ((0, 256), (256, 256), (512, 512))
PARTS = 2
LOW = jnp.bfloat16
F32 = jnp.float32
NN = (((1,), (0,)), ((), ()))
NT = (((1,), (1,)), ((), ()))
TN = (((0,), (0,)), ((), ()))


def dot(a, b, dims=NN):
    return lax.dot_general(a, b, dims, preferred_element_type=F32)


MESH = pl.DeviceIdType.MESH


def params(identity=None):
    if identity is None:
        return pltpu.CompilerParams(vmem_limit_bytes=60 * 2**20)
    return pltpu.CompilerParams(vmem_limit_bytes=60 * 2**20, collective_id=identity, has_side_effects=True)


def partner():
    return (lax.axis_index("group"), 1 - lax.axis_index("fsdp"), lax.axis_index("tensor"))


def greet_partner():
    barrier = pltpu.get_barrier_semaphore()
    pl.semaphore_signal(barrier, inc=1, device_id=partner(), device_id_type=MESH)
    pl.semaphore_wait(barrier, 1)


def to_partner(sent, received, sends, receives, n):
    return pltpu.make_async_remote_copy(
        src_ref=sent.at[n],
        dst_ref=received.at[n],
        send_sem=sends.at[n],
        recv_sem=receives.at[n],
        device_id=partner(),
        device_id_type=MESH,
    )


def bands(depth):
    f = lax.axis_index("fsdp")
    return pl.ds(pl.multiple_of(f * depth, depth), depth), pl.ds(pl.multiple_of((1 - f) * depth, depth), depth)


def exchange_scratch(steps, shape):
    dma = pltpu.SemaphoreType.DMA
    return [
        pltpu.VMEM((steps, *shape), F32),
        pltpu.VMEM((steps, *shape), LOW),
        pltpu.VMEM((steps, *shape), LOW),
        dma((steps,)),
        dma((steps,)),
    ]


def cost(flops, moved, special=0):
    return pl.CostEstimate(flops=int(flops), bytes_accessed=int(moved), transcendentals=int(special))


def padded(rows):
    return -(-rows // 16) * 16


def centred(source):
    centre = source - jnp.mean(source, axis=-1, keepdims=True)
    spread = jnp.mean(centre * centre, axis=-1, keepdims=True)
    inverse = lax.rsqrt(spread + EPSILON)
    return centre * inverse, inverse


def norm_back(upstream, normal, inverse, gain):
    pulled = upstream * gain
    mean_one = jnp.mean(pulled, axis=-1, keepdims=True)
    mean_two = jnp.mean(pulled * normal, axis=-1, keepdims=True)
    return inverse * (pulled - mean_one - normal * mean_two)


def project_kernel(images, seq, x_ref, w_ref, vec_ref, n_ref, out_ref, n_scr):
    j, t = pl.program_id(0), pl.program_id(1)
    span = n_scr.shape[0] // images

    @pl.when((j == 0) & (t == 0))
    def _():
        n_scr[...] = jnp.zeros_like(n_scr)
        for i in range(images):
            normal, _ = centred(x_ref[i].astype(F32))
            n_scr[pl.ds(i * span, seq), :] = (normal * vec_ref[0:1] + vec_ref[1:2]).astype(LOW)
        n_ref[...] = n_scr[...]

    cols = out_ref.shape[-1]
    out = dot(n_scr[...], w_ref[0, 0])
    at = pl.ds(pl.multiple_of(t * cols, cols), cols)
    bias = jnp.where(j == 0, vec_ref[4:5, at], jnp.where(j == 2, vec_ref[5:6, at], 0.0))
    out_ref[0] = (out + bias).astype(LOW)


def project(patches, w_attn, vec):
    images, seq, width = patches.shape
    shards, _, _, cols = w_attn.shape
    rows = images * padded(seq)
    return pl.pallas_call(
        functools.partial(project_kernel, images, seq),
        grid=(3, shards),
        in_specs=[
            pl.BlockSpec((images, seq, width), lambda j, t: (0, 0, 0)),
            pl.BlockSpec((1, 1, width, cols), lambda j, t: (t, j, 0, 0)),
            pl.BlockSpec(vec.shape, lambda j, t: (0, 0)),
        ],
        out_specs=[
            pl.BlockSpec((rows, width), lambda j, t: (0, 0)),
            pl.BlockSpec((1, rows, cols), lambda j, t: (j, 0, t)),
        ],
        out_shape=[
            jax.ShapeDtypeStruct((rows, width), LOW),
            jax.ShapeDtypeStruct((3, rows, width), LOW),
        ],
        scratch_shapes=[pltpu.VMEM((rows, width), LOW)],
        compiler_params=params(),
        cost_estimate=cost(6 * rows * width * width, 16 * rows * width),
        name="project",
    )(patches, w_attn, vec)


def half_lanes(value, which):
    lane = lax.broadcasted_iota(jnp.int32, value.shape, 1)
    return jnp.where((lane >= HD) == bool(which), value, jnp.zeros_like(value))


def attend_kernel(seq, q_ref, k_ref, v_ref, out_ref):
    span = q_ref.shape[1]
    scale = HD**-0.5
    q, k, v = q_ref[0], k_ref[0], v_ref[0]
    parts = []
    for h in range(2):
        scores = dot(q, half_lanes(k, h), NT)
        lane = lax.broadcasted_iota(jnp.int32, scores.shape, 1)
        scores = jnp.where(lane < seq, scores, -1e30)
        top = jnp.max(scores, axis=1, keepdims=True)
        raised = jnp.exp((scores - top) * scale)
        total = jnp.sum(raised, axis=1, keepdims=True)
        probs = (raised * (1.0 / total)).astype(LOW)
        parts.append(dot(probs, v))
    lane = lax.broadcasted_iota(jnp.int32, (span, 2 * HD), 1)
    out_ref[...] = jnp.where(lane < HD, parts[0], parts[1]).astype(LOW)


def attend(qkv, images, seq):
    _, rows, width = qkv.shape
    span = rows // images
    pair = 2 * HD

    def take(j):
        return pl.BlockSpec((1, span, pair), lambda i, h: (j, i, h))

    return pl.pallas_call(
        functools.partial(attend_kernel, seq),
        grid=(images, width // pair),
        in_specs=[take(0), take(1), take(2)],
        out_specs=pl.BlockSpec((span, pair), lambda i, h: (i, h)),
        out_shape=jax.ShapeDtypeStruct((rows, width), LOW),
        compiler_params=params(),
        cost_estimate=cost(16 * rows * span * width, 8 * rows * width, rows * span * (width // HD)),
        name="attend",
    )(qkv, qkv, qkv)


def mix_kernel(seq, alive_ref, att_ref, x_ref, g_ref, w_ref, vec_ref, resid_ref, n_ref, g2_ref, x_scr):
    i = pl.program_id(0)
    shards, _, _, cols = w_ref.shape
    x_scr[...] = jnp.zeros_like(x_scr)
    x_scr[0:seq, :] = x_ref[0].astype(F32)
    total = x_scr[...] + vec_ref[6:7]
    for t in range(shards):
        total = total + dot(att_ref[:, t * cols : (t + 1) * cols], w_ref[t, 0], NT)
    resid_ref[...] = total
    normal, _ = centred(total)
    n_ref[...] = (normal * vec_ref[2:3] + vec_ref[3:4]).astype(LOW)
    x_scr[0:seq, :] = g_ref[0].astype(F32) * alive_ref[i]
    g2_ref[...] = x_scr[...].astype(LOW)


def mix(alive, attended, patches, cotangent, w_attn, vec):
    images, seq, width = patches.shape
    rows = attended.shape[0]
    span = rows // images
    shards, _, _, cols = w_attn.shape
    block = pl.BlockSpec((span, width), lambda i: (i, 0))
    whole = jax.ShapeDtypeStruct((rows, width), LOW)
    return pl.pallas_call(
        functools.partial(mix_kernel, seq),
        grid=(images,),
        in_specs=[
            pl.BlockSpec(memory_space=pltpu.SMEM),
            block,
            pl.BlockSpec((1, seq, width), lambda i: (i, 0, 0)),
            pl.BlockSpec((1, seq, width), lambda i: (i, 0, 0)),
            pl.BlockSpec((shards, 1, width, cols), lambda i: (0, 3, 0, 0)),
            pl.BlockSpec(vec.shape, lambda i: (0, 0)),
        ],
        out_specs=[block, block, block],
        out_shape=[jax.ShapeDtypeStruct((rows, width), F32), whole, whole],
        scratch_shapes=[pltpu.VMEM((span, width), F32)],
        compiler_params=params(),
        cost_estimate=cost(2 * rows * width * width, 16 * rows * width),
        name="mix",
    )(alive, attended, patches, cotangent, w_attn, vec)


def mlp_kernel(first, pairwise, n_ref, g_ref, w1_ref, w2_ref, bias_ref, *refs):
    if not first:
        yi_ref, gi_ref, *refs = refs
    y_ref, gn_ref, dw_ref, db_ref, h_scr, p_scr, loaded, *exchange = refs
    step = pl.program_id(0)
    each, _, width, cols = w1_ref.shape
    if not first:
        loads = (
            pltpu.make_async_copy(yi_ref, y_ref, loaded.at[0]),
            pltpu.make_async_copy(gi_ref, gn_ref, loaded.at[1]),
        )

    @pl.when(step == 0)
    def _():
        if not first:
            for load in loads:
                load.start()
        else:
            y_ref[...] = jnp.zeros_like(y_ref)
            gn_ref[...] = jnp.zeros_like(gn_ref)
        if pairwise:
            greet_partner()

    w1 = jnp.concatenate([w1_ref[t, 0] for t in range(each)], axis=1)
    w2 = jnp.concatenate([w2_ref[t, 0] for t in range(each)], axis=1)
    bias = jnp.concatenate([bias_ref[t] for t in range(each)], axis=1)
    pre = dot(n_ref[...], w1) + bias
    cdf = 0.5 * (1.0 + lax.erf(pre * 0.7071067811865476))
    h_scr[...] = (pre * cdf).astype(LOW)
    slope = cdf + pre * jnp.exp(-0.5 * pre * pre) * 0.3989422804014327
    p_scr[...] = (dot(g_ref[...], w2) * slope).astype(LOW)
    sums = jnp.sum(p_scr[...].astype(F32), axis=0, keepdims=True)
    for t in range(each):
        db_ref[t] = sums[:, t * cols : (t + 1) * cols]

    if pairwise:
        own, sent, received, sends, receives = exchange
        ours, theirs = bands(width // 2)

        slot = lax.rem(step, 2)

        def collect(n):
            at = lax.rem(n, 2)
            to_partner(sent, received, sends, receives, at).wait()
            for which in range(2):
                total = (own[at, which] + received[at, which].astype(F32)).astype(LOW)
                for t in range(each):
                    dw_ref[n * each + t, which] = total[:, t * cols : (t + 1) * cols]

        @pl.when(step > 0)
        def _():
            collect(step - 1)

        sent[slot, 0] = dot(n_ref[:, theirs], p_scr[...], TN).astype(LOW)
        sent[slot, 1] = dot(g_ref[:, theirs], h_scr[...], TN).astype(LOW)
        to_partner(sent, received, sends, receives, slot).start()
        own[slot, 0] = dot(n_ref[:, ours], p_scr[...], TN)
        own[slot, 1] = dot(g_ref[:, ours], h_scr[...], TN)

    else:
        shards, depth = dw_ref.shape[0], dw_ref.shape[3]
        d1 = dot(n_ref[...], p_scr[...], TN).astype(LOW)
        d2 = dot(g_ref[...], h_scr[...], TN).astype(LOW)
        for f in range(shards):
            for t in range(each):
                dw_ref[f, t, 0] = d1[f * depth : (f + 1) * depth, t * cols : (t + 1) * cols]
                dw_ref[f, t, 1] = d2[f * depth : (f + 1) * depth, t * cols : (t + 1) * cols]

    if not first:

        @pl.when(step == 0)
        def _():
            for load in loads:
                load.wait()

    y_ref[...] += dot(h_scr[...], w2, NT)
    gn_ref[...] += dot(p_scr[...], w1, NT)
    if pairwise:

        @pl.when(step == pl.num_programs(0) - 1)
        def _():
            collect(step)


def mlp(part, start, cols, normed, grad_two, w_mlp, bias, carried, fsdp):
    rows, width = normed.shape
    shards = w_mlp.shape[0]
    each = max(512 // cols, 1)
    at = start // cols
    first, pairwise = carried is None, fsdp == 2
    single = pl.Buffered(1)
    full = pl.BlockSpec((rows, width), lambda s: (0, 0), pipeline_mode=single)
    depth = width // fsdp
    steps = shards // each
    acc_shape = jax.ShapeDtypeStruct((rows, width), F32)
    if pairwise:
        out_w = pl.BlockSpec((shards, 2, depth, cols), lambda s: (0, 0, 0, 0), pipeline_mode=single)
        w_shape = jax.ShapeDtypeStruct((shards, 2, depth, cols), LOW)
        extra = exchange_scratch(2, (2, depth, each * cols))
    else:
        out_w = pl.BlockSpec((fsdp, each, 2, depth, cols), lambda s: (0, s, 0, 0, 0))
        w_shape = jax.ShapeDtypeStruct((fsdp, shards, 2, depth, cols), LOW)
        extra = []
    return pl.pallas_call(
        functools.partial(mlp_kernel, first, pairwise),
        grid=(steps,),
        in_specs=[
            full,
            full,
            pl.BlockSpec((each, 1, width, cols), lambda s: (s, 0, 0, at)),
            pl.BlockSpec((each, 1, width, cols), lambda s: (s, 1, 0, at)),
            pl.BlockSpec((each, 1, cols), lambda s: (s, 0, at)),
        ]
        + ([] if first else [pl.BlockSpec(memory_space=pl.ANY)] * 2),
        out_specs=[full, full, out_w, pl.BlockSpec((each, 1, cols), lambda s: (s, 0, 0))],
        out_shape=[acc_shape, acc_shape, w_shape, jax.ShapeDtypeStruct((shards, 1, cols), F32)],
        scratch_shapes=[
            pltpu.VMEM((rows, each * cols), LOW),
            pltpu.VMEM((rows, each * cols), LOW),
            pltpu.SemaphoreType.DMA((2,)),
            *extra,
        ],
        compiler_params=params(2 + part if pairwise else None),
        cost_estimate=cost(12 * rows * width * cols * shards, 24 * rows * width),
        name=f"mlp_{part}",
    )(normed, grad_two, w_mlp, w_mlp, bias, *([] if first else carried))


def turn_kernel(seq, pairwise, alive_ref, resid_ref, y_ref, gn_ref, g2_ref, att_ref, w_ref, vec_ref,
                out_ref, gr_ref, ga_ref, dw_ref, sums_ref, dw_scr, *exchange):
    i = pl.program_id(0)
    if pairwise:
        pl.when(i == 0)(greet_partner)
    shards, _, _, cols = w_ref.shape
    resid = resid_ref[...]
    out_ref[0] = ((resid + y_ref[...] + vec_ref[7:8]) * alive_ref[i]).astype(LOW)[0:seq]
    normal, inverse = centred(resid)
    upstream = gn_ref[...]
    grad_out = g2_ref[...].astype(F32)
    grad_resid = grad_out + norm_back(upstream, normal, inverse, vec_ref[2:3])
    gr_ref[...] = grad_resid
    low = grad_resid.astype(LOW)
    rows = [
        jnp.sum(upstream * normal, axis=0, keepdims=True),
        jnp.sum(upstream, axis=0, keepdims=True),
        jnp.sum(grad_resid, axis=0, keepdims=True),
        jnp.sum(grad_out, axis=0, keepdims=True),
    ]
    rows = jnp.concatenate(rows, axis=0)

    @pl.when(i == 0)
    def _():
        sums_ref[...] = rows

    @pl.when(i != 0)
    def _():
        sums_ref[...] += rows

    for t in range(shards):
        ga_ref[:, t * cols : (t + 1) * cols] = dot(low, w_ref[t, 0]).astype(LOW)
    part = dot(low, att_ref[...], TN)

    @pl.when(i == 0)
    def _():
        dw_scr[...] = part

    @pl.when(i != 0)
    def _():
        dw_scr[...] += part

    @pl.when(i == pl.num_programs(0) - 1)
    def _():
        if pairwise:
            sent, received, sends, receives = exchange
            ours, theirs = bands(dw_scr.shape[0] // 2)
            sent[0] = dw_scr[theirs, :].astype(LOW)
            copy = to_partner(sent, received, sends, receives, 0)
            copy.start()
            copy.wait()
            total = (dw_scr[ours, :] + received[0].astype(F32)).astype(LOW)
            for t in range(shards):
                dw_ref[t, 0] = total[:, t * cols : (t + 1) * cols]
            return
        depth = dw_ref.shape[3]
        for f in range(dw_ref.shape[0]):
            for t in range(shards):
                dw_ref[f, t, 0] = dw_scr[f * depth : (f + 1) * depth, t * cols : (t + 1) * cols].astype(LOW)


def turn(alive, resid, branch, grad_normed, grad_two, attended, w_attn, vec, images, seq, fsdp):
    rows, width = resid.shape
    span = rows // images
    shards, _, _, cols = w_attn.shape
    depth = width // fsdp
    pairwise = fsdp == 2
    lead = () if pairwise else (fsdp,)
    block = pl.BlockSpec((span, width), lambda i: (i, 0))
    return pl.pallas_call(
        functools.partial(turn_kernel, seq, pairwise),
        grid=(images,),
        in_specs=[
            pl.BlockSpec(memory_space=pltpu.SMEM),
            block, block, block, block, block,
            pl.BlockSpec((shards, 1, width, cols), lambda i: (0, 3, 0, 0)),
            pl.BlockSpec(vec.shape, lambda i: (0, 0)),
        ],
        out_specs=[
            pl.BlockSpec((1, seq, width), lambda i: (i, 0, 0)),
            block, block,
            pl.BlockSpec((*lead, shards, 1, depth, cols), lambda i: (0,) * (4 + len(lead))),
            pl.BlockSpec((4, width), lambda i: (0, 0)),
        ],
        out_shape=[
            jax.ShapeDtypeStruct((images, seq, width), LOW),
            jax.ShapeDtypeStruct((rows, width), F32),
            jax.ShapeDtypeStruct((rows, width), LOW),
            jax.ShapeDtypeStruct((*lead, shards, 1, depth, cols), LOW),
            jax.ShapeDtypeStruct((4, width), F32),
        ],
        scratch_shapes=[pltpu.VMEM((width, width), F32)] + (exchange_scratch(1, (depth, width))[1:] if pairwise else []),
        compiler_params=params(6 if pairwise else None),
        cost_estimate=cost(4 * rows * width * width, 24 * rows * width),
        name="turn",
    )(alive, resid, branch, grad_normed, grad_two, attended, w_attn, vec)


def carrier(groups, paired, diff_ref, total_ref, mine, landed, sends, receives, loaded):
    g, f, t = lax.axis_index("group"), lax.axis_index("fsdp"), lax.axis_index("tensor")
    quarter = landed.shape[1]

    def rows(n):
        return pl.ds(pl.multiple_of(n * quarter, quarter), quarter)

    def other(k):
        return (lax.rem(g + k, groups), f, t)

    def part(k):
        return pltpu.make_async_remote_copy(
            src_ref=diff_ref.at[rows(lax.rem(g + k, groups)), :],
            dst_ref=landed.at[k],
            send_sem=sends.at[k],
            recv_sem=receives.at[k],
            device_id=other(k),
            device_id_type=MESH,
        )

    keep = pltpu.make_async_copy(diff_ref.at[rows(g), :], mine, loaded.at[0])

    def begin():
        barrier = pltpu.get_barrier_semaphore()
        if paired:
            pl.semaphore_signal(barrier, inc=1, device_id=partner(), device_id_type=MESH)
        for k in range(1, groups):
            pl.semaphore_signal(barrier, inc=1, device_id=other(k), device_id_type=MESH)
        pl.semaphore_wait(barrier, groups - 1 + int(paired))
        for k in range(1, groups):
            part(k).start()
        keep.start()

    def end():
        keep.wait()
        total = mine[...].astype(F32)
        for k in range(1, groups):
            part(k).wait()
            total = total + landed[k].astype(F32)
        total_ref[...] = total.astype(LOW)

    return begin, end


def carrier_scratch(groups, quarter, lanes):
    dma = pltpu.SemaphoreType.DMA
    return [
        pltpu.VMEM((quarter, lanes), LOW),
        pltpu.VMEM((groups, quarter, lanes), LOW),
        dma((groups,)),
        dma((groups,)),
        dma((1,)),
    ]


def unattend_kernel(seq, groups, q_ref, k_ref, v_ref, g_ref, *refs):
    if groups:
        diff_ref, out_ref, total_ref, *scratch = refs
        begin, end = carrier(groups, False, diff_ref, total_ref, *scratch)
        pl.when((pl.program_id(0) == 0) & (pl.program_id(1) == 0))(begin)
    else:
        (out_ref,) = refs
    span = q_ref.shape[1]
    scale = HD**-0.5
    q, k, v, g = q_ref[0], k_ref[0], v_ref[0], g_ref[...]
    parts = []
    for h in range(2):
        scores = dot(half_lanes(k, h), q, NT)
        row = lax.broadcasted_iota(jnp.int32, scores.shape, 0)
        scores = jnp.where(row < seq, scores, -1e30)
        top = jnp.max(scores, axis=0, keepdims=True)
        raised = jnp.exp((scores - top) * scale)
        total = jnp.sum(raised, axis=0, keepdims=True)
        probs = raised * (1.0 / total)
        gp = dot(half_lanes(v, h), g, NT)
        delta = jnp.sum(probs * gp, axis=0, keepdims=True)
        gs = (probs * (gp - delta)).astype(LOW)
        dv = dot(probs.astype(LOW), g)
        dk = dot(gs, q)
        dq = dot(gs, k, TN)
        parts.append((dq, dk, dv))
    lane = lax.broadcasted_iota(jnp.int32, (span, 2 * HD), 1) < HD
    out_ref[0] = (jnp.where(lane, parts[0][0], parts[1][0]) * scale).astype(LOW)
    out_ref[1] = (jnp.where(lane, parts[0][1], parts[1][1]) * scale).astype(LOW)
    out_ref[2] = jnp.where(lane, parts[0][2], parts[1][2]).astype(LOW)
    if groups:
        at_end = (pl.program_id(0) == pl.num_programs(0) - 1) & (pl.program_id(1) == pl.num_programs(1) - 1)
        pl.when(at_end)(end)


def unattend(qkv, grad_attended, images, seq, part, parts, shards, diff=None, groups=0):
    _, rows, width = qkv.shape
    span = rows // images
    pair = 2 * HD
    each = width // shards // parts // pair

    def spot(h):
        return (h // each) * (each * parts) + part * each + h % each

    def take(j):
        return pl.BlockSpec((1, span, pair), lambda i, h: (j, i, spot(h)))

    in_specs = [take(0), take(1), take(2), pl.BlockSpec((span, pair), lambda i, h: (i, spot(h)))]
    out_specs = [pl.BlockSpec((3, span, pair), lambda i, h: (0, i, h))]
    out_shape = [jax.ShapeDtypeStruct((3, rows, width // parts), LOW)]
    scratch = []
    if groups:
        quarter, lanes = diff.shape[0] // groups, diff.shape[1]
        in_specs.append(pl.BlockSpec(memory_space=pl.ANY))
        out_specs.append(pl.BlockSpec((quarter, lanes), lambda i, h: (0, 0)))
        out_shape.append(jax.ShapeDtypeStruct((quarter, lanes), LOW))
        scratch = carrier_scratch(groups, quarter, lanes)
    return pl.pallas_call(
        functools.partial(unattend_kernel, seq, groups),
        grid=(images, width // pair // parts),
        in_specs=in_specs,
        out_specs=out_specs,
        out_shape=out_shape,
        scratch_shapes=scratch,
        compiler_params=params(9 if groups else None),
        cost_estimate=cost(
            40 * rows * span * width // parts, 14 * rows * width // parts, rows * span * (width // HD) // parts
        ),
        name=f"unattend_{part}",
    )(qkv, qkv, qkv, grad_attended, *([diff] if groups else []))


def close_kernel(pairwise, groups, first, final, n_ref, grad_ref, w_ref, *refs):
    if not first:
        carry_ref, *refs = refs
    elif pairwise:
        more_ref, *refs = refs
    if pairwise and final:
        diff_ref, acc_ref, total_ref, *refs = refs
    else:
        acc_ref, *refs = refs
    dw_ref, sums_ref, acc_scr, *exchange = refs
    j = pl.program_id(0)
    shards, _, _, cols = w_ref.shape
    if pairwise:
        own, sent, received, sends, receives, *exchange = exchange
        if not final:
            pl.when(j == 0)(greet_partner)
    if pairwise and final:
        begin, end = carrier(groups, True, diff_ref, total_ref, *exchange)
        pl.when(j == 0)(begin)

    @pl.when(j == 0)
    def _():
        acc_scr[...] = jnp.zeros_like(acc_scr) if first else carry_ref[...]

    sums = jnp.sum(grad_ref[0].astype(F32), axis=0, keepdims=True)
    for n, matrix in enumerate((0, 2)):

        @pl.when(j == matrix)
        def _():
            sums_ref[n : n + 1, :] = sums

    def spread(n, total, f=None):
        for t in range(shards):
            piece = total[:, t * cols : (t + 1) * cols]
            if f is None:
                dw_ref[t, n] = piece
            else:
                dw_ref[f, t, 0] = piece

    weight = jnp.concatenate([w_ref[t, 0] for t in range(shards)], axis=1)
    if pairwise:
        ours, theirs = bands(n_ref.shape[1] // 2)
        sent[j] = dot(n_ref[:, theirs], grad_ref[0], TN).astype(LOW)
        to_partner(sent, received, sends, receives, j).start()
        own[j] = dot(n_ref[:, ours], grad_ref[0], TN)
    else:
        depth = dw_ref.shape[3]
        dw = dot(n_ref[...], grad_ref[0], TN).astype(LOW)
        for f in range(dw_ref.shape[0]):
            spread(0, dw[f * depth : (f + 1) * depth], f)
    acc_scr[...] += dot(grad_ref[0], weight, NT)

    @pl.when(j == 2)
    def _():
        if pairwise:
            for n in range(own.shape[0]):
                to_partner(sent, received, sends, receives, n).wait()
                spread(n, (own[n] + received[n].astype(F32)).astype(LOW))
            if first:
                for t in range(shards):
                    for n in range(dw_ref.shape[1] - 3):
                        dw_ref[t, 3 + n] = more_ref[t, 0, :, n * cols : (n + 1) * cols]
        acc_ref[...] = acc_scr[...]
        if pairwise and final:
            end()


def close(part, parts, normed, grads, w_attn, carry, more, ending, fsdp, groups):
    rows, width = normed.shape
    shards, _, _, cols = w_attn.shape
    cols = cols // parts
    lanes = shards * cols
    depth = width // fsdp
    pairwise, first, final = fsdp == 2, carry is None, ending is not None
    single = pl.Buffered(1)
    stack = pl.BlockSpec((1, rows, lanes), lambda j: (j, 0, 0))
    full = pl.BlockSpec((rows, width), lambda j: (0, 0), pipeline_mode=single)
    if pairwise:
        many = 3 + parts if first else 3
        dw_spec = pl.BlockSpec((shards, many, depth, cols), lambda j: (0, 0, 0, 0), pipeline_mode=single)
        dw_shape = jax.ShapeDtypeStruct((shards, many, depth, cols), LOW)
        extra = exchange_scratch(3, (depth, lanes))
    else:
        dw_spec = pl.BlockSpec((fsdp, shards, 1, depth, cols), lambda j: (0, 0, j, 0, 0))
        dw_shape = jax.ShapeDtypeStruct((fsdp, shards, 3, depth, cols), LOW)
        extra = []
    in_specs = [full, stack, pl.BlockSpec((shards, 1, width, cols), lambda j: (0, j, 0, part))]
    out_specs, out_shape = [], []
    if not first:
        in_specs.append(full)
    elif pairwise:
        in_specs.append(pl.BlockSpec(more.shape, lambda j: (0, 0, 0, 0), pipeline_mode=single))
    out_specs.append(full)
    out_shape.append(jax.ShapeDtypeStruct((rows, width), F32))
    if pairwise and final:
        quarter, lanes_two = ending.shape[0] // groups, ending.shape[1]
        in_specs.append(pl.BlockSpec(memory_space=pl.ANY))
        out_specs.append(pl.BlockSpec((quarter, lanes_two), lambda j: (0, 0), pipeline_mode=single))
        out_shape.append(jax.ShapeDtypeStruct((quarter, lanes_two), LOW))
        extra = [*extra, *carrier_scratch(groups, quarter, lanes_two)]
    return pl.pallas_call(
        functools.partial(close_kernel, pairwise, groups, first, final),
        grid=(3,),
        in_specs=in_specs,
        out_specs=[*out_specs, dw_spec, pl.BlockSpec((2, lanes), lambda j: (0, 0))],
        out_shape=[*out_shape, dw_shape, jax.ShapeDtypeStruct((2, lanes), F32)],
        scratch_shapes=[pltpu.VMEM((rows, width), F32), *extra],
        compiler_params=params(7 + part if pairwise else None),
        cost_estimate=cost(12 * rows * width * lanes, 20 * rows * width),
        name=f"close_{part}",
    )(normed, grads, w_attn, *([carry] if not first else [more] if pairwise else []), *([ending] if pairwise and final else []))


def finish_kernel(acc_ref, gr_ref, x_ref, vec_ref, out_ref, norm_ref):
    i = pl.program_id(0)
    seq = out_ref.shape[1]
    normal, inverse = centred(x_ref[...].astype(F32))
    upstream = acc_ref[...]
    grad = gr_ref[...] + norm_back(upstream, normal, inverse, vec_ref[0:1])
    out_ref[0, :, 0, :] = grad[0:seq]
    sums = [jnp.sum(upstream * normal, axis=0, keepdims=True), jnp.sum(upstream, axis=0, keepdims=True)]
    sums = jnp.concatenate(sums, axis=0)

    @pl.when(i == 0)
    def _():
        norm_ref[...] = sums

    @pl.when(i != 0)
    def _():
        norm_ref[...] += sums


def finish(acc, grad_resid, x_rows, vec, images, seq):
    rows, width = acc.shape
    block = pl.BlockSpec((rows // images, width), lambda i: (i, 0))
    return pl.pallas_call(
        finish_kernel,
        grid=(images,),
        in_specs=[block, block, block, pl.BlockSpec(vec.shape, lambda i: (0, 0))],
        out_specs=[pl.BlockSpec((1, seq, 1, width), lambda i: (i, 0, 0, 0)), pl.BlockSpec((2, width), lambda i: (0, 0))],
        out_shape=[
            jax.ShapeDtypeStruct((images, seq, 1, width), F32),
            jax.ShapeDtypeStruct((2, width), F32),
        ],
        compiler_params=params(),
        cost_estimate=cost(20 * rows * width, 14 * rows * width),
        name="finish",
    )(acc, grad_resid, x_rows, vec)


def attend_pair(seq, q, k, v):
    scale = HD**-0.5
    parts = []
    for h in range(2):
        scores = dot(q, half_lanes(k, h), NT)
        lane = lax.broadcasted_iota(jnp.int32, scores.shape, 1)
        scores = jnp.where(lane < seq, scores, -1e30)
        top = jnp.max(scores, axis=1, keepdims=True)
        raised = jnp.exp((scores - top) * scale)
        total = jnp.sum(raised, axis=1, keepdims=True)
        probs = (raised * (1.0 / total)).astype(LOW)
        parts.append(dot(probs, v))
    lane = lax.broadcasted_iota(jnp.int32, parts[0].shape, 1)
    return jnp.where(lane < HD, parts[0], parts[1]).astype(LOW)


def front_kernel(
    images, seq, alive_ref, a_in, m_in, x_ref, g_ref, vec_ref,
    a_out, m_out, n_out, qkv_out, att_out, resid_out, n2_out, g2_out, x_out,
    a_wide, m_wide, a_hold, m_hold, n_scr, qkv_scr, att_scr, w_scr, o_scr, resid_scr, n2_scr, g2_scr, x_all,
    zs, zr, xs, xr, ys, yr, xfs, xfr, yfs, yfr, cs, cr, ls, ws,
):
    g, f, z = lax.axis_index("group"), lax.axis_index("fsdp"), lax.axis_index("tensor")
    shards = lax.axis_size("tensor")
    last = shards - 1
    x_at, y_at = g % 2, g // 2
    east, north = y_at * 2 + (1 - x_at), (1 - y_at) * 2 + x_at
    depth, cols = a_in.shape[1:]
    band = depth // 4
    shared = band * 3 // 8
    rest = band - 2 * shared
    span = n_scr.shape[0] // images

    def place(column):
        cx, cy = column % 2, column // 2
        return 2 * (cx + cy - 2 * cx * cy) + cy

    mine, of_east, of_north = place(g), place(east), place(north)
    z_row = mine * band - shared * (mine % 2)
    lead_east = of_east * band + shared * (of_east % 2)
    lead_north = of_north * band + shared * (of_north % 2)
    chunks = ((a_out, 0, 3), (a_out, 3, 1), (m_out, 0, 1), (m_out, 1, 1))

    def tile(n):
        return pl.multiple_of(n, 16)

    def held(n, t, row, rows):
        out, j, many = chunks[n]
        return out.at[t, pl.ds(j, many), pl.ds(tile(f * depth + row), rows), :]

    def send(part, sems, semr, n, t, to):
        return pltpu.make_async_remote_copy(
            src_ref=part, dst_ref=part, send_sem=sems.at[n, t], recv_sem=semr.at[n, t], device_id=to, device_id_type=MESH
        )

    def along(n, t, up):
        part = held(n, t, z_row, band + shared)
        return pltpu.make_async_remote_copy(
            src_ref=part,
            dst_ref=part,
            send_sem=zs.at[n, t, 0 if up else 1],
            recv_sem=zr.at[n, t],
            device_id=(g, f, z + 1 if up else z - 1),
            device_id_type=MESH,
        )

    def to_east(n, t):
        return send(held(n, t, mine * band, band), xs, xr, n, t, (east, f, z))

    def to_north(n, t):
        return send(held(n, t, mine * band, band), ys, yr, n, t, (north, f, z))

    def north_to_east(n, t):
        return send(held(n, t, lead_north, shared), xfs, xfr, n, t, (east, f, z))

    def east_to_north(n, t):
        return send(held(n, t, lead_east + shared, rest), yfs, yfr, n, t, (north, f, z))

    def across(n, t):
        return send(held(n, t, 0, depth), cs, cr, n, t, (g, 1 - f, z))

    rows = pl.ds(tile(f * depth), depth)
    loads = (
        pltpu.make_async_copy(a_in, a_wide, ls.at[0]),
        pltpu.make_async_copy(m_in, m_wide, ls.at[1]),
    )
    keeps = (
        pltpu.make_async_copy(a_hold, a_out.at[z, :, rows, :], ls.at[2]),
        pltpu.make_async_copy(m_hold, m_out.at[z, :, rows, :], ls.at[3]),
    )
    loads[0].start()

    barrier = pltpu.get_barrier_semaphore()

    def greet(to):
        pl.semaphore_signal(barrier, inc=1, device_id=to, device_id_type=MESH)

    for to in ((east, f, z), (north, f, z), (g, 1 - f, z)):
        greet(to)

    @pl.when(z > 0)
    def _():
        greet((g, f, z - 1))

    @pl.when(z < last)
    def _():
        greet((g, f, z + 1))

    loads[0].wait()
    a_hold[...] = a_wide[...].astype(LOW)
    keeps[0].start()
    pl.semaphore_wait(barrier, 3 + jnp.minimum(z, 1) + jnp.minimum(last - z, 1))
    keeps[0].wait()

    count = len(chunks)

    def when_real(k, up, run):
        @pl.when(z - k >= 0 if up else z + k <= last)
        def _():
            run(z - k if up else z + k)

    def own(n):
        @pl.when(z < last)
        def _():
            along(n, z, True).start()

        @pl.when(z > 0)
        def _():
            along(n, z, False).start()

        across(n, z).start()

    def land(n, k, up):
        def run(t):
            along(n, t, up).wait_recv()

            @pl.when(z < last if up else z > 0)
            def _():
                along(n, t, up).start()

            to_east(n, t).start()
            to_north(n, t).start()

        when_real(k, up, run)

    def relay(n, k, up):
        def run(t):
            to_east(n, t).wait_recv()
            east_to_north(n, t).start()
            to_north(n, t).wait_recv()
            north_to_east(n, t).start()

        when_real(k, up, run)

    def finish(n, k, up):
        def run(t):
            east_to_north(n, t).wait_recv()
            north_to_east(n, t).wait_recv()
            across(n, t).start()

        when_real(k, up, run)

    def both(run, n, k):
        for up in (True, False):
            run(n, k, up)

    def fetch(t):
        return pltpu.make_async_copy(a_out.at[t, pl.ds(0, 3)], w_scr, ws.at[0])

    def maps(t):
        across(0, t).wait_recv()
        fetch(t).start()
        fetch(t).wait()
        here = pl.ds(pl.multiple_of(t * cols, cols), cols)

        def body(j, carry):
            bias = jnp.where(j == 0, vec_ref[4:5, here], jnp.where(j == 2, vec_ref[5:6, here], 0.0))
            qkv_scr[j, :, here] = (dot(n_scr[...], w_scr[j]) + bias).astype(LOW)
            return carry

        lax.fori_loop(0, 3, body, 0)

    def project(k):
        def body(d, carry):
            t = z - k + 2 * k * d

            @pl.when((t >= 0) & (t <= last))
            def _():
                maps(t)

            return carry

        lax.fori_loop(0, 2, body, 0)

    own(0)
    loads[1].start()
    n_scr[...] = jnp.zeros_like(n_scr)
    x_all[...] = jnp.zeros_like(x_all)
    g2_scr[...] = jnp.zeros_like(g2_scr)

    def norm_image(i):
        here = pl.ds(i * span, seq)
        image = x_ref[:, i, :]
        x_all[here, :] = image
        normal, _ = centred(image.astype(F32))
        n_scr[here, :] = (normal * vec_ref[0:1] + vec_ref[1:2]).astype(LOW)

    norm_image(0)
    both(land, 0, 1)
    for i in range(1, images):
        norm_image(i)
    puts = [
        pltpu.make_async_copy(n_scr, n_out, ws.at[1]),
        pltpu.make_async_copy(x_all, x_out, ws.at[7]),
    ]
    for put in puts:
        put.start()
    both(land, 0, 2)
    both(relay, 0, 1)
    loads[1].wait()
    m_hold[...] = m_wide[...].astype(LOW)
    keeps[1].start()
    maps(z)
    keeps[1].wait()
    both(land, 0, 3)
    for n in range(1, count):
        own(n)
    both(relay, 0, 2)
    both(finish, 0, 1)
    both(relay, 0, 3)
    both(finish, 0, 2)
    project(1)
    both(finish, 0, 3)
    project(2)

    rest_items = [(n, k) for k in range(1, last + 1) for n in range(1, count)]
    total = len(rest_items) + 2

    def advance(at):
        if at < len(rest_items):
            both(land, *rest_items[at])
        if 0 <= at - 1 < len(rest_items):
            both(relay, *rest_items[at - 1])
        if 0 <= at - 2 < len(rest_items):
            both(finish, *rest_items[at - 2])

    advance(0)
    project(3)
    puts.append(pltpu.make_async_copy(qkv_scr, qkv_out, ws.at[2]))
    puts[-1].start()

    pair = 2 * HD
    pairs = qkv_scr.shape[2] // pair
    stretch = max(pairs // 4, 1)
    segments = images * pairs // stretch

    def segment(n, carry):
        def body(m, carry):
            at = n * stretch + m
            lanes = pl.ds(pl.multiple_of(lax.rem(at, pairs) * pair, pair), pair)
            here = pl.ds(pl.multiple_of(at // pairs * span, 16), span)
            att_scr[here, lanes] = attend_pair(
                seq, qkv_scr[0, here, lanes], qkv_scr[1, here, lanes], qkv_scr[2, here, lanes]
            )
            return carry

        lax.fori_loop(0, stretch, body, 0)
        for c in range(min(segments, total - 3)):
            pl.when(n == c)(functools.partial(advance, 1 + c))
        return carry

    lax.fori_loop(0, segments, segment, 0)
    at = 1 + min(segments, total - 3)
    puts.append(pltpu.make_async_copy(att_scr, att_out, ws.at[3]))
    puts[-1].start()
    for i in range(images):
        g2_scr[pl.ds(i * span, seq), :] = (g_ref[:, i, :].astype(F32) * alive_ref[i]).astype(LOW)
    while at < total - 2:
        advance(at)
        at += 1

    for t in range(shards):
        across(1, t).wait_recv()
    take = pltpu.make_async_copy(a_out.at[:, 3], o_scr, ws.at[0])
    take.start()
    take.wait()

    def mix_image(i, carry):
        here = pl.ds(pl.multiple_of(i * span, 16), span)
        out = x_all[here, :].astype(F32) + vec_ref[6:7]
        for t in range(shards):
            out = out + dot(att_scr[here, t * cols : (t + 1) * cols], o_scr[t], NT)
        resid_scr[here, :] = out
        normal, _ = centred(out)
        n2_scr[here, :] = (normal * vec_ref[2:3] + vec_ref[3:4]).astype(LOW)
        for c in range(min(images, total - at)):
            pl.when(i == c)(functools.partial(advance, at + c))
        return carry

    lax.fori_loop(0, images, mix_image, 0)
    at += min(images, total - at)
    for n, (src, dst) in enumerate(((resid_scr, resid_out), (n2_scr, n2_out), (g2_scr, g2_out))):
        puts.append(pltpu.make_async_copy(src, dst, ws.at[4 + n]))
        puts[-1].start()
    while at < total:
        advance(at)
        at += 1
    for put in puts:
        put.wait()

    for n in range(count):
        @pl.when(z < last)
        def _():
            along(n, z, True).wait_send()

        @pl.when(z > 0)
        def _():
            along(n, z, False).wait_send()

        for t in range(shards):
            across(n, t).wait_send()
            if n > 1:
                across(n, t).wait_recv()

    def settle(n, k, up):
        def run(t):
            @pl.when(z < last if up else z > 0)
            def _():
                along(n, t, up).wait_send()

            to_east(n, t).wait_send()
            to_north(n, t).wait_send()
            east_to_north(n, t).wait_send()
            north_to_east(n, t).wait_send()

        when_real(k, up, run)

    for n in range(count):
        for k in range(1, last + 1):
            both(settle, n, k)


def front(alive, attn_master, mlp_master, patches, cotangent, vec, shards):
    _, depth, a_cols = attn_master.shape
    _, _, m_cols = mlp_master.shape
    seq, images, width = patches.shape
    rows = images * padded(seq)
    anywhere = pl.BlockSpec(memory_space=pl.ANY)
    inside = pl.BlockSpec(memory_space=pltpu.VMEM)
    dma = pltpu.SemaphoreType.DMA
    low = jax.ShapeDtypeStruct((rows, width), LOW)
    return pl.pallas_call(
        functools.partial(front_kernel, images, seq),
        in_specs=[pl.BlockSpec(memory_space=pltpu.SMEM), anywhere, anywhere, inside, inside, inside],
        out_specs=[anywhere] * 9,
        out_shape=[
            jax.ShapeDtypeStruct((shards, 4, width, a_cols), LOW),
            jax.ShapeDtypeStruct((shards, 2, width, m_cols), LOW),
            low,
            jax.ShapeDtypeStruct((3, rows, width), LOW),
            low,
            jax.ShapeDtypeStruct((rows, width), F32),
            low,
            low,
            low,
        ],
        scratch_shapes=[
            pltpu.VMEM(attn_master.shape, F32),
            pltpu.VMEM(mlp_master.shape, F32),
            pltpu.VMEM(attn_master.shape, LOW),
            pltpu.VMEM(mlp_master.shape, LOW),
            pltpu.VMEM((rows, width), LOW),
            pltpu.VMEM((3, rows, width), LOW),
            pltpu.VMEM((rows, width), LOW),
            pltpu.VMEM((3, width, a_cols), LOW),
            pltpu.VMEM((shards, width, a_cols), LOW),
            pltpu.VMEM((rows, width), F32),
            pltpu.VMEM((rows, width), LOW),
            pltpu.VMEM((rows, width), LOW),
            pltpu.VMEM((rows, width), LOW),
            dma((4, shards, 2)),
        ]
        + [dma((4, shards))] * 11
        + [dma((4,)), dma((8,))],
        compiler_params=params(1),
        cost_estimate=cost(8 * rows * width * width, 30 * rows * width),
        name="front",
    )(alive, attn_master, mlp_master, patches, cotangent, vec)


def inner_adamw(master, gradient, first, second, step_rate, decay_rate):
    first_moment = 0.9 * first + 0.1 * gradient
    second_moment = 0.95 * second + 0.05 * gradient * gradient
    step_ratio = (
        first_moment / (1.0 - 0.9**STEP) / (jnp.sqrt(second_moment / (1.0 - 0.95**STEP)) + 1e-08)
    )
    return (master - step_rate * (step_ratio + decay_rate * master), second_moment)


def outer_nesterov(master, outer_old, difference):
    momentum = OUTER_MOMENTUM * outer_old + difference
    return momentum, master - OUTER_RATE * (difference + OUTER_MOMENTUM * momentum)


def inner_kernel(join, count, *refs):
    pieces, (master_ref, moment_ref, *_, inner_ref, diff_ref) = refs[:count], refs[count:]
    gradient = join(*[piece[0] for piece in pieces]).astype(F32)
    master = master_ref[0]
    new, second = inner_adamw(master, gradient, moment_ref[0, 0, 0], moment_ref[0, 1, 0], INNER_RATE, WEIGHT_DECAY)
    inner_ref[0, 0, 0] = gradient
    inner_ref[0, 1, 0] = second
    diff_ref[0] = (master - new).astype(LOW)


def inner_step(join, pieces, unit, units, cols, master, moments, into, name):
    depth = master.shape[1]
    rows = min(depth, 524288 // cols)
    block = pl.BlockSpec((1, rows, cols), lambda u, r: (unit(u)[0], r, unit(u)[1]))
    both = pl.BlockSpec((1, 2, 1, rows, cols), lambda u, r: (0, 0, unit(u)[0], r, unit(u)[1]))
    piece_specs = [pl.BlockSpec((1, rows, piece.shape[2]), lambda u, r: (u, r, 0)) for piece in pieces]
    count = len(pieces)
    return pl.pallas_call(
        functools.partial(inner_kernel, join, count),
        grid=(units, depth // rows),
        in_specs=[*piece_specs, block, both] + ([] if into is None else [pl.BlockSpec(memory_space=pl.ANY)]),
        out_specs=[both, pl.BlockSpec((1, rows, cols), lambda u, r: (u, r, 0))],
        out_shape=[
            jax.ShapeDtypeStruct(moments.shape, F32),
            jax.ShapeDtypeStruct((units, depth, cols), LOW),
        ],
        input_output_aliases={} if into is None else {count + 2: 0},
        compiler_params=params(),
        cost_estimate=cost(30 * units * depth * cols, 24 * units * depth * cols),
        name=name,
    )(*pieces, master, moments, *([] if into is None else [into]))


def outer_kernel(groups, slots, each, g_ref, *refs):
    totals, (master_ref, outer_ref, *_, state_ref, copy_ref) = refs[:slots], refs[slots:]
    rows = copy_ref.shape[1]
    if slots == 1:
        total = totals[0][0]
    else:
        at = pl.program_id(0) * pl.num_programs(1) + pl.program_id(1)
        slot = lax.rem(g_ref[0] + groups - at // each, groups)
        here = pl.ds(pl.multiple_of(lax.rem(at, each) * rows, rows), rows)
        total = totals[0][here, :]
        for n in range(1, slots):
            total = jnp.where(slot == n, totals[n][here, :], total)
    difference = total.astype(F32) / groups
    momentum, fresh = outer_nesterov(master_ref[0], outer_ref[0], difference)
    state_ref[0, 0] = difference
    state_ref[1, 0] = momentum
    state_ref[2, 0] = fresh
    copy_ref[0] = fresh.astype(LOW)


def outer_step(groups, me, totals, unit, units, cols, master, outer_old, into, name):
    depth = master.shape[1]
    slots = len(totals)
    rows = min(depth, 524288 // cols, totals[0].shape[-2])
    each = totals[0].shape[-2] // rows
    block = pl.BlockSpec((1, rows, cols), lambda u, r, g: (unit(u)[0], r, unit(u)[1]))
    state = pl.BlockSpec((3, 1, rows, cols), lambda u, r, g: (0, unit(u)[0], r, unit(u)[1]))
    if slots == 1:
        total = pl.BlockSpec((1, rows, cols), lambda u, r, g: (u, r, 0))
    else:
        total = pl.BlockSpec(totals[0].shape, lambda u, r, g: (0, 0))
    aliased = [] if into is None else [pl.BlockSpec(memory_space=pl.ANY)] * 2
    return pl.pallas_call(
        functools.partial(outer_kernel, groups, slots, each),
        grid_spec=pltpu.PrefetchScalarGridSpec(
            num_scalar_prefetch=1,
            grid=(units, depth // rows),
            in_specs=[*[total] * slots, block, block, *aliased],
            out_specs=[state, block],
        ),
        out_shape=[
            jax.ShapeDtypeStruct((3, *master.shape), F32),
            jax.ShapeDtypeStruct(master.shape, LOW),
        ],
        input_output_aliases={} if into is None else {slots + 3: 0, slots + 4: 1},
        compiler_params=params(),
        cost_estimate=cost(10 * units * depth * cols, 24 * units * depth * cols),
        name=name,
    )(me, *totals, master, outer_old, *([] if into is None else into))


def group_kernel(groups, shards, vectors, diff_ref, *refs):
    if vectors:
        part_ref, master_ref, moment_ref, outer_ref, total_ref, inner_ref, state_ref, copy_ref, *refs = refs
    else:
        total_ref, *refs = refs
    landed, summed, sends, receives, sends_two, receives_two, *small = refs
    g, f, t = lax.axis_index("group"), lax.axis_index("fsdp"), lax.axis_index("tensor")
    span = landed.shape[1]

    def rows(n):
        return pl.ds(pl.multiple_of(n * span, span), span)

    def other(k):
        return lax.rem(g + k, groups)

    def back(k):
        return lax.rem(g + groups - k, groups)

    def copy(src, dst, sems, semr, k, to):
        return pltpu.make_async_remote_copy(
            src_ref=src, dst_ref=dst, send_sem=sems.at[k], recv_sem=semr.at[k], device_id=to, device_id_type=MESH
        )

    def part(k):
        return copy(diff_ref.at[rows(other(k)), :], landed.at[k], sends, receives, k, (other(k), f, t))

    def result(k):
        return copy(summed, landed.at[groups + k], sends_two, receives_two, k, (other(k), f, t))

    barrier = pltpu.get_barrier_semaphore()
    for k in range(1, groups):
        pl.semaphore_signal(barrier, inc=1, device_id=(other(k), f, t), device_id_type=MESH)
    if vectors:
        stage, pair, mine, line, whole, few, diffs, ss, rs, ls, lr, gs, gr = small
        half = part_ref.shape[0] // 2
        halves = (pl.ds(0, half), pl.ds(half, half))

        def pick(ref):
            return jnp.where(f == 0, ref[halves[0], :], ref[halves[1], :])

        def line_copy(k):
            return copy(mine, line.at[k], ls, lr, k, (g, f, lax.rem(t + k, shards)))

        def few_copy(k):
            return copy(diffs.at[f], few.at[k], gs, gr, k, (other(k), f, t))

        pair_copy = copy(stage.at[1 - f], pair, ss, rs, 0, partner())
        whole_copy = copy(whole.at[f], whole.at[f], ss, rs, 1, partner())
        final_copy = copy(mine, stage.at[f], ss, rs, 2, partner())
        pl.semaphore_signal(barrier, inc=1, device_id=partner(), device_id_type=MESH)
        for k in range(1, shards):
            pl.semaphore_signal(barrier, inc=1, device_id=(g, f, lax.rem(t + k, shards)), device_id_type=MESH)
        stage[...] = jnp.zeros_like(stage)
        diffs[...] = jnp.zeros_like(diffs)
        for n in range(2):
            stage[n, 0:half] = part_ref[halves[n], :]
    pl.semaphore_wait(barrier, groups - 1 + (shards if vectors else 0))

    for k in range(1, groups):
        part(k).start()
    if vectors:
        pair_copy.start()
        pair_copy.wait()
        mine[...] = stage[f] + pair[...]
        for k in range(1, shards):
            line_copy(k).start()
        line[0] = mine[...]
        for k in range(1, shards):
            line_copy(k).wait()
        gradient = jnp.zeros(mine.shape, F32)
        for n in range(shards):
            gradient = gradient + line[lax.rem(t + shards - n, shards)]
        whole[f] = gradient
        whole_copy.start()
        new, _ = inner_adamw(
            pick(master_ref), gradient[0:half], pick(moment_ref.at[0]), pick(moment_ref.at[1]), VECTOR_RATE, 0.0
        )
        diffs[f, 0:half] = pick(master_ref) - new
        for k in range(1, groups):
            few_copy(k).start()
        few[0] = diffs[f]
        whole_copy.wait()
        for n in range(2):
            own = whole[n, 0:half]
            _, second = inner_adamw(
                master_ref[halves[n], :], own, moment_ref[0, halves[n], :], moment_ref[1, halves[n], :], VECTOR_RATE, 0.0
            )
            inner_ref[0, halves[n], :] = own
            inner_ref[1, halves[n], :] = second
    total = diff_ref[rows(g), :].astype(F32)
    for k in range(1, groups):
        part(k).wait_recv()
        total = total + landed[k].astype(F32)
    summed[...] = total.astype(LOW)
    for k in range(1, groups):
        result(k).start()
    total_ref[rows(g), :] = summed[...]
    if vectors:
        for k in range(1, groups):
            few_copy(k).wait()
        difference = jnp.zeros(mine.shape, F32)
        for n in range(groups):
            difference = difference + few[lax.rem(g + groups - n, groups)]
        mine[...] = difference / groups
        stage[f] = mine[...]
        final_copy.start()
        final_copy.wait()
        for n in range(2):
            difference = stage[n, 0:half]
            momentum, fresh = outer_nesterov(master_ref[halves[n], :], outer_ref[halves[n], :], difference)
            state_ref[0, halves[n], :] = difference
            state_ref[1, halves[n], :] = momentum
            state_ref[2, halves[n], :] = fresh
            copy_ref[halves[n], :] = fresh.astype(LOW)
    for k in range(1, groups):
        result(k).wait_recv()
        total_ref[rows(back(k)), :] = landed[groups + k]
    for k in range(1, groups):
        part(k).wait_send()
        result(k).wait_send()


def group_sum(diff, groups, identity, name, vectors=None, shards=0):
    flat = diff.reshape(-1, diff.shape[-1])
    span, cols = flat.shape[0] // groups, flat.shape[1]
    dma = pltpu.SemaphoreType.DMA
    whole = pl.BlockSpec(memory_space=pltpu.VMEM)
    out_shape = [jax.ShapeDtypeStruct(flat.shape, LOW)]
    extra = []
    if vectors:
        shape = vectors[0].shape
        half = (-(-shape[0] // 16) * 8, shape[1])
        out_shape += [
            jax.ShapeDtypeStruct((2, *shape), F32),
            jax.ShapeDtypeStruct((3, *shape), F32),
            jax.ShapeDtypeStruct(shape, LOW),
        ]
        extra = [
            pltpu.VMEM((2, *half), F32),
            pltpu.VMEM(half, F32),
            pltpu.VMEM(half, F32),
            pltpu.VMEM((shards, *half), F32),
            pltpu.VMEM((2, *half), F32),
            pltpu.VMEM((groups, *half), F32),
            pltpu.VMEM((2, *half), F32),
            dma((3,)),
            dma((3,)),
            dma((shards,)),
            dma((shards,)),
            dma((groups,)),
            dma((groups,)),
        ]
    total, *rest = pl.pallas_call(
        functools.partial(group_kernel, groups, shards, bool(vectors)),
        in_specs=[whole] * (5 if vectors else 1),
        out_specs=[whole] * len(out_shape),
        out_shape=out_shape,
        scratch_shapes=[
            pltpu.VMEM((2 * groups, span, cols), LOW),
            pltpu.VMEM((span, cols), LOW),
            *[dma((groups,))] * 4,
            *extra,
        ],
        compiler_params=params(identity),
        cost_estimate=cost(4 * flat.size, 8 * flat.size),
        name=name,
    )(flat, *(vectors or []))
    return total.reshape(diff.shape), *rest


def gather_weights(shard):
    whole = lax.all_gather(shard, "tensor", axis=0)
    return lax.all_gather(whole, "fsdp", axis=2, tiled=True)


def around(array, k, groups):
    return lax.ppermute(array, "group", [(i, (i + k) % groups) for i in range(groups)])


def exchange_parts(diff, groups):
    g = lax.axis_index("group")
    quarters = diff.reshape(groups, -1, diff.shape[-1])
    parts = [lax.dynamic_index_in_dim(quarters, lax.rem(g + k, groups), 0, keepdims=False) for k in range(groups)]
    total = sum([around(parts[k], k, groups).astype(F32) for k in range(1, groups)], parts[0].astype(F32))
    return total.astype(LOW)


def exchange_total(own, groups):
    return [own] + [around(own, k, groups) for k in range(1, groups)]


def scatter_gradient(gradient):
    half = gradient if gradient.ndim == 4 else lax.psum_scatter(gradient, "fsdp", scatter_dimension=0)
    return lax.psum_scatter(half, "tensor", scatter_dimension=0)


def local(
    patches,
    output_grad,
    live_counts,
    attn_master,
    mlp_master,
    vector_master,
    attn_moments,
    mlp_moments,
    vector_moments,
    attn_outer,
    mlp_outer,
    vector_outer,
):
    vec = vector_master
    tensor_size, fsdp = lax.axis_size("tensor"), lax.axis_size("fsdp")
    groups = lax.axis_size("group")
    local_images, seq, width = patches.shape[2:]
    slot = (lax.axis_index("fsdp") * tensor_size + lax.axis_index("tensor")) * local_images
    slot = slot + jnp.arange(local_images)
    counts = jnp.take(live_counts[0], slot // IMG_DEV, axis=1)
    alive = ((slot % IMG_DEV)[None, :] < counts).astype(F32).reshape(-1)
    x = patches.reshape(-1, seq, width)
    cotangent = output_grad.reshape(-1, seq, width)
    images = x.shape[0]

    if (groups, fsdp) == (4, 2):
        beside_images = [
            jnp.moveaxis(v.reshape(images, seq, width), 0, 1) for v in (patches, output_grad)
        ]
        w_attn, w_mlp, normed_one, qkv, attended, resid, normed_two, grad_two, x_rows = front(
            alive, attn_master, mlp_master, *beside_images, vec, tensor_size
        )
    else:
        w_attn = gather_weights(attn_master.astype(LOW))
        w_mlp = gather_weights(mlp_master.astype(LOW))
        normed_one, qkv = project(x, w_attn, vec)
        attended = attend(qkv, images, seq)
        resid, normed_two, grad_two = mix(alive, attended, x, cotangent, w_attn, vec)
        x_rows = jnp.pad(x, ((0, 0), (0, padded(seq) - seq), (0, 0))).reshape(-1, width)
    bias = vec[8:].reshape(tensor_size, 1, -1)
    carried = None
    mlp_grads, bias_parts = [], []
    for part, (start, cols) in enumerate(PIECES):
        *carried, dw, db = mlp(part, start, cols, normed_two, grad_two, w_mlp, bias, carried, fsdp)
        mlp_grads.append(scatter_gradient(dw))
        bias_parts.append(db)
    branch, grad_normed = carried
    block_output, grad_resid, grad_attended, dw_out, sums_two = turn(
        alive, resid, branch, grad_normed, grad_two, attended, w_attn, vec, images, seq, fsdp
    )
    def beside(*parts):
        return jnp.concatenate(parts, axis=-1)

    pairwise = fsdp == 2
    me = lax.axis_index("group").astype(jnp.int32).reshape(1)
    half = attn_master.shape[2] // PARTS
    (grads,) = unattend(qkv, grad_attended, images, seq, 0, PARTS, tensor_size)
    grads, mlp_grads[0] = lax.optimization_barrier((grads, mlp_grads[0]))
    carry, dw_early, head_sums = close(
        0, PARTS, normed_one, grads, w_attn, None, dw_out, None, fsdp, groups
    )
    if not pairwise:
        halves = jnp.moveaxis(dw_out.reshape(*dw_out.shape[:-1], PARTS, half), -2, 2)
        dw_early = jnp.concatenate([dw_early, halves[:, :, :, 0]], axis=2)
    early_grad = scatter_gradient(dw_early)
    head_sums = [head_sums]
    carry, mlp_grads[1] = lax.optimization_barrier((carry, mlp_grads[1]))
    hidden = mlp_master.shape[2] // 2
    mlp_inner, diff_one = inner_step(
        beside, mlp_grads[:2], lambda u: (u, 0), 2, hidden, mlp_master, mlp_moments, None, "inner_mlp_0"
    )
    riding = groups if pairwise else 0
    grads, *own_one = unattend(
        qkv, grad_attended, images, seq, 1, PARTS, tensor_size, diff_one.reshape(-1, hidden), riding
    )
    mlp_grads[2], grads = lax.optimization_barrier((mlp_grads[2], grads))
    mlp_inner, diff_two = inner_step(
        beside, mlp_grads[2:], lambda u: (u, 1), 2, hidden, mlp_master, mlp_moments, mlp_inner, "inner_mlp_1"
    )
    carry, diff_two = lax.optimization_barrier((carry, diff_two))
    carry, *own_two, dw_late, sums = close(
        1, PARTS, normed_one, grads, w_attn, carry, None, diff_two.reshape(-1, hidden), fsdp, groups
    )
    mlp_own = [beside(*own_one, *own_two)] if pairwise else []
    mlp_diff = beside(diff_one, diff_two)
    patches_grad, sums_one = finish(carry, grad_resid, x_rows, vec, images, seq)
    if not pairwise:
        mlp_own = [exchange_parts(mlp_diff, groups)]
    mlp_total = exchange_total(mlp_own[0], groups)
    late_grad = scatter_gradient(dw_late)
    head_sums.append(sums)

    def early(u):
        return jnp.minimum(u, 3), jnp.maximum(u - 3, 0)

    def late(u):
        return u, 1

    def first(piece):
        return piece

    attn_inner, early_diff = inner_step(
        first, [early_grad], early, 3 + PARTS, half, attn_master, attn_moments, None, "inner_early"
    )
    head_rows = jnp.concatenate([v.reshape(2, tensor_size, -1) for v in head_sums], axis=-1).reshape(2, width)
    hidden_bias = jnp.concatenate(bias_parts, axis=-1).reshape(-1, width)
    vector_part = jnp.concatenate([sums_one, sums_two[:2], head_rows, sums_two[2:], hidden_bias])

    if pairwise:
        early_total, vector_inner, vector_state, vector_copy = group_sum(
            early_diff,
            groups,
            10,
            "group_early",
            [vector_part, vec, vector_moments[0], vector_outer],
            tensor_size,
        )
    else:
        (early_total,) = group_sum(early_diff, groups, 10, "group_early")
        vector_grad = lax.psum(vector_part, ("fsdp", "tensor"))
        new_vector, second_vector = inner_adamw(
            vec, vector_grad, vector_moments[0, 0], vector_moments[0, 1], VECTOR_RATE, 0.0
        )
        diff_vector = lax.psum(vec - new_vector, "group") / groups
        momentum, fresh = outer_nesterov(vec, vector_outer, diff_vector)
        vector_inner = jnp.stack([vector_grad, second_vector])
        vector_state, vector_copy = jnp.stack([diff_vector, momentum, fresh]), fresh.astype(LOW)
    attn_state, attn_copy = outer_step(
        groups, me, [early_total], early, 3 + PARTS, half, attn_master, attn_outer, None, "outer_early"
    )
    attn_copy, *mlp_total = lax.optimization_barrier((attn_copy, *mlp_total))
    mlp_state, mlp_copy = outer_step(
        groups,
        me,
        mlp_total,
        lambda u: (u, 0),
        2,
        mlp_master.shape[2],
        mlp_master,
        mlp_outer,
        None,
        "outer_mlp",
    )
    late_grad, mlp_state = lax.optimization_barrier((late_grad, mlp_state))
    attn_inner, late_diff = inner_step(
        first, [late_grad], late, 3, half, attn_master, attn_moments, attn_inner, "inner_late"
    )
    (late_total,) = group_sum(late_diff, groups, 11, "group_late")
    attn_state, attn_copy = outer_step(
        groups, me, [late_total], late, 3, half, attn_master, attn_outer, (attn_state, attn_copy), "outer_late"
    )
    return (
        block_output.reshape(patches.shape),
        patches_grad.reshape(patches.shape),
        attn_inner,
        attn_state,
        attn_copy,
        mlp_inner,
        mlp_state,
        mlp_copy,
        vector_inner[None],
        vector_state,
        vector_copy,
    )


def solution(mesh):
    placed = (
        P("group", None, ("fsdp", "tensor"), None, None),
        P("group", None, ("fsdp", "tensor"), None, None),
        P("group", None, None),
        P(None, "fsdp", "tensor"),
        P(None, "fsdp", "tensor"),
        P(),
        P("group", None, None, "fsdp", "tensor"),
        P("group", None, None, "fsdp", "tensor"),
        P("group", None, None, None),
        P(None, "fsdp", "tensor"),
        P(None, "fsdp", "tensor"),
        P(),
    )
    return jax.shard_map(
        local,
        mesh=mesh,
        in_specs=placed,
        out_specs=(
            P("group", None, ("fsdp", "tensor"), None, None),
            P("group", None, ("fsdp", "tensor"), None, None),
            P("group", None, None, "fsdp", "tensor"),
            P(None, None, "fsdp", "tensor"),
            P(None, "fsdp", "tensor"),
            P("group", None, None, "fsdp", "tensor"),
            P(None, None, "fsdp", "tensor"),
            P(None, "fsdp", "tensor"),
            P("group", None, None, None),
            P(),
            P(),
        ),
        check_vma=False,
    )
```

```python
import functools

import jax
import jax.numpy as jnp
from jax import lax
from jax.experimental import pallas as pl
from jax.experimental.pallas import tpu as pltpu
from jax.sharding import PartitionSpec as P

HD = 64
STEP = 8
IMG_DEV = 4
EPSILON = 1e-06
INNER_RATE = 0.02
VECTOR_RATE = 0.2
WEIGHT_DECAY = 0.1
OUTER_RATE = 0.7
OUTER_MOMENTUM = 0.9
PIECES = ((0, 256), (256, 256), (512, 512))
PARTS = 2
LOW = jnp.bfloat16
F32 = jnp.float32
NN = (((1,), (0,)), ((), ()))
NT = (((1,), (1,)), ((), ()))
TN = (((0,), (0,)), ((), ()))


def dot(a, b, dims=NN):
    return lax.dot_general(a, b, dims, preferred_element_type=F32)


MESH = pl.DeviceIdType.MESH


def params(identity=None):
    if identity is None:
        return pltpu.CompilerParams(vmem_limit_bytes=60 * 2**20)
    return pltpu.CompilerParams(vmem_limit_bytes=60 * 2**20, collective_id=identity, has_side_effects=True)


def partner():
    return (lax.axis_index("group"), 1 - lax.axis_index("fsdp"), lax.axis_index("tensor"))


def greet_partner():
    barrier = pltpu.get_barrier_semaphore()
    pl.semaphore_signal(barrier, inc=1, device_id=partner(), device_id_type=MESH)
    pl.semaphore_wait(barrier, 1)


def to_partner(sent, received, sends, receives, n):
    return pltpu.make_async_remote_copy(
        src_ref=sent.at[n],
        dst_ref=received.at[n],
        send_sem=sends.at[n],
        recv_sem=receives.at[n],
        device_id=partner(),
        device_id_type=MESH,
    )


def bands(depth):
    f = lax.axis_index("fsdp")
    return pl.ds(pl.multiple_of(f * depth, depth), depth), pl.ds(pl.multiple_of((1 - f) * depth, depth), depth)


def exchange_scratch(steps, shape):
    dma = pltpu.SemaphoreType.DMA
    return [
        pltpu.VMEM((steps, *shape), F32),
        pltpu.VMEM((steps, *shape), LOW),
        pltpu.VMEM((steps, *shape), LOW),
        dma((steps,)),
        dma((steps,)),
    ]


def cost(flops, moved, special=0):
    return pl.CostEstimate(flops=int(flops), bytes_accessed=int(moved), transcendentals=int(special))


def padded(rows):
    return -(-rows // 16) * 16


def centred(source):
    centre = source - jnp.mean(source, axis=-1, keepdims=True)
    spread = jnp.mean(centre * centre, axis=-1, keepdims=True)
    inverse = lax.rsqrt(spread + EPSILON)
    return centre * inverse, inverse


def norm_back(upstream, normal, inverse, gain):
    pulled = upstream * gain
    mean_one = jnp.mean(pulled, axis=-1, keepdims=True)
    mean_two = jnp.mean(pulled * normal, axis=-1, keepdims=True)
    return inverse * (pulled - mean_one - normal * mean_two)


def project_kernel(images, seq, x_ref, w_ref, vec_ref, n_ref, out_ref, n_scr):
    j, t = pl.program_id(0), pl.program_id(1)
    span = n_scr.shape[0] // images

    @pl.when((j == 0) & (t == 0))
    def _():
        n_scr[...] = jnp.zeros_like(n_scr)
        for i in range(images):
            normal, _ = centred(x_ref[i].astype(F32))
            n_scr[pl.ds(i * span, seq), :] = (normal * vec_ref[0:1] + vec_ref[1:2]).astype(LOW)
        n_ref[...] = n_scr[...]

    cols = out_ref.shape[-1]
    out = dot(n_scr[...], w_ref[0, 0])
    at = pl.ds(pl.multiple_of(t * cols, cols), cols)
    bias = jnp.where(j == 0, vec_ref[4:5, at], jnp.where(j == 2, vec_ref[5:6, at], 0.0))
    out_ref[0] = (out + bias).astype(LOW)


def project(patches, w_attn, vec):
    images, seq, width = patches.shape
    shards, _, _, cols = w_attn.shape
    rows = images * padded(seq)
    return pl.pallas_call(
        functools.partial(project_kernel, images, seq),
        grid=(3, shards),
        in_specs=[
            pl.BlockSpec((images, seq, width), lambda j, t: (0, 0, 0)),
            pl.BlockSpec((1, 1, width, cols), lambda j, t: (t, j, 0, 0)),
            pl.BlockSpec(vec.shape, lambda j, t: (0, 0)),
        ],
        out_specs=[
            pl.BlockSpec((rows, width), lambda j, t: (0, 0)),
            pl.BlockSpec((1, rows, cols), lambda j, t: (j, 0, t)),
        ],
        out_shape=[
            jax.ShapeDtypeStruct((rows, width), LOW),
            jax.ShapeDtypeStruct((3, rows, width), LOW),
        ],
        scratch_shapes=[pltpu.VMEM((rows, width), LOW)],
        compiler_params=params(),
        cost_estimate=cost(6 * rows * width * width, 16 * rows * width),
        name="project",
    )(patches, w_attn, vec)


def half_lanes(value, which):
    lane = lax.broadcasted_iota(jnp.int32, value.shape, 1)
    return jnp.where((lane >= HD) == bool(which), value, jnp.zeros_like(value))


def attend_kernel(seq, q_ref, k_ref, v_ref, out_ref):
    span = q_ref.shape[1]
    scale = HD**-0.5
    q, k, v = q_ref[0], k_ref[0], v_ref[0]
    parts = []
    for h in range(2):
        scores = dot(q, half_lanes(k, h), NT)
        lane = lax.broadcasted_iota(jnp.int32, scores.shape, 1)
        scores = jnp.where(lane < seq, scores, -1e30)
        top = jnp.max(scores, axis=1, keepdims=True)
        raised = jnp.exp((scores - top) * scale)
        total = jnp.sum(raised, axis=1, keepdims=True)
        probs = (raised * (1.0 / total)).astype(LOW)
        parts.append(dot(probs, v))
    lane = lax.broadcasted_iota(jnp.int32, (span, 2 * HD), 1)
    out_ref[...] = jnp.where(lane < HD, parts[0], parts[1]).astype(LOW)


def attend(qkv, images, seq):
    _, rows, width = qkv.shape
    span = rows // images
    pair = 2 * HD

    def take(j):
        return pl.BlockSpec((1, span, pair), lambda i, h: (j, i, h))

    return pl.pallas_call(
        functools.partial(attend_kernel, seq),
        grid=(images, width // pair),
        in_specs=[take(0), take(1), take(2)],
        out_specs=pl.BlockSpec((span, pair), lambda i, h: (i, h)),
        out_shape=jax.ShapeDtypeStruct((rows, width), LOW),
        compiler_params=params(),
        cost_estimate=cost(16 * rows * span * width, 8 * rows * width, rows * span * (width // HD)),
        name="attend",
    )(qkv, qkv, qkv)


def mix_kernel(seq, alive_ref, att_ref, x_ref, g_ref, w_ref, vec_ref, resid_ref, n_ref, g2_ref, x_scr):
    i = pl.program_id(0)
    shards, _, _, cols = w_ref.shape
    x_scr[...] = jnp.zeros_like(x_scr)
    x_scr[0:seq, :] = x_ref[0].astype(F32)
    total = x_scr[...] + vec_ref[6:7]
    for t in range(shards):
        total = total + dot(att_ref[:, t * cols : (t + 1) * cols], w_ref[t, 0], NT)
    resid_ref[...] = total
    normal, _ = centred(total)
    n_ref[...] = (normal * vec_ref[2:3] + vec_ref[3:4]).astype(LOW)
    x_scr[0:seq, :] = g_ref[0].astype(F32) * alive_ref[i]
    g2_ref[...] = x_scr[...].astype(LOW)


def mix(alive, attended, patches, cotangent, w_attn, vec):
    images, seq, width = patches.shape
    rows = attended.shape[0]
    span = rows // images
    shards, _, _, cols = w_attn.shape
    block = pl.BlockSpec((span, width), lambda i: (i, 0))
    whole = jax.ShapeDtypeStruct((rows, width), LOW)
    return pl.pallas_call(
        functools.partial(mix_kernel, seq),
        grid=(images,),
        in_specs=[
            pl.BlockSpec(memory_space=pltpu.SMEM),
            block,
            pl.BlockSpec((1, seq, width), lambda i: (i, 0, 0)),
            pl.BlockSpec((1, seq, width), lambda i: (i, 0, 0)),
            pl.BlockSpec((shards, 1, width, cols), lambda i: (0, 3, 0, 0)),
            pl.BlockSpec(vec.shape, lambda i: (0, 0)),
        ],
        out_specs=[block, block, block],
        out_shape=[jax.ShapeDtypeStruct((rows, width), F32), whole, whole],
        scratch_shapes=[pltpu.VMEM((span, width), F32)],
        compiler_params=params(),
        cost_estimate=cost(2 * rows * width * width, 16 * rows * width),
        name="mix",
    )(alive, attended, patches, cotangent, w_attn, vec)


def mlp_kernel(first, pairwise, n_ref, g_ref, w1_ref, w2_ref, bias_ref, *refs):
    if not first:
        yi_ref, gi_ref, *refs = refs
    y_ref, gn_ref, dw_ref, db_ref, h_scr, p_scr, loaded, *exchange = refs
    step = pl.program_id(0)
    each, _, width, cols = w1_ref.shape
    if not first:
        loads = (
            pltpu.make_async_copy(yi_ref, y_ref, loaded.at[0]),
            pltpu.make_async_copy(gi_ref, gn_ref, loaded.at[1]),
        )

    @pl.when(step == 0)
    def _():
        if not first:
            for load in loads:
                load.start()
        else:
            y_ref[...] = jnp.zeros_like(y_ref)
            gn_ref[...] = jnp.zeros_like(gn_ref)
        if pairwise:
            greet_partner()

    w1 = jnp.concatenate([w1_ref[t, 0] for t in range(each)], axis=1)
    w2 = jnp.concatenate([w2_ref[t, 0] for t in range(each)], axis=1)
    bias = jnp.concatenate([bias_ref[t] for t in range(each)], axis=1)
    pre = dot(n_ref[...], w1) + bias
    cdf = 0.5 * (1.0 + lax.erf(pre * 0.7071067811865476))
    h_scr[...] = (pre * cdf).astype(LOW)
    slope = cdf + pre * jnp.exp(-0.5 * pre * pre) * 0.3989422804014327
    p_scr[...] = (dot(g_ref[...], w2) * slope).astype(LOW)
    sums = jnp.sum(p_scr[...].astype(F32), axis=0, keepdims=True)
    for t in range(each):
        db_ref[t] = sums[:, t * cols : (t + 1) * cols]

    if pairwise:
        own, sent, received, sends, receives = exchange
        ours, theirs = bands(width // 2)

        slot = lax.rem(step, 2)

        def collect(n):
            at = lax.rem(n, 2)
            to_partner(sent, received, sends, receives, at).wait()
            for which in range(2):
                total = (own[at, which] + received[at, which].astype(F32)).astype(LOW)
                for t in range(each):
                    dw_ref[n * each + t, which] = total[:, t * cols : (t + 1) * cols]

        @pl.when(step > 0)
        def _():
            collect(step - 1)

        sent[slot, 0] = dot(n_ref[:, theirs], p_scr[...], TN).astype(LOW)
        sent[slot, 1] = dot(g_ref[:, theirs], h_scr[...], TN).astype(LOW)
        to_partner(sent, received, sends, receives, slot).start()
        own[slot, 0] = dot(n_ref[:, ours], p_scr[...], TN)
        own[slot, 1] = dot(g_ref[:, ours], h_scr[...], TN)

    else:
        shards, depth = dw_ref.shape[0], dw_ref.shape[3]
        d1 = dot(n_ref[...], p_scr[...], TN).astype(LOW)
        d2 = dot(g_ref[...], h_scr[...], TN).astype(LOW)
        for f in range(shards):
            for t in range(each):
                dw_ref[f, t, 0] = d1[f * depth : (f + 1) * depth, t * cols : (t + 1) * cols]
                dw_ref[f, t, 1] = d2[f * depth : (f + 1) * depth, t * cols : (t + 1) * cols]

    if not first:

        @pl.when(step == 0)
        def _():
            for load in loads:
                load.wait()

    y_ref[...] += dot(h_scr[...], w2, NT)
    gn_ref[...] += dot(p_scr[...], w1, NT)
    if pairwise:

        @pl.when(step == pl.num_programs(0) - 1)
        def _():
            collect(step)


def mlp(part, start, cols, normed, grad_two, w_mlp, bias, carried, fsdp):
    rows, width = normed.shape
    shards = w_mlp.shape[0]
    each = max(512 // cols, 1)
    at = start // cols
    first, pairwise = carried is None, fsdp == 2
    single = pl.Buffered(1)
    full = pl.BlockSpec((rows, width), lambda s: (0, 0), pipeline_mode=single)
    depth = width // fsdp
    steps = shards // each
    acc_shape = jax.ShapeDtypeStruct((rows, width), F32)
    if pairwise:
        out_w = pl.BlockSpec((shards, 2, depth, cols), lambda s: (0, 0, 0, 0), pipeline_mode=single)
        w_shape = jax.ShapeDtypeStruct((shards, 2, depth, cols), LOW)
        extra = exchange_scratch(2, (2, depth, each * cols))
    else:
        out_w = pl.BlockSpec((fsdp, each, 2, depth, cols), lambda s: (0, s, 0, 0, 0))
        w_shape = jax.ShapeDtypeStruct((fsdp, shards, 2, depth, cols), LOW)
        extra = []
    return pl.pallas_call(
        functools.partial(mlp_kernel, first, pairwise),
        grid=(steps,),
        in_specs=[
            full,
            full,
            pl.BlockSpec((each, 1, width, cols), lambda s: (s, 0, 0, at)),
            pl.BlockSpec((each, 1, width, cols), lambda s: (s, 1, 0, at)),
            pl.BlockSpec((each, 1, cols), lambda s: (s, 0, at)),
        ]
        + ([] if first else [pl.BlockSpec(memory_space=pl.ANY)] * 2),
        out_specs=[full, full, out_w, pl.BlockSpec((each, 1, cols), lambda s: (s, 0, 0))],
        out_shape=[acc_shape, acc_shape, w_shape, jax.ShapeDtypeStruct((shards, 1, cols), F32)],
        scratch_shapes=[
            pltpu.VMEM((rows, each * cols), LOW),
            pltpu.VMEM((rows, each * cols), LOW),
            pltpu.SemaphoreType.DMA((2,)),
            *extra,
        ],
        compiler_params=params(2 + part if pairwise else None),
        cost_estimate=cost(12 * rows * width * cols * shards, 24 * rows * width),
        name=f"mlp_{part}",
    )(normed, grad_two, w_mlp, w_mlp, bias, *([] if first else carried))


def turn_kernel(seq, pairwise, alive_ref, resid_ref, y_ref, gn_ref, g2_ref, att_ref, w_ref, vec_ref,
                out_ref, gr_ref, ga_ref, dw_ref, sums_ref, dw_scr, *exchange):
    i = pl.program_id(0)
    if pairwise:
        pl.when(i == 0)(greet_partner)
    shards, _, _, cols = w_ref.shape
    resid = resid_ref[...]
    out_ref[0] = ((resid + y_ref[...] + vec_ref[7:8]) * alive_ref[i]).astype(LOW)[0:seq]
    normal, inverse = centred(resid)
    upstream = gn_ref[...]
    grad_out = g2_ref[...].astype(F32)
    grad_resid = grad_out + norm_back(upstream, normal, inverse, vec_ref[2:3])
    gr_ref[...] = grad_resid
    low = grad_resid.astype(LOW)
    rows = [
        jnp.sum(upstream * normal, axis=0, keepdims=True),
        jnp.sum(upstream, axis=0, keepdims=True),
        jnp.sum(grad_resid, axis=0, keepdims=True),
        jnp.sum(grad_out, axis=0, keepdims=True),
    ]
    rows = jnp.concatenate(rows, axis=0)

    @pl.when(i == 0)
    def _():
        sums_ref[...] = rows

    @pl.when(i != 0)
    def _():
        sums_ref[...] += rows

    for t in range(shards):
        ga_ref[:, t * cols : (t + 1) * cols] = dot(low, w_ref[t, 0]).astype(LOW)
    part = dot(low, att_ref[...], TN)

    @pl.when(i == 0)
    def _():
        dw_scr[...] = part

    @pl.when(i != 0)
    def _():
        dw_scr[...] += part

    @pl.when(i == pl.num_programs(0) - 1)
    def _():
        if pairwise:
            sent, received, sends, receives = exchange
            ours, theirs = bands(dw_scr.shape[0] // 2)
            sent[0] = dw_scr[theirs, :].astype(LOW)
            copy = to_partner(sent, received, sends, receives, 0)
            copy.start()
            copy.wait()
            total = (dw_scr[ours, :] + received[0].astype(F32)).astype(LOW)
            for t in range(shards):
                dw_ref[t, 0] = total[:, t * cols : (t + 1) * cols]
            return
        depth = dw_ref.shape[3]
        for f in range(dw_ref.shape[0]):
            for t in range(shards):
                dw_ref[f, t, 0] = dw_scr[f * depth : (f + 1) * depth, t * cols : (t + 1) * cols].astype(LOW)


def turn(alive, resid, branch, grad_normed, grad_two, attended, w_attn, vec, images, seq, fsdp):
    rows, width = resid.shape
    span = rows // images
    shards, _, _, cols = w_attn.shape
    depth = width // fsdp
    pairwise = fsdp == 2
    lead = () if pairwise else (fsdp,)
    block = pl.BlockSpec((span, width), lambda i: (i, 0))
    return pl.pallas_call(
        functools.partial(turn_kernel, seq, pairwise),
        grid=(images,),
        in_specs=[
            pl.BlockSpec(memory_space=pltpu.SMEM),
            block, block, block, block, block,
            pl.BlockSpec((shards, 1, width, cols), lambda i: (0, 3, 0, 0)),
            pl.BlockSpec(vec.shape, lambda i: (0, 0)),
        ],
        out_specs=[
            pl.BlockSpec((1, seq, width), lambda i: (i, 0, 0)),
            block, block,
            pl.BlockSpec((*lead, shards, 1, depth, cols), lambda i: (0,) * (4 + len(lead))),
            pl.BlockSpec((4, width), lambda i: (0, 0)),
        ],
        out_shape=[
            jax.ShapeDtypeStruct((images, seq, width), LOW),
            jax.ShapeDtypeStruct((rows, width), F32),
            jax.ShapeDtypeStruct((rows, width), LOW),
            jax.ShapeDtypeStruct((*lead, shards, 1, depth, cols), LOW),
            jax.ShapeDtypeStruct((4, width), F32),
        ],
        scratch_shapes=[pltpu.VMEM((width, width), F32)] + (exchange_scratch(1, (depth, width))[1:] if pairwise else []),
        compiler_params=params(6 if pairwise else None),
        cost_estimate=cost(4 * rows * width * width, 24 * rows * width),
        name="turn",
    )(alive, resid, branch, grad_normed, grad_two, attended, w_attn, vec)


def carrier(groups, paired, diff_ref, total_ref, mine, landed, sends, receives, loaded):
    g, f, t = lax.axis_index("group"), lax.axis_index("fsdp"), lax.axis_index("tensor")
    quarter = landed.shape[1]

    def rows(n):
        return pl.ds(pl.multiple_of(n * quarter, quarter), quarter)

    def other(k):
        return (lax.rem(g + k, groups), f, t)

    def part(k):
        return pltpu.make_async_remote_copy(
            src_ref=diff_ref.at[rows(lax.rem(g + k, groups)), :],
            dst_ref=landed.at[k],
            send_sem=sends.at[k],
            recv_sem=receives.at[k],
            device_id=other(k),
            device_id_type=MESH,
        )

    keep = pltpu.make_async_copy(diff_ref.at[rows(g), :], mine, loaded.at[0])

    def begin():
        barrier = pltpu.get_barrier_semaphore()
        if paired:
            pl.semaphore_signal(barrier, inc=1, device_id=partner(), device_id_type=MESH)
        for k in range(1, groups):
            pl.semaphore_signal(barrier, inc=1, device_id=other(k), device_id_type=MESH)
        pl.semaphore_wait(barrier, groups - 1 + int(paired))
        for k in range(1, groups):
            part(k).start()
        keep.start()

    def end():
        keep.wait()
        total = mine[...].astype(F32)
        for k in range(1, groups):
            part(k).wait()
            total = total + landed[k].astype(F32)
        total_ref[...] = total.astype(LOW)

    return begin, end


def carrier_scratch(groups, quarter, lanes):
    dma = pltpu.SemaphoreType.DMA
    return [
        pltpu.VMEM((quarter, lanes), LOW),
        pltpu.VMEM((groups, quarter, lanes), LOW),
        dma((groups,)),
        dma((groups,)),
        dma((1,)),
    ]


def unattend_kernel(seq, groups, q_ref, k_ref, v_ref, g_ref, *refs):
    if groups:
        diff_ref, out_ref, total_ref, *scratch = refs
        begin, end = carrier(groups, False, diff_ref, total_ref, *scratch)
        pl.when((pl.program_id(0) == 0) & (pl.program_id(1) == 0))(begin)
    else:
        (out_ref,) = refs
    span = q_ref.shape[1]
    scale = HD**-0.5
    q, k, v, g = q_ref[0], k_ref[0], v_ref[0], g_ref[...]
    scaled = (k.astype(F32) * scale).astype(LOW)
    parts = []
    for h in range(2):
        scores = dot(half_lanes(scaled, h), q, NT)
        row = lax.broadcasted_iota(jnp.int32, scores.shape, 0)
        scores = jnp.where(row < seq, scores, -1e30)
        top = jnp.max(scores, axis=0, keepdims=True)
        raised = jnp.exp(scores - top)
        total = jnp.sum(raised, axis=0, keepdims=True)
        probs = raised * (1.0 / total)
        gp = dot(half_lanes(v, h), g, NT)
        delta = jnp.sum(probs * gp, axis=0, keepdims=True)
        gs = (probs * (gp - delta)).astype(LOW)
        dv = dot(probs.astype(LOW), g)
        dk = dot(gs, q)
        dq = dot(gs, k, TN)
        parts.append((dq, dk, dv))
    lane = lax.broadcasted_iota(jnp.int32, (span, 2 * HD), 1) < HD
    out_ref[0] = (jnp.where(lane, parts[0][0], parts[1][0]) * scale).astype(LOW)
    out_ref[1] = (jnp.where(lane, parts[0][1], parts[1][1]) * scale).astype(LOW)
    out_ref[2] = jnp.where(lane, parts[0][2], parts[1][2]).astype(LOW)
    if groups:
        at_end = (pl.program_id(0) == pl.num_programs(0) - 1) & (pl.program_id(1) == pl.num_programs(1) - 1)
        pl.when(at_end)(end)


def unattend(qkv, grad_attended, images, seq, part, parts, shards, diff=None, groups=0):
    _, rows, width = qkv.shape
    span = rows // images
    pair = 2 * HD
    each = width // shards // parts // pair

    def spot(h):
        return (h // each) * (each * parts) + part * each + h % each

    def take(j):
        return pl.BlockSpec((1, span, pair), lambda i, h: (j, i, spot(h)))

    in_specs = [take(0), take(1), take(2), pl.BlockSpec((span, pair), lambda i, h: (i, spot(h)))]
    out_specs = [pl.BlockSpec((3, span, pair), lambda i, h: (0, i, h))]
    out_shape = [jax.ShapeDtypeStruct((3, rows, width // parts), LOW)]
    scratch = []
    if groups:
        quarter, lanes = diff.shape[0] // groups, diff.shape[1]
        in_specs.append(pl.BlockSpec(memory_space=pl.ANY))
        out_specs.append(pl.BlockSpec((quarter, lanes), lambda i, h: (0, 0)))
        out_shape.append(jax.ShapeDtypeStruct((quarter, lanes), LOW))
        scratch = carrier_scratch(groups, quarter, lanes)
    return pl.pallas_call(
        functools.partial(unattend_kernel, seq, groups),
        grid=(images, width // pair // parts),
        in_specs=in_specs,
        out_specs=out_specs,
        out_shape=out_shape,
        scratch_shapes=scratch,
        compiler_params=params(9 if groups else None),
        cost_estimate=cost(
            40 * rows * span * width // parts, 14 * rows * width // parts, rows * span * (width // HD) // parts
        ),
        name=f"unattend_{part}",
    )(qkv, qkv, qkv, grad_attended, *([diff] if groups else []))


def close_kernel(pairwise, groups, first, final, n_ref, grad_ref, w_ref, *refs):
    if not first:
        carry_ref, *refs = refs
    elif pairwise:
        more_ref, *refs = refs
    if pairwise and final:
        diff_ref, acc_ref, total_ref, *refs = refs
    else:
        acc_ref, *refs = refs
    dw_ref, sums_ref, acc_scr, *exchange = refs
    j = pl.program_id(0)
    shards, _, _, cols = w_ref.shape
    if pairwise:
        own, sent, received, sends, receives, *exchange = exchange
        if not final:
            pl.when(j == 0)(greet_partner)
    if pairwise and final:
        begin, end = carrier(groups, True, diff_ref, total_ref, *exchange)
        pl.when(j == 0)(begin)

    @pl.when(j == 0)
    def _():
        acc_scr[...] = jnp.zeros_like(acc_scr) if first else carry_ref[...]

    sums = jnp.sum(grad_ref[0].astype(F32), axis=0, keepdims=True)
    for n, matrix in enumerate((0, 2)):

        @pl.when(j == matrix)
        def _():
            sums_ref[n : n + 1, :] = sums

    def spread(n, total, f=None):
        for t in range(shards):
            piece = total[:, t * cols : (t + 1) * cols]
            if f is None:
                dw_ref[t, n] = piece
            else:
                dw_ref[f, t, 0] = piece

    weight = jnp.concatenate([w_ref[t, 0] for t in range(shards)], axis=1)
    if pairwise:
        ours, theirs = bands(n_ref.shape[1] // 2)
        sent[j] = dot(n_ref[:, theirs], grad_ref[0], TN).astype(LOW)
        to_partner(sent, received, sends, receives, j).start()
        own[j] = dot(n_ref[:, ours], grad_ref[0], TN)
    else:
        depth = dw_ref.shape[3]
        dw = dot(n_ref[...], grad_ref[0], TN).astype(LOW)
        for f in range(dw_ref.shape[0]):
            spread(0, dw[f * depth : (f + 1) * depth], f)
    acc_scr[...] += dot(grad_ref[0], weight, NT)

    @pl.when(j == 2)
    def _():
        if pairwise:
            for n in range(own.shape[0]):
                to_partner(sent, received, sends, receives, n).wait()
                spread(n, (own[n] + received[n].astype(F32)).astype(LOW))
            if first:
                for t in range(shards):
                    for n in range(dw_ref.shape[1] - 3):
                        dw_ref[t, 3 + n] = more_ref[t, 0, :, n * cols : (n + 1) * cols]
        acc_ref[...] = acc_scr[...]
        if pairwise and final:
            end()


def close(part, parts, normed, grads, w_attn, carry, more, ending, fsdp, groups):
    rows, width = normed.shape
    shards, _, _, cols = w_attn.shape
    cols = cols // parts
    lanes = shards * cols
    depth = width // fsdp
    pairwise, first, final = fsdp == 2, carry is None, ending is not None
    single = pl.Buffered(1)
    stack = pl.BlockSpec((1, rows, lanes), lambda j: (j, 0, 0))
    full = pl.BlockSpec((rows, width), lambda j: (0, 0), pipeline_mode=single)
    if pairwise:
        many = 3 + parts if first else 3
        dw_spec = pl.BlockSpec((shards, many, depth, cols), lambda j: (0, 0, 0, 0), pipeline_mode=single)
        dw_shape = jax.ShapeDtypeStruct((shards, many, depth, cols), LOW)
        extra = exchange_scratch(3, (depth, lanes))
    else:
        dw_spec = pl.BlockSpec((fsdp, shards, 1, depth, cols), lambda j: (0, 0, j, 0, 0))
        dw_shape = jax.ShapeDtypeStruct((fsdp, shards, 3, depth, cols), LOW)
        extra = []
    in_specs = [full, stack, pl.BlockSpec((shards, 1, width, cols), lambda j: (0, j, 0, part))]
    out_specs, out_shape = [], []
    if not first:
        in_specs.append(full)
    elif pairwise:
        in_specs.append(pl.BlockSpec(more.shape, lambda j: (0, 0, 0, 0), pipeline_mode=single))
    out_specs.append(full)
    out_shape.append(jax.ShapeDtypeStruct((rows, width), F32))
    if pairwise and final:
        quarter, lanes_two = ending.shape[0] // groups, ending.shape[1]
        in_specs.append(pl.BlockSpec(memory_space=pl.ANY))
        out_specs.append(pl.BlockSpec((quarter, lanes_two), lambda j: (0, 0), pipeline_mode=single))
        out_shape.append(jax.ShapeDtypeStruct((quarter, lanes_two), LOW))
        extra = [*extra, *carrier_scratch(groups, quarter, lanes_two)]
    return pl.pallas_call(
        functools.partial(close_kernel, pairwise, groups, first, final),
        grid=(3,),
        in_specs=in_specs,
        out_specs=[*out_specs, dw_spec, pl.BlockSpec((2, lanes), lambda j: (0, 0))],
        out_shape=[*out_shape, dw_shape, jax.ShapeDtypeStruct((2, lanes), F32)],
        scratch_shapes=[pltpu.VMEM((rows, width), F32), *extra],
        compiler_params=params(7 + part if pairwise else None),
        cost_estimate=cost(12 * rows * width * lanes, 20 * rows * width),
        name=f"close_{part}",
    )(normed, grads, w_attn, *([carry] if not first else [more] if pairwise else []), *([ending] if pairwise and final else []))


def finish_kernel(acc_ref, gr_ref, x_ref, vec_ref, out_ref, norm_ref):
    i = pl.program_id(0)
    seq = out_ref.shape[1]
    normal, inverse = centred(x_ref[...].astype(F32))
    upstream = acc_ref[...]
    grad = gr_ref[...] + norm_back(upstream, normal, inverse, vec_ref[0:1])
    out_ref[0, :, 0, :] = grad[0:seq]
    sums = [jnp.sum(upstream * normal, axis=0, keepdims=True), jnp.sum(upstream, axis=0, keepdims=True)]
    sums = jnp.concatenate(sums, axis=0)

    @pl.when(i == 0)
    def _():
        norm_ref[...] = sums

    @pl.when(i != 0)
    def _():
        norm_ref[...] += sums


def finish(acc, grad_resid, x_rows, vec, images, seq):
    rows, width = acc.shape
    block = pl.BlockSpec((rows // images, width), lambda i: (i, 0))
    return pl.pallas_call(
        finish_kernel,
        grid=(images,),
        in_specs=[block, block, block, pl.BlockSpec(vec.shape, lambda i: (0, 0))],
        out_specs=[pl.BlockSpec((1, seq, 1, width), lambda i: (i, 0, 0, 0)), pl.BlockSpec((2, width), lambda i: (0, 0))],
        out_shape=[
            jax.ShapeDtypeStruct((images, seq, 1, width), F32),
            jax.ShapeDtypeStruct((2, width), F32),
        ],
        compiler_params=params(),
        cost_estimate=cost(20 * rows * width, 14 * rows * width),
        name="finish",
    )(acc, grad_resid, x_rows, vec)


def attend_pair(seq, q, k, v):
    scale = HD**-0.5
    parts = []
    for h in range(2):
        scores = dot(q, half_lanes(k, h), NT)
        lane = lax.broadcasted_iota(jnp.int32, scores.shape, 1)
        scores = jnp.where(lane < seq, scores, -1e30)
        top = jnp.max(scores, axis=1, keepdims=True)
        raised = jnp.exp((scores - top) * scale)
        total = jnp.sum(raised, axis=1, keepdims=True)
        probs = (raised * (1.0 / total)).astype(LOW)
        parts.append(dot(probs, v))
    lane = lax.broadcasted_iota(jnp.int32, parts[0].shape, 1)
    return jnp.where(lane < HD, parts[0], parts[1]).astype(LOW)


def front_kernel(
    images, seq, alive_ref, a_in, m_in, x_ref, g_ref, vec_ref,
    a_out, m_out, n_out, qkv_out, att_out, resid_out, n2_out, g2_out, x_out,
    a_wide, m_wide, a_hold, m_hold, n_scr, qkv_scr, att_scr, w_scr, o_scr, resid_scr, n2_scr, g2_scr, x_all,
    zs, zr, xs, xr, ys, yr, xfs, xfr, yfs, yfr, cs, cr, ls, ws,
):
    g, f, z = lax.axis_index("group"), lax.axis_index("fsdp"), lax.axis_index("tensor")
    shards = lax.axis_size("tensor")
    last = shards - 1
    x_at, y_at = g % 2, g // 2
    east, north = y_at * 2 + (1 - x_at), (1 - y_at) * 2 + x_at
    depth, cols = a_in.shape[1:]
    band = depth // 4
    shared = band * 3 // 8
    rest = band - 2 * shared
    span = n_scr.shape[0] // images

    def place(column):
        cx, cy = column % 2, column // 2
        return 2 * (cx + cy - 2 * cx * cy) + cy

    mine, of_east, of_north = place(g), place(east), place(north)
    z_row = mine * band - shared * (mine % 2)
    lead_east = of_east * band + shared * (of_east % 2)
    lead_north = of_north * band + shared * (of_north % 2)
    chunks = ((a_out, 0, 3), (a_out, 3, 1), (m_out, 0, 1), (m_out, 1, 1))

    def tile(n):
        return pl.multiple_of(n, 16)

    def held(n, t, row, rows):
        out, j, many = chunks[n]
        return out.at[t, pl.ds(j, many), pl.ds(tile(f * depth + row), rows), :]

    def send(part, sems, semr, n, t, to):
        return pltpu.make_async_remote_copy(
            src_ref=part, dst_ref=part, send_sem=sems.at[n, t], recv_sem=semr.at[n, t], device_id=to, device_id_type=MESH
        )

    def along(n, t, up):
        part = held(n, t, z_row, band + shared)
        return pltpu.make_async_remote_copy(
            src_ref=part,
            dst_ref=part,
            send_sem=zs.at[n, t, 0 if up else 1],
            recv_sem=zr.at[n, t],
            device_id=(g, f, z + 1 if up else z - 1),
            device_id_type=MESH,
        )

    def to_east(n, t):
        return send(held(n, t, mine * band, band), xs, xr, n, t, (east, f, z))

    def to_north(n, t):
        return send(held(n, t, mine * band, band), ys, yr, n, t, (north, f, z))

    def north_to_east(n, t):
        return send(held(n, t, lead_north, shared), xfs, xfr, n, t, (east, f, z))

    def east_to_north(n, t):
        return send(held(n, t, lead_east + shared, rest), yfs, yfr, n, t, (north, f, z))

    def across(n, t):
        return send(held(n, t, 0, depth), cs, cr, n, t, (g, 1 - f, z))

    rows = pl.ds(tile(f * depth), depth)
    loads = (
        pltpu.make_async_copy(a_in, a_wide, ls.at[0]),
        pltpu.make_async_copy(m_in, m_wide, ls.at[1]),
    )
    keeps = (
        pltpu.make_async_copy(a_hold, a_out.at[z, :, rows, :], ls.at[2]),
        pltpu.make_async_copy(m_hold, m_out.at[z, :, rows, :], ls.at[3]),
    )
    loads[0].start()

    barrier = pltpu.get_barrier_semaphore()

    def greet(to):
        pl.semaphore_signal(barrier, inc=1, device_id=to, device_id_type=MESH)

    for to in ((east, f, z), (north, f, z), (g, 1 - f, z)):
        greet(to)

    @pl.when(z > 0)
    def _():
        greet((g, f, z - 1))

    @pl.when(z < last)
    def _():
        greet((g, f, z + 1))

    loads[0].wait()
    a_hold[...] = a_wide[...].astype(LOW)
    keeps[0].start()
    pl.semaphore_wait(barrier, 3 + jnp.minimum(z, 1) + jnp.minimum(last - z, 1))
    keeps[0].wait()

    count = len(chunks)

    def when_real(k, up, run):
        @pl.when(z - k >= 0 if up else z + k <= last)
        def _():
            run(z - k if up else z + k)

    def own(n):
        @pl.when(z < last)
        def _():
            along(n, z, True).start()

        @pl.when(z > 0)
        def _():
            along(n, z, False).start()

        across(n, z).start()

    def land(n, k, up):
        def run(t):
            along(n, t, up).wait_recv()

            @pl.when(z < last if up else z > 0)
            def _():
                along(n, t, up).start()

            to_east(n, t).start()
            to_north(n, t).start()

        when_real(k, up, run)

    def relay(n, k, up):
        def run(t):
            to_east(n, t).wait_recv()
            east_to_north(n, t).start()
            to_north(n, t).wait_recv()
            north_to_east(n, t).start()

        when_real(k, up, run)

    def finish(n, k, up):
        def run(t):
            east_to_north(n, t).wait_recv()
            north_to_east(n, t).wait_recv()
            across(n, t).start()

        when_real(k, up, run)

    def both(run, n, k):
        for up in (True, False):
            run(n, k, up)

    def fetch(t):
        return pltpu.make_async_copy(a_out.at[t, pl.ds(0, 3)], w_scr, ws.at[0])

    def maps(t):
        across(0, t).wait_recv()
        fetch(t).start()
        fetch(t).wait()
        here = pl.ds(pl.multiple_of(t * cols, cols), cols)

        def body(j, carry):
            bias = jnp.where(j == 0, vec_ref[4:5, here], jnp.where(j == 2, vec_ref[5:6, here], 0.0))
            qkv_scr[j, :, here] = (dot(n_scr[...], w_scr[j]) + bias).astype(LOW)
            return carry

        lax.fori_loop(0, 3, body, 0)

    def project(k):
        def body(d, carry):
            t = z - k + 2 * k * d

            @pl.when((t >= 0) & (t <= last))
            def _():
                maps(t)

            return carry

        lax.fori_loop(0, 2, body, 0)

    own(0)
    loads[1].start()
    n_scr[...] = jnp.zeros_like(n_scr)
    x_all[...] = jnp.zeros_like(x_all)
    g2_scr[...] = jnp.zeros_like(g2_scr)

    def norm_image(i):
        here = pl.ds(i * span, seq)
        image = x_ref[:, i, :]
        x_all[here, :] = image
        normal, _ = centred(image.astype(F32))
        n_scr[here, :] = (normal * vec_ref[0:1] + vec_ref[1:2]).astype(LOW)

    norm_image(0)
    both(land, 0, 1)
    for i in range(1, images):
        norm_image(i)
    puts = [
        pltpu.make_async_copy(n_scr, n_out, ws.at[1]),
        pltpu.make_async_copy(x_all, x_out, ws.at[7]),
    ]
    for put in puts:
        put.start()
    both(land, 0, 2)
    both(relay, 0, 1)
    loads[1].wait()
    m_hold[...] = m_wide[...].astype(LOW)
    keeps[1].start()
    maps(z)
    keeps[1].wait()
    both(land, 0, 3)
    for n in range(1, count):
        own(n)
    both(relay, 0, 2)
    both(finish, 0, 1)
    both(relay, 0, 3)
    both(finish, 0, 2)
    project(1)
    both(finish, 0, 3)
    project(2)

    rest_items = [(n, k) for k in range(1, last + 1) for n in range(1, count)]
    total = len(rest_items) + 2

    def advance(at):
        if at < len(rest_items):
            both(land, *rest_items[at])
        if 0 <= at - 1 < len(rest_items):
            both(relay, *rest_items[at - 1])
        if 0 <= at - 2 < len(rest_items):
            both(finish, *rest_items[at - 2])

    advance(0)
    project(3)
    puts.append(pltpu.make_async_copy(qkv_scr, qkv_out, ws.at[2]))
    puts[-1].start()

    pair = 2 * HD
    pairs = qkv_scr.shape[2] // pair
    stretch = max(pairs // 4, 1)
    segments = images * pairs // stretch

    def segment(n, carry):
        def body(m, carry):
            at = n * stretch + m
            lanes = pl.ds(pl.multiple_of(lax.rem(at, pairs) * pair, pair), pair)
            here = pl.ds(pl.multiple_of(at // pairs * span, 16), span)
            att_scr[here, lanes] = attend_pair(
                seq, qkv_scr[0, here, lanes], qkv_scr[1, here, lanes], qkv_scr[2, here, lanes]
            )
            return carry

        lax.fori_loop(0, stretch, body, 0)
        for c in range(min(segments, total - 3)):
            pl.when(n == c)(functools.partial(advance, 1 + c))
        return carry

    lax.fori_loop(0, segments, segment, 0)
    at = 1 + min(segments, total - 3)
    puts.append(pltpu.make_async_copy(att_scr, att_out, ws.at[3]))
    puts[-1].start()
    for i in range(images):
        g2_scr[pl.ds(i * span, seq), :] = (g_ref[:, i, :].astype(F32) * alive_ref[i]).astype(LOW)
    while at < total - 2:
        advance(at)
        at += 1

    for t in range(shards):
        across(1, t).wait_recv()
    take = pltpu.make_async_copy(a_out.at[:, 3], o_scr, ws.at[0])
    take.start()
    take.wait()

    def mix_image(i, carry):
        here = pl.ds(pl.multiple_of(i * span, 16), span)
        out = x_all[here, :].astype(F32) + vec_ref[6:7]
        for t in range(shards):
            out = out + dot(att_scr[here, t * cols : (t + 1) * cols], o_scr[t], NT)
        resid_scr[here, :] = out
        normal, _ = centred(out)
        n2_scr[here, :] = (normal * vec_ref[2:3] + vec_ref[3:4]).astype(LOW)
        for c in range(min(images, total - at)):
            pl.when(i == c)(functools.partial(advance, at + c))
        return carry

    lax.fori_loop(0, images, mix_image, 0)
    at += min(images, total - at)
    for n, (src, dst) in enumerate(((resid_scr, resid_out), (n2_scr, n2_out), (g2_scr, g2_out))):
        puts.append(pltpu.make_async_copy(src, dst, ws.at[4 + n]))
        puts[-1].start()
    while at < total:
        advance(at)
        at += 1
    for put in puts:
        put.wait()

    for n in range(count):
        @pl.when(z < last)
        def _():
            along(n, z, True).wait_send()

        @pl.when(z > 0)
        def _():
            along(n, z, False).wait_send()

        for t in range(shards):
            across(n, t).wait_send()
            if n > 1:
                across(n, t).wait_recv()

    def settle(n, k, up):
        def run(t):
            @pl.when(z < last if up else z > 0)
            def _():
                along(n, t, up).wait_send()

            to_east(n, t).wait_send()
            to_north(n, t).wait_send()
            east_to_north(n, t).wait_send()
            north_to_east(n, t).wait_send()

        when_real(k, up, run)

    for n in range(count):
        for k in range(1, last + 1):
            both(settle, n, k)


def front(alive, attn_master, mlp_master, patches, cotangent, vec, shards):
    _, depth, a_cols = attn_master.shape
    _, _, m_cols = mlp_master.shape
    seq, images, width = patches.shape
    rows = images * padded(seq)
    anywhere = pl.BlockSpec(memory_space=pl.ANY)
    inside = pl.BlockSpec(memory_space=pltpu.VMEM)
    dma = pltpu.SemaphoreType.DMA
    low = jax.ShapeDtypeStruct((rows, width), LOW)
    return pl.pallas_call(
        functools.partial(front_kernel, images, seq),
        in_specs=[pl.BlockSpec(memory_space=pltpu.SMEM), anywhere, anywhere, inside, inside, inside],
        out_specs=[anywhere] * 9,
        out_shape=[
            jax.ShapeDtypeStruct((shards, 4, width, a_cols), LOW),
            jax.ShapeDtypeStruct((shards, 2, width, m_cols), LOW),
            low,
            jax.ShapeDtypeStruct((3, rows, width), LOW),
            low,
            jax.ShapeDtypeStruct((rows, width), F32),
            low,
            low,
            low,
        ],
        scratch_shapes=[
            pltpu.VMEM(attn_master.shape, F32),
            pltpu.VMEM(mlp_master.shape, F32),
            pltpu.VMEM(attn_master.shape, LOW),
            pltpu.VMEM(mlp_master.shape, LOW),
            pltpu.VMEM((rows, width), LOW),
            pltpu.VMEM((3, rows, width), LOW),
            pltpu.VMEM((rows, width), LOW),
            pltpu.VMEM((3, width, a_cols), LOW),
            pltpu.VMEM((shards, width, a_cols), LOW),
            pltpu.VMEM((rows, width), F32),
            pltpu.VMEM((rows, width), LOW),
            pltpu.VMEM((rows, width), LOW),
            pltpu.VMEM((rows, width), LOW),
            dma((4, shards, 2)),
        ]
        + [dma((4, shards))] * 11
        + [dma((4,)), dma((8,))],
        compiler_params=params(1),
        cost_estimate=cost(8 * rows * width * width, 30 * rows * width),
        name="front",
    )(alive, attn_master, mlp_master, patches, cotangent, vec)


def inner_adamw(master, gradient, first, second, step_rate, decay_rate):
    first_moment = 0.9 * first + 0.1 * gradient
    second_moment = 0.95 * second + 0.05 * gradient * gradient
    step_ratio = (
        first_moment / (1.0 - 0.9**STEP) / (jnp.sqrt(second_moment / (1.0 - 0.95**STEP)) + 1e-08)
    )
    return (master - step_rate * (step_ratio + decay_rate * master), second_moment)


def outer_nesterov(master, outer_old, difference):
    momentum = OUTER_MOMENTUM * outer_old + difference
    return momentum, master - OUTER_RATE * (difference + OUTER_MOMENTUM * momentum)


def inner_kernel(join, count, *refs):
    pieces, (master_ref, moment_ref, *_, inner_ref, diff_ref) = refs[:count], refs[count:]
    gradient = join(*[piece[0] for piece in pieces]).astype(F32)
    master = master_ref[0]
    new, second = inner_adamw(master, gradient, moment_ref[0, 0, 0], moment_ref[0, 1, 0], INNER_RATE, WEIGHT_DECAY)
    inner_ref[0, 0, 0] = gradient
    inner_ref[0, 1, 0] = second
    diff_ref[0] = (master - new).astype(LOW)


def inner_step(join, pieces, unit, units, cols, master, moments, into, name):
    depth = master.shape[1]
    rows = min(depth, 524288 // cols)
    block = pl.BlockSpec((1, rows, cols), lambda u, r: (unit(u)[0], r, unit(u)[1]))
    both = pl.BlockSpec((1, 2, 1, rows, cols), lambda u, r: (0, 0, unit(u)[0], r, unit(u)[1]))
    piece_specs = [pl.BlockSpec((1, rows, piece.shape[2]), lambda u, r: (u, r, 0)) for piece in pieces]
    count = len(pieces)
    return pl.pallas_call(
        functools.partial(inner_kernel, join, count),
        grid=(units, depth // rows),
        in_specs=[*piece_specs, block, both] + ([] if into is None else [pl.BlockSpec(memory_space=pl.ANY)]),
        out_specs=[both, pl.BlockSpec((1, rows, cols), lambda u, r: (u, r, 0))],
        out_shape=[
            jax.ShapeDtypeStruct(moments.shape, F32),
            jax.ShapeDtypeStruct((units, depth, cols), LOW),
        ],
        input_output_aliases={} if into is None else {count + 2: 0},
        compiler_params=params(),
        cost_estimate=cost(30 * units * depth * cols, 24 * units * depth * cols),
        name=name,
    )(*pieces, master, moments, *([] if into is None else [into]))


def outer_kernel(groups, slots, each, g_ref, *refs):
    totals, (master_ref, outer_ref, *_, state_ref, copy_ref) = refs[:slots], refs[slots:]
    rows = copy_ref.shape[1]
    if slots == 1:
        total = totals[0][0]
    else:
        at = pl.program_id(0) * pl.num_programs(1) + pl.program_id(1)
        slot = lax.rem(g_ref[0] + groups - at // each, groups)
        here = pl.ds(pl.multiple_of(lax.rem(at, each) * rows, rows), rows)
        total = totals[0][here, :]
        for n in range(1, slots):
            total = jnp.where(slot == n, totals[n][here, :], total)
    difference = total.astype(F32) / groups
    momentum, fresh = outer_nesterov(master_ref[0], outer_ref[0], difference)
    state_ref[0, 0] = difference
    state_ref[1, 0] = momentum
    state_ref[2, 0] = fresh
    copy_ref[0] = fresh.astype(LOW)


def outer_step(groups, me, totals, unit, units, cols, master, outer_old, into, name):
    depth = master.shape[1]
    slots = len(totals)
    rows = min(depth, 524288 // cols, totals[0].shape[-2])
    each = totals[0].shape[-2] // rows
    block = pl.BlockSpec((1, rows, cols), lambda u, r, g: (unit(u)[0], r, unit(u)[1]))
    state = pl.BlockSpec((3, 1, rows, cols), lambda u, r, g: (0, unit(u)[0], r, unit(u)[1]))
    if slots == 1:
        total = pl.BlockSpec((1, rows, cols), lambda u, r, g: (u, r, 0))
    else:
        total = pl.BlockSpec(totals[0].shape, lambda u, r, g: (0, 0))
    aliased = [] if into is None else [pl.BlockSpec(memory_space=pl.ANY)] * 2
    return pl.pallas_call(
        functools.partial(outer_kernel, groups, slots, each),
        grid_spec=pltpu.PrefetchScalarGridSpec(
            num_scalar_prefetch=1,
            grid=(units, depth // rows),
            in_specs=[*[total] * slots, block, block, *aliased],
            out_specs=[state, block],
        ),
        out_shape=[
            jax.ShapeDtypeStruct((3, *master.shape), F32),
            jax.ShapeDtypeStruct(master.shape, LOW),
        ],
        input_output_aliases={} if into is None else {slots + 3: 0, slots + 4: 1},
        compiler_params=params(),
        cost_estimate=cost(10 * units * depth * cols, 24 * units * depth * cols),
        name=name,
    )(me, *totals, master, outer_old, *([] if into is None else into))


def group_kernel(groups, shards, vectors, diff_ref, *refs):
    if vectors:
        part_ref, master_ref, moment_ref, outer_ref, total_ref, inner_ref, state_ref, copy_ref, *refs = refs
    else:
        total_ref, *refs = refs
    landed, summed, sends, receives, sends_two, receives_two, *small = refs
    g, f, t = lax.axis_index("group"), lax.axis_index("fsdp"), lax.axis_index("tensor")
    span = landed.shape[1]

    def rows(n):
        return pl.ds(pl.multiple_of(n * span, span), span)

    def other(k):
        return lax.rem(g + k, groups)

    def back(k):
        return lax.rem(g + groups - k, groups)

    def copy(src, dst, sems, semr, k, to):
        return pltpu.make_async_remote_copy(
            src_ref=src, dst_ref=dst, send_sem=sems.at[k], recv_sem=semr.at[k], device_id=to, device_id_type=MESH
        )

    def part(k):
        return copy(diff_ref.at[rows(other(k)), :], landed.at[k], sends, receives, k, (other(k), f, t))

    def result(k):
        return copy(summed, landed.at[groups + k], sends_two, receives_two, k, (other(k), f, t))

    barrier = pltpu.get_barrier_semaphore()
    for k in range(1, groups):
        pl.semaphore_signal(barrier, inc=1, device_id=(other(k), f, t), device_id_type=MESH)
    if vectors:
        stage, pair, mine, line, whole, few, diffs, ss, rs, ls, lr, gs, gr = small
        half = part_ref.shape[0] // 2
        halves = (pl.ds(0, half), pl.ds(half, half))

        def pick(ref):
            return jnp.where(f == 0, ref[halves[0], :], ref[halves[1], :])

        def line_copy(k):
            return copy(mine, line.at[k], ls, lr, k, (g, f, lax.rem(t + k, shards)))

        def few_copy(k):
            return copy(diffs.at[f], few.at[k], gs, gr, k, (other(k), f, t))

        pair_copy = copy(stage.at[1 - f], pair, ss, rs, 0, partner())
        whole_copy = copy(whole.at[f], whole.at[f], ss, rs, 1, partner())
        final_copy = copy(mine, stage.at[f], ss, rs, 2, partner())
        pl.semaphore_signal(barrier, inc=1, device_id=partner(), device_id_type=MESH)
        for k in range(1, shards):
            pl.semaphore_signal(barrier, inc=1, device_id=(g, f, lax.rem(t + k, shards)), device_id_type=MESH)
        stage[...] = jnp.zeros_like(stage)
        diffs[...] = jnp.zeros_like(diffs)
        for n in range(2):
            stage[n, 0:half] = part_ref[halves[n], :]
    pl.semaphore_wait(barrier, groups - 1 + (shards if vectors else 0))

    for k in range(1, groups):
        part(k).start()
    if vectors:
        pair_copy.start()
        pair_copy.wait()
        mine[...] = stage[f] + pair[...]
        for k in range(1, shards):
            line_copy(k).start()
        line[0] = mine[...]
        for k in range(1, shards):
            line_copy(k).wait()
        gradient = jnp.zeros(mine.shape, F32)
        for n in range(shards):
            gradient = gradient + line[lax.rem(t + shards - n, shards)]
        whole[f] = gradient
        whole_copy.start()
        new, _ = inner_adamw(
            pick(master_ref), gradient[0:half], pick(moment_ref.at[0]), pick(moment_ref.at[1]), VECTOR_RATE, 0.0
        )
        diffs[f, 0:half] = pick(master_ref) - new
        for k in range(1, groups):
            few_copy(k).start()
        few[0] = diffs[f]
        whole_copy.wait()
        for n in range(2):
            own = whole[n, 0:half]
            _, second = inner_adamw(
                master_ref[halves[n], :], own, moment_ref[0, halves[n], :], moment_ref[1, halves[n], :], VECTOR_RATE, 0.0
            )
            inner_ref[0, halves[n], :] = own
            inner_ref[1, halves[n], :] = second
    total = diff_ref[rows(g), :].astype(F32)
    for k in range(1, groups):
        part(k).wait_recv()
        total = total + landed[k].astype(F32)
    summed[...] = total.astype(LOW)
    for k in range(1, groups):
        result(k).start()
    total_ref[rows(g), :] = summed[...]
    if vectors:
        for k in range(1, groups):
            few_copy(k).wait()
        difference = jnp.zeros(mine.shape, F32)
        for n in range(groups):
            difference = difference + few[lax.rem(g + groups - n, groups)]
        mine[...] = difference / groups
        stage[f] = mine[...]
        final_copy.start()
        final_copy.wait()
        for n in range(2):
            difference = stage[n, 0:half]
            momentum, fresh = outer_nesterov(master_ref[halves[n], :], outer_ref[halves[n], :], difference)
            state_ref[0, halves[n], :] = difference
            state_ref[1, halves[n], :] = momentum
            state_ref[2, halves[n], :] = fresh
            copy_ref[halves[n], :] = fresh.astype(LOW)
    for k in range(1, groups):
        result(k).wait_recv()
        total_ref[rows(back(k)), :] = landed[groups + k]
    for k in range(1, groups):
        part(k).wait_send()
        result(k).wait_send()


def group_sum(diff, groups, identity, name, vectors=None, shards=0):
    flat = diff.reshape(-1, diff.shape[-1])
    span, cols = flat.shape[0] // groups, flat.shape[1]
    dma = pltpu.SemaphoreType.DMA
    whole = pl.BlockSpec(memory_space=pltpu.VMEM)
    out_shape = [jax.ShapeDtypeStruct(flat.shape, LOW)]
    extra = []
    if vectors:
        shape = vectors[0].shape
        half = (-(-shape[0] // 16) * 8, shape[1])
        out_shape += [
            jax.ShapeDtypeStruct((2, *shape), F32),
            jax.ShapeDtypeStruct((3, *shape), F32),
            jax.ShapeDtypeStruct(shape, LOW),
        ]
        extra = [
            pltpu.VMEM((2, *half), F32),
            pltpu.VMEM(half, F32),
            pltpu.VMEM(half, F32),
            pltpu.VMEM((shards, *half), F32),
            pltpu.VMEM((2, *half), F32),
            pltpu.VMEM((groups, *half), F32),
            pltpu.VMEM((2, *half), F32),
            dma((3,)),
            dma((3,)),
            dma((shards,)),
            dma((shards,)),
            dma((groups,)),
            dma((groups,)),
        ]
    total, *rest = pl.pallas_call(
        functools.partial(group_kernel, groups, shards, bool(vectors)),
        in_specs=[whole] * (5 if vectors else 1),
        out_specs=[whole] * len(out_shape),
        out_shape=out_shape,
        scratch_shapes=[
            pltpu.VMEM((2 * groups, span, cols), LOW),
            pltpu.VMEM((span, cols), LOW),
            *[dma((groups,))] * 4,
            *extra,
        ],
        compiler_params=params(identity),
        cost_estimate=cost(4 * flat.size, 8 * flat.size),
        name=name,
    )(flat, *(vectors or []))
    return total.reshape(diff.shape), *rest


def gather_weights(shard):
    whole = lax.all_gather(shard, "tensor", axis=0)
    return lax.all_gather(whole, "fsdp", axis=2, tiled=True)


def around(array, k, groups):
    return lax.ppermute(array, "group", [(i, (i + k) % groups) for i in range(groups)])


def exchange_parts(diff, groups):
    g = lax.axis_index("group")
    quarters = diff.reshape(groups, -1, diff.shape[-1])
    parts = [lax.dynamic_index_in_dim(quarters, lax.rem(g + k, groups), 0, keepdims=False) for k in range(groups)]
    total = sum([around(parts[k], k, groups).astype(F32) for k in range(1, groups)], parts[0].astype(F32))
    return total.astype(LOW)


def exchange_total(own, groups):
    return [own] + [around(own, k, groups) for k in range(1, groups)]


def scatter_gradient(gradient):
    half = gradient if gradient.ndim == 4 else lax.psum_scatter(gradient, "fsdp", scatter_dimension=0)
    return lax.psum_scatter(half, "tensor", scatter_dimension=0)


def local(
    patches,
    output_grad,
    live_counts,
    attn_master,
    mlp_master,
    vector_master,
    attn_moments,
    mlp_moments,
    vector_moments,
    attn_outer,
    mlp_outer,
    vector_outer,
):
    vec = vector_master
    tensor_size, fsdp = lax.axis_size("tensor"), lax.axis_size("fsdp")
    groups = lax.axis_size("group")
    local_images, seq, width = patches.shape[2:]
    slot = (lax.axis_index("fsdp") * tensor_size + lax.axis_index("tensor")) * local_images
    slot = slot + jnp.arange(local_images)
    counts = jnp.take(live_counts[0], slot // IMG_DEV, axis=1)
    alive = ((slot % IMG_DEV)[None, :] < counts).astype(F32).reshape(-1)
    x = patches.reshape(-1, seq, width)
    cotangent = output_grad.reshape(-1, seq, width)
    images = x.shape[0]

    if (groups, fsdp) == (4, 2):
        beside_images = [
            jnp.moveaxis(v.reshape(images, seq, width), 0, 1) for v in (patches, output_grad)
        ]
        w_attn, w_mlp, normed_one, qkv, attended, resid, normed_two, grad_two, x_rows = front(
            alive, attn_master, mlp_master, *beside_images, vec, tensor_size
        )
    else:
        w_attn = gather_weights(attn_master.astype(LOW))
        w_mlp = gather_weights(mlp_master.astype(LOW))
        normed_one, qkv = project(x, w_attn, vec)
        attended = attend(qkv, images, seq)
        resid, normed_two, grad_two = mix(alive, attended, x, cotangent, w_attn, vec)
        x_rows = jnp.pad(x, ((0, 0), (0, padded(seq) - seq), (0, 0))).reshape(-1, width)
    bias = vec[8:].reshape(tensor_size, 1, -1)
    carried = None
    mlp_grads, bias_parts = [], []
    for part, (start, cols) in enumerate(PIECES):
        *carried, dw, db = mlp(part, start, cols, normed_two, grad_two, w_mlp, bias, carried, fsdp)
        mlp_grads.append(scatter_gradient(dw))
        bias_parts.append(db)
    branch, grad_normed = carried
    block_output, grad_resid, grad_attended, dw_out, sums_two = turn(
        alive, resid, branch, grad_normed, grad_two, attended, w_attn, vec, images, seq, fsdp
    )
    def beside(*parts):
        return jnp.concatenate(parts, axis=-1)

    pairwise = fsdp == 2
    me = lax.axis_index("group").astype(jnp.int32).reshape(1)
    half = attn_master.shape[2] // PARTS
    (grads,) = unattend(qkv, grad_attended, images, seq, 0, PARTS, tensor_size)
    grads, mlp_grads[0] = lax.optimization_barrier((grads, mlp_grads[0]))
    carry, dw_early, head_sums = close(
        0, PARTS, normed_one, grads, w_attn, None, dw_out, None, fsdp, groups
    )
    if not pairwise:
        halves = jnp.moveaxis(dw_out.reshape(*dw_out.shape[:-1], PARTS, half), -2, 2)
        dw_early = jnp.concatenate([dw_early, halves[:, :, :, 0]], axis=2)
    early_grad = scatter_gradient(dw_early)
    head_sums = [head_sums]
    carry, mlp_grads[1] = lax.optimization_barrier((carry, mlp_grads[1]))
    hidden = mlp_master.shape[2] // 2
    mlp_inner, diff_one = inner_step(
        beside, mlp_grads[:2], lambda u: (u, 0), 2, hidden, mlp_master, mlp_moments, None, "inner_mlp_0"
    )
    riding = groups if pairwise else 0
    grads, *own_one = unattend(
        qkv, grad_attended, images, seq, 1, PARTS, tensor_size, diff_one.reshape(-1, hidden), riding
    )
    mlp_grads[2], grads = lax.optimization_barrier((mlp_grads[2], grads))
    mlp_inner, diff_two = inner_step(
        beside, mlp_grads[2:], lambda u: (u, 1), 2, hidden, mlp_master, mlp_moments, mlp_inner, "inner_mlp_1"
    )
    carry, diff_two = lax.optimization_barrier((carry, diff_two))
    carry, *own_two, dw_late, sums = close(
        1, PARTS, normed_one, grads, w_attn, carry, None, diff_two.reshape(-1, hidden), fsdp, groups
    )
    mlp_own = [beside(*own_one, *own_two)] if pairwise else []
    mlp_diff = beside(diff_one, diff_two)
    patches_grad, sums_one = finish(carry, grad_resid, x_rows, vec, images, seq)
    if not pairwise:
        mlp_own = [exchange_parts(mlp_diff, groups)]
    mlp_total = exchange_total(mlp_own[0], groups)
    late_grad = scatter_gradient(dw_late)
    head_sums.append(sums)

    def early(u):
        return jnp.minimum(u, 3), jnp.maximum(u - 3, 0)

    def late(u):
        return u, 1

    def first(piece):
        return piece

    attn_inner, early_diff = inner_step(
        first, [early_grad], early, 3 + PARTS, half, attn_master, attn_moments, None, "inner_early"
    )
    head_rows = jnp.concatenate([v.reshape(2, tensor_size, -1) for v in head_sums], axis=-1).reshape(2, width)
    hidden_bias = jnp.concatenate(bias_parts, axis=-1).reshape(-1, width)
    vector_part = jnp.concatenate([sums_one, sums_two[:2], head_rows, sums_two[2:], hidden_bias])

    if pairwise:
        early_total, vector_inner, vector_state, vector_copy = group_sum(
            early_diff,
            groups,
            10,
            "group_early",
            [vector_part, vec, vector_moments[0], vector_outer],
            tensor_size,
        )
    else:
        (early_total,) = group_sum(early_diff, groups, 10, "group_early")
        vector_grad = lax.psum(vector_part, ("fsdp", "tensor"))
        new_vector, second_vector = inner_adamw(
            vec, vector_grad, vector_moments[0, 0], vector_moments[0, 1], VECTOR_RATE, 0.0
        )
        diff_vector = lax.psum(vec - new_vector, "group") / groups
        momentum, fresh = outer_nesterov(vec, vector_outer, diff_vector)
        vector_inner = jnp.stack([vector_grad, second_vector])
        vector_state, vector_copy = jnp.stack([diff_vector, momentum, fresh]), fresh.astype(LOW)
    attn_state, attn_copy = outer_step(
        groups, me, [early_total], early, 3 + PARTS, half, attn_master, attn_outer, None, "outer_early"
    )
    attn_copy, *mlp_total = lax.optimization_barrier((attn_copy, *mlp_total))
    mlp_state, mlp_copy = outer_step(
        groups,
        me,
        mlp_total,
        lambda u: (u, 0),
        2,
        mlp_master.shape[2],
        mlp_master,
        mlp_outer,
        None,
        "outer_mlp",
    )
    late_grad, mlp_state = lax.optimization_barrier((late_grad, mlp_state))
    attn_inner, late_diff = inner_step(
        first, [late_grad], late, 3, half, attn_master, attn_moments, attn_inner, "inner_late"
    )
    (late_total,) = group_sum(late_diff, groups, 11, "group_late")
    attn_state, attn_copy = outer_step(
        groups, me, [late_total], late, 3, half, attn_master, attn_outer, (attn_state, attn_copy), "outer_late"
    )
    return (
        block_output.reshape(patches.shape),
        patches_grad.reshape(patches.shape),
        attn_inner,
        attn_state,
        attn_copy,
        mlp_inner,
        mlp_state,
        mlp_copy,
        vector_inner[None],
        vector_state,
        vector_copy,
    )


def solution(mesh):
    placed = (
        P("group", None, ("fsdp", "tensor"), None, None),
        P("group", None, ("fsdp", "tensor"), None, None),
        P("group", None, None),
        P(None, "fsdp", "tensor"),
        P(None, "fsdp", "tensor"),
        P(),
        P("group", None, None, "fsdp", "tensor"),
        P("group", None, None, "fsdp", "tensor"),
        P("group", None, None, None),
        P(None, "fsdp", "tensor"),
        P(None, "fsdp", "tensor"),
        P(),
    )
    return jax.shard_map(
        local,
        mesh=mesh,
        in_specs=placed,
        out_specs=(
            P("group", None, ("fsdp", "tensor"), None, None),
            P("group", None, ("fsdp", "tensor"), None, None),
            P("group", None, None, "fsdp", "tensor"),
            P(None, None, "fsdp", "tensor"),
            P(None, "fsdp", "tensor"),
            P("group", None, None, "fsdp", "tensor"),
            P(None, None, "fsdp", "tensor"),
            P(None, "fsdp", "tensor"),
            P("group", None, None, None),
            P(),
            P(),
        ),
        check_vma=False,
    )
```
